32 devices in a mesh: rep: 2 (over x), fsdp: 16 (over z, y, core).
Axes of the slice: x: 2, y: 2, z: 4, core: 2. Of those that a mesh axis runs over, the one named last changes fastest.
Arguments:
- x_in: bfloat16 [32, 256, 1536], P(('rep', 'fsdp')), may hold values from -6 to 6
- doc_ids: int32 [32, 256], P(('rep', 'fsdp')), may hold values from 0 to 3, never falling along the last dimension, each value on 1 to 128 neighbouring positions
- w_qkv: bfloat16 [1536, 4608], P('fsdp'), may hold values from -0.15625 to 0.15625
- w_out: bfloat16 [1536, 1536], P('fsdp'), may hold values from -0.15625 to 0.15625
- gain_attn: bfloat16 [1536], P('fsdp'), may hold values from 0.5 to 1.5
- gain_group: bfloat16 [1536], P('fsdp'), may hold values from 0.5 to 1.5
- conv_kernel: float32 [16, 6, 11], replicated, may hold values from -0.8 to 0.8
- head_mix: float32 [16, 2], replicated, may hold values from 0.1 to 1
- gain_ffn: bfloat16 [1536], P('fsdp'), may hold values from 0.5 to 1.5
- w_gate: bfloat16 [1536, 4096], P('fsdp'), may hold values from -0.15625 to 0.15625
- w_up: bfloat16 [1536, 4096], P('fsdp'), may hold values from -0.15625 to 0.15625
- w_down: bfloat16 [4096, 1536], P('fsdp'), may hold values from -0.09375 to 0.09375
- cotangent: bfloat16 [32, 256, 1536], P(('rep', 'fsdp')), may hold values from -6 to 6
Outputs:
- out: bfloat16 [32, 256, 1536], P(('rep', 'fsdp'))
- grad_x: float32 [32, 256, 1536], P(('rep', 'fsdp'))
- grad_qkv: float32 [1536, 4608], P('fsdp')
- grad_out: float32 [1536, 1536], P('fsdp')
- grad_gain_attn: float32 [1536], P('fsdp')
- grad_gain_group: float32 [1536], P('fsdp')
- grad_conv: float32 [16, 6, 11], replicated
- grad_mix: float32 [16, 2], replicated
- grad_gain_ffn: float32 [1536], P('fsdp')
- grad_gate: float32 [1536, 4096], P('fsdp')
- grad_up: float32 [1536, 4096], P('fsdp')
- grad_down: float32 [4096, 1536], P('fsdp')
The draws below stay inside these ranges and needn't reach their ends.
Inputs may be any that keep to these rules, and one draw needn't show every extreme that they name: `doc_ids`: within each packed row the document ids never fall, and each document holds at most 128 tokens.
All inputs are finite; a program needn't handle non-finite values.
Results may differ from the reference program's by a relative error of at most 0.017.
Values may be sent and summed in bfloat16 or wider, within the bound.
A program may use at most 320 MiB of HBM per device.

```python
import math
import jax
import jax.numpy as jnp
import numpy as np
from jax import lax

MODEL_WIDTH = 1536
H = 16
E = 96
FF = 4096
QWIN = 6
KWIN = 11
TOK_DEV = 256
ROWS = 32
DOCS = 4


def levels(rng, dims, split, least, high):
    def one(position, shards_of):
        steps = jax.random.uniform(jax.random.fold_in(jax.random.fold_in(rng, 6), position), (shards_of,), jnp.float32, least / len(split), high / len(split))
        return jnp.repeat(jnp.exp(steps), dims[position] // shards_of).reshape((-1,) + (1,) * (len(dims) - position - 1))

    factor_of = one(*split[0])
    for cut in split[1:]:
        factor_of = factor_of * one(*cut)
    return factor_of


def length_profile(amount, total, bound, skew):
    portions = [(1 << 20) // math.isqrt(rank ** skew) + 1 for rank in range(2, amount + 1)]
    spare, holding = total - bound - (amount - 1), [1] * (amount - 1)
    while spare > 0:
        candidates = [i for i in range(amount - 1) if holding[i] < bound]
        pool, left = sum([portions[i] for i in candidates]), spare
        for i in candidates:
            more = min(bound - holding[i], max(1, left * portions[i] // pool), spare)
            holding[i] = holding[i] + more
            spare = spare - more
    return np.array([bound] + holding)


def ragged(stream_key, number_of, total, bound, skew):
    if number_of == 2:
        one = jax.random.randint(stream_key, (), max(1, total - bound), min(bound, total - 1) + 1)
        return jnp.stack([one, total - one])
    lengths = jnp.asarray(length_profile(number_of, total, bound, skew), jnp.int32)
    twos = (number_of - 1) // 2
    source_of, sink = lengths[1:1 + 2 * twos:2], lengths[2:2 + 2 * twos:2]
    slack = jnp.minimum(source_of - 1, bound - sink)
    passed = jax.random.randint(jax.random.fold_in(stream_key, 1), (twos,), 0, 1 << 20) % (slack + 1)
    lengths = lengths.at[1:1 + 2 * twos:2].set(source_of - passed).at[2:2 + 2 * twos:2].set(sink + passed)
    return lengths[jax.random.permutation(jax.random.fold_in(stream_key, 2), number_of)]


def gaussian(stream_key, dims, width, most, split=(), held_as=jnp.bfloat16):
    array = jax.random.normal(stream_key, dims, jnp.float32) * width
    if len(split) > 0:
        array = levels(stream_key, dims, split, -0.22, 0.18) * array
    return jnp.clip(array, min=-most, max=most).astype(held_as)


def setup_inputs(seed: int = 0) -> dict:
    key_of = jax.random.split(jax.random.key(seed), 14)
    x_in = gaussian(key_of[0], (ROWS, TOK_DEV, MODEL_WIDTH), 1.0, 6.0, ((0, 32),))
    doc_ids = jax.vmap(lambda own: jnp.searchsorted(jnp.cumsum(ragged(own, DOCS, TOK_DEV, TOK_DEV // 2, 1)), jnp.arange(TOK_DEV), side="right"))(jax.random.split(key_of[1], ROWS)).reshape((ROWS, TOK_DEV)).astype(jnp.int32)
    w_qkv = gaussian(key_of[2], (MODEL_WIDTH, 3 * MODEL_WIDTH), MODEL_WIDTH ** -0.5, 0.15625, ((0, 16),))
    w_out = gaussian(key_of[3], (MODEL_WIDTH, MODEL_WIDTH), MODEL_WIDTH ** -0.5, 0.15625, ((0, 16),))
    gain_attn = jnp.clip(1.0 + 0.1 * jax.random.normal(key_of[4], (MODEL_WIDTH,), jnp.float32), 0.5, 1.5).astype(jnp.bfloat16)
    gain_group = jnp.clip(1.0 + 0.1 * jax.random.normal(key_of[5], (MODEL_WIDTH,), jnp.float32), 0.5, 1.5).astype(jnp.bfloat16)
    conv_kernel = gaussian(key_of[6], (H, QWIN, KWIN), 0.2, 0.8, (), jnp.float32)
    head_mix = jnp.clip(jax.random.uniform(key_of[7], (H, 2), jnp.float32, 0.1, 1.0), 0.1, 1.0)
    gain_ffn = jnp.clip(1.0 + 0.1 * jax.random.normal(key_of[8], (MODEL_WIDTH,), jnp.float32), 0.5, 1.5).astype(jnp.bfloat16)
    w_gate = gaussian(key_of[9], (MODEL_WIDTH, FF), MODEL_WIDTH ** -0.5, 0.15625, ((0, 16),))
    w_up = gaussian(key_of[10], (MODEL_WIDTH, FF), MODEL_WIDTH ** -0.5, 0.15625, ((0, 16),))
    w_down = gaussian(key_of[11], (FF, MODEL_WIDTH), FF ** -0.5, 0.09375, ((0, 16),))
    cotangent = gaussian(key_of[12], (ROWS, TOK_DEV, MODEL_WIDTH), 1.0, 6.0, ((0, 32),))
    return dict(x_in=x_in, doc_ids=doc_ids, w_qkv=w_qkv, w_out=w_out, gain_attn=gain_attn, gain_group=gain_group, conv_kernel=conv_kernel, head_mix=head_mix, gain_ffn=gain_ffn, w_gate=w_gate, w_up=w_up, w_down=w_down, cotangent=cotangent)


@jax.custom_vjp
def low(v):
    return lax.optimization_barrier(v.astype(jnp.bfloat16)).astype(jnp.float32)

@jax.custom_vjp
def low_back(v):
    return v

def low_keep(v):
    return (low(v), None)

def low_pass(kept, grad):
    return (grad,)

def back_keep(v):
    return (v, None)

def back_low(kept, grad):
    return (low(grad),)
low.defvjp(low_keep, low_pass)
low_back.defvjp(back_keep, back_low)

def matmul(left, right):
    return jnp.dot(left, right, precision=lax.Precision.HIGHEST)

def rms_scale(values, epsilon):
    return lax.rsqrt(lax.optimization_barrier(jnp.mean(values * values, axis=1, keepdims=True)) + epsilon)

def convolve(scores, allowed, kernel):
    zeroed = jnp.where(allowed, scores, 0.0)
    padded = jnp.pad(zeroed, ((0, 0), (QWIN - 1, 0), (KWIN - 1, 0)))
    sequence_length = scores.shape[1]
    total = jnp.zeros_like(scores)
    for row_shift in range(QWIN):
        for col_shift in range(KWIN):
            row_start = QWIN - 1 - row_shift
            col_start = KWIN - 1 - col_shift
            window = padded[:, row_start:row_start + sequence_length, col_start:col_start + sequence_length]
            total = total + kernel[:, row_shift, col_shift][:, None, None] * window
    return total

def forward_row(tokens, allowed, w_qkv, w_out, gain_attn, gain_group, conv_kernel, head_mix, gain_ffn, w_gate, w_up, w_down):
    sequence_length = tokens.shape[0]
    scale = 1.0 / math.sqrt(E)
    highest = lax.Precision.HIGHEST
    normed_in = low(tokens * rms_scale(tokens, 1e-06) * gain_attn)
    projected = matmul(normed_in, w_qkv)
    queries = low(low_back(projected[:, :MODEL_WIDTH])).reshape(sequence_length, H, E)
    key_rows = low(low_back(projected[:, MODEL_WIDTH:2 * MODEL_WIDTH])).reshape(sequence_length, H, E)
    value_rows = low(low_back(projected[:, 2 * MODEL_WIDTH:])).reshape(sequence_length, H, E)
    raw_scores = low_back(jnp.einsum('ihe,jhe->hij', queries, key_rows, precision=highest) * scale)
    convolved = convolve(raw_scores, allowed, conv_kernel)
    masked = jnp.where(allowed, convolved, -jnp.inf)
    top_score = lax.optimization_barrier(jnp.max(masked, axis=2, keepdims=True))
    exp_scores = jnp.exp(masked - top_score)
    probs = exp_scores / lax.optimization_barrier(jnp.sum(exp_scores, axis=2, keepdims=True))
    grouped = probs.reshape(H // 2, 2, sequence_length, sequence_length)
    table = head_mix.reshape(H // 2, 2, 2)
    mixed = low((table[:, :, 0, None, None] * grouped[:, 0:1] + table[:, :, 1, None, None] * grouped[:, 1:2]).reshape(H, sequence_length, sequence_length))
    heads_out = low_back(jnp.einsum('hij,jhe->ihe', mixed, value_rows, precision=highest))
    mean_removed = heads_out - lax.optimization_barrier(jnp.mean(heads_out, axis=2, keepdims=True))
    inverse_deviation = lax.rsqrt(lax.optimization_barrier(jnp.mean(mean_removed * mean_removed, axis=2, keepdims=True)) + 1e-05)
    head_normalized = low((mean_removed * inverse_deviation * gain_group.reshape(H, E)).reshape(sequence_length, MODEL_WIDTH))
    resid = tokens + low_back(matmul(head_normalized, w_out))
    normed_mid = low(resid * rms_scale(resid, 1e-06) * gain_ffn)
    gate_act = low_back(matmul(normed_mid, w_gate))
    up_act = low_back(matmul(normed_mid, w_up))
    hidden = low(jax.nn.silu(gate_act) * up_act)
    return resid + low_back(matmul(hidden, w_down))

def reference(x_in, doc_ids, w_qkv, w_out, gain_attn, gain_group, conv_kernel, head_mix, gain_ffn, w_gate, w_up, w_down, cotangent):
    params = (w_qkv.astype(jnp.float32), w_out.astype(jnp.float32), gain_attn.astype(jnp.float32), gain_group.astype(jnp.float32), conv_kernel.astype(jnp.float32), head_mix.astype(jnp.float32), gain_ffn.astype(jnp.float32), w_gate.astype(jnp.float32), w_up.astype(jnp.float32), w_down.astype(jnp.float32))
    positions = jnp.arange(TOK_DEV)
    causal = positions[None, :] <= positions[:, None]

    def one_row(totals, row_data):
        tokens, documents, upstream = row_data
        allowed = causal & (documents[:, None] == documents[None, :])

        def run(token_rows, *weights):
            return forward_row(token_rows, allowed, *weights)
        result, pullback = jax.vjp(run, tokens.astype(jnp.float32), *params)
        grads = pullback(upstream.astype(jnp.float32))
        updated = tuple((total + update for total, update in zip(totals, grads[1:])))
        return (updated, (result.astype(jnp.bfloat16), grads[0]))
    start = tuple((jnp.zeros_like(weight) for weight in params))
    totals, (outputs, grad_tokens) = lax.scan(one_row, start, (x_in, doc_ids, cotangent))
    return (outputs, grad_tokens, totals[0], totals[1], totals[2], totals[3], totals[4], totals[5], totals[6], totals[7], totals[8], totals[9])
```

```python
import math

import jax
import jax.numpy as jnp
from jax import lax
from jax.experimental import pallas as pl
from jax.experimental.pallas import tpu as pltpu
from jax.sharding import PartitionSpec as P

MODEL_WIDTH = 1536
H = 16
E = 96
EP = 128
QWIN = 6
KWIN = 11
bf16, f32 = jnp.bfloat16, jnp.float32


def allowed_mask(doc_col, doc_row):
    n = doc_row.shape[-1]
    i = lax.broadcasted_iota(jnp.int32, (n, n), 0)
    j = lax.broadcasted_iota(jnp.int32, (n, n), 1)
    return (j <= i) & (doc_col == doc_row)


def down(v, a):
    if a == 0:
        return v
    i = lax.broadcasted_iota(jnp.int32, v.shape, 0)
    return jnp.where(i >= a, pltpu.roll(v, a, 0), 0.0)


def up(v, a):
    if a == 0:
        return v
    n = v.shape[0]
    i = lax.broadcasted_iota(jnp.int32, v.shape, 0)
    return jnp.where(i < n - a, pltpu.roll(v, n - a, 0), 0.0)


def dot(a, b, ca=1, cb=0):
    return lax.dot_general(a, b, (((ca,), (cb,)), ((), ())), preferred_element_type=f32)


def split(v):
    hi = v.astype(bf16)
    return hi, (v - hi.astype(f32)).astype(bf16)


def fwd_kernel(mix_ref, qkv_ref, dcol_ref, drow_ref, th_ref, tl_ref, gain_ref,
               normed_ref, xhat_ref, s_ref, p_ref, z_ref):
    allowed = allowed_mask(dcol_ref[0], drow_ref[0])
    scale = 1.0 / math.sqrt(E)
    probs = []
    for h in range(2):
        q = qkv_ref[0, :, h * EP:(h + 1) * EP]
        k = qkv_ref[0, :, (2 + h) * EP:(3 + h) * EP]
        zeroed = jnp.where(allowed, dot(q, k, 1, 1) * scale, 0.0)
        z_ref[0, h] = zeroed.astype(bf16)
        his, los = [], []
        for a in range(QWIN):
            hi, lo = split(down(zeroed, a))
            his.append(hi)
            los.append(lo)
        his, los = jnp.concatenate(his, 1), jnp.concatenate(los, 1)
        th, tl = th_ref[h], tl_ref[h]
        conv = dot(his, th) + (dot(his, tl) + dot(los, th))
        masked = jnp.where(allowed, conv, -jnp.inf)
        e = jnp.exp(masked - jnp.max(masked, axis=1, keepdims=True))
        p = e / jnp.sum(e, axis=1, keepdims=True)
        p_ref[0, h] = p
        probs.append(p)
    lane = lax.broadcasted_iota(jnp.int32, (1, EP), 1)
    for h in range(2):
        v = qkv_ref[0, :, (4 + h) * EP:(5 + h) * EP]
        mixed = (mix_ref[h, 0] * probs[0] + mix_ref[h, 1] * probs[1]).astype(bf16)
        ho = dot(mixed, v)
        centered = jnp.where(lane < E, ho - jnp.sum(ho, axis=1, keepdims=True) / E, 0.0)
        s = lax.rsqrt(jnp.sum(centered * centered, axis=1, keepdims=True) / E + 1e-05)
        xhat = centered * s
        cols = slice(h * EP, (h + 1) * EP)
        xhat_ref[0, :, cols] = xhat
        s_ref[0, :, cols] = jnp.broadcast_to(s, xhat.shape)
        normed_ref[0, :, cols] = (xhat * gain_ref[0:1, cols]).astype(bf16)


def attend(mix, qkv, dcol, drow, th, tl, gain):
    n, t, _ = qkv.shape
    row = lambda *s: pl.BlockSpec((1,) + s, lambda i: (i,) + (0,) * len(s))
    full = lambda a: pl.BlockSpec(a.shape, lambda i: (0,) * a.ndim)
    return pl.pallas_call(
        fwd_kernel,
        grid=(n,),
        in_specs=[pl.BlockSpec(memory_space=pltpu.SMEM), row(t, 6 * EP), row(t, 1), row(1, t), full(th), full(tl), full(gain)],
        out_specs=[row(t, 2 * EP), row(t, 2 * EP), row(t, 2 * EP), row(2, t, t), row(2, t, t)],
        out_shape=[
            jax.ShapeDtypeStruct((n, t, 2 * EP), bf16),
            jax.ShapeDtypeStruct((n, t, 2 * EP), f32),
            jax.ShapeDtypeStruct((n, t, 2 * EP), f32),
            jax.ShapeDtypeStruct((n, 2, t, t), f32),
            jax.ShapeDtypeStruct((n, 2, t, t), bf16),
        ],
        cost_estimate=pl.CostEstimate(flops=n * 2 * 3 * 2 * t * t * QWIN * t, bytes_accessed=n * t * t * 20, transcendentals=n * 2 * t * t),
        name="attend",
    )(mix, qkv, dcol, drow, th, tl, gain)


def bwd_kernel(mix_ref, qkv_ref, dcol_ref, drow_ref, tt_ref, gain_ref, dn_ref, xhat_ref, s_ref, p_ref, z_ref,
               dqkv_ref, gconv_ref, gmix_ref, gg_ref, m_ref):
    step, steps = pl.program_id(0), pl.num_programs(0)
    t = p_ref.shape[-1]

    @pl.when(step == 0)
    def _():
        m_ref[...] = jnp.zeros_like(m_ref)
        gmix_ref[...] = jnp.zeros_like(gmix_ref)
        gg_ref[...] = jnp.zeros_like(gg_ref)

    allowed = allowed_mask(dcol_ref[0], drow_ref[0])
    scale = 1.0 / math.sqrt(E)
    lane = lax.broadcasted_iota(jnp.int32, (1, EP), 1)
    p = [p_ref[0, 0], p_ref[0, 1]]
    dmixed = []
    for h in range(2):
        cols = slice(h * EP, (h + 1) * EP)
        dn, xhat = dn_ref[0, :, cols], xhat_ref[0, :, cols]
        gg_ref[0:1, cols] += jnp.sum(dn * xhat, axis=0, keepdims=True)
        dc = dn * gain_ref[0:1, cols]
        m1 = jnp.sum(dc, axis=1, keepdims=True) / E
        m2 = jnp.sum(dc * xhat, axis=1, keepdims=True) / E
        dh = jnp.where(lane < E, s_ref[0, :, cols] * (dc - m1 - xhat * m2), 0.0).astype(bf16)
        v = qkv_ref[0, :, (4 + h) * EP:(5 + h) * EP]
        mixed = (mix_ref[h, 0] * p[0] + mix_ref[h, 1] * p[1]).astype(bf16)
        dmixed.append(dot(dh, v, 1, 1))
        dqkv_ref[0, :, (4 + h) * EP:(5 + h) * EP] = dot(mixed, dh, 0, 0).astype(bf16)
    for h in range(2):
        for c in range(2):
            r = 2 * h + c
            gmix_ref[r:r + 1, :] += jnp.sum(dmixed[h] * p[c], axis=0, keepdims=True)
    for c in range(2):
        dp = mix_ref[0, c] * dmixed[0] + mix_ref[1, c] * dmixed[1]
        dconv = p[c] * (dp - jnp.sum(dp * p[c], axis=1, keepdims=True))
        ahead = jnp.concatenate([up(dconv, a).astype(bf16) for a in range(QWIN)], 1)
        m_ref[c] += dot(z_ref[0, c], ahead, 0, 0)
        ds = jnp.where(allowed, dot(ahead, tt_ref[c]), 0.0).astype(bf16)
        q = qkv_ref[0, :, c * EP:(c + 1) * EP]
        k = qkv_ref[0, :, (2 + c) * EP:(3 + c) * EP]
        dqkv_ref[0, :, c * EP:(c + 1) * EP] = (dot(ds, k) * scale).astype(bf16)
        dqkv_ref[0, :, (2 + c) * EP:(3 + c) * EP] = (dot(ds, q, 0, 0) * scale).astype(bf16)

    @pl.when(step == steps - 1)
    def _():
        lanes = lax.broadcasted_iota(jnp.int32, (8, t), 1)
        for h in range(2):
            for a in range(QWIN):
                total = jnp.zeros((8, t), f32)
                for first in range(0, t, 8):
                    rows = m_ref[h, first:first + 8, a * t:(a + 1) * t]
                    turned = pltpu.roll(rows, t - first, 1) if first else rows
                    total = total + jnp.where(lanes < t - first, turned, 0.0)
                gconv_ref[h, a] = total[:, :EP]


def attend_back(mix, qkv, dcol, drow, tt, gain, dn, xhat, s, p, z):
    n, t, _ = qkv.shape
    row = lambda *sh: pl.BlockSpec((1,) + sh, lambda i: (i,) + (0,) * len(sh))
    full = lambda a: pl.BlockSpec(a.shape, lambda i: (0,) * a.ndim)
    keep = lambda *sh: pl.BlockSpec(sh, lambda i: (0,) * len(sh))
    return pl.pallas_call(
        bwd_kernel,
        grid=(n,),
        in_specs=[pl.BlockSpec(memory_space=pltpu.SMEM), row(t, 6 * EP), row(t, 1), row(1, t), full(tt), full(gain),
                  row(t, 2 * EP), row(t, 2 * EP), row(t, 2 * EP), row(2, t, t), row(2, t, t)],
        out_specs=[row(t, 6 * EP), keep(2, QWIN, 8, EP), keep(8, t), keep(8, 2 * EP)],
        out_shape=[
            jax.ShapeDtypeStruct((n, t, 6 * EP), bf16),
            jax.ShapeDtypeStruct((2, QWIN, 8, EP), f32),
            jax.ShapeDtypeStruct((8, t), f32),
            jax.ShapeDtypeStruct((8, 2 * EP), f32),
        ],
        scratch_shapes=[pltpu.VMEM((2, t, QWIN * t), f32)],
        cost_estimate=pl.CostEstimate(flops=n * 2 * 2 * 2 * t * t * QWIN * t, bytes_accessed=n * t * t * 20, transcendentals=0),
        name="attend_back",
    )(mix, qkv, dcol, drow, tt, gain, dn, xhat, s, p, z)


def bands(kernel, t):
    diff = jnp.arange(t)[None, :] - jnp.arange(t)[:, None]
    band = jnp.zeros((2, QWIN, t, t), f32)
    back = jnp.zeros((2, QWIN, t, t), f32)
    for b in range(KWIN):
        tap = kernel[:, :, b][:, :, None, None]
        band = band + jnp.where(diff == b, tap, 0.0)
        back = back + jnp.where(diff == -b, tap, 0.0)
    th, tl = split(band)
    flat = lambda v: v.reshape(2, QWIN * t, t)
    return flat(th), flat(tl), flat(back.astype(bf16))


def diagonals(tiles):
    return sum(tiles[:, :, i, i:i + KWIN] for i in range(8))


FF = 4096


def rms_scale(values):
    return lax.rsqrt(jnp.mean(values * values, axis=1, keepdims=True) + 1e-06)


class Links:
    def __init__(self, fsdp):
        self.fsdp = fsdp
        index = lax.axis_index("fsdp")
        self.x = lax.axis_index("rep")
        self.z, self.y, self.c = index // 4, (index // 2) % 2, index % 2

    def across(self, flip, v):
        if flip == "x":
            return lax.ppermute(v, "rep", [(0, 1), (1, 0)])
        bit = {"y": 2, "c": 1}[flip]
        return lax.ppermute(v, "fsdp", [(f, f ^ bit) for f in range(self.fsdp)])

    def along(self, v, step):
        pairs = [(f, f + 4 * step) for f in range(self.fsdp) if 0 <= f + 4 * step < self.fsdp]
        return lax.ppermute(v, "fsdp", pairs)

    def ordered(self, bit, mine, other, axis):
        first, second = jnp.where(bit == 0, mine, other), jnp.where(bit == 0, other, mine)
        return jnp.stack([first, second], axis)

    def gather_z(self, v):
        left, right = [], []
        a = b = v
        for _ in range(3):
            a, b = self.along(a, 1), self.along(b, -1)
            left.append(a)
            right.append(b)
        line = jnp.stack(left[::-1] + [v] + right)
        return lax.dynamic_slice_in_dim(line, 3 - self.z, 4, 0)

    def scatter_z(self, parts):
        zero = jnp.zeros((3,) + parts.shape[1:], parts.dtype)
        line = lax.dynamic_slice_in_dim(jnp.concatenate([zero, parts, zero]), self.z, 7, 0)
        low = lambda v: v.astype(bf16)
        a = self.along(low(line[6]), 1)
        b = self.along(low(line[0]), -1)
        for step in (1, 2):
            a = self.along(low(line[6 - step] + a.astype(f32)), 1)
            b = self.along(low(line[step] + b.astype(f32)), -1)
        return line[3] + a.astype(f32) + b.astype(f32)

    def gather_plane(self, v):
        n = v.shape[0] // 2
        vx, vy = self.across("x", v), self.across("y", v)
        vd = jnp.concatenate([self.across("y", vx[:n]), self.across("x", vy[n:])])
        return [jnp.concatenate([u, self.across("c", u)]) for u in (v, vx, vy, vd)]

    def scatter_plane(self, parts):
        low = lambda v: v.astype(bf16)
        n = parts[0].shape[0] // 2
        s = [p[:n] + self.across("c", low(p[n:])).astype(f32) for p in parts]
        m = n // 2
        dx, dy = self.across("x", low(s[3][:m])), self.across("y", low(s[3][m:]))
        to_x = jnp.concatenate([s[1][:m], s[1][m:] + dy.astype(f32)])
        to_y = jnp.concatenate([s[2][:m] + dx.astype(f32), s[2][m:]])
        return s[0] + self.across("x", low(to_x)).astype(f32) + self.across("y", low(to_y)).astype(f32)


class Weights:
    def __init__(self, links):
        self.links = links
        self.line = links.fsdp == 16
        x, y, c = links.x, links.y, links.c
        self.pair = 4 * x + 2 * c + y
        self.slot = 4 * x + 2 * y + c

    def spread(self, shard, dims):
        l = self.links
        ax, ay, ac = dims
        v = lax.dynamic_index_in_dim(shard, l.x, ax, keepdims=True)
        keep = lax.dynamic_index_in_dim(v, l.y, ay, keepdims=True)
        sent = l.across("y", lax.dynamic_index_in_dim(v, 1 - l.y, ay, keepdims=True))
        v = l.ordered(l.y, keep, sent, 0)
        keep = lax.dynamic_index_in_dim(v, l.c, ac + 1, keepdims=True)
        sent = l.across("c", lax.dynamic_index_in_dim(v, 1 - l.c, ac + 1, keepdims=True))
        v = l.ordered(l.c, keep, sent, 1)
        return l.gather_z(v)

    def collect(self, grad, dims):
        l = self.links
        ax, ay, ac = dims
        low = lambda v: v.astype(bf16)
        v = l.scatter_z(grad)
        keep = lax.dynamic_index_in_dim(v, l.c, 1, keepdims=False)
        sent = l.across("c", low(lax.dynamic_index_in_dim(v, 1 - l.c, 1, keepdims=False)))
        v = self.join(l.c, keep, sent.astype(f32), ac + 1)
        keep = lax.dynamic_index_in_dim(v, l.y, 0, keepdims=False)
        sent = l.across("y", low(lax.dynamic_index_in_dim(v, 1 - l.y, 0, keepdims=False)))
        v = low(self.join(l.y, keep, sent.astype(f32), ay))
        return self.join(l.x, v, l.across("x", v), ax).astype(f32)

    def join(self, bit, mine, other, axis):
        first, second = jnp.where(bit == 0, mine, other), jnp.where(bit == 0, other, mine)
        return jnp.concatenate([first, second], axis)

    def whole(self, shard):
        return lax.all_gather(shard, "fsdp", axis=0, tiled=True)

    def owned(self, grad):
        part = lax.psum_scatter(grad, "fsdp", scatter_dimension=0, tiled=True)
        return lax.psum(part.astype(bf16), "rep").astype(f32)

    def qkv(self, shard):
        rows = shard.shape[0]
        if self.line:
            v = self.spread(shard.reshape(rows, 3, 2, 2, 2, 2 * E), (2, 4, 3))
            v = v.reshape(MODEL_WIDTH, 3, 2, E)
        else:
            v = self.whole(shard).reshape(MODEL_WIDTH, 3, 8, 2, E)
            v = lax.dynamic_index_in_dim(v, self.pair, 2, keepdims=False)
        return jnp.pad(v, ((0, 0), (0, 0), (0, 0), (0, EP - E))).reshape(MODEL_WIDTH, 6 * EP)

    def qkv_back(self, grad):
        g = grad.reshape(MODEL_WIDTH, 3, 2, EP)[..., :E]
        if self.line:
            return self.collect(g.reshape(4, 2, 2, -1, 3, 1, 1, 1, 2 * E), (2, 4, 3)).reshape(-1, 3 * MODEL_WIDTH)
        zero = jnp.zeros((MODEL_WIDTH, 3, 8, 2, E), f32)
        return self.owned(lax.dynamic_update_index_in_dim(zero, g, self.pair, 2).reshape(MODEL_WIDTH, 3 * MODEL_WIDTH))

    def out(self, shard):
        l = self.links
        if self.line:
            v = l.gather_z(shard)
            keep = lax.dynamic_index_in_dim(v, 2 * l.x + l.c, 0, keepdims=False)
            sent = l.across("c", lax.dynamic_index_in_dim(v, 2 * l.x + 1 - l.c, 0, keepdims=False))
            v = l.ordered(l.c, keep, sent, 0)
        else:
            v = self.whole(shard).reshape(8, 2, E, MODEL_WIDTH)
            v = lax.dynamic_index_in_dim(v, self.pair, 0, keepdims=False)
        return jnp.pad(v, ((0, 0), (0, EP - E), (0, 0))).reshape(2 * EP, MODEL_WIDTH)

    def out_back(self, grad):
        l = self.links
        g = grad.reshape(2, EP, MODEL_WIDTH)[:, :E]
        if self.line:
            keep = lax.dynamic_index_in_dim(g, l.c, 0, keepdims=False)
            sent = l.across("c", lax.dynamic_index_in_dim(g, 1 - l.c, 0, keepdims=False).astype(bf16)).astype(f32)
            at = jnp.arange(4)[:, None, None]
            parts = jnp.where(at == 2 * l.x + l.c, keep[None], jnp.where(at == 2 * l.x + 1 - l.c, sent[None], 0.0))
            v = l.scatter_z(parts).astype(bf16)
            return (v + l.across("x", v)).astype(f32)
        zero = jnp.zeros((8, 2, E, MODEL_WIDTH), f32)
        return self.owned(lax.dynamic_update_index_in_dim(zero, g, self.pair, 0).reshape(MODEL_WIDTH, MODEL_WIDTH))

    def ffn_in(self, gate, up_):
        rows = gate.shape[0]
        both = jnp.stack([gate, up_], 1)
        if self.line:
            v = self.spread(both.reshape(rows, 2, 4, 2, 2, 2, FF // 32), (5, 3, 4))
            return v.reshape(MODEL_WIDTH, FF // 4)
        v = self.whole(both).reshape(MODEL_WIDTH, 2, 8, FF // 8)
        return lax.dynamic_index_in_dim(v, self.slot, 2, keepdims=False).reshape(MODEL_WIDTH, FF // 4)

    def ffn_in_back(self, grad):
        if self.line:
            v = self.collect(grad.reshape(4, 2, 2, -1, 2, 4, 1, 1, 1, FF // 32), (5, 3, 4)).reshape(-1, 2, FF)
        else:
            zero = jnp.zeros((MODEL_WIDTH, 2, 8, FF // 8), f32)
            g = grad.reshape(MODEL_WIDTH, 2, FF // 8)
            v = self.owned(lax.dynamic_update_index_in_dim(zero, g, self.slot, 2).reshape(MODEL_WIDTH, 2, FF))
        return v[:, 0], v[:, 1]

    def ffn_out(self, shard):
        l = self.links
        if self.line:
            v = lax.dynamic_index_in_dim(shard.reshape(2, FF // 32, MODEL_WIDTH), l.x, 0, keepdims=False)
            return l.gather_z(v).reshape(FF // 8, MODEL_WIDTH)
        v = self.whole(shard).reshape(8, FF // 8, MODEL_WIDTH)
        return lax.dynamic_index_in_dim(v, self.slot, 0, keepdims=False)

    def ffn_out_back(self, grad):
        l = self.links
        if self.line:
            v = l.scatter_z(grad.reshape(4, FF // 32, MODEL_WIDTH)).astype(bf16)
            return self.join(l.x, v, l.across("x", v), 0).astype(f32)
        zero = jnp.zeros((8, FF // 8, MODEL_WIDTH), f32)
        return self.owned(lax.dynamic_update_index_in_dim(zero, grad, self.slot, 0).reshape(FF, MODEL_WIDTH))

    def gains(self, *shards):
        l = self.links
        v = jnp.stack(shards)
        if self.line:
            v = l.ordered(l.c, v, l.across("c", v), 0)
            v = l.ordered(l.y, v, l.across("y", v), 0)
            v = l.gather_z(v)
            v = v.reshape(16, len(shards), -1).transpose(1, 0, 2).reshape(len(shards), MODEL_WIDTH)
        else:
            v = lax.all_gather(v, "fsdp", axis=1, tiled=True)
        return [v[i].astype(f32) for i in range(len(shards))]


def per_device(
    fsdp,
    x_in,
    doc_ids,
    w_qkv,
    w_out,
    gain_attn,
    gain_group,
    conv_kernel,
    head_mix,
    gain_ffn,
    w_gate,
    w_up,
    w_down,
    cotangent,
):
    links = Links(fsdp)
    weights = Weights(links)
    tokens = x_in.shape[1]

    x_all = jnp.concatenate(links.gather_plane(x_in[0]))
    qkv_w = weights.qkv(w_qkv)
    gain_a, gain_g, gain_f = weights.gains(gain_attn, gain_group, gain_ffn)
    docs = doc_ids
    for flip in ("y", "x"):
        docs = jnp.concatenate([docs, links.across(flip, docs)])
    docs = jnp.stack([docs, links.across("c", docs)], 1)
    docs = docs[jnp.array([0, 2, 1, 3])].reshape(8, tokens)
    out_w = weights.out(w_out)
    in_w = weights.ffn_in(w_gate, w_up)
    down_w = weights.ffn_out(w_down)
    upstream_chips = links.gather_plane(cotangent[0])

    kernel = lax.dynamic_slice_in_dim(conv_kernel, 2 * weights.pair, 2, 0)
    mix = lax.dynamic_slice_in_dim(head_mix, 2 * weights.pair, 2, 0)
    th, tl, tt = bands(kernel, tokens)
    group = lax.dynamic_slice_in_dim(gain_g.reshape(8, 2, E), weights.pair, 1, 0)
    group = jnp.pad(group, ((0, 0), (0, 0), (0, EP - E))).reshape(1, 2 * EP)
    doc_col, doc_row = docs[:, :, None], docs[:, None, :]

    xf_all = x_all.astype(f32)
    a1 = (xf_all * rms_scale(xf_all) * gain_a).astype(bf16)
    qkv = dot(a1, qkv_w).astype(bf16).reshape(8, tokens, 6 * EP)
    normed, xhat, s, probs, zeroed = attend(mix, qkv, doc_col, doc_row, th, tl, group)
    normed = normed.reshape(4, 2 * tokens, 2 * EP)
    xf = x_in[0].astype(f32)
    resid = xf + links.scatter_plane([dot(normed[i], out_w) for i in range(4)])

    r2 = rms_scale(resid)
    a2_chips = links.gather_plane((resid * r2 * gain_f).astype(bf16))
    out_parts, back_parts, hiddens, dgus = [], [], [], []
    half = FF // 8
    for a2, dffn in zip(a2_chips, upstream_chips):
        gu = dot(a2, in_w)
        gate, up_act = gu[:, :half], gu[:, half:]
        sig = jax.nn.sigmoid(gate)
        silu = gate * sig
        hidden = (silu * up_act).astype(bf16)
        dhidden = dot(dffn, down_w, 1, 1)
        dgate = (dhidden * up_act * sig * (1.0 + gate * (1.0 - sig))).astype(bf16)
        dup = (dhidden * silu).astype(bf16)
        dgu = jnp.concatenate([dgate, dup], 1)
        hiddens.append(hidden)
        dgus.append(dgu)
        back_parts.append(dot(dgu, in_w, 1, 1))
        out_parts.append(dot(hidden, down_w))
    da2 = links.scatter_plane(back_parts)
    output = (resid + links.scatter_plane(out_parts)).astype(bf16)

    dy = cotangent[0].astype(f32)
    sum_gain_ffn = jnp.sum(da2 * resid * r2, axis=0)
    dn2 = da2 * gain_f
    dresid = dy + r2 * (dn2 - resid * r2 * r2 * jnp.mean(dn2 * resid, axis=1, keepdims=True))
    dattn = jnp.concatenate(links.gather_plane(dresid.astype(bf16)))

    a2_all, dgu_all = jnp.concatenate(a2_chips), jnp.concatenate(dgus)
    hidden_all, dffn_all = jnp.concatenate(hiddens), jnp.concatenate(upstream_chips)
    grad_gate, grad_up = weights.ffn_in_back(dot(a2_all, dgu_all, 0, 0))
    grad_down = weights.ffn_out_back(dot(hidden_all, dffn_all, 0, 0))

    dnormed = dot(dattn, out_w, 1, 1).reshape(8, tokens, 2 * EP)
    dqkv, conv_tiles, mix_sums, group_sums = attend_back(
        mix, qkv, doc_col, doc_row, tt, group, dnormed, xhat, s, probs, zeroed
    )
    dqkv = dqkv.reshape(4, 2 * tokens, 6 * EP)
    da1 = links.scatter_plane([dot(dqkv[i], qkv_w, 1, 1) for i in range(4)])
    grad_out = weights.out_back(dot(normed.reshape(8 * tokens, 2 * EP), dattn, 0, 0))
    grad_qkv = weights.qkv_back(dot(a1, dqkv.reshape(8 * tokens, 6 * EP), 0, 0))

    r1 = rms_scale(xf)
    sum_gain_attn = jnp.sum(da1 * xf * r1, axis=0)
    dn1 = da1 * gain_a
    grad_x = dresid + r1 * (dn1 - xf * r1 * r1 * jnp.mean(dn1 * xf, axis=1, keepdims=True))

    place = lambda v: lax.dynamic_update_index_in_dim(jnp.zeros((8,) + v.shape, f32), v, weights.pair, 0)
    small = [
        sum_gain_attn,
        sum_gain_ffn,
        place(group_sums[0].reshape(2, EP)[:, :E].reshape(-1)),
        place(diagonals(conv_tiles)),
        place(jnp.sum(mix_sums[:4], axis=1)),
    ]
    sizes = [v.size for v in small]
    total = lax.psum(jnp.concatenate([v.reshape(-1) for v in small]), ("rep", "fsdp"))
    cut = [0]
    for size in sizes:
        cut.append(cut[-1] + size)
    gain_a_sum, gain_f_sum, group_sum, conv_sum, mix_sum = (total[cut[i] : cut[i + 1]] for i in range(5))
    rows = gain_attn.shape[0]
    own = lambda v: lax.dynamic_slice_in_dim(v, lax.axis_index("fsdp") * rows, rows, 0)
    return (
        output[None],
        grad_x[None],
        grad_qkv,
        grad_out,
        own(gain_a_sum),
        own(group_sum),
        conv_sum.reshape(H, QWIN, KWIN),
        mix_sum.reshape(H, 2),
        own(gain_f_sum),
        grad_gate,
        grad_up,
        grad_down,
    )


def solution(mesh):
    fsdp = mesh.shape["fsdp"]
    assert mesh.shape["rep"] == 2 and fsdp % 4 == 0
    rows, shard, part = P(("rep", "fsdp"), None, None), P("fsdp", None), P("fsdp")
    placed = (rows, P(("rep", "fsdp"), None), shard, shard, part, part, P(), P(), part, shard, shard, shard, rows)
    return jax.shard_map(
        lambda *args: per_device(fsdp, *args),
        mesh=mesh,
        in_specs=placed,
        out_specs=(rows, rows, shard, shard, part, part, P(), P(), part, shard, shard, shard),
        check_vma=False,
    )
```

```python
import math

import jax
import jax.numpy as jnp
from jax import lax
from jax.experimental import pallas as pl
from jax.experimental.pallas import tpu as pltpu
from jax.sharding import PartitionSpec as P

MODEL_WIDTH = 1536
H = 16
E = 96
EP = 128
QWIN = 6
KWIN = 11
bf16, f32 = jnp.bfloat16, jnp.float32


def allowed_mask(doc_col, doc_row):
    n = doc_row.shape[-1]
    i = lax.broadcasted_iota(jnp.int32, (n, n), 0)
    j = lax.broadcasted_iota(jnp.int32, (n, n), 1)
    return (j <= i) & (doc_col == doc_row)


def down(v, a):
    if a == 0:
        return v
    i = lax.broadcasted_iota(jnp.int32, v.shape, 0)
    return jnp.where(i >= a, pltpu.roll(v, a, 0), 0.0)


def up(v, a):
    if a == 0:
        return v
    n = v.shape[0]
    i = lax.broadcasted_iota(jnp.int32, v.shape, 0)
    return jnp.where(i < n - a, pltpu.roll(v, n - a, 0), 0.0)


def dot(a, b, ca=1, cb=0):
    return lax.dot_general(a, b, (((ca,), (cb,)), ((), ())), preferred_element_type=f32)


def split(v):
    hi = v.astype(bf16)
    return hi, (v - hi.astype(f32)).astype(bf16)


def fwd_kernel(mix_ref, qkv_ref, dcol_ref, drow_ref, th_ref, tl_ref, gain_ref,
               normed_ref, xhat_ref, s_ref, p_ref, z_ref):
    allowed = allowed_mask(dcol_ref[0], drow_ref[0])
    scale = 1.0 / math.sqrt(E)
    probs = []
    for h in range(2):
        q = qkv_ref[0, :, h * EP:(h + 1) * EP]
        k = qkv_ref[0, :, (2 + h) * EP:(3 + h) * EP]
        zeroed = jnp.where(allowed, dot(q, k, 1, 1) * scale, 0.0)
        z_ref[0, h] = zeroed.astype(bf16)
        his, los = [], []
        for a in range(QWIN):
            hi, lo = split(down(zeroed, a))
            his.append(hi)
            los.append(lo)
        his, los = jnp.concatenate(his, 1), jnp.concatenate(los, 1)
        th, tl = th_ref[h], tl_ref[h]
        conv = dot(his, th) + (dot(his, tl) + dot(los, th))
        masked = jnp.where(allowed, conv, -jnp.inf)
        e = jnp.exp(masked - jnp.max(masked, axis=1, keepdims=True))
        p = e / jnp.sum(e, axis=1, keepdims=True)
        p_ref[0, h] = p
        probs.append(p)
    lane = lax.broadcasted_iota(jnp.int32, (1, EP), 1)
    for h in range(2):
        v = qkv_ref[0, :, (4 + h) * EP:(5 + h) * EP]
        mixed = (mix_ref[h, 0] * probs[0] + mix_ref[h, 1] * probs[1]).astype(bf16)
        ho = dot(mixed, v)
        centered = jnp.where(lane < E, ho - jnp.sum(ho, axis=1, keepdims=True) / E, 0.0)
        s = lax.rsqrt(jnp.sum(centered * centered, axis=1, keepdims=True) / E + 1e-05)
        xhat = centered * s
        cols = slice(h * EP, (h + 1) * EP)
        xhat_ref[0, :, cols] = xhat
        s_ref[0, :, cols] = jnp.broadcast_to(s, xhat.shape)
        normed_ref[0, :, cols] = (xhat * gain_ref[0:1, cols]).astype(bf16)


def attend(mix, qkv, dcol, drow, th, tl, gain):
    n, t, _ = qkv.shape
    row = lambda *s: pl.BlockSpec((1,) + s, lambda i: (i,) + (0,) * len(s))
    full = lambda a: pl.BlockSpec(a.shape, lambda i: (0,) * a.ndim)
    return pl.pallas_call(
        fwd_kernel,
        grid=(n,),
        in_specs=[pl.BlockSpec(memory_space=pltpu.SMEM), row(t, 6 * EP), row(t, 1), row(1, t), full(th), full(tl), full(gain)],
        out_specs=[row(t, 2 * EP), row(t, 2 * EP), row(t, 2 * EP), row(2, t, t), row(2, t, t)],
        out_shape=[
            jax.ShapeDtypeStruct((n, t, 2 * EP), bf16),
            jax.ShapeDtypeStruct((n, t, 2 * EP), f32),
            jax.ShapeDtypeStruct((n, t, 2 * EP), f32),
            jax.ShapeDtypeStruct((n, 2, t, t), f32),
            jax.ShapeDtypeStruct((n, 2, t, t), bf16),
        ],
        cost_estimate=pl.CostEstimate(flops=n * 2 * 3 * 2 * t * t * QWIN * t, bytes_accessed=n * t * t * 20, transcendentals=n * 2 * t * t),
        name="attend",
    )(mix, qkv, dcol, drow, th, tl, gain)


def bwd_kernel(mix_ref, qkv_ref, dcol_ref, drow_ref, tt_ref, gain_ref, dn_ref, xhat_ref, s_ref, p_ref, z_ref,
               dqkv_ref, gconv_ref, gmix_ref, gg_ref, m_ref):
    step, steps = pl.program_id(0), pl.num_programs(0)
    t = p_ref.shape[-1]

    @pl.when(step == 0)
    def _():
        m_ref[...] = jnp.zeros_like(m_ref)
        gmix_ref[...] = jnp.zeros_like(gmix_ref)
        gg_ref[...] = jnp.zeros_like(gg_ref)

    allowed = allowed_mask(dcol_ref[0], drow_ref[0])
    scale = 1.0 / math.sqrt(E)
    lane = lax.broadcasted_iota(jnp.int32, (1, EP), 1)
    p = [p_ref[0, 0], p_ref[0, 1]]
    dmixed = []
    for h in range(2):
        cols = slice(h * EP, (h + 1) * EP)
        dn, xhat = dn_ref[0, :, cols], xhat_ref[0, :, cols]
        gg_ref[0:1, cols] += jnp.sum(dn * xhat, axis=0, keepdims=True)
        dc = dn * gain_ref[0:1, cols]
        m1 = jnp.sum(dc, axis=1, keepdims=True) / E
        m2 = jnp.sum(dc * xhat, axis=1, keepdims=True) / E
        dh = jnp.where(lane < E, s_ref[0, :, cols] * (dc - m1 - xhat * m2), 0.0).astype(bf16)
        v = qkv_ref[0, :, (4 + h) * EP:(5 + h) * EP]
        mixed = (mix_ref[h, 0] * p[0] + mix_ref[h, 1] * p[1]).astype(bf16)
        dmixed.append(dot(dh, v, 1, 1))
        dqkv_ref[0, :, (4 + h) * EP:(5 + h) * EP] = dot(mixed, dh, 0, 0).astype(bf16)
    for h in range(2):
        for c in range(2):
            r = 2 * h + c
            gmix_ref[r:r + 1, :] += jnp.sum(dmixed[h] * p[c], axis=0, keepdims=True)
    for c in range(2):
        dp = mix_ref[0, c] * dmixed[0] + mix_ref[1, c] * dmixed[1]
        dconv = p[c] * (dp - jnp.sum(dp * p[c], axis=1, keepdims=True))
        ahead = jnp.concatenate([up(dconv, a).astype(bf16) for a in range(QWIN)], 1)
        m_ref[c] += dot(z_ref[0, c], ahead, 0, 0)
        ds = jnp.where(allowed, dot(ahead, tt_ref[c]), 0.0).astype(bf16)
        q = qkv_ref[0, :, c * EP:(c + 1) * EP]
        k = qkv_ref[0, :, (2 + c) * EP:(3 + c) * EP]
        dqkv_ref[0, :, c * EP:(c + 1) * EP] = (dot(ds, k) * scale).astype(bf16)
        dqkv_ref[0, :, (2 + c) * EP:(3 + c) * EP] = (dot(ds, q, 0, 0) * scale).astype(bf16)

    @pl.when(step == steps - 1)
    def _():
        lanes = lax.broadcasted_iota(jnp.int32, (8, t), 1)
        for h in range(2):
            for a in range(QWIN):
                total = jnp.zeros((8, t), f32)
                for first in range(0, t, 8):
                    rows = m_ref[h, first:first + 8, a * t:(a + 1) * t]
                    turned = pltpu.roll(rows, t - first, 1) if first else rows
                    total = total + jnp.where(lanes < t - first, turned, 0.0)
                gconv_ref[h, a] = total[:, :EP]


def attend_back(mix, qkv, dcol, drow, tt, gain, dn, xhat, s, p, z):
    n, t, _ = qkv.shape
    row = lambda *sh: pl.BlockSpec((1,) + sh, lambda i: (i,) + (0,) * len(sh))
    full = lambda a: pl.BlockSpec(a.shape, lambda i: (0,) * a.ndim)
    keep = lambda *sh: pl.BlockSpec(sh, lambda i: (0,) * len(sh))
    return pl.pallas_call(
        bwd_kernel,
        grid=(n,),
        in_specs=[pl.BlockSpec(memory_space=pltpu.SMEM), row(t, 6 * EP), row(t, 1), row(1, t), full(tt), full(gain),
                  row(t, 2 * EP), row(t, 2 * EP), row(t, 2 * EP), row(2, t, t), row(2, t, t)],
        out_specs=[row(t, 6 * EP), keep(2, QWIN, 8, EP), keep(8, t), keep(8, 2 * EP)],
        out_shape=[
            jax.ShapeDtypeStruct((n, t, 6 * EP), bf16),
            jax.ShapeDtypeStruct((2, QWIN, 8, EP), f32),
            jax.ShapeDtypeStruct((8, t), f32),
            jax.ShapeDtypeStruct((8, 2 * EP), f32),
        ],
        scratch_shapes=[pltpu.VMEM((2, t, QWIN * t), f32)],
        cost_estimate=pl.CostEstimate(flops=n * 2 * 2 * 2 * t * t * QWIN * t, bytes_accessed=n * t * t * 20, transcendentals=0),
        name="attend_back",
    )(mix, qkv, dcol, drow, tt, gain, dn, xhat, s, p, z)


def bands(kernel, t):
    diff = jnp.arange(t)[None, :] - jnp.arange(t)[:, None]
    band = jnp.zeros((2, QWIN, t, t), f32)
    back = jnp.zeros((2, QWIN, t, t), f32)
    for b in range(KWIN):
        tap = kernel[:, :, b][:, :, None, None]
        band = band + jnp.where(diff == b, tap, 0.0)
        back = back + jnp.where(diff == -b, tap, 0.0)
    th, tl = split(band)
    flat = lambda v: v.reshape(2, QWIN * t, t)
    return flat(th), flat(tl), flat(back.astype(bf16))


def diagonals(tiles):
    return sum(tiles[:, :, i, i:i + KWIN] for i in range(8))


FF = 4096
MESH = pl.DeviceIdType.MESH


class Net:
    def __init__(self):
        self.x, self.f = lax.axis_index("rep"), lax.axis_index("fsdp")
        self.z, self.y, self.c = self.f // 4, (self.f // 2) % 2, self.f % 2
        self.k = self.f % 4
        nx, fy, fc = 1 - self.x, 2 - 4 * self.y, 1 - 2 * self.c
        self.to = {
            "x": (nx, self.f),
            "y": (self.x, self.f + fy),
            "c": (self.x, self.f + fc),
            "xy": (nx, self.f + fy),
            "xc": (nx, self.f + fc),
            "yc": (self.x, self.f + fy + fc),
            "xyc": (nx, self.f + fy + fc),
            "up": (self.x, self.f + 4),
            "down": (self.x, self.f - 4),
        }

    def greet(self, names, line=True):
        barrier = pltpu.get_barrier_semaphore()
        for name in names:
            pl.semaphore_signal(barrier, inc=1, device_id=self.to[name], device_id_type=MESH)
        count = len(names)
        if line:

            @pl.when(self.z < 3)
            def _():
                pl.semaphore_signal(barrier, inc=1, device_id=self.to["up"], device_id_type=MESH)

            @pl.when(self.z > 0)
            def _():
                pl.semaphore_signal(barrier, inc=1, device_id=self.to["down"], device_id_type=MESH)

            count = count + (self.z + 3) // 4 + (6 - self.z) // 4
        pl.semaphore_wait(barrier, count)

    def copy(self, src, dst, sems, i, name):
        return pltpu.make_async_remote_copy(
            src_ref=src, dst_ref=dst, send_sem=sems[0].at[i], recv_sem=sems[1].at[i],
            device_id=self.to[name], device_id_type=MESH,
        )

    def send(self, src, dst, sems, i, name):
        copy = self.copy(src, dst, sems, i, name)
        copy.start()
        return copy


def tiles(start, size, body, step=32):
    def one(i, _):
        body(pl.ds(pl.multiple_of(start + i * step, step), step))
        return 0

    lax.fori_loop(0, size // step, one, 0)


def wide(v):
    return v.astype(f32)


class GatherLine:
    def __init__(self, net, src, out, sems, base, keep=None):
        self.net, self.src, self.out, self.sems, self.base = net, src, out, sems, base
        self.keep = keep or (lambda slot: net.z >= 0)

    def go(self, d, way, act):
        net = self.net
        slot = net.z - d if way == "up" else net.z + d
        inside = (net.z >= d) & (net.z < 3) if way == "up" else (net.z < 4 - d) & (net.z > 0)
        i = self.base + d + (0 if way == "up" else 3)

        @pl.when(inside & self.keep(slot))
        def _():
            src = self.src if d == 0 else self.out.at[slot]
            act(net.copy(src, self.out.at[slot], self.sems, i, way))

    def came(self, d, way):
        net = self.net
        slot = net.z - d if way == "up" else net.z + d
        inside = net.z >= d if way == "up" else net.z < 4 - d
        i = self.base + d - 1 + (0 if way == "up" else 3)

        @pl.when(inside & self.keep(slot))
        def _():
            net.copy(self.out.at[slot], self.out.at[slot], self.sems, i, way).wait_recv()

    def step(self, d):
        for way in ("up", "down"):
            if d > 0:
                self.came(d, way)
            if d < 3:
                self.go(d, way, lambda copy: copy.start())

    def finish(self):
        for d in range(3):
            for way in ("up", "down"):
                self.go(d, way, lambda copy: copy.wait_send())


class ScatterLine:
    def __init__(self, net, parts, got, made, sems, base):
        self.net, self.parts, self.got, self.made, self.sems, self.base = net, parts, got, made, sems, base
        self.n = parts.shape[1]

    def each(self, d, way):
        net = self.net
        t = net.z + (3 - d) if way == 0 else net.z - (3 - d)
        inside = (t < 4) if way == 0 else (t >= 0)
        first = (net.z == 0) if way == 0 else (net.z == 3)
        return t, inside, first, self.base + d + 3 * way, ("up", "down")[way]

    def step(self, d):
        for way in range(2):
            t, inside, first, i, name = self.each(d, way)

            @pl.when(inside & first)
            def _():
                self.net.copy(self.parts.at[t], self.got.at[way, d], self.sems, i, name).start()

            if d == 0:
                continue

            @pl.when(inside & jnp.logical_not(first))
            def _():
                self.net.copy(self.got.at[way, d - 1], self.got.at[way, d - 1], self.sems, i - 1, name).wait_recv()

                def body(rows):
                    self.made[way, d - 1, rows] = (wide(self.parts[t, rows]) + wide(self.got[way, d - 1, rows])).astype(bf16)

                tiles(0, self.n, body)
                self.net.copy(self.made.at[way, d - 1], self.got.at[way, d], self.sems, i, name).start()

    def finish(self, store):
        net = self.net
        below, above = net.z > 0, net.z < 3

        @pl.when(below)
        def _():
            net.copy(self.got.at[0, 2], self.got.at[0, 2], self.sems, self.base + 2, "up").wait_recv()

        @pl.when(above)
        def _():
            net.copy(self.got.at[1, 2], self.got.at[1, 2], self.sems, self.base + 5, "down").wait_recv()

        def put(low, high):
            def body(rows):
                total = wide(self.parts[net.z, rows])
                if low:
                    total = total + wide(self.got[0, 2, rows])
                if high:
                    total = total + wide(self.got[1, 2, rows])
                store(rows, total)

            tiles(0, self.n, body)

        @pl.when(below & above)
        def _():
            put(True, True)

        @pl.when(jnp.logical_not(below))
        def _():
            put(False, True)

        @pl.when(jnp.logical_not(above))
        def _():
            put(True, False)

        for d in range(3):
            for way in range(2):
                t, inside, first, i, name = self.each(d, way)

                @pl.when(inside & first)
                def _():
                    net.copy(self.parts.at[t], self.got.at[way, d], self.sems, i, name).wait_send()

                if d > 0:

                    @pl.when(inside & jnp.logical_not(first))
                    def _():
                        net.copy(self.made.at[way, d - 1], self.got.at[way, d], self.sems, i, name).wait_send()


def line_scratch(n, w):
    return [pltpu.VMEM((2, 3, n, w), bf16), pltpu.VMEM((2, 2, n, w), bf16)]


LINE_COPIES = 6


def gather_rows(net, v, out, sems, base, ready, poll):
    n = v.shape[0]
    A, B = pl.ds(0, n // 2), pl.ds(n // 2, n // 2)
    go = {}
    ready(0)
    go["xA"] = net.send(v.at[A], out.at[1, 0, A], sems, base + 0, "x")
    go["yA"] = net.send(v.at[A], out.at[2, 0, A], sems, base + 3, "y")
    go["0A"] = net.send(v.at[A], out.at[0, 1, A], sems, base + 4, "c")
    ready(1)
    go["yB"] = net.send(v.at[B], out.at[2, 0, B], sems, base + 2, "y")
    go["xB"] = net.send(v.at[B], out.at[1, 0, B], sems, base + 1, "x")
    go["0B"] = net.send(v.at[B], out.at[0, 1, B], sems, base + 5, "c")
    poll()
    go["xA"].wait_recv()
    go["dA"] = net.send(out.at[1, 0, A], out.at[3, 0, A], sems, base + 6, "y")
    go["1A"] = net.send(out.at[1, 0, A], out.at[1, 1, A], sems, base + 8, "c")
    go["yA"].wait_recv()
    go["2A"] = net.send(out.at[2, 0, A], out.at[2, 1, A], sems, base + 10, "c")
    poll()
    go["yB"].wait_recv()
    go["dB"] = net.send(out.at[2, 0, B], out.at[3, 0, B], sems, base + 7, "x")
    go["2B"] = net.send(out.at[2, 0, B], out.at[2, 1, B], sems, base + 9, "c")
    go["xB"].wait_recv()
    go["1B"] = net.send(out.at[1, 0, B], out.at[1, 1, B], sems, base + 11, "c")
    poll()
    go["dA"].wait_recv()
    go["3A"] = net.send(out.at[3, 0, A], out.at[3, 1, A], sems, base + 12, "c")
    go["dB"].wait_recv()
    go["3B"] = net.send(out.at[3, 0, B], out.at[3, 1, B], sems, base + 13, "c")
    poll()
    for name in ("0A", "0B", "1A", "2B", "2A", "1B", "3A", "3B"):
        go[name].wait_recv()
    for copy in go.values():
        copy.wait_send()


GATHER_COPIES = 14
SCATTER_COPIES = 10


def scatter_rows(net, parts, rc, rd, rx, ry, td, tx, ty, sems, base, poll):
    n = parts.shape[2]
    A, B = pl.ds(0, n // 2), pl.ds(n // 2, n // 2)
    go = {}
    for i, chip in enumerate((3, 1, 2, 0)):
        go[chip] = net.send(parts.at[chip, 1], rc.at[chip], sems, base + i, "c")

    def add(dst, chip, start, more=None):
        def body(rows):
            total = wide(parts[chip, 0, rows]) + wide(rc[chip, rows])
            if more is not None:
                total = total + wide(more[rows])
            dst[rows] = total.astype(bf16)

        tiles(start, n // 2, body)

    go[3].wait_recv()
    add(td, 3, 0)
    go["dA"] = net.send(td.at[A], rd.at[A], sems, base + 4, "x")
    add(td, 3, n // 2)
    go["dB"] = net.send(td.at[B], rd.at[B], sems, base + 5, "y")
    go[1].wait_recv()
    add(tx, 1, 0)
    go["xA"] = net.send(tx.at[A], rx.at[A], sems, base + 6, "x")
    go[2].wait_recv()
    add(ty, 2, n // 2)
    go["yB"] = net.send(ty.at[B], ry.at[B], sems, base + 7, "y")
    poll()
    go["dA"].wait_recv()
    add(ty, 2, 0, rd)
    go["yA"] = net.send(ty.at[A], ry.at[A], sems, base + 8, "y")
    go["dB"].wait_recv()
    add(tx, 1, n // 2, rd)
    go["xB"] = net.send(tx.at[B], rx.at[B], sems, base + 9, "x")
    go[0].wait_recv()

    def done(half):
        for name in (("xA", "yA"), ("xB", "yB"))[half]:
            go[name].wait_recv()
        if half == 1:
            for copy in go.values():
                copy.wait_send()

    return done


def scatter_scratch(n, w):
    return [pltpu.VMEM((4, n, w), bf16)] + [pltpu.VMEM((n, w), bf16)] * 6


def dma_sems(count):
    return [pltpu.SemaphoreType.DMA((count,)), pltpu.SemaphoreType.DMA((count,))]


VM = pl.BlockSpec(memory_space=pltpu.VMEM)
ANY = pl.BlockSpec(memory_space=pl.ANY)


def polls(*acts):
    left = list(acts)

    def poll():
        if left:
            left.pop(0)()

    def drain():
        while left:
            poll()

    return poll, drain


def comm_call(body, name, ident, ins, in_specs, outs, out_specs, scratch):
    return pl.pallas_call(
        body,
        in_specs=in_specs,
        out_specs=out_specs,
        out_shape=outs,
        scratch_shapes=scratch,
        compiler_params=pltpu.CompilerParams(collective_id=ident, has_side_effects=True, vmem_limit_bytes=60 << 20),
        name=name,
    )(*ins)


def shape(dims, dtype):
    return jax.ShapeDtypeStruct(dims, dtype)


PLANE = ("x", "y", "c", "xy", "xc", "yc", "xyc")
PLACES = {"c": (0, 1), "x": (1, 0), "xc": (1, 1), "y": (2, 0), "yc": (2, 1), "xy": (3, 0), "xyc": (3, 1)}


def start_call(x, dy, docs, gains, w_qkv, w_gate, w_up, w_out, ident):
    n, w = x.shape
    rows = w_qkv.shape[0]

    def body(x_ref, dy_ref, docs_ref, g_ref, wq_ref, gate_ref, up_ref, wo_ref,
             xs_ref, dys_ref, docs_out, gains_out, qkv_out, gu_out, wo_out, slots, gus, local, send, recv):
        net = Net()
        sems = (send, recv)
        base = 2 * GATHER_COPIES
        line_q = GatherLine(net, qkv_out.at[net.z], qkv_out, sems, base)
        line_o = GatherLine(net, wo_ref, wo_out, sems, base + 6, lambda slot: slot // 2 == net.x)
        line_g = GatherLine(net, gains_out.at[net.z], gains_out, sems, base + 12)
        base += 18
        slots[...] = jnp.zeros_like(slots)
        for half in range(2):

            @pl.when(net.x == half)
            def _():
                for k in range(4):
                    pair = 4 * half + 2 * (k % 2) + k // 2
                    for m in range(6):
                        col = (m // 2) * MODEL_WIDTH + (2 * pair + m % 2) * E
                        slots[k, :, m * EP : m * EP + E] = wq_ref[:, col : col + E]
                    for m in range(8):
                        src = gate_ref if m < 4 else up_ref
                        col = 256 * (4 * (m % 4) + k) + 128 * half
                        gus[k, :, m * 128 : (m + 1) * 128] = src[:, col : col + 128]

        net.greet(PLANE)
        own = [
            pltpu.make_async_copy(x_ref, xs_ref.at[0, 0], local.at[0]),
            pltpu.make_async_copy(dy_ref, dys_ref.at[0, 0], local.at[1]),
            pltpu.make_async_copy(slots.at[net.k], qkv_out.at[net.z, net.k], local.at[2]),
            pltpu.make_async_copy(gus.at[net.k], gu_out.at[net.k], local.at[3]),
            pltpu.make_async_copy(g_ref, gains_out.at[net.z, net.k], local.at[4]),
            pltpu.make_async_copy(docs_ref, docs_out.at[0, 0], local.at[5]),
            pltpu.make_async_copy(wo_ref, wo_out.at[net.z], local.at[6]),
        ]
        for copy in own:
            copy.start()
        shares, small = [], []
        flips = {"c": net.k + 1 - 2 * net.c, "y": net.k + 2 - 4 * net.y, "yc": net.k + 1 - 2 * net.c + 2 - 4 * net.y}
        for j, name in enumerate(("y", "yc", "c")):
            other = flips[name]
            shares.append(net.send(slots.at[other], qkv_out.at[net.z, net.k], sems, base + j, name))
            small.append(net.send(g_ref, gains_out.at[net.z, net.k], sems, base + 6 + j, name))
        for j, (name, (chip, core)) in enumerate(PLACES.items()):
            small.append(net.send(docs_ref, docs_out.at[chip, core], sems, base + 9 + j, name))

        def rest():
            for j, name in enumerate(("y", "yc", "c")):
                small.append(net.send(gus.at[flips[name]], gu_out.at[net.k], sems, base + 3 + j, name))

        def line0():
            own[2].wait()
            own[4].wait()
            for copy in shares:
                copy.wait_recv()
            for copy in small[:3]:
                copy.wait_recv()
            line_q.step(0)
            line_g.step(0)
            line_o.step(0)

        def both(d):
            def act():
                line_q.step(d)
                line_g.step(d)

            return act

        first, _ = polls(line0, both(1))
        gather_rows(net, x_ref, xs_ref, sems, 0, lambda half: None, first)
        rest()
        second, drain = polls(both(2), lambda: line_o.step(1), both(3), lambda: line_o.step(2))
        gather_rows(net, dy_ref, dys_ref, sems, GATHER_COPIES, lambda half: None, second)
        drain()
        line_o.step(3)
        for line in (line_q, line_g, line_o):
            line.finish()
        for copy in own[:2] + [own[3]] + own[5:]:
            copy.wait()
        for copy in small[3:]:
            copy.wait_recv()
        for copy in shares + small:
            copy.wait_send()

    return comm_call(
        body, "start", ident, (x, dy, docs, gains, w_qkv, w_gate, w_up, w_out), [VM] * 7 + [ANY],
        [shape((4, 2, n, w), bf16), shape((4, 2, n, w), bf16), shape((4, 2) + docs.shape, docs.dtype), shape((4, 4) + gains.shape, bf16),
         shape((4, 4, rows, 6 * EP), bf16), shape((4, rows, FF // 4), bf16), shape((4, rows, MODEL_WIDTH), bf16)],
        [ANY] * 7,
        [pltpu.VMEM((4, rows, 6 * EP), bf16), pltpu.VMEM((4, rows, FF // 4), bf16), pltpu.SemaphoreType.DMA((7,))]
        + dma_sems(2 * GATHER_COPIES + 18 + 16),
    )


def mid_call(parts, x, gain, gu, w_down, ident):
    n, w = parts.shape[2:]
    down = w_down.shape[0] // 2

    def body(p_ref, x_ref, g_ref, gu_ref, wd_ref, resid_ref, out_ref, gu_out, wd_out, v, local, rc, rd, rx, ry, td, tx, ty, send, recv):
        net = Net()
        sems = (send, recv)
        net.greet("xyc")
        base = SCATTER_COPIES + GATHER_COPIES
        mine = wd_ref.at[pl.ds(pl.multiple_of(down * net.x, down), down)]
        line_g = GatherLine(net, gu_ref, gu_out, sems, base)
        line_d = GatherLine(net, mine, wd_out, sems, base + LINE_COPIES)
        lines = (line_g, line_d)
        own = [pltpu.make_async_copy(gu_ref, gu_out.at[net.z], local.at[1]), pltpu.make_async_copy(mine, wd_out.at[net.z], local.at[2])]
        for copy in own:
            copy.start()
        for line in lines:
            line.step(0)
        poll, drain = polls(*[lambda d=d, line=line: line.step(d) for d in (1, 2, 3) for line in lines])
        done = scatter_rows(net, p_ref, rc, rd, rx, ry, td, tx, ty, sems, 0, poll)
        poll()

        def ready(half):
            done(half)

            def rows_of(rows):
                total = wide(p_ref[0, 0, rows]) + wide(rc[0, rows]) + wide(rx[rows]) + wide(ry[rows])
                resid = wide(x_ref[rows]) + total
                resid_ref[rows] = resid
                r = lax.rsqrt(jnp.mean(resid * resid, axis=1, keepdims=True) + 1e-06)
                v[rows] = (resid * r * g_ref[...]).astype(bf16)

            tiles(half * (n // 2), n // 2, rows_of)

        gather_rows(net, v, out_ref, sems, SCATTER_COPIES, ready, poll)
        drain()
        last = pltpu.make_async_copy(v, out_ref.at[0, 0], local.at[0])
        last.start()
        for line in lines:
            line.finish()
        for copy in own:
            copy.wait()
        last.wait()

    return comm_call(
        body, "mid", ident, (parts, x, gain, gu, w_down), [VM] * 3 + [ANY] * 2,
        [shape((n, w), f32), shape((4, 2, n, w), bf16), shape((4,) + gu.shape, bf16), shape((4, down, w), bf16)], [VM, ANY, ANY, ANY],
        [pltpu.VMEM((n, w), bf16), pltpu.SemaphoreType.DMA((3,))] + scatter_scratch(n, w)
        + dma_sems(SCATTER_COPIES + GATHER_COPIES + 2 * LINE_COPIES),
    )


def mid_back_call(parts, dy, resid, gain, gu, down, ident):
    n, w = parts.shape[2:]

    def body(p_ref, dy_ref, r_ref, g_ref, gu_ref, down_ref, dresid_ref, out_ref, sum_ref, gu_out, down_out,
             v, local, rc, rd, rx, ry, td, tx, ty, g_got, g_made, d_got, d_made, send, recv):
        net = Net()
        sems = (send, recv)
        net.greet("xyc")
        base = SCATTER_COPIES + GATHER_COPIES
        line_g = ScatterLine(net, gu_ref, g_got, g_made, sems, base)
        line_d = ScatterLine(net, down_ref, d_got, d_made, sems, base + LINE_COPIES)
        lines = (line_g, line_d)
        for line in lines:
            line.step(0)
        acts = [lambda d=d, line=line: line.step(d) for d in (1, 2) for line in lines]
        poll, drain = polls(acts[0], acts[1], lambda: None, acts[2], acts[3])
        sum_ref[...] = jnp.zeros_like(sum_ref)
        done = scatter_rows(net, p_ref, rc, rd, rx, ry, td, tx, ty, sems, 0, poll)
        poll()

        def ready(half):
            done(half)

            def rows_of(rows):
                da2 = wide(p_ref[0, 0, rows]) + wide(rc[0, rows]) + wide(rx[rows]) + wide(ry[rows])
                res = r_ref[rows]
                r = lax.rsqrt(jnp.mean(res * res, axis=1, keepdims=True) + 1e-06)
                unit = res * r
                sum_ref[0:1] += jnp.sum(da2 * unit, axis=0, keepdims=True)
                dn = da2 * g_ref[...]
                dresid = wide(dy_ref[rows]) + r * (dn - unit * r * jnp.mean(dn * res, axis=1, keepdims=True))
                dresid_ref[rows] = dresid
                v[rows] = dresid.astype(bf16)

            tiles(half * (n // 2), n // 2, rows_of)

        gather_rows(net, v, out_ref, sems, SCATTER_COPIES, ready, poll)
        drain()
        last = pltpu.make_async_copy(v, out_ref.at[0, 0], local)
        last.start()

        def put(ref):
            def store(rows, total):
                ref[rows] = total.astype(bf16)

            return store

        line_g.finish(put(gu_out))
        line_d.finish(put(down_out))
        last.wait()

    return comm_call(
        body, "mid_back", ident, (parts, dy, resid, gain, gu, down), [VM] * 6,
        [shape((n, w), f32), shape((4, 2, n, w), bf16), shape((8, w), f32), shape(gu.shape[1:], bf16), shape(down.shape[1:], bf16)],
        [VM, ANY, VM, VM, VM],
        [pltpu.VMEM((n, w), bf16), pltpu.SemaphoreType.DMA] + scatter_scratch(n, w) + line_scratch(*gu.shape[1:]) + line_scratch(*down.shape[1:])
        + dma_sems(SCATTER_COPIES + GATHER_COPIES + 2 * LINE_COPIES),
    )


def end_call(da_parts, out_parts, qkv, wo, small, x, resid, dresid, gain, ident):
    n, w = da_parts.shape[2:]
    rows_q = qkv.shape[1] // 4
    rows_o = wo.shape[1]

    def body(da_ref, op_ref, q_ref, wo_ref, small_ref, x_ref, resid_ref, dresid_ref, g_ref,
             out_ref, gx_ref, gq_ref, go_ref, total_ref,
             rc, rd, rx, ry, td, tx, ty, rc2, rd2, rx2, ry2, td2, tx2, ty2,
             q_got, q_made, o_got, o_made, zq, cq, fq, po, ro, s_got, s_sum, s_line, send, recv):
        net = Net()
        sems = (send, recv)
        net.greet("xyc")
        z, x, y, c = net.z, net.x, net.y, net.c
        base = 2 * SCATTER_COPIES
        line_q = ScatterLine(net, q_ref, q_got, q_made, sems, base)
        line_o = ScatterLine(net, po, o_got, o_made, sems, base + 6)
        line_s = GatherLine(net, s_sum.at[2], s_line, sems, base + 12)
        base += 18
        line_q.step(0)
        to_c = net.send(wo_ref.at[1 - c], po.at[2 * x + c], sems, base, "c")
        hop = net.send(small_ref, s_got.at[0], sems, base + 1, "c")
        hops = [hop]
        po[2 * (1 - x)] = jnp.zeros((rows_o, w), bf16)
        po[2 * (1 - x) + 1] = jnp.zeros((rows_o, w), bf16)
        po[2 * x + c] = wo_ref[c]

        def small_step(i):
            hops[i].wait_recv()
            s_sum[i] = (small_ref[...] if i == 0 else s_sum[i - 1]) + s_got[i]
            if i < 2:
                hops.append(net.send(s_sum.at[i], s_got.at[i + 1], sems, base + 2 + i, "yx"[i]))
            else:
                line_s.step(0)

        def begin():
            small_step(0)
            to_c.wait_recv()
            line_o.step(0)

        poll, _ = polls(begin)
        done = scatter_rows(net, da_ref, rc, rd, rx, ry, td, tx, ty, sems, 0, poll)
        line_q.step(1)
        small_step(1)
        line_o.step(1)

        def later():
            line_q.step(2)
            small_step(2)

        poll, _ = polls(later)
        done2 = scatter_rows(net, op_ref, rc2, rd2, rx2, ry2, td2, tx2, ty2, sems, SCATTER_COPIES, poll)
        line_o.step(2)
        line_s.step(1)
        for half in range(2):
            done(half)

            def rows_of(rows):
                da = wide(da_ref[0, 0, rows]) + wide(rc[0, rows]) + wide(rx[rows]) + wide(ry[rows])
                xf = wide(x_ref[rows])
                r = lax.rsqrt(jnp.mean(xf * xf, axis=1, keepdims=True) + 1e-06)
                dn = da * g_ref[...]
                gx_ref[rows] = dresid_ref[rows] + r * (dn - xf * r * r * jnp.mean(dn * xf, axis=1, keepdims=True))

            tiles(half * (n // 2), n // 2, rows_of)

        def put_q(rows, total):
            zq[rows] = total.astype(bf16)

        def put_o(rows, total):
            ro[0, rows] = total.astype(bf16)

        line_q.finish(put_q)
        block = lambda i, j: pl.ds(pl.multiple_of((2 * i + j) * rows_q, rows_q), rows_q)
        swaps = [net.send(zq.at[block(i, 1 - c)], cq.at[i, c], sems, base + 4 + i, "c") for i in range(2)]
        for i in range(2):
            cq[i, c] = zq[block(i, c)]
        for copy in swaps:
            copy.wait_recv()
        swaps.append(net.send(cq.at[1 - y], fq.at[x, y], sems, base + 6, "y"))
        fq[x, y] = cq[y]
        line_s.step(2)
        line_o.finish(put_o)
        swaps.append(net.send(ro.at[0], ro.at[1], sems, base + 7, "x"))
        swaps[2].wait_recv()
        swaps.append(net.send(fq.at[x], fq.at[x], sems, base + 8, "x"))
        line_s.step(3)
        s_line[z] = s_sum[2]
        total_ref[...] = (s_line[0] + s_line[1]) + (s_line[2] + s_line[3])
        for half in range(2):
            done2(half)

            def sum_of(rows):
                total = wide(op_ref[0, 0, rows]) + wide(rc2[0, rows]) + wide(rx2[rows]) + wide(ry2[rows])
                out_ref[rows] = (resid_ref[rows] + total).astype(bf16)

            tiles(half * (n // 2), n // 2, sum_of)
        swaps[3].wait_recv()
        go_ref[...] = wide(ro[0]) + wide(ro[1])
        swaps[4].wait_recv()
        for i in range(2):
            for k in range(4):
                pair = 4 * i + 2 * (k % 2) + k // 2
                for m in range(6):
                    col = (m // 2) * MODEL_WIDTH + (2 * pair + m % 2) * E
                    gq_ref[:, col : col + E] = wide(fq[i, k // 2, k % 2, :, m * EP : m * EP + E])
        line_s.finish()
        for copy in swaps + hops + [to_c]:
            copy.wait_send()

    stages = [pltpu.VMEM((2, rows_o, w), bf16), pltpu.VMEM((3,) + small.shape, f32), pltpu.VMEM((3,) + small.shape, f32),
              pltpu.VMEM((4,) + small.shape, f32)]
    return comm_call(
        body, "end", ident, (da_parts, out_parts, qkv, wo, small, x, resid, dresid, gain), [VM] * 9,
        [shape((n, w), bf16), shape((n, w), f32), shape((rows_q, 3 * MODEL_WIDTH), f32), shape((rows_o, w), f32), shape(small.shape, f32)],
        [VM] * 5,
        scatter_scratch(n, w) * 2 + line_scratch(*qkv.shape[1:]) + line_scratch(rows_o, w)
        + [pltpu.VMEM(qkv.shape[1:], bf16), pltpu.VMEM((2, 2, rows_q, 6 * EP), bf16), pltpu.VMEM((2, 2, 2, rows_q, 6 * EP), bf16),
           pltpu.VMEM((4, rows_o, w), bf16)]
        + stages + dma_sems(2 * SCATTER_COPIES + 18 + 9),
    )


def place_gu(pieces):
    rows = pieces.shape[3]

    def body(p_ref, gate_ref, up_ref):
        for i in range(2):
            for k in range(4):
                for m in range(8):
                    col = 256 * (4 * (m % 4) + k) + 128 * i
                    dst = gate_ref if m < 4 else up_ref
                    dst[:, col : col + 128] = wide(p_ref[i, k // 2, k % 2, :, m * 128 : (m + 1) * 128])

    return pl.pallas_call(
        body, in_specs=[VM], out_specs=[VM] * 2, out_shape=[shape((rows, FF), f32)] * 2, name="place_gu",
        compiler_params=pltpu.CompilerParams(vmem_limit_bytes=16 << 20),
    )(pieces)


def rms_scale(values):
    return lax.rsqrt(jnp.mean(values * values, axis=1, keepdims=True) + 1e-06)


class Links:
    def __init__(self, fsdp):
        self.fsdp = fsdp
        index = lax.axis_index("fsdp")
        self.x = lax.axis_index("rep")
        self.z, self.y, self.c = index // 4, (index // 2) % 2, index % 2

    def across(self, flip, v):
        if flip == "x":
            return lax.ppermute(v, "rep", [(0, 1), (1, 0)])
        bit = {"y": 2, "c": 1}[flip]
        return lax.ppermute(v, "fsdp", [(f, f ^ bit) for f in range(self.fsdp)])

    def along(self, v, step):
        pairs = [(f, f + 4 * step) for f in range(self.fsdp) if 0 <= f + 4 * step < self.fsdp]
        return lax.ppermute(v, "fsdp", pairs)

    def ordered(self, bit, mine, other, axis):
        first, second = jnp.where(bit == 0, mine, other), jnp.where(bit == 0, other, mine)
        return jnp.stack([first, second], axis)

    def gather_z(self, v):
        left, right = [], []
        a = b = v
        for _ in range(3):
            a, b = self.along(a, 1), self.along(b, -1)
            left.append(a)
            right.append(b)
        line = jnp.stack(left[::-1] + [v] + right)
        return lax.dynamic_slice_in_dim(line, 3 - self.z, 4, 0)

    def scatter_z(self, parts):
        zero = jnp.zeros((3,) + parts.shape[1:], parts.dtype)
        line = lax.dynamic_slice_in_dim(jnp.concatenate([zero, parts, zero]), self.z, 7, 0)
        low = lambda v: v.astype(bf16)
        a = self.along(low(line[6]), 1)
        b = self.along(low(line[0]), -1)
        for step in (1, 2):
            a = self.along(low(line[6 - step] + a.astype(f32)), 1)
            b = self.along(low(line[step] + b.astype(f32)), -1)
        return line[3] + a.astype(f32) + b.astype(f32)

    def gather_plane(self, v):
        n = v.shape[0] // 2
        vx, vy = self.across("x", v), self.across("y", v)
        vd = jnp.concatenate([self.across("y", vx[:n]), self.across("x", vy[n:])])
        return [jnp.concatenate([u, self.across("c", u)]) for u in (v, vx, vy, vd)]

    def scatter_plane(self, parts):
        low = lambda v: v.astype(bf16)
        n = parts[0].shape[0] // 2
        s = [p[:n] + self.across("c", low(p[n:])).astype(f32) for p in parts]
        m = n // 2
        dx, dy = self.across("x", low(s[3][:m])), self.across("y", low(s[3][m:]))
        to_x = jnp.concatenate([s[1][:m], s[1][m:] + dy.astype(f32)])
        to_y = jnp.concatenate([s[2][:m] + dx.astype(f32), s[2][m:]])
        return s[0] + self.across("x", low(to_x)).astype(f32) + self.across("y", low(to_y)).astype(f32)


class Weights:
    def __init__(self, links):
        self.links = links
        self.line = links.fsdp == 16
        x, y, c = links.x, links.y, links.c
        self.pair = 4 * x + 2 * c + y
        self.slot = 4 * x + 2 * y + c

    def spread(self, shard, dims):
        l = self.links
        ax, ay, ac = dims
        v = lax.dynamic_index_in_dim(shard, l.x, ax, keepdims=True)
        keep = lax.dynamic_index_in_dim(v, l.y, ay, keepdims=True)
        sent = l.across("y", lax.dynamic_index_in_dim(v, 1 - l.y, ay, keepdims=True))
        v = l.ordered(l.y, keep, sent, 0)
        keep = lax.dynamic_index_in_dim(v, l.c, ac + 1, keepdims=True)
        sent = l.across("c", lax.dynamic_index_in_dim(v, 1 - l.c, ac + 1, keepdims=True))
        v = l.ordered(l.c, keep, sent, 1)
        return l.gather_z(v)

    def collect(self, grad, dims):
        l = self.links
        ax, ay, ac = dims
        low = lambda v: v.astype(bf16)
        v = l.scatter_z(grad)
        keep = lax.dynamic_index_in_dim(v, l.c, 1, keepdims=False)
        sent = l.across("c", low(lax.dynamic_index_in_dim(v, 1 - l.c, 1, keepdims=False)))
        v = self.join(l.c, keep, sent.astype(f32), ac + 1)
        keep = lax.dynamic_index_in_dim(v, l.y, 0, keepdims=False)
        sent = l.across("y", low(lax.dynamic_index_in_dim(v, 1 - l.y, 0, keepdims=False)))
        v = low(self.join(l.y, keep, sent.astype(f32), ay))
        return self.join(l.x, v, l.across("x", v), ax).astype(f32)

    def join(self, bit, mine, other, axis):
        first, second = jnp.where(bit == 0, mine, other), jnp.where(bit == 0, other, mine)
        return jnp.concatenate([first, second], axis)

    def whole(self, shard):
        return lax.all_gather(shard, "fsdp", axis=0, tiled=True)

    def owned(self, grad):
        part = lax.psum_scatter(grad, "fsdp", scatter_dimension=0, tiled=True)
        return lax.psum(part.astype(bf16), "rep").astype(f32)

    def qkv(self, shard):
        rows = shard.shape[0]
        if self.line:
            v = self.spread(shard.reshape(rows, 3, 2, 2, 2, 2 * E), (2, 4, 3))
            v = v.reshape(MODEL_WIDTH, 3, 2, E)
        else:
            v = self.whole(shard).reshape(MODEL_WIDTH, 3, 8, 2, E)
            v = lax.dynamic_index_in_dim(v, self.pair, 2, keepdims=False)
        return jnp.pad(v, ((0, 0), (0, 0), (0, 0), (0, EP - E))).reshape(MODEL_WIDTH, 6 * EP)

    def qkv_back(self, grad):
        g = grad.reshape(MODEL_WIDTH, 3, 2, EP)[..., :E]
        if self.line:
            return self.collect(g.reshape(4, 2, 2, -1, 3, 1, 1, 1, 2 * E), (2, 4, 3)).reshape(-1, 3 * MODEL_WIDTH)
        zero = jnp.zeros((MODEL_WIDTH, 3, 8, 2, E), f32)
        return self.owned(lax.dynamic_update_index_in_dim(zero, g, self.pair, 2).reshape(MODEL_WIDTH, 3 * MODEL_WIDTH))

    def out(self, shard):
        l = self.links
        if self.line:
            v = l.gather_z(shard)
            keep = lax.dynamic_index_in_dim(v, 2 * l.x + l.c, 0, keepdims=False)
            sent = l.across("c", lax.dynamic_index_in_dim(v, 2 * l.x + 1 - l.c, 0, keepdims=False))
            v = l.ordered(l.c, keep, sent, 0)
        else:
            v = self.whole(shard).reshape(8, 2, E, MODEL_WIDTH)
            v = lax.dynamic_index_in_dim(v, self.pair, 0, keepdims=False)
        return jnp.pad(v, ((0, 0), (0, EP - E), (0, 0))).reshape(2 * EP, MODEL_WIDTH)

    def out_back(self, grad):
        l = self.links
        g = grad.reshape(2, EP, MODEL_WIDTH)[:, :E]
        if self.line:
            keep = lax.dynamic_index_in_dim(g, l.c, 0, keepdims=False)
            sent = l.across("c", lax.dynamic_index_in_dim(g, 1 - l.c, 0, keepdims=False).astype(bf16)).astype(f32)
            at = jnp.arange(4)[:, None, None]
            parts = jnp.where(at == 2 * l.x + l.c, keep[None], jnp.where(at == 2 * l.x + 1 - l.c, sent[None], 0.0))
            v = l.scatter_z(parts).astype(bf16)
            return (v + l.across("x", v)).astype(f32)
        zero = jnp.zeros((8, 2, E, MODEL_WIDTH), f32)
        return self.owned(lax.dynamic_update_index_in_dim(zero, g, self.pair, 0).reshape(MODEL_WIDTH, MODEL_WIDTH))

    def ffn_in(self, gate, up_):
        rows = gate.shape[0]
        both = jnp.stack([gate, up_], 1)
        if self.line:
            v = self.spread(both.reshape(rows, 2, 4, 2, 2, 2, FF // 32), (5, 3, 4))
            return v.reshape(MODEL_WIDTH, FF // 4)
        v = self.whole(both).reshape(MODEL_WIDTH, 2, 8, FF // 8)
        return lax.dynamic_index_in_dim(v, self.slot, 2, keepdims=False).reshape(MODEL_WIDTH, FF // 4)

    def ffn_in_back(self, grad):
        if self.line:
            v = self.collect(grad.reshape(4, 2, 2, -1, 2, 4, 1, 1, 1, FF // 32), (5, 3, 4)).reshape(-1, 2, FF)
        else:
            zero = jnp.zeros((MODEL_WIDTH, 2, 8, FF // 8), f32)
            g = grad.reshape(MODEL_WIDTH, 2, FF // 8)
            v = self.owned(lax.dynamic_update_index_in_dim(zero, g, self.slot, 2).reshape(MODEL_WIDTH, 2, FF))
        return v[:, 0], v[:, 1]

    def ffn_out(self, shard):
        l = self.links
        if self.line:
            v = lax.dynamic_index_in_dim(shard.reshape(2, FF // 32, MODEL_WIDTH), l.x, 0, keepdims=False)
            return l.gather_z(v).reshape(FF // 8, MODEL_WIDTH)
        v = self.whole(shard).reshape(8, FF // 8, MODEL_WIDTH)
        return lax.dynamic_index_in_dim(v, self.slot, 0, keepdims=False)

    def ffn_out_back(self, grad):
        l = self.links
        if self.line:
            v = l.scatter_z(grad.reshape(4, FF // 32, MODEL_WIDTH)).astype(bf16)
            return self.join(l.x, v, l.across("x", v), 0).astype(f32)
        zero = jnp.zeros((8, FF // 8, MODEL_WIDTH), f32)
        return self.owned(lax.dynamic_update_index_in_dim(zero, grad, self.slot, 0).reshape(FF, MODEL_WIDTH))

    def gains(self, *shards):
        l = self.links
        v = jnp.stack(shards)
        if self.line:
            v = l.ordered(l.c, v, l.across("c", v), 0)
            v = l.ordered(l.y, v, l.across("y", v), 0)
            v = l.gather_z(v)
            v = v.reshape(16, len(shards), -1).transpose(1, 0, 2).reshape(len(shards), MODEL_WIDTH)
        else:
            v = lax.all_gather(v, "fsdp", axis=1, tiled=True)
        return [v[i].astype(f32) for i in range(len(shards))]


def per_device(
    fsdp,
    x_in,
    doc_ids,
    w_qkv,
    w_out,
    gain_attn,
    gain_group,
    conv_kernel,
    head_mix,
    gain_ffn,
    w_gate,
    w_up,
    w_down,
    cotangent,
):
    links = Links(fsdp)
    weights = Weights(links)
    tokens = x_in.shape[1]

    x_all = jnp.concatenate(links.gather_plane(x_in[0]))
    qkv_w = weights.qkv(w_qkv)
    gain_a, gain_g, gain_f = weights.gains(gain_attn, gain_group, gain_ffn)
    docs = doc_ids
    for flip in ("y", "x"):
        docs = jnp.concatenate([docs, links.across(flip, docs)])
    docs = jnp.stack([docs, links.across("c", docs)], 1)
    docs = docs[jnp.array([0, 2, 1, 3])].reshape(8, tokens)
    out_w = weights.out(w_out)
    in_w = weights.ffn_in(w_gate, w_up)
    down_w = weights.ffn_out(w_down)
    upstream_chips = links.gather_plane(cotangent[0])

    kernel = lax.dynamic_slice_in_dim(conv_kernel, 2 * weights.pair, 2, 0)
    mix = lax.dynamic_slice_in_dim(head_mix, 2 * weights.pair, 2, 0)
    th, tl, tt = bands(kernel, tokens)
    group = lax.dynamic_slice_in_dim(gain_g.reshape(8, 2, E), weights.pair, 1, 0)
    group = jnp.pad(group, ((0, 0), (0, 0), (0, EP - E))).reshape(1, 2 * EP)
    doc_col, doc_row = docs[:, :, None], docs[:, None, :]

    xf_all = x_all.astype(f32)
    a1 = (xf_all * rms_scale(xf_all) * gain_a).astype(bf16)
    qkv = dot(a1, qkv_w).astype(bf16).reshape(8, tokens, 6 * EP)
    normed, xhat, s, probs, zeroed = attend(mix, qkv, doc_col, doc_row, th, tl, group)
    normed = normed.reshape(4, 2 * tokens, 2 * EP)
    xf = x_in[0].astype(f32)
    resid = xf + links.scatter_plane([dot(normed[i], out_w) for i in range(4)])

    r2 = rms_scale(resid)
    a2_chips = links.gather_plane((resid * r2 * gain_f).astype(bf16))
    out_parts, back_parts, hiddens, dgus = [], [], [], []
    half = FF // 8
    for a2, dffn in zip(a2_chips, upstream_chips):
        gu = dot(a2, in_w)
        gate, up_act = gu[:, :half], gu[:, half:]
        sig = jax.nn.sigmoid(gate)
        silu = gate * sig
        hidden = (silu * up_act).astype(bf16)
        dhidden = dot(dffn, down_w, 1, 1)
        dgate = (dhidden * up_act * sig * (1.0 + gate * (1.0 - sig))).astype(bf16)
        dup = (dhidden * silu).astype(bf16)
        dgu = jnp.concatenate([dgate, dup], 1)
        hiddens.append(hidden)
        dgus.append(dgu)
        back_parts.append(dot(dgu, in_w, 1, 1))
        out_parts.append(dot(hidden, down_w))
    da2 = links.scatter_plane(back_parts)
    output = (resid + links.scatter_plane(out_parts)).astype(bf16)

    dy = cotangent[0].astype(f32)
    sum_gain_ffn = jnp.sum(da2 * resid * r2, axis=0)
    dn2 = da2 * gain_f
    dresid = dy + r2 * (dn2 - resid * r2 * r2 * jnp.mean(dn2 * resid, axis=1, keepdims=True))
    dattn = jnp.concatenate(links.gather_plane(dresid.astype(bf16)))

    a2_all, dgu_all = jnp.concatenate(a2_chips), jnp.concatenate(dgus)
    hidden_all, dffn_all = jnp.concatenate(hiddens), jnp.concatenate(upstream_chips)
    grad_gate, grad_up = weights.ffn_in_back(dot(a2_all, dgu_all, 0, 0))
    grad_down = weights.ffn_out_back(dot(hidden_all, dffn_all, 0, 0))

    dnormed = dot(dattn, out_w, 1, 1).reshape(8, tokens, 2 * EP)
    dqkv, conv_tiles, mix_sums, group_sums = attend_back(
        mix, qkv, doc_col, doc_row, tt, group, dnormed, xhat, s, probs, zeroed
    )
    dqkv = dqkv.reshape(4, 2 * tokens, 6 * EP)
    da1 = links.scatter_plane([dot(dqkv[i], qkv_w, 1, 1) for i in range(4)])
    grad_out = weights.out_back(dot(normed.reshape(8 * tokens, 2 * EP), dattn, 0, 0))
    grad_qkv = weights.qkv_back(dot(a1, dqkv.reshape(8 * tokens, 6 * EP), 0, 0))

    r1 = rms_scale(xf)
    sum_gain_attn = jnp.sum(da1 * xf * r1, axis=0)
    dn1 = da1 * gain_a
    grad_x = dresid + r1 * (dn1 - xf * r1 * r1 * jnp.mean(dn1 * xf, axis=1, keepdims=True))

    place = lambda v: lax.dynamic_update_index_in_dim(jnp.zeros((8,) + v.shape, f32), v, weights.pair, 0)
    small = [
        sum_gain_attn,
        sum_gain_ffn,
        place(group_sums[0].reshape(2, EP)[:, :E].reshape(-1)),
        place(diagonals(conv_tiles)),
        place(jnp.sum(mix_sums[:4], axis=1)),
    ]
    sizes = [v.size for v in small]
    total = lax.psum(jnp.concatenate([v.reshape(-1) for v in small]), ("rep", "fsdp"))
    cut = [0]
    for size in sizes:
        cut.append(cut[-1] + size)
    gain_a_sum, gain_f_sum, group_sum, conv_sum, mix_sum = (total[cut[i] : cut[i + 1]] for i in range(5))
    rows = gain_attn.shape[0]
    own = lambda v: lax.dynamic_slice_in_dim(v, lax.axis_index("fsdp") * rows, rows, 0)
    return (
        output[None],
        grad_x[None],
        grad_qkv,
        grad_out,
        own(gain_a_sum),
        own(group_sum),
        conv_sum.reshape(H, QWIN, KWIN),
        mix_sum.reshape(H, 2),
        own(gain_f_sum),
        grad_gate,
        grad_up,
        grad_down,
    )


def join(bit, mine, other, axis):
    first, second = jnp.where(bit == 0, mine, other), jnp.where(bit == 0, other, mine)
    return jnp.stack([first, second], axis)


def fast(
    x_in,
    doc_ids,
    w_qkv,
    w_out,
    gain_attn,
    gain_group,
    conv_kernel,
    head_mix,
    gain_ffn,
    w_gate,
    w_up,
    w_down,
    cotangent,
):
    links = Links(16)
    pair = 4 * links.x + 2 * links.c + links.y
    tokens = x_in.shape[1]
    x, dy = x_in[0], cotangent[0]
    rows = w_qkv.shape[0]

    gains = jnp.pad(jnp.stack([gain_attn, gain_group, gain_ffn]), ((0, 13), (0, 128 - rows)))
    docs = jnp.broadcast_to(doc_ids, (8, tokens))
    x_all, dffn_all, docs, gains, qkv_w, gu_plane, out_w = start_call(x, dy, docs, gains, w_qkv, w_gate, w_up, w_out, 1)
    docs = docs.reshape(8, 8, tokens)[:, 0]
    gains = gains.reshape(16, 16, 128)[:, :3, :rows].astype(f32).transpose(1, 0, 2).reshape(3, MODEL_WIDTH)
    gain_a, gain_g, gain_f = gains[0:1], gains[1], gains[2:3]
    qkv_w = qkv_w.reshape(MODEL_WIDTH, 6 * EP)
    keep = lax.dynamic_index_in_dim(out_w, 2 * links.x + links.c, 0, keepdims=False)
    other = links.across("c", lax.dynamic_index_in_dim(out_w, 2 * links.x + 1 - links.c, 0, keepdims=False))
    out_w = jnp.pad(join(links.c, keep, other, 0), ((0, 0), (0, EP - E), (0, 0))).reshape(2 * EP, MODEL_WIDTH)

    kernel = lax.dynamic_slice_in_dim(conv_kernel, 2 * pair, 2, 0)
    mix = lax.dynamic_slice_in_dim(head_mix, 2 * pair, 2, 0)
    th, tl, tt = bands(kernel, tokens)
    group = lax.dynamic_slice_in_dim(gain_g.reshape(8, 2, E), pair, 1, 0)
    group = jnp.pad(group, ((0, 0), (0, 0), (0, EP - E))).reshape(1, 2 * EP)
    doc_col, doc_row = docs[:, :, None], docs[:, None, :]

    x_all = x_all.reshape(8 * tokens, MODEL_WIDTH)
    dffn_all = dffn_all.reshape(8 * tokens, MODEL_WIDTH)
    xf_all = x_all.astype(f32)
    a1 = (xf_all * rms_scale(xf_all) * gain_a).astype(bf16)
    qkv = dot(a1, qkv_w).astype(bf16).reshape(8, tokens, 6 * EP)
    normed, xhat, s, probs, zeroed = attend(mix, qkv, doc_col, doc_row, th, tl, group)
    normed = normed.reshape(8 * tokens, 2 * EP)
    by_chip = lambda v: v.astype(bf16).reshape(4, 2, tokens, MODEL_WIDTH)
    resid, a2, gu_w, down_w = mid_call(by_chip(dot(normed, out_w)), x, gain_f, gu_plane, w_down, 2)

    a2 = a2.reshape(8 * tokens, MODEL_WIDTH)
    gu_w = gu_w.reshape(MODEL_WIDTH, FF // 4)
    down_w = down_w.reshape(FF // 8, MODEL_WIDTH)
    half = FF // 8
    gu = dot(a2, gu_w)
    gate, up_act = gu[:, :half], gu[:, half:]
    sig = jax.nn.sigmoid(gate)
    silu = gate * sig
    hidden = (silu * up_act).astype(bf16)
    dhidden = dot(dffn_all, down_w, 1, 1)
    dgate = (dhidden * up_act * sig * (1.0 + gate * (1.0 - sig))).astype(bf16)
    dup = (dhidden * silu).astype(bf16)
    dgu = jnp.concatenate([dgate, dup], 1)
    grad_gu = dot(a2, dgu, 0, 0).astype(bf16).reshape(4, 4 * rows, FF // 4)
    grad_down = dot(hidden, dffn_all, 0, 0).astype(bf16).reshape(4, FF // 32, MODEL_WIDTH)
    out_parts = by_chip(dot(hidden, down_w))
    dresid, dattn, sum_f, grad_gu, grad_down = mid_back_call(
        by_chip(dot(dgu, gu_w, 1, 1)), dy, resid, gain_f, grad_gu, grad_down, 3
    )
    v = grad_gu.reshape(2, 2, rows, FF // 4)
    sent = links.across("c", lax.dynamic_index_in_dim(v, 1 - links.c, 1, keepdims=False))
    v = join(links.c, lax.dynamic_index_in_dim(v, links.c, 1, keepdims=False), sent, 1)
    sent = links.across("y", lax.dynamic_index_in_dim(v, 1 - links.y, 0, keepdims=False))
    v = join(links.y, lax.dynamic_index_in_dim(v, links.y, 0, keepdims=False), sent, 0)
    grad_gate, grad_up = place_gu(join(links.x, v, links.across("x", v), 0))
    grad_down = join(links.x, grad_down, links.across("x", grad_down), 0).reshape(-1, MODEL_WIDTH).astype(f32)

    dattn = dattn.reshape(8 * tokens, MODEL_WIDTH)
    dnormed = dot(dattn, out_w, 1, 1).reshape(8, tokens, 2 * EP)
    dqkv, conv_tiles, mix_sums, group_sums = attend_back(
        mix, qkv, doc_col, doc_row, tt, group, dnormed, xhat, s, probs, zeroed
    )
    dqkv = dqkv.reshape(8 * tokens, 6 * EP)
    grad_qkv = dot(a1, dqkv, 0, 0)
    sum_a = jnp.sum(grad_qkv * qkv_w.astype(f32), axis=1) / gain_a[0]
    grad_out = dot(normed, dattn, 0, 0).astype(bf16).reshape(2, EP, MODEL_WIDTH)[:, :rows]
    place = lambda v: lax.dynamic_update_index_in_dim(jnp.zeros((8,) + v.shape, f32), v, pair, 0)
    small = [
        sum_a,
        sum_f[0],
        place(group_sums[0].reshape(2, EP)[:, :E].reshape(-1)),
        place(diagonals(conv_tiles)),
        place(jnp.sum(mix_sums[:4], axis=1)),
    ]
    cut = [0]
    for v in small:
        cut.append(cut[-1] + v.size)
    room = 48 * 128
    flat = jnp.concatenate([v.reshape(-1) for v in small] + [jnp.zeros((room - cut[-1],), f32)]).reshape(48, 128)
    out, grad_x, grad_qkv, grad_out, total = end_call(
        by_chip(dot(dqkv, qkv_w, 1, 1)),
        out_parts,
        grad_qkv.astype(bf16).reshape(4, 4 * rows, 6 * EP),
        grad_out,
        flat,
        x,
        resid,
        dresid,
        gain_a,
        4,
    )
    total = total.reshape(-1)
    gain_a_sum, gain_f_sum, group_sum, conv_sum, mix_sum = (total[cut[i] : cut[i + 1]] for i in range(5))
    own = lambda v: lax.dynamic_slice_in_dim(v, lax.axis_index("fsdp") * rows, rows, 0)
    return (
        out[None],
        grad_x[None],
        grad_qkv,
        grad_out,
        own(gain_a_sum),
        own(group_sum),
        conv_sum.reshape(H, QWIN, KWIN),
        mix_sum.reshape(H, 2),
        own(gain_f_sum),
        grad_gate,
        grad_up,
        grad_down,
    )


def solution(mesh):
    fsdp = mesh.shape["fsdp"]
    assert mesh.shape["rep"] == 2 and fsdp % 4 == 0
    rows, shard, part = P(("rep", "fsdp"), None, None), P("fsdp", None), P("fsdp")
    placed = (rows, P(("rep", "fsdp"), None), shard, shard, part, part, P(), P(), part, shard, shard, shard, rows)
    return jax.shard_map(
        fast if fsdp == 16 else (lambda *args: per_device(fsdp, *args)),
        mesh=mesh,
        in_specs=placed,
        out_specs=(rows, rows, shard, shard, part, part, P(), P(), part, shard, shard, shard),
        check_vma=False,
    )
```

```python
import math

import jax
import jax.numpy as jnp
from jax import lax
from jax.experimental import pallas as pl
from jax.experimental.pallas import tpu as pltpu
from jax.sharding import PartitionSpec as P

MODEL_WIDTH = 1536
H = 16
E = 96
EP = 128
QWIN = 6
KWIN = 11
bf16, f32 = jnp.bfloat16, jnp.float32


def allowed_mask(doc_col, doc_row):
    n = doc_row.shape[-1]
    i = lax.broadcasted_iota(jnp.int32, (n, n), 0)
    j = lax.broadcasted_iota(jnp.int32, (n, n), 1)
    return (j <= i) & (doc_col == doc_row)


def down(v, a):
    if a == 0:
        return v
    i = lax.broadcasted_iota(jnp.int32, v.shape, 0)
    return jnp.where(i >= a, pltpu.roll(v, a, 0), 0.0)


def up(v, a):
    if a == 0:
        return v
    n = v.shape[0]
    i = lax.broadcasted_iota(jnp.int32, v.shape, 0)
    return jnp.where(i < n - a, pltpu.roll(v, n - a, 0), 0.0)


def dot(a, b, ca=1, cb=0):
    return lax.dot_general(a, b, (((ca,), (cb,)), ((), ())), preferred_element_type=f32)


def split(v):
    hi = v.astype(bf16)
    return hi, (v - hi.astype(f32)).astype(bf16)


def fwd_kernel(mix_ref, qkv_ref, dcol_ref, drow_ref, th_ref, tl_ref, gain_ref,
               normed_ref, xhat_ref, s_ref, p_ref, z_ref):
    allowed = allowed_mask(dcol_ref[0], drow_ref[0])
    scale = 1.0 / math.sqrt(E)
    probs = []
    for h in range(2):
        q = qkv_ref[0, :, h * EP:(h + 1) * EP]
        k = qkv_ref[0, :, (2 + h) * EP:(3 + h) * EP]
        zeroed = jnp.where(allowed, dot(q, k, 1, 1) * scale, 0.0)
        z_ref[0, h] = zeroed.astype(bf16)
        his, los = [], []
        for a in range(QWIN):
            hi, lo = split(down(zeroed, a))
            his.append(hi)
            los.append(lo)
        his, los = jnp.concatenate(his, 1), jnp.concatenate(los, 1)
        th, tl = th_ref[h], tl_ref[h]
        conv = dot(his, th) + (dot(his, tl) + dot(los, th))
        masked = jnp.where(allowed, conv, -jnp.inf)
        e = jnp.exp(masked - jnp.max(masked, axis=1, keepdims=True))
        p = e / jnp.sum(e, axis=1, keepdims=True)
        p_ref[0, h] = p
        probs.append(p)
    lane = lax.broadcasted_iota(jnp.int32, (1, EP), 1)
    for h in range(2):
        v = qkv_ref[0, :, (4 + h) * EP:(5 + h) * EP]
        mixed = (mix_ref[h, 0] * probs[0] + mix_ref[h, 1] * probs[1]).astype(bf16)
        ho = dot(mixed, v)
        centered = jnp.where(lane < E, ho - jnp.sum(ho, axis=1, keepdims=True) / E, 0.0)
        s = lax.rsqrt(jnp.sum(centered * centered, axis=1, keepdims=True) / E + 1e-05)
        xhat = centered * s
        cols = slice(h * EP, (h + 1) * EP)
        xhat_ref[0, :, cols] = xhat
        s_ref[0, :, cols] = jnp.broadcast_to(s, xhat.shape)
        normed_ref[0, :, cols] = (xhat * gain_ref[0:1, cols]).astype(bf16)


def attend(mix, qkv, dcol, drow, th, tl, gain):
    n, t, _ = qkv.shape
    row = lambda *s: pl.BlockSpec((1,) + s, lambda i: (i,) + (0,) * len(s))
    full = lambda a: pl.BlockSpec(a.shape, lambda i: (0,) * a.ndim)
    return pl.pallas_call(
        fwd_kernel,
        grid=(n,),
        in_specs=[pl.BlockSpec(memory_space=pltpu.SMEM), row(t, 6 * EP), row(t, 1), row(1, t), full(th), full(tl), full(gain)],
        out_specs=[row(t, 2 * EP), row(t, 2 * EP), row(t, 2 * EP), row(2, t, t), row(2, t, t)],
        out_shape=[
            jax.ShapeDtypeStruct((n, t, 2 * EP), bf16),
            jax.ShapeDtypeStruct((n, t, 2 * EP), f32),
            jax.ShapeDtypeStruct((n, t, 2 * EP), f32),
            jax.ShapeDtypeStruct((n, 2, t, t), f32),
            jax.ShapeDtypeStruct((n, 2, t, t), bf16),
        ],
        cost_estimate=pl.CostEstimate(flops=n * 2 * 3 * 2 * t * t * QWIN * t, bytes_accessed=n * t * t * 20, transcendentals=n * 2 * t * t),
        name="attend",
    )(mix, qkv, dcol, drow, th, tl, gain)


def bwd_kernel(mix_ref, qkv_ref, dcol_ref, drow_ref, tt_ref, gain_ref, dn_ref, xhat_ref, s_ref, p_ref, z_ref,
               dqkv_ref, gconv_ref, gmix_ref, gg_ref, m_ref):
    step, steps = pl.program_id(0), pl.num_programs(0)
    t = p_ref.shape[-1]

    @pl.when(step == 0)
    def _():
        m_ref[...] = jnp.zeros_like(m_ref)
        gmix_ref[...] = jnp.zeros_like(gmix_ref)
        gg_ref[...] = jnp.zeros_like(gg_ref)

    allowed = allowed_mask(dcol_ref[0], drow_ref[0])
    scale = 1.0 / math.sqrt(E)
    lane = lax.broadcasted_iota(jnp.int32, (1, EP), 1)
    p = [p_ref[0, 0], p_ref[0, 1]]
    dmixed = []
    for h in range(2):
        cols = slice(h * EP, (h + 1) * EP)
        dn, xhat = dn_ref[0, :, cols], xhat_ref[0, :, cols]
        gg_ref[0:1, cols] += jnp.sum(dn * xhat, axis=0, keepdims=True)
        dc = dn * gain_ref[0:1, cols]
        m1 = jnp.sum(dc, axis=1, keepdims=True) / E
        m2 = jnp.sum(dc * xhat, axis=1, keepdims=True) / E
        dh = jnp.where(lane < E, s_ref[0, :, cols] * (dc - m1 - xhat * m2), 0.0).astype(bf16)
        v = qkv_ref[0, :, (4 + h) * EP:(5 + h) * EP]
        mixed = (mix_ref[h, 0] * p[0] + mix_ref[h, 1] * p[1]).astype(bf16)
        dmixed.append(dot(dh, v, 1, 1))
        dqkv_ref[0, :, (4 + h) * EP:(5 + h) * EP] = dot(mixed, dh, 0, 0).astype(bf16)
    for h in range(2):
        for c in range(2):
            r = 2 * h + c
            gmix_ref[r:r + 1, :] += jnp.sum(dmixed[h] * p[c], axis=0, keepdims=True)
    for c in range(2):
        dp = mix_ref[0, c] * dmixed[0] + mix_ref[1, c] * dmixed[1]
        dconv = p[c] * (dp - jnp.sum(dp * p[c], axis=1, keepdims=True))
        ahead = jnp.concatenate([up(dconv, a).astype(bf16) for a in range(QWIN)], 1)
        m_ref[c] += dot(z_ref[0, c], ahead, 0, 0)
        ds = jnp.where(allowed, dot(ahead, tt_ref[c]), 0.0).astype(bf16)
        q = qkv_ref[0, :, c * EP:(c + 1) * EP]
        k = qkv_ref[0, :, (2 + c) * EP:(3 + c) * EP]
        dqkv_ref[0, :, c * EP:(c + 1) * EP] = (dot(ds, k) * scale).astype(bf16)
        dqkv_ref[0, :, (2 + c) * EP:(3 + c) * EP] = (dot(ds, q, 0, 0) * scale).astype(bf16)

    @pl.when(step == steps - 1)
    def _():
        lanes = lax.broadcasted_iota(jnp.int32, (8, t), 1)
        for h in range(2):
            for a in range(QWIN):
                total = jnp.zeros((8, t), f32)
                for first in range(0, t, 8):
                    rows = m_ref[h, first:first + 8, a * t:(a + 1) * t]
                    turned = pltpu.roll(rows, t - first, 1) if first else rows
                    total = total + jnp.where(lanes < t - first, turned, 0.0)
                gconv_ref[h, a] = total[:, :EP]


def attend_back(mix, qkv, dcol, drow, tt, gain, dn, xhat, s, p, z):
    n, t, _ = qkv.shape
    row = lambda *sh: pl.BlockSpec((1,) + sh, lambda i: (i,) + (0,) * len(sh))
    full = lambda a: pl.BlockSpec(a.shape, lambda i: (0,) * a.ndim)
    keep = lambda *sh: pl.BlockSpec(sh, lambda i: (0,) * len(sh))
    return pl.pallas_call(
        bwd_kernel,
        grid=(n,),
        in_specs=[pl.BlockSpec(memory_space=pltpu.SMEM), row(t, 6 * EP), row(t, 1), row(1, t), full(tt), full(gain),
                  row(t, 2 * EP), row(t, 2 * EP), row(t, 2 * EP), row(2, t, t), row(2, t, t)],
        out_specs=[row(t, 6 * EP), keep(2, QWIN, 8, EP), keep(8, t), keep(8, 2 * EP)],
        out_shape=[
            jax.ShapeDtypeStruct((n, t, 6 * EP), bf16),
            jax.ShapeDtypeStruct((2, QWIN, 8, EP), f32),
            jax.ShapeDtypeStruct((8, t), f32),
            jax.ShapeDtypeStruct((8, 2 * EP), f32),
        ],
        scratch_shapes=[pltpu.VMEM((2, t, QWIN * t), f32)],
        cost_estimate=pl.CostEstimate(flops=n * 2 * 2 * 2 * t * t * QWIN * t, bytes_accessed=n * t * t * 20, transcendentals=0),
        name="attend_back",
    )(mix, qkv, dcol, drow, tt, gain, dn, xhat, s, p, z)


def bands(kernel, t):
    diff = jnp.arange(t)[None, :] - jnp.arange(t)[:, None]
    band = jnp.zeros((2, QWIN, t, t), f32)
    back = jnp.zeros((2, QWIN, t, t), f32)
    for b in range(KWIN):
        tap = kernel[:, :, b][:, :, None, None]
        band = band + jnp.where(diff == b, tap, 0.0)
        back = back + jnp.where(diff == -b, tap, 0.0)
    th, tl = split(band)
    flat = lambda v: v.reshape(2, QWIN * t, t)
    return flat(th), flat(tl), flat(back.astype(bf16))


def diagonals(tiles):
    return sum(tiles[:, :, i, i:i + KWIN] for i in range(8))


FF = 4096
MESH = pl.DeviceIdType.MESH


class Net:
    def __init__(self):
        self.x, self.f = lax.axis_index("rep"), lax.axis_index("fsdp")
        self.z, self.y, self.c = self.f // 4, (self.f // 2) % 2, self.f % 2
        self.k = self.f % 4
        nx, fy, fc = 1 - self.x, 2 - 4 * self.y, 1 - 2 * self.c
        self.to = {
            "x": (nx, self.f),
            "y": (self.x, self.f + fy),
            "c": (self.x, self.f + fc),
            "xy": (nx, self.f + fy),
            "xc": (nx, self.f + fc),
            "yc": (self.x, self.f + fy + fc),
            "xyc": (nx, self.f + fy + fc),
            "up": (self.x, self.f + 4),
            "down": (self.x, self.f - 4),
        }

    def greet(self, names, line=True):
        barrier = pltpu.get_barrier_semaphore()
        for name in names:
            pl.semaphore_signal(barrier, inc=1, device_id=self.to[name], device_id_type=MESH)
        count = len(names)
        if line:

            @pl.when(self.z < 3)
            def _():
                pl.semaphore_signal(barrier, inc=1, device_id=self.to["up"], device_id_type=MESH)

            @pl.when(self.z > 0)
            def _():
                pl.semaphore_signal(barrier, inc=1, device_id=self.to["down"], device_id_type=MESH)

            count = count + (self.z + 3) // 4 + (6 - self.z) // 4
        pl.semaphore_wait(barrier, count)

    def copy(self, src, dst, sems, i, name):
        return pltpu.make_async_remote_copy(
            src_ref=src, dst_ref=dst, send_sem=sems[0].at[i], recv_sem=sems[1].at[i],
            device_id=self.to[name], device_id_type=MESH,
        )

    def send(self, src, dst, sems, i, name):
        copy = self.copy(src, dst, sems, i, name)
        copy.start()
        return copy


def tiles(start, size, body, step=32):
    def one(i, _):
        body(pl.ds(pl.multiple_of(start + i * step, step), step))
        return 0

    lax.fori_loop(0, size // step, one, 0)


def wide(v):
    return v.astype(f32)


class GatherLine:
    def __init__(self, net, src, out, sems, base, keep=None):
        self.net, self.src, self.out, self.sems, self.base = net, src, out, sems, base
        self.keep = keep or (lambda slot: net.z >= 0)

    def go(self, d, way, act):
        net = self.net
        slot = net.z - d if way == "up" else net.z + d
        inside = (net.z >= d) & (net.z < 3) if way == "up" else (net.z < 4 - d) & (net.z > 0)
        i = self.base + d + (0 if way == "up" else 3)

        @pl.when(inside & self.keep(slot))
        def _():
            src = self.src if d == 0 else self.out.at[slot]
            act(net.copy(src, self.out.at[slot], self.sems, i, way))

    def came(self, d, way):
        net = self.net
        slot = net.z - d if way == "up" else net.z + d
        inside = net.z >= d if way == "up" else net.z < 4 - d
        i = self.base + d - 1 + (0 if way == "up" else 3)

        @pl.when(inside & self.keep(slot))
        def _():
            net.copy(self.out.at[slot], self.out.at[slot], self.sems, i, way).wait_recv()

    def step(self, d):
        for way in ("up", "down"):
            if d > 0:
                self.came(d, way)
            if d < 3:
                self.go(d, way, lambda copy: copy.start())

    def finish(self):
        for d in range(3):
            for way in ("up", "down"):
                self.go(d, way, lambda copy: copy.wait_send())


class ScatterLine:
    def __init__(self, net, parts, got, made, sems, base):
        self.net, self.parts, self.got, self.made, self.sems, self.base = net, parts, got, made, sems, base
        self.n = parts.shape[1]

    def each(self, d, way):
        net = self.net
        t = net.z + (3 - d) if way == 0 else net.z - (3 - d)
        inside = (t < 4) if way == 0 else (t >= 0)
        first = (net.z == 0) if way == 0 else (net.z == 3)
        return t, inside, first, self.base + d + 3 * way, ("up", "down")[way]

    def step(self, d):
        for way in range(2):
            t, inside, first, i, name = self.each(d, way)

            @pl.when(inside & first)
            def _():
                self.net.copy(self.parts.at[t], self.got.at[way, d], self.sems, i, name).start()

            if d == 0:
                continue

            @pl.when(inside & jnp.logical_not(first))
            def _():
                self.net.copy(self.got.at[way, d - 1], self.got.at[way, d - 1], self.sems, i - 1, name).wait_recv()

                def body(rows):
                    self.made[way, d - 1, rows] = (wide(self.parts[t, rows]) + wide(self.got[way, d - 1, rows])).astype(bf16)

                tiles(0, self.n, body)
                self.net.copy(self.made.at[way, d - 1], self.got.at[way, d], self.sems, i, name).start()

    def finish(self, store):
        net = self.net
        below, above = net.z > 0, net.z < 3

        @pl.when(below)
        def _():
            net.copy(self.got.at[0, 2], self.got.at[0, 2], self.sems, self.base + 2, "up").wait_recv()

        @pl.when(above)
        def _():
            net.copy(self.got.at[1, 2], self.got.at[1, 2], self.sems, self.base + 5, "down").wait_recv()

        def put(low, high):
            def body(rows):
                total = wide(self.parts[net.z, rows])
                if low:
                    total = total + wide(self.got[0, 2, rows])
                if high:
                    total = total + wide(self.got[1, 2, rows])
                store(rows, total)

            tiles(0, self.n, body)

        @pl.when(below & above)
        def _():
            put(True, True)

        @pl.when(jnp.logical_not(below))
        def _():
            put(False, True)

        @pl.when(jnp.logical_not(above))
        def _():
            put(True, False)

        for d in range(3):
            for way in range(2):
                t, inside, first, i, name = self.each(d, way)

                @pl.when(inside & first)
                def _():
                    net.copy(self.parts.at[t], self.got.at[way, d], self.sems, i, name).wait_send()

                if d > 0:

                    @pl.when(inside & jnp.logical_not(first))
                    def _():
                        net.copy(self.made.at[way, d - 1], self.got.at[way, d], self.sems, i, name).wait_send()


def line_scratch(n, w):
    return [pltpu.VMEM((2, 3, n, w), bf16), pltpu.VMEM((2, 2, n, w), bf16)]


LINE_COPIES = 6


def gather_steps(net, v, out, sems, base, ready):
    n = v.shape[0]
    A, B = pl.ds(0, n // 2), pl.ds(n // 2, n // 2)
    go = {}
    ready(0)
    go["xA"] = net.send(v.at[A], out.at[1, 0, A], sems, base + 0, "x")
    go["yA"] = net.send(v.at[A], out.at[2, 0, A], sems, base + 3, "y")
    go["0A"] = net.send(v.at[A], out.at[0, 1, A], sems, base + 4, "c")
    ready(1)
    go["yB"] = net.send(v.at[B], out.at[2, 0, B], sems, base + 2, "y")
    go["xB"] = net.send(v.at[B], out.at[1, 0, B], sems, base + 1, "x")
    go["0B"] = net.send(v.at[B], out.at[0, 1, B], sems, base + 5, "c")
    yield
    go["xA"].wait_recv()
    go["dA"] = net.send(out.at[1, 0, A], out.at[3, 0, A], sems, base + 6, "y")
    go["1A"] = net.send(out.at[1, 0, A], out.at[1, 1, A], sems, base + 8, "c")
    go["yA"].wait_recv()
    go["2A"] = net.send(out.at[2, 0, A], out.at[2, 1, A], sems, base + 10, "c")
    yield
    go["yB"].wait_recv()
    go["dB"] = net.send(out.at[2, 0, B], out.at[3, 0, B], sems, base + 7, "x")
    go["2B"] = net.send(out.at[2, 0, B], out.at[2, 1, B], sems, base + 9, "c")
    go["xB"].wait_recv()
    go["1B"] = net.send(out.at[1, 0, B], out.at[1, 1, B], sems, base + 11, "c")
    yield
    go["dA"].wait_recv()
    go["3A"] = net.send(out.at[3, 0, A], out.at[3, 1, A], sems, base + 12, "c")
    go["dB"].wait_recv()
    go["3B"] = net.send(out.at[3, 0, B], out.at[3, 1, B], sems, base + 13, "c")
    yield
    for name in ("0A", "0B", "1A", "2B", "2A", "1B", "3A", "3B"):
        go[name].wait_recv()
    for copy in go.values():
        copy.wait_send()


def gather_rows(net, v, out, sems, base, ready, poll):
    for _ in gather_steps(net, v, out, sems, base, ready):
        poll()


GATHER_COPIES = 14
SCATTER_COPIES = 10


class Later:
    def __init__(self, make):
        self.make = make
        make().start()

    def wait_recv(self):
        self.make().wait_recv()

    def wait_send(self):
        self.make().wait_send()


def scatter_steps(net, parts, rc, rd, rx, ry, td, tx, ty, sems, base):
    n = parts.shape[2]
    A, B = pl.ds(0, n // 2), pl.ds(n // 2, n // 2)
    go = {}
    for i, chip in enumerate((3, 1, 2, 0)):
        go[chip] = Later(lambda i=i, chip=chip: net.copy(parts.at[chip, 1], rc.at[chip], sems, base + i, "c"))

    def add(dst, chip, start, more=None):
        def body(rows):
            total = wide(parts[chip, 0, rows]) + wide(rc[chip, rows])
            if more is not None:
                total = total + wide(more[rows])
            dst[rows] = total.astype(bf16)

        tiles(start, n // 2, body)

    yield None
    go[3].wait_recv()
    add(td, 3, 0)
    go["dA"] = Later(lambda: net.copy(td.at[A], rd.at[A], sems, base + 4, "x"))
    add(td, 3, n // 2)
    go["dB"] = Later(lambda: net.copy(td.at[B], rd.at[B], sems, base + 5, "y"))
    go[1].wait_recv()
    add(tx, 1, 0)
    go["xA"] = Later(lambda: net.copy(tx.at[A], rx.at[A], sems, base + 6, "x"))
    go[2].wait_recv()
    add(ty, 2, n // 2)
    go["yB"] = Later(lambda: net.copy(ty.at[B], ry.at[B], sems, base + 7, "y"))
    yield None
    go["dA"].wait_recv()
    add(ty, 2, 0, rd)
    go["yA"] = Later(lambda: net.copy(ty.at[A], ry.at[A], sems, base + 8, "y"))
    go["dB"].wait_recv()
    add(tx, 1, n // 2, rd)
    go["xB"] = Later(lambda: net.copy(tx.at[B], rx.at[B], sems, base + 9, "x"))
    go[0].wait_recv()

    def done(half):
        for name in (("xA", "yA"), ("xB", "yB"))[half]:
            go[name].wait_recv()
        if half == 1:
            for copy in go.values():
                copy.wait_send()

    yield done


def scatter_rows(net, parts, rc, rd, rx, ry, td, tx, ty, sems, base, poll):
    steps = scatter_steps(net, parts, rc, rd, rx, ry, td, tx, ty, sems, base)
    next(steps)
    next(steps)
    poll()
    return next(steps)


def scatter_scratch(n, w):
    return [pltpu.VMEM((4, n, w), bf16)] + [pltpu.VMEM((n, w), bf16)] * 6


def dma_sems(count):
    return [pltpu.SemaphoreType.DMA((count,)), pltpu.SemaphoreType.DMA((count,))]


VM = pl.BlockSpec(memory_space=pltpu.VMEM)
ANY = pl.BlockSpec(memory_space=pl.ANY)


def polls(*acts):
    left = list(acts)

    def poll():
        if left:
            left.pop(0)()

    def drain():
        while left:
            poll()

    return poll, drain


def comm_call(body, name, ident, ins, in_specs, outs, out_specs, scratch):
    return pl.pallas_call(
        body,
        in_specs=in_specs,
        out_specs=out_specs,
        out_shape=outs,
        scratch_shapes=scratch,
        compiler_params=pltpu.CompilerParams(collective_id=ident, has_side_effects=True, vmem_limit_bytes=60 << 20),
        name=name,
    )(*ins)


def shape(dims, dtype):
    return jax.ShapeDtypeStruct(dims, dtype)


PLANE = ("x", "y", "c", "xy", "xc", "yc", "xyc")
PLACES = {"c": (0, 1), "x": (1, 0), "xc": (1, 1), "y": (2, 0), "yc": (2, 1), "xy": (3, 0), "xyc": (3, 1)}


def start_call(x, dy, docs, gains, taps, w_qkv, w_gate, w_up, w_out, ident):
    n, w = x.shape
    rows = w_qkv.shape[0]

    def body(x_ref, dy_ref, docs_ref, g_ref, taps_ref, wq_ref, gate_ref, up_ref, wo_ref,
             a1_ref, dys_ref, docs_out, gains_ref, qkv_out, gu_out, wo_out, th_ref, tl_ref, tt_ref,
             xs, gains_out, slots, gus, local, send, recv):
        net = Net()
        sems = (send, recv)
        base = 2 * GATHER_COPIES
        line_q = GatherLine(net, qkv_out.at[net.z], qkv_out, sems, base)
        line_o = GatherLine(net, wo_ref, wo_out, sems, base + 6, lambda slot: slot // 2 == net.x)
        line_g = GatherLine(net, gains_out.at[net.z], gains_out, sems, base + 12)
        base += 18
        gains_out[net.z, net.k] = g_ref[...]
        slots[...] = jnp.zeros_like(slots)
        for half in range(2):

            @pl.when(net.x == half)
            def _():
                for k in range(4):
                    pair = 4 * half + 2 * (k % 2) + k // 2
                    for m in range(6):
                        col = (m // 2) * MODEL_WIDTH + (2 * pair + m % 2) * E
                        slots[k, :, m * EP : m * EP + E] = wq_ref[:, col : col + E]
                    for m in range(8):
                        src = gate_ref if m < 4 else up_ref
                        col = 256 * (4 * (m % 4) + k) + 128 * half
                        gus[k, :, m * 128 : (m + 1) * 128] = src[:, col : col + 128]

        net.greet(PLANE)
        own = [
            pltpu.make_async_copy(slots.at[net.k], qkv_out.at[net.z, net.k], local.at[0]),
            pltpu.make_async_copy(dy_ref, dys_ref.at[0, 0], local.at[1]),
            pltpu.make_async_copy(gus.at[net.k], gu_out.at[net.k], local.at[2]),
            pltpu.make_async_copy(docs_ref, docs_out.at[0, 0], local.at[3]),
            pltpu.make_async_copy(wo_ref, wo_out.at[net.z], local.at[4]),
        ]
        for copy in own:
            copy.start()
        qkv_parts, gain_parts, small = [], [], []
        flips = {"c": net.k + 1 - 2 * net.c, "y": net.k + 2 - 4 * net.y, "yc": net.k + 1 - 2 * net.c + 2 - 4 * net.y}
        for j, name in enumerate(("y", "yc", "c")):
            gain_parts.append(net.send(g_ref, gains_out.at[net.z, net.k], sems, base + 6 + j, name))
            qkv_parts.append(net.send(slots.at[flips[name]], qkv_out.at[net.z, net.k], sems, base + j, name))
        line_o.step(0)
        for j, (name, (chip, core)) in enumerate(PLACES.items()):
            small.append(net.send(docs_ref, docs_out.at[chip, core], sems, base + 9 + j, name))
        gather_x = gather_steps(net, x_ref, xs, sems, 0, lambda half: None)
        next(gather_x)
        gather_dy = gather_steps(net, dy_ref, dys_ref, sems, GATHER_COPIES, lambda half: None)
        next(gather_dy)
        for copy in gain_parts:
            copy.wait_recv()
        line_g.step(0)
        own[0].wait()
        for copy in qkv_parts:
            copy.wait_recv()
        line_q.step(0)
        line_g.step(1)

        diff = lax.broadcasted_iota(jnp.int32, (n, n), 1) - lax.broadcasted_iota(jnp.int32, (n, n), 0)

        def bands_of(first, count):
            def one(i, _):
                band = jnp.zeros((n, n), f32)
                back = jnp.zeros((n, n), f32)
                for b in range(KWIN):
                    tap = taps_ref[(first + i) * KWIN + b]
                    band = jnp.where(diff == b, tap, band)
                    back = jnp.where(diff == -b, tap, back)
                h, a = (first + i) // QWIN, (first + i) % QWIN
                at = pl.ds(pl.multiple_of(a * n, n), n)
                th_ref[h, at], tl_ref[h, at] = split(band)
                tt_ref[h, at] = back.astype(bf16)
                return 0

            lax.fori_loop(0, count, one, 0)

        bands_of(0, QWIN)
        line_g.step(2)
        next(gather_x)
        line_q.step(1)
        line_g.step(3)
        line_o.step(1)
        for i in range(16):
            gains_ref[:, i * rows : (i + 1) * rows] = wide(gains_out[i // 4, i % 4, 0:8, 0:rows])
        bands_of(QWIN, QWIN)
        next(gather_x)
        next(gather_dy)
        for j, name in enumerate(("y", "yc", "c")):
            small.append(net.send(gus.at[flips[name]], gu_out.at[net.k], sems, base + 3 + j, name))
        next(gather_dy)
        gain = gains_ref[0:1]

        def norm(chip, core, src):
            def body(at):
                xf = wide(src[at])
                r = lax.rsqrt(jnp.mean(xf * xf, axis=1, keepdims=True) + 1e-06)
                a1_ref[chip, core, at] = (xf * r * gain).astype(bf16)

            tiles(0, n, body)

        norm(0, 0, x_ref)
        line_q.step(2)
        line_o.step(2)
        for _ in gather_x:
            pass
        next(gather_dy)
        for chip in range(4):
            for core in range(2):
                if (chip, core) != (0, 0):
                    norm(chip, core, xs.at[chip, core])
        line_q.step(3)
        line_o.step(3)
        for _ in gather_dy:
            pass
        for line in (line_q, line_g, line_o):
            line.finish()
        for copy in own[1:]:
            copy.wait()
        for copy in small:
            copy.wait_recv()
        for copy in qkv_parts + gain_parts + small:
            copy.wait_send()

    return comm_call(
        body, "start", ident, (x, dy, docs, gains, taps, w_qkv, w_gate, w_up, w_out),
        [VM] * 4 + [pl.BlockSpec(memory_space=pltpu.SMEM)] + [VM] * 4,
        [shape((4, 2, n, w), bf16), shape((4, 2, n, w), bf16), shape((4, 2) + docs.shape, docs.dtype), shape((8, w), f32),
         shape((4, 4, rows, 6 * EP), bf16), shape((4, rows, FF // 4), bf16), shape((4, rows, MODEL_WIDTH), bf16)]
        + [shape((2, QWIN * n, n), bf16)] * 3,
        [VM, ANY, ANY, VM, ANY, ANY, ANY, VM, VM, VM],
        [pltpu.VMEM((4, 2, n, w), bf16), pltpu.VMEM((4, 4) + gains.shape, bf16),
         pltpu.VMEM((4, rows, 6 * EP), bf16), pltpu.VMEM((4, rows, FF // 4), bf16), pltpu.SemaphoreType.DMA((5,))]
        + dma_sems(2 * GATHER_COPIES + 18 + 16),
    )


def mid_call(parts, x, gain, gu, w_down, ident):
    n, w = parts.shape[2:]
    down = w_down.shape[0] // 2

    def body(p_ref, x_ref, g_ref, gu_ref, wd_ref, resid_ref, out_ref, gu_out, wd_out, v, local, rc, rd, rx, ry, td, tx, ty, send, recv):
        net = Net()
        sems = (send, recv)
        net.greet("xyc")
        base = SCATTER_COPIES + GATHER_COPIES
        mine = wd_ref.at[pl.ds(pl.multiple_of(down * net.x, down), down)]
        line_g = GatherLine(net, gu_ref, gu_out, sems, base)
        line_d = GatherLine(net, mine, wd_out, sems, base + LINE_COPIES)
        lines = (line_g, line_d)
        own = [pltpu.make_async_copy(gu_ref, gu_out.at[net.z], local.at[1]), pltpu.make_async_copy(mine, wd_out.at[net.z], local.at[2])]
        for copy in own:
            copy.start()
        for line in lines:
            line.step(0)
        poll, drain = polls(*[lambda d=d, line=line: line.step(d) for d in (1, 2, 3) for line in lines])
        done = scatter_rows(net, p_ref, rc, rd, rx, ry, td, tx, ty, sems, 0, poll)
        poll()

        def ready(half):
            done(half)

            def rows_of(rows):
                total = wide(p_ref[0, 0, rows]) + wide(rc[0, rows]) + wide(rx[rows]) + wide(ry[rows])
                resid = wide(x_ref[rows]) + total
                resid_ref[rows] = resid
                r = lax.rsqrt(jnp.mean(resid * resid, axis=1, keepdims=True) + 1e-06)
                v[rows] = (resid * r * g_ref[...]).astype(bf16)

            tiles(half * (n // 2), n // 2, rows_of)

        gather_rows(net, v, out_ref, sems, SCATTER_COPIES, ready, poll)
        drain()
        last = pltpu.make_async_copy(v, out_ref.at[0, 0], local.at[0])
        last.start()
        for line in lines:
            line.finish()
        for copy in own:
            copy.wait()
        last.wait()

    return comm_call(
        body, "mid", ident, (parts, x, gain, gu, w_down), [VM] * 5,
        [shape((n, w), f32), shape((4, 2, n, w), bf16), shape((4,) + gu.shape, bf16), shape((4, down, w), bf16)], [VM, ANY, ANY, ANY],
        [pltpu.VMEM((n, w), bf16), pltpu.SemaphoreType.DMA((3,))] + scatter_scratch(n, w)
        + dma_sems(SCATTER_COPIES + GATHER_COPIES + 2 * LINE_COPIES),
    )


def mid_back_call(parts, dy, resid, gain, down, ident):
    n, w = parts.shape[2:]

    def body(p_ref, dy_ref, r_ref, g_ref, down_ref, dresid_ref, out_ref, sum_ref, down_out,
             v, local, rc, rd, rx, ry, td, tx, ty, d_got, d_made, send, recv):
        net = Net()
        sems = (send, recv)
        net.greet("xyc")
        base = SCATTER_COPIES + GATHER_COPIES
        line_d = ScatterLine(net, down_ref, d_got, d_made, sems, base)
        line_d.step(0)
        poll, drain = polls(lambda: line_d.step(1), lambda: None, lambda: line_d.step(2))
        sum_ref[...] = jnp.zeros_like(sum_ref)
        done = scatter_rows(net, p_ref, rc, rd, rx, ry, td, tx, ty, sems, 0, poll)
        poll()

        def ready(half):
            done(half)

            def rows_of(rows):
                da2 = wide(p_ref[0, 0, rows]) + wide(rc[0, rows]) + wide(rx[rows]) + wide(ry[rows])
                res = r_ref[rows]
                r = lax.rsqrt(jnp.mean(res * res, axis=1, keepdims=True) + 1e-06)
                unit = res * r
                sum_ref[0:1] += jnp.sum(da2 * unit, axis=0, keepdims=True)
                dn = da2 * g_ref[...]
                dresid = wide(dy_ref[rows]) + r * (dn - unit * r * jnp.mean(dn * res, axis=1, keepdims=True))
                dresid_ref[rows] = dresid
                v[rows] = dresid.astype(bf16)

            tiles(half * (n // 2), n // 2, rows_of)

        gather_rows(net, v, out_ref, sems, SCATTER_COPIES, ready, poll)
        drain()
        last = pltpu.make_async_copy(v, out_ref.at[0, 0], local)
        last.start()

        def put(ref):
            def store(rows, total):
                ref[rows] = total.astype(bf16)

            return store

        line_d.finish(put(down_out))
        last.wait()

    return comm_call(
        body, "mid_back", ident, (parts, dy, resid, gain, down), [VM] * 5,
        [shape((n, w), f32), shape((4, 2, n, w), bf16), shape((8, w), f32), shape(down.shape[1:], bf16)],
        [VM, ANY, VM, VM],
        [pltpu.VMEM((n, w), bf16), pltpu.SemaphoreType.DMA] + scatter_scratch(n, w) + line_scratch(*down.shape[1:])
        + dma_sems(SCATTER_COPIES + GATHER_COPIES + LINE_COPIES),
    )


def end_call(da_parts, qkv, wo, gu, down, small, x, dresid, gain, ident):
    n, w = da_parts.shape[2:]
    rows_q = qkv.shape[1] // 4
    rows_o = wo.shape[1]

    def body(da_ref, q_ref, wo_ref, zg, down_ref, small_ref, x_ref, dresid_ref, g_ref,
             gx_ref, gq_ref, go_ref, gate_ref, up_ref, gd_ref, total_ref,
             rc, rd, rx, ry, td, tx, ty,
             q_got, q_made, o_got, o_made, zq, cq, fq, cg, fg, fd, po, ro, s_got, s_sum, s_line, send, recv):
        net = Net()
        sems = (send, recv)
        net.greet("xyc")
        z, x, y, c = net.z, net.x, net.y, net.c
        base = SCATTER_COPIES
        line_q = ScatterLine(net, q_ref, q_got, q_made, sems, base)
        line_o = ScatterLine(net, po, o_got, o_made, sems, base + 6)
        line_s = GatherLine(net, s_sum.at[2], s_line, sems, base + 12)
        base += 18
        line_q.step(0)
        to_c = net.send(wo_ref.at[1 - c], po.at[2 * x + c], sems, base, "c")
        hop = net.send(small_ref, s_got.at[0], sems, base + 1, "c")
        hops = [hop]
        po[2 * (1 - x)] = jnp.zeros((rows_o, w), bf16)
        po[2 * (1 - x) + 1] = jnp.zeros((rows_o, w), bf16)
        po[2 * x + c] = wo_ref[c]
        block = lambda i, j: pl.ds(pl.multiple_of((2 * i + j) * rows_q, rows_q), rows_q)
        gu_swaps = [net.send(zg.at[block(i, 1 - c)], cg.at[i, c], sems, base + 9 + i, "c") for i in range(2)]
        for i in range(2):
            cg[i, c] = zg[block(i, c)]
        fd[x] = down_ref[...]

        def small_step(i):
            hops[i].wait_recv()
            s_sum[i] = (small_ref[...] if i == 0 else s_sum[i - 1]) + s_got[i]
            if i < 2:
                hops.append(net.send(s_sum.at[i], s_got.at[i + 1], sems, base + 2 + i, "yx"[i]))
            else:
                line_s.step(0)

        def begin():
            small_step(0)
            to_c.wait_recv()
            line_o.step(0)

        poll, _ = polls(begin)
        done = scatter_rows(net, da_ref, rc, rd, rx, ry, td, tx, ty, sems, 0, poll)
        line_q.step(1)
        small_step(1)
        line_o.step(1)
        down_swap = net.send(down_ref, fd.at[x], sems, base + 13, "x")
        for copy in gu_swaps:
            copy.wait_recv()
        gu_swaps.append(net.send(cg.at[1 - y], fg.at[x, y], sems, base + 11, "y"))
        fg[x, y] = cg[y]

        line_q.step(2)
        small_step(2)
        line_o.step(2)
        line_s.step(1)
        gu_swaps[2].wait_recv()
        gu_swaps.append(net.send(fg.at[x], fg.at[x], sems, base + 12, "x"))
        for half in range(2):
            done(half)

            def rows_of(rows):
                da = wide(da_ref[0, 0, rows]) + wide(rc[0, rows]) + wide(rx[rows]) + wide(ry[rows])
                xf = wide(x_ref[rows])
                r = lax.rsqrt(jnp.mean(xf * xf, axis=1, keepdims=True) + 1e-06)
                dn = da * g_ref[...]
                gx_ref[rows] = dresid_ref[rows] + r * (dn - xf * r * r * jnp.mean(dn * xf, axis=1, keepdims=True))

            tiles(half * (n // 2), n // 2, rows_of)

        def put_q(rows, total):
            zq[rows] = total.astype(bf16)

        def put_o(rows, total):
            ro[0, rows] = total.astype(bf16)

        line_q.finish(put_q)
        swaps = [net.send(zq.at[block(i, 1 - c)], cq.at[i, c], sems, base + 4 + i, "c") for i in range(2)]
        for i in range(2):
            cq[i, c] = zq[block(i, c)]
        for copy in swaps:
            copy.wait_recv()
        swaps.append(net.send(cq.at[1 - y], fq.at[x, y], sems, base + 6, "y"))
        fq[x, y] = cq[y]
        line_s.step(2)
        line_o.finish(put_o)
        swaps.append(net.send(ro.at[0], ro.at[1], sems, base + 7, "x"))
        swaps[2].wait_recv()
        swaps.append(net.send(fq.at[x], fq.at[x], sems, base + 8, "x"))
        line_s.step(3)
        s_line[z] = s_sum[2]
        total_ref[...] = (s_line[0] + s_line[1]) + (s_line[2] + s_line[3])
        down_swap.wait_recv()
        for i in range(2):
            gd_ref[i * down.shape[0] : (i + 1) * down.shape[0]] = wide(fd[i])
        gu_swaps[3].wait_recv()
        for i in range(2):
            for k in range(4):
                for m in range(8):
                    col = 256 * (4 * (m % 4) + k) + 128 * i
                    dst = gate_ref if m < 4 else up_ref
                    dst[:, col : col + 128] = wide(fg[i, k // 2, k % 2, :, m * 128 : (m + 1) * 128])
        swaps[3].wait_recv()
        go_ref[...] = wide(ro[0]) + wide(ro[1])
        swaps[4].wait_recv()
        for i in range(2):
            for k in range(4):
                pair = 4 * i + 2 * (k % 2) + k // 2
                for m in range(6):
                    col = (m // 2) * MODEL_WIDTH + (2 * pair + m % 2) * E
                    gq_ref[:, col : col + E] = wide(fq[i, k // 2, k % 2, :, m * EP : m * EP + E])
        line_s.finish()
        for copy in swaps + hops + gu_swaps + [to_c, down_swap]:
            copy.wait_send()

    stages = [pltpu.VMEM((2, rows_o, w), bf16), pltpu.VMEM((3,) + small.shape, f32), pltpu.VMEM((3,) + small.shape, f32),
              pltpu.VMEM((4,) + small.shape, f32)]
    return comm_call(
        body, "end", ident, (da_parts, qkv, wo, gu, down, small, x, dresid, gain), [VM] * 9,
        [shape((n, w), f32), shape((rows_q, 3 * MODEL_WIDTH), f32), shape((rows_o, w), f32),
         shape((rows_q, FF), f32), shape((rows_q, FF), f32), shape((2 * down.shape[0], w), f32), shape(small.shape, f32)],
        [VM] * 7,
        scatter_scratch(n, w) + line_scratch(*qkv.shape[1:]) + line_scratch(rows_o, w)
        + [pltpu.VMEM(qkv.shape[1:], bf16), pltpu.VMEM((2, 2, rows_q, 6 * EP), bf16), pltpu.VMEM((2, 2, 2, rows_q, 6 * EP), bf16),
           pltpu.VMEM((2, 2, rows_q, FF // 4), bf16), pltpu.VMEM((2, 2, 2, rows_q, FF // 4), bf16), pltpu.VMEM((2,) + down.shape, bf16),
           pltpu.VMEM((4, rows_o, w), bf16)]
        + stages + dma_sems(SCATTER_COPIES + 18 + 14),
    )


def back_call(mix, qkv, dcol, drow, tt, gain, dattn, xhat, s, p, z, normed, a1, out_w, qkv_w, out_parts, gu, resid, ident):
    rows, t, _ = qkv.shape
    n, w = out_parts.shape[2:]

    def body(mix_ref, qkv_ref, dcol_ref, drow_ref, tt_ref, gain_ref, dattn_ref, xhat_ref, s_ref, p_ref, z_ref, normed_ref, a1_ref,
             ow_ref, qw_ref, op_ref, gu_ref, resid_ref,
             da_ref, gq_ref, go_ref, gconv_ref, gmix_ref, gg_ref, out_ref, gu_out,
             m_ref, dq, rc, rd, rx, ry, td, tx, ty, g_got, g_made, send, recv):
        net = Net()
        sems = (send, recv)
        step = pl.program_id(0)
        line = ScatterLine(net, gu_ref, g_got, g_made, sems, SCATTER_COPIES)
        scatter = scatter_steps(net, op_ref, rc, rd, rx, ry, td, tx, ty, sems, 0)

        @pl.when(step == 0)
        def _():
            net.greet("xyc")
            line.step(0)
            next(scatter)
            m_ref[...] = jnp.zeros_like(m_ref)
            gmix_ref[...] = jnp.zeros_like(gmix_ref)
            gg_ref[...] = jnp.zeros_like(gg_ref)
            gq_ref[...] = jnp.zeros_like(gq_ref)
            go_ref[...] = jnp.zeros_like(go_ref)

        allowed = allowed_mask(dcol_ref[0], drow_ref[0])
        scale = 1.0 / math.sqrt(E)
        lane = lax.broadcasted_iota(jnp.int32, (1, EP), 1)
        prob = [p_ref[0, 0], p_ref[0, 1]]
        go_ref[...] += dot(normed_ref[0], dattn_ref[0], 0, 0)
        dmixed = []
        for h in range(2):
            cols = slice(h * EP, (h + 1) * EP)
            dn, xh = dot(dattn_ref[0], ow_ref[cols], 1, 1), xhat_ref[0, :, cols]
            gg_ref[0:1, cols] += jnp.sum(dn * xh, axis=0, keepdims=True)
            dc = dn * gain_ref[0:1, cols]
            m1 = jnp.sum(dc, axis=1, keepdims=True) / E
            m2 = jnp.sum(dc * xh, axis=1, keepdims=True) / E
            dh = jnp.where(lane < E, s_ref[0, :, cols] * (dc - m1 - xh * m2), 0.0).astype(bf16)
            v = qkv_ref[0, :, (4 + h) * EP : (5 + h) * EP]
            mixed = (mix_ref[h, 0] * prob[0] + mix_ref[h, 1] * prob[1]).astype(bf16)
            dmixed.append(dot(dh, v, 1, 1))
            dq[:, (4 + h) * EP : (5 + h) * EP] = dot(mixed, dh, 0, 0).astype(bf16)
        for h in range(2):
            for c in range(2):
                r = 2 * h + c
                gmix_ref[r : r + 1, :] += jnp.sum(dmixed[h] * prob[c], axis=0, keepdims=True)
        for c in range(2):
            dp = mix_ref[0, c] * dmixed[0] + mix_ref[1, c] * dmixed[1]
            dconv = prob[c] * (dp - jnp.sum(dp * prob[c], axis=1, keepdims=True))
            ahead = jnp.concatenate([up(dconv, a).astype(bf16) for a in range(QWIN)], 1)
            m_ref[c] += dot(z_ref[0, c], ahead, 0, 0)
            ds = jnp.where(allowed, dot(ahead, tt_ref[c]), 0.0).astype(bf16)
            q = qkv_ref[0, :, c * EP : (c + 1) * EP]
            k = qkv_ref[0, :, (2 + c) * EP : (3 + c) * EP]
            dq[:, c * EP : (c + 1) * EP] = (dot(ds, k) * scale).astype(bf16)
            dq[:, (2 + c) * EP : (3 + c) * EP] = (dot(ds, q, 0, 0) * scale).astype(bf16)
        da_ref[0] = dot(dq[...], qw_ref[...], 1, 1).astype(bf16)
        for i in range(0, w, 384):
            gq_ref[i : i + 384] += dot(a1_ref[0, :, i : i + 384], dq[...], 0, 0)

        @pl.when(step == 1)
        def _():
            next(scatter)

        @pl.when(step == 3)
        def _():
            line.step(1)

        done = []

        @pl.when(step == 2)
        def _():
            done.append(next(scatter))

        @pl.when(step == 5)
        def _():
            line.step(2)

        @pl.when(step == rows - 1)
        def _():
            lanes = lax.broadcasted_iota(jnp.int32, (8, t), 1)
            for h in range(2):
                for a in range(QWIN):
                    total = jnp.zeros((8, t), f32)
                    for first in range(0, t, 8):
                        part = m_ref[h, first : first + 8, a * t : (a + 1) * t]
                        turned = pltpu.roll(part, t - first, 1) if first else part
                        total = total + jnp.where(lanes < t - first, turned, 0.0)
                    gconv_ref[h, a] = total[:, :EP]
            for half in range(2):
                done[0](half)

                def sum_of(at):
                    total = wide(op_ref[0, 0, at]) + wide(rc[0, at]) + wide(rx[at]) + wide(ry[at])
                    out_ref[at] = (resid_ref[at] + total).astype(bf16)

                tiles(half * (n // 2), n // 2, sum_of)

            def put(at, total):
                gu_out[at] = total.astype(bf16)

            line.finish(put)

    row = lambda *sh: pl.BlockSpec((1,) + sh, lambda i: (i,) + (0,) * len(sh))
    full = lambda v: pl.BlockSpec(v.shape, lambda i: (0,) * v.ndim, pipeline_mode=pl.Buffered(1))
    keep = lambda *sh: pl.BlockSpec(sh, lambda i: (0,) * len(sh))
    return pl.pallas_call(
        body,
        grid=(rows,),
        in_specs=[pl.BlockSpec(memory_space=pltpu.SMEM), row(t, 6 * EP), row(t, 1), row(1, t), full(tt), full(gain),
                  row(t, w), row(t, 2 * EP), row(t, 2 * EP), row(2, t, t), row(2, t, t), row(t, 2 * EP), row(t, w),
                  full(out_w), full(qkv_w), full(out_parts), full(gu), full(resid)],
        out_specs=[row(t, w), keep(w, 6 * EP), keep(2 * EP, w), keep(2, QWIN, 8, EP), keep(8, t), keep(8, 2 * EP), keep(n, w),
                   keep(*gu.shape[1:])],
        out_shape=[
            shape((rows, t, w), bf16),
            shape((w, 6 * EP), f32),
            shape((2 * EP, w), f32),
            shape((2, QWIN, 8, EP), f32),
            shape((8, t), f32),
            shape((8, 2 * EP), f32),
            shape((n, w), bf16),
            shape(gu.shape[1:], bf16),
        ],
        scratch_shapes=[pltpu.VMEM((2, t, QWIN * t), f32), pltpu.VMEM((t, 6 * EP), bf16)] + scatter_scratch(n, w)
        + line_scratch(*gu.shape[1:]) + dma_sems(SCATTER_COPIES + LINE_COPIES),
        compiler_params=pltpu.CompilerParams(collective_id=ident, has_side_effects=True, vmem_limit_bytes=63 << 20),
        name="back",
    )(mix, qkv, dcol, drow, tt, gain, dattn, xhat, s, p, z, normed, a1, out_w, qkv_w, out_parts, gu, resid)


def rms_scale(values):
    return lax.rsqrt(jnp.mean(values * values, axis=1, keepdims=True) + 1e-06)


class Links:
    def __init__(self, fsdp):
        self.fsdp = fsdp
        index = lax.axis_index("fsdp")
        self.x = lax.axis_index("rep")
        self.z, self.y, self.c = index // 4, (index // 2) % 2, index % 2

    def across(self, flip, v):
        if flip == "x":
            return lax.ppermute(v, "rep", [(0, 1), (1, 0)])
        bit = {"y": 2, "c": 1}[flip]
        return lax.ppermute(v, "fsdp", [(f, f ^ bit) for f in range(self.fsdp)])

    def along(self, v, step):
        pairs = [(f, f + 4 * step) for f in range(self.fsdp) if 0 <= f + 4 * step < self.fsdp]
        return lax.ppermute(v, "fsdp", pairs)

    def ordered(self, bit, mine, other, axis):
        first, second = jnp.where(bit == 0, mine, other), jnp.where(bit == 0, other, mine)
        return jnp.stack([first, second], axis)

    def gather_z(self, v):
        left, right = [], []
        a = b = v
        for _ in range(3):
            a, b = self.along(a, 1), self.along(b, -1)
            left.append(a)
            right.append(b)
        line = jnp.stack(left[::-1] + [v] + right)
        return lax.dynamic_slice_in_dim(line, 3 - self.z, 4, 0)

    def scatter_z(self, parts):
        zero = jnp.zeros((3,) + parts.shape[1:], parts.dtype)
        line = lax.dynamic_slice_in_dim(jnp.concatenate([zero, parts, zero]), self.z, 7, 0)
        low = lambda v: v.astype(bf16)
        a = self.along(low(line[6]), 1)
        b = self.along(low(line[0]), -1)
        for step in (1, 2):
            a = self.along(low(line[6 - step] + a.astype(f32)), 1)
            b = self.along(low(line[step] + b.astype(f32)), -1)
        return line[3] + a.astype(f32) + b.astype(f32)

    def gather_plane(self, v):
        n = v.shape[0] // 2
        vx, vy = self.across("x", v), self.across("y", v)
        vd = jnp.concatenate([self.across("y", vx[:n]), self.across("x", vy[n:])])
        return [jnp.concatenate([u, self.across("c", u)]) for u in (v, vx, vy, vd)]

    def scatter_plane(self, parts):
        low = lambda v: v.astype(bf16)
        n = parts[0].shape[0] // 2
        s = [p[:n] + self.across("c", low(p[n:])).astype(f32) for p in parts]
        m = n // 2
        dx, dy = self.across("x", low(s[3][:m])), self.across("y", low(s[3][m:]))
        to_x = jnp.concatenate([s[1][:m], s[1][m:] + dy.astype(f32)])
        to_y = jnp.concatenate([s[2][:m] + dx.astype(f32), s[2][m:]])
        return s[0] + self.across("x", low(to_x)).astype(f32) + self.across("y", low(to_y)).astype(f32)


class Weights:
    def __init__(self, links):
        self.links = links
        self.line = links.fsdp == 16
        x, y, c = links.x, links.y, links.c
        self.pair = 4 * x + 2 * c + y
        self.slot = 4 * x + 2 * y + c

    def spread(self, shard, dims):
        l = self.links
        ax, ay, ac = dims
        v = lax.dynamic_index_in_dim(shard, l.x, ax, keepdims=True)
        keep = lax.dynamic_index_in_dim(v, l.y, ay, keepdims=True)
        sent = l.across("y", lax.dynamic_index_in_dim(v, 1 - l.y, ay, keepdims=True))
        v = l.ordered(l.y, keep, sent, 0)
        keep = lax.dynamic_index_in_dim(v, l.c, ac + 1, keepdims=True)
        sent = l.across("c", lax.dynamic_index_in_dim(v, 1 - l.c, ac + 1, keepdims=True))
        v = l.ordered(l.c, keep, sent, 1)
        return l.gather_z(v)

    def collect(self, grad, dims):
        l = self.links
        ax, ay, ac = dims
        low = lambda v: v.astype(bf16)
        v = l.scatter_z(grad)
        keep = lax.dynamic_index_in_dim(v, l.c, 1, keepdims=False)
        sent = l.across("c", low(lax.dynamic_index_in_dim(v, 1 - l.c, 1, keepdims=False)))
        v = self.join(l.c, keep, sent.astype(f32), ac + 1)
        keep = lax.dynamic_index_in_dim(v, l.y, 0, keepdims=False)
        sent = l.across("y", low(lax.dynamic_index_in_dim(v, 1 - l.y, 0, keepdims=False)))
        v = low(self.join(l.y, keep, sent.astype(f32), ay))
        return self.join(l.x, v, l.across("x", v), ax).astype(f32)

    def join(self, bit, mine, other, axis):
        first, second = jnp.where(bit == 0, mine, other), jnp.where(bit == 0, other, mine)
        return jnp.concatenate([first, second], axis)

    def whole(self, shard):
        return lax.all_gather(shard, "fsdp", axis=0, tiled=True)

    def owned(self, grad):
        part = lax.psum_scatter(grad, "fsdp", scatter_dimension=0, tiled=True)
        return lax.psum(part.astype(bf16), "rep").astype(f32)

    def qkv(self, shard):
        rows = shard.shape[0]
        if self.line:
            v = self.spread(shard.reshape(rows, 3, 2, 2, 2, 2 * E), (2, 4, 3))
            v = v.reshape(MODEL_WIDTH, 3, 2, E)
        else:
            v = self.whole(shard).reshape(MODEL_WIDTH, 3, 8, 2, E)
            v = lax.dynamic_index_in_dim(v, self.pair, 2, keepdims=False)
        return jnp.pad(v, ((0, 0), (0, 0), (0, 0), (0, EP - E))).reshape(MODEL_WIDTH, 6 * EP)

    def qkv_back(self, grad):
        g = grad.reshape(MODEL_WIDTH, 3, 2, EP)[..., :E]
        if self.line:
            return self.collect(g.reshape(4, 2, 2, -1, 3, 1, 1, 1, 2 * E), (2, 4, 3)).reshape(-1, 3 * MODEL_WIDTH)
        zero = jnp.zeros((MODEL_WIDTH, 3, 8, 2, E), f32)
        return self.owned(lax.dynamic_update_index_in_dim(zero, g, self.pair, 2).reshape(MODEL_WIDTH, 3 * MODEL_WIDTH))

    def out(self, shard):
        l = self.links
        if self.line:
            v = l.gather_z(shard)
            keep = lax.dynamic_index_in_dim(v, 2 * l.x + l.c, 0, keepdims=False)
            sent = l.across("c", lax.dynamic_index_in_dim(v, 2 * l.x + 1 - l.c, 0, keepdims=False))
            v = l.ordered(l.c, keep, sent, 0)
        else:
            v = self.whole(shard).reshape(8, 2, E, MODEL_WIDTH)
            v = lax.dynamic_index_in_dim(v, self.pair, 0, keepdims=False)
        return jnp.pad(v, ((0, 0), (0, EP - E), (0, 0))).reshape(2 * EP, MODEL_WIDTH)

    def out_back(self, grad):
        l = self.links
        g = grad.reshape(2, EP, MODEL_WIDTH)[:, :E]
        if self.line:
            keep = lax.dynamic_index_in_dim(g, l.c, 0, keepdims=False)
            sent = l.across("c", lax.dynamic_index_in_dim(g, 1 - l.c, 0, keepdims=False).astype(bf16)).astype(f32)
            at = jnp.arange(4)[:, None, None]
            parts = jnp.where(at == 2 * l.x + l.c, keep[None], jnp.where(at == 2 * l.x + 1 - l.c, sent[None], 0.0))
            v = l.scatter_z(parts).astype(bf16)
            return (v + l.across("x", v)).astype(f32)
        zero = jnp.zeros((8, 2, E, MODEL_WIDTH), f32)
        return self.owned(lax.dynamic_update_index_in_dim(zero, g, self.pair, 0).reshape(MODEL_WIDTH, MODEL_WIDTH))

    def ffn_in(self, gate, up_):
        rows = gate.shape[0]
        both = jnp.stack([gate, up_], 1)
        if self.line:
            v = self.spread(both.reshape(rows, 2, 4, 2, 2, 2, FF // 32), (5, 3, 4))
            return v.reshape(MODEL_WIDTH, FF // 4)
        v = self.whole(both).reshape(MODEL_WIDTH, 2, 8, FF // 8)
        return lax.dynamic_index_in_dim(v, self.slot, 2, keepdims=False).reshape(MODEL_WIDTH, FF // 4)

    def ffn_in_back(self, grad):
        if self.line:
            v = self.collect(grad.reshape(4, 2, 2, -1, 2, 4, 1, 1, 1, FF // 32), (5, 3, 4)).reshape(-1, 2, FF)
        else:
            zero = jnp.zeros((MODEL_WIDTH, 2, 8, FF // 8), f32)
            g = grad.reshape(MODEL_WIDTH, 2, FF // 8)
            v = self.owned(lax.dynamic_update_index_in_dim(zero, g, self.slot, 2).reshape(MODEL_WIDTH, 2, FF))
        return v[:, 0], v[:, 1]

    def ffn_out(self, shard):
        l = self.links
        if self.line:
            v = lax.dynamic_index_in_dim(shard.reshape(2, FF // 32, MODEL_WIDTH), l.x, 0, keepdims=False)
            return l.gather_z(v).reshape(FF // 8, MODEL_WIDTH)
        v = self.whole(shard).reshape(8, FF // 8, MODEL_WIDTH)
        return lax.dynamic_index_in_dim(v, self.slot, 0, keepdims=False)

    def ffn_out_back(self, grad):
        l = self.links
        if self.line:
            v = l.scatter_z(grad.reshape(4, FF // 32, MODEL_WIDTH)).astype(bf16)
            return self.join(l.x, v, l.across("x", v), 0).astype(f32)
        zero = jnp.zeros((8, FF // 8, MODEL_WIDTH), f32)
        return self.owned(lax.dynamic_update_index_in_dim(zero, grad, self.slot, 0).reshape(FF, MODEL_WIDTH))

    def gains(self, *shards):
        l = self.links
        v = jnp.stack(shards)
        if self.line:
            v = l.ordered(l.c, v, l.across("c", v), 0)
            v = l.ordered(l.y, v, l.across("y", v), 0)
            v = l.gather_z(v)
            v = v.reshape(16, len(shards), -1).transpose(1, 0, 2).reshape(len(shards), MODEL_WIDTH)
        else:
            v = lax.all_gather(v, "fsdp", axis=1, tiled=True)
        return [v[i].astype(f32) for i in range(len(shards))]


def per_device(
    fsdp,
    x_in,
    doc_ids,
    w_qkv,
    w_out,
    gain_attn,
    gain_group,
    conv_kernel,
    head_mix,
    gain_ffn,
    w_gate,
    w_up,
    w_down,
    cotangent,
):
    links = Links(fsdp)
    weights = Weights(links)
    tokens = x_in.shape[1]

    x_all = jnp.concatenate(links.gather_plane(x_in[0]))
    qkv_w = weights.qkv(w_qkv)
    gain_a, gain_g, gain_f = weights.gains(gain_attn, gain_group, gain_ffn)
    docs = doc_ids
    for flip in ("y", "x"):
        docs = jnp.concatenate([docs, links.across(flip, docs)])
    docs = jnp.stack([docs, links.across("c", docs)], 1)
    docs = docs[jnp.array([0, 2, 1, 3])].reshape(8, tokens)
    out_w = weights.out(w_out)
    in_w = weights.ffn_in(w_gate, w_up)
    down_w = weights.ffn_out(w_down)
    upstream_chips = links.gather_plane(cotangent[0])

    kernel = lax.dynamic_slice_in_dim(conv_kernel, 2 * weights.pair, 2, 0)
    mix = lax.dynamic_slice_in_dim(head_mix, 2 * weights.pair, 2, 0)
    th, tl, tt = bands(kernel, tokens)
    group = lax.dynamic_slice_in_dim(gain_g.reshape(8, 2, E), weights.pair, 1, 0)
    group = jnp.pad(group, ((0, 0), (0, 0), (0, EP - E))).reshape(1, 2 * EP)
    doc_col, doc_row = docs[:, :, None], docs[:, None, :]

    xf_all = x_all.astype(f32)
    a1 = (xf_all * rms_scale(xf_all) * gain_a).astype(bf16)
    qkv = dot(a1, qkv_w).astype(bf16).reshape(8, tokens, 6 * EP)
    normed, xhat, s, probs, zeroed = attend(mix, qkv, doc_col, doc_row, th, tl, group)
    normed = normed.reshape(4, 2 * tokens, 2 * EP)
    xf = x_in[0].astype(f32)
    resid = xf + links.scatter_plane([dot(normed[i], out_w) for i in range(4)])

    r2 = rms_scale(resid)
    a2_chips = links.gather_plane((resid * r2 * gain_f).astype(bf16))
    out_parts, back_parts, hiddens, dgus = [], [], [], []
    half = FF // 8
    for a2, dffn in zip(a2_chips, upstream_chips):
        gu = dot(a2, in_w)
        gate, up_act = gu[:, :half], gu[:, half:]
        sig = jax.nn.sigmoid(gate)
        silu = gate * sig
        hidden = (silu * up_act).astype(bf16)
        dhidden = dot(dffn, down_w, 1, 1)
        dgate = (dhidden * up_act * sig * (1.0 + gate * (1.0 - sig))).astype(bf16)
        dup = (dhidden * silu).astype(bf16)
        dgu = jnp.concatenate([dgate, dup], 1)
        hiddens.append(hidden)
        dgus.append(dgu)
        back_parts.append(dot(dgu, in_w, 1, 1))
        out_parts.append(dot(hidden, down_w))
    da2 = links.scatter_plane(back_parts)
    output = (resid + links.scatter_plane(out_parts)).astype(bf16)

    dy = cotangent[0].astype(f32)
    sum_gain_ffn = jnp.sum(da2 * resid * r2, axis=0)
    dn2 = da2 * gain_f
    dresid = dy + r2 * (dn2 - resid * r2 * r2 * jnp.mean(dn2 * resid, axis=1, keepdims=True))
    dattn = jnp.concatenate(links.gather_plane(dresid.astype(bf16)))

    a2_all, dgu_all = jnp.concatenate(a2_chips), jnp.concatenate(dgus)
    hidden_all, dffn_all = jnp.concatenate(hiddens), jnp.concatenate(upstream_chips)
    grad_gate, grad_up = weights.ffn_in_back(dot(a2_all, dgu_all, 0, 0))
    grad_down = weights.ffn_out_back(dot(hidden_all, dffn_all, 0, 0))

    dnormed = dot(dattn, out_w, 1, 1).reshape(8, tokens, 2 * EP)
    dqkv, conv_tiles, mix_sums, group_sums = attend_back(
        mix, qkv, doc_col, doc_row, tt, group, dnormed, xhat, s, probs, zeroed
    )
    dqkv = dqkv.reshape(4, 2 * tokens, 6 * EP)
    da1 = links.scatter_plane([dot(dqkv[i], qkv_w, 1, 1) for i in range(4)])
    grad_out = weights.out_back(dot(normed.reshape(8 * tokens, 2 * EP), dattn, 0, 0))
    grad_qkv = weights.qkv_back(dot(a1, dqkv.reshape(8 * tokens, 6 * EP), 0, 0))

    r1 = rms_scale(xf)
    sum_gain_attn = jnp.sum(da1 * xf * r1, axis=0)
    dn1 = da1 * gain_a
    grad_x = dresid + r1 * (dn1 - xf * r1 * r1 * jnp.mean(dn1 * xf, axis=1, keepdims=True))

    place = lambda v: lax.dynamic_update_index_in_dim(jnp.zeros((8,) + v.shape, f32), v, weights.pair, 0)
    small = [
        sum_gain_attn,
        sum_gain_ffn,
        place(group_sums[0].reshape(2, EP)[:, :E].reshape(-1)),
        place(diagonals(conv_tiles)),
        place(jnp.sum(mix_sums[:4], axis=1)),
    ]
    sizes = [v.size for v in small]
    total = lax.psum(jnp.concatenate([v.reshape(-1) for v in small]), ("rep", "fsdp"))
    cut = [0]
    for size in sizes:
        cut.append(cut[-1] + size)
    gain_a_sum, gain_f_sum, group_sum, conv_sum, mix_sum = (total[cut[i] : cut[i + 1]] for i in range(5))
    rows = gain_attn.shape[0]
    own = lambda v: lax.dynamic_slice_in_dim(v, lax.axis_index("fsdp") * rows, rows, 0)
    return (
        output[None],
        grad_x[None],
        grad_qkv,
        grad_out,
        own(gain_a_sum),
        own(group_sum),
        conv_sum.reshape(H, QWIN, KWIN),
        mix_sum.reshape(H, 2),
        own(gain_f_sum),
        grad_gate,
        grad_up,
        grad_down,
    )


def join(bit, mine, other, axis):
    first, second = jnp.where(bit == 0, mine, other), jnp.where(bit == 0, other, mine)
    return jnp.stack([first, second], axis)


def fast(
    x_in,
    doc_ids,
    w_qkv,
    w_out,
    gain_attn,
    gain_group,
    conv_kernel,
    head_mix,
    gain_ffn,
    w_gate,
    w_up,
    w_down,
    cotangent,
):
    links = Links(16)
    pair = 4 * links.x + 2 * links.c + links.y
    tokens = x_in.shape[1]
    x, dy = x_in[0], cotangent[0]
    rows = w_qkv.shape[0]

    kernel = lax.dynamic_slice_in_dim(conv_kernel, 2 * pair, 2, 0)
    mix = lax.dynamic_slice_in_dim(head_mix, 2 * pair, 2, 0)
    gains = jnp.pad(jnp.stack([gain_attn, gain_group, gain_ffn]), ((0, 13), (0, 128 - rows)))
    docs = jnp.broadcast_to(doc_ids, (8, tokens))
    a1, dffn_all, docs, gains, qkv_w, gu_plane, out_w, th, tl, tt = start_call(
        x, dy, docs, gains, kernel.reshape(-1), w_qkv, w_gate, w_up, w_out, 1
    )
    docs = docs.reshape(8, 8, tokens)[:, 0]
    gain_a, gain_g, gain_f = gains[0:1], gains[1], gains[2:3]
    qkv_w = qkv_w.reshape(MODEL_WIDTH, 6 * EP)
    keep = lax.dynamic_index_in_dim(out_w, 2 * links.x + links.c, 0, keepdims=False)
    other = links.across("c", lax.dynamic_index_in_dim(out_w, 2 * links.x + 1 - links.c, 0, keepdims=False))
    out_w = jnp.pad(join(links.c, keep, other, 0), ((0, 0), (0, EP - E), (0, 0))).reshape(2 * EP, MODEL_WIDTH)

    group = lax.dynamic_slice_in_dim(gain_g.reshape(8, 2, E), pair, 1, 0)
    group = jnp.pad(group, ((0, 0), (0, 0), (0, EP - E))).reshape(1, 2 * EP)
    doc_col, doc_row = docs[:, :, None], docs[:, None, :]

    dffn_all = dffn_all.reshape(8 * tokens, MODEL_WIDTH)
    a1 = a1.reshape(8 * tokens, MODEL_WIDTH)
    qkv = dot(a1, qkv_w).astype(bf16).reshape(8, tokens, 6 * EP)
    normed, xhat, s, probs, zeroed = attend(mix, qkv, doc_col, doc_row, th, tl, group)
    normed = normed.reshape(8 * tokens, 2 * EP)
    by_chip = lambda v: v.astype(bf16).reshape(4, 2, tokens, MODEL_WIDTH)
    resid, a2, gu_w, down_w = mid_call(by_chip(dot(normed, out_w)), x, gain_f, gu_plane, w_down, 2)

    a2 = a2.reshape(8 * tokens, MODEL_WIDTH)
    gu_w = gu_w.reshape(MODEL_WIDTH, FF // 4)
    down_w = down_w.reshape(FF // 8, MODEL_WIDTH)
    half = FF // 8
    gu = dot(a2, gu_w)
    gate, up_act = gu[:, :half], gu[:, half:]
    sig = jax.nn.sigmoid(gate)
    silu = gate * sig
    hidden = (silu * up_act).astype(bf16)
    dhidden = dot(dffn_all, down_w, 1, 1)
    dgate = (dhidden * up_act * sig * (1.0 + gate * (1.0 - sig))).astype(bf16)
    dup = (dhidden * silu).astype(bf16)
    dgu = jnp.concatenate([dgate, dup], 1)
    grad_gu = dot(a2, dgu, 0, 0).astype(bf16).reshape(4, 4 * rows, FF // 4)
    grad_down = dot(hidden, dffn_all, 0, 0).astype(bf16).reshape(4, FF // 32, MODEL_WIDTH)
    out_parts = by_chip(dot(hidden, down_w))
    dresid, dattn, sum_f, grad_down = mid_back_call(by_chip(dot(dgu, gu_w, 1, 1)), dy, resid, gain_f, grad_down, 3)
    by_row = lambda v: v.reshape(8, tokens, -1)
    da_parts, grad_qkv, grad_out, conv_tiles, mix_sums, group_sums, out, grad_gu = back_call(
        mix, qkv, doc_col, doc_row, tt, group, by_row(dattn), xhat, s, probs, zeroed, by_row(normed), by_row(a1), out_w, qkv_w,
        out_parts, grad_gu, resid, 5
    )
    sum_a = jnp.sum(grad_qkv * qkv_w.astype(f32), axis=1) / gain_a[0]
    grad_out = grad_out.astype(bf16).reshape(2, EP, MODEL_WIDTH)[:, :rows]
    place = lambda v: lax.dynamic_update_index_in_dim(jnp.zeros((8,) + v.shape, f32), v, pair, 0)
    small = [
        sum_a,
        sum_f[0],
        place(group_sums[0].reshape(2, EP)[:, :E].reshape(-1)),
        place(diagonals(conv_tiles)),
        place(jnp.sum(mix_sums[:4], axis=1)),
    ]
    cut = [0]
    for v in small:
        cut.append(cut[-1] + v.size)
    room = 48 * 128
    flat = jnp.concatenate([v.reshape(-1) for v in small] + [jnp.zeros((room - cut[-1],), f32)]).reshape(48, 128)
    grad_x, grad_qkv, grad_out, grad_gate, grad_up, grad_down, total = end_call(
        by_chip(da_parts),
        grad_qkv.astype(bf16).reshape(4, 4 * rows, 6 * EP),
        grad_out,
        grad_gu,
        grad_down,
        flat,
        x,
        dresid,
        gain_a,
        4,
    )
    total = total.reshape(-1)
    gain_a_sum, gain_f_sum, group_sum, conv_sum, mix_sum = (total[cut[i] : cut[i + 1]] for i in range(5))
    own = lambda v: lax.dynamic_slice_in_dim(v, lax.axis_index("fsdp") * rows, rows, 0)
    return (
        out[None],
        grad_x[None],
        grad_qkv,
        grad_out,
        own(gain_a_sum),
        own(group_sum),
        conv_sum.reshape(H, QWIN, KWIN),
        mix_sum.reshape(H, 2),
        own(gain_f_sum),
        grad_gate,
        grad_up,
        grad_down,
    )


def solution(mesh):
    fsdp = mesh.shape["fsdp"]
    assert mesh.shape["rep"] == 2 and fsdp % 4 == 0
    rows, shard, part = P(("rep", "fsdp"), None, None), P("fsdp", None), P("fsdp")
    placed = (rows, P(("rep", "fsdp"), None), shard, shard, part, part, P(), P(), part, shard, shard, shard, rows)
    return jax.shard_map(
        fast if fsdp == 16 else (lambda *args: per_device(fsdp, *args)),
        mesh=mesh,
        in_specs=placed,
        out_specs=(rows, rows, shard, shard, part, part, P(), P(), part, shard, shard, shard),
        check_vma=False,
    )
```

```python
import math

import jax
import jax.numpy as jnp
from jax import lax
from jax.experimental import pallas as pl
from jax.experimental.pallas import tpu as pltpu
from jax.sharding import PartitionSpec as P

MODEL_WIDTH = 1536
H = 16
E = 96
EP = 128
QWIN = 6
KWIN = 11
bf16, f32 = jnp.bfloat16, jnp.float32


def allowed_mask(doc_col, doc_row):
    n = doc_row.shape[-1]
    i = lax.broadcasted_iota(jnp.int32, (n, n), 0)
    j = lax.broadcasted_iota(jnp.int32, (n, n), 1)
    return (j <= i) & (doc_col == doc_row)


def down(v, a):
    if a == 0:
        return v
    i = lax.broadcasted_iota(jnp.int32, v.shape, 0)
    return jnp.where(i >= a, pltpu.roll(v, a, 0), 0.0)


def up(v, a):
    if a == 0:
        return v
    n = v.shape[0]
    i = lax.broadcasted_iota(jnp.int32, v.shape, 0)
    return jnp.where(i < n - a, pltpu.roll(v, n - a, 0), 0.0)


def dot(a, b, ca=1, cb=0):
    return lax.dot_general(a, b, (((ca,), (cb,)), ((), ())), preferred_element_type=f32)


def split(v):
    hi = v.astype(bf16)
    return hi, (v - hi.astype(f32)).astype(bf16)


def attend_row(mix_ref, qkv_ref, dcol_ref, drow_ref, th_ref, tl_ref, gain_ref,
               normed_ref, xhat_ref, s_ref, p_ref, z_ref):
    allowed = allowed_mask(dcol_ref[0], drow_ref[0])
    scale = 1.0 / math.sqrt(E)
    probs = []
    for h in range(2):
        q = qkv_ref[0, :, h * EP:(h + 1) * EP]
        k = qkv_ref[0, :, (2 + h) * EP:(3 + h) * EP]
        zeroed = jnp.where(allowed, dot(q, k, 1, 1) * scale, 0.0)
        z_ref[0, h] = zeroed.astype(bf16)
        his, los = [], []
        for a in range(QWIN):
            hi, lo = split(down(zeroed, a))
            his.append(hi)
            los.append(lo)
        his, los = jnp.concatenate(his, 1), jnp.concatenate(los, 1)
        th, tl = th_ref[h], tl_ref[h]
        conv = dot(his, th) + (dot(his, tl) + dot(los, th))
        masked = jnp.where(allowed, conv, -jnp.inf)
        e = jnp.exp(masked - jnp.max(masked, axis=1, keepdims=True))
        p = e / jnp.sum(e, axis=1, keepdims=True)
        p_ref[0, h] = p
        probs.append(p)
    lane = lax.broadcasted_iota(jnp.int32, (1, EP), 1)
    for h in range(2):
        v = qkv_ref[0, :, (4 + h) * EP:(5 + h) * EP]
        mixed = (mix_ref[h, 0] * probs[0] + mix_ref[h, 1] * probs[1]).astype(bf16)
        ho = dot(mixed, v)
        centered = jnp.where(lane < E, ho - jnp.sum(ho, axis=1, keepdims=True) / E, 0.0)
        s = lax.rsqrt(jnp.sum(centered * centered, axis=1, keepdims=True) / E + 1e-05)
        xhat = centered * s
        cols = slice(h * EP, (h + 1) * EP)
        xhat_ref[0, :, cols] = xhat
        s_ref[0, :, cols] = jnp.broadcast_to(s, xhat.shape)
        normed_ref[0, :, cols] = (xhat * gain_ref[0:1, cols]).astype(bf16)


def attend(mix, qkv, dcol, drow, th, tl, gain):
    n, t, _ = qkv.shape
    row = lambda *s: pl.BlockSpec((1,) + s, lambda i: (i,) + (0,) * len(s))
    full = lambda a: pl.BlockSpec(a.shape, lambda i: (0,) * a.ndim)
    return pl.pallas_call(
        attend_row,
        grid=(n,),
        in_specs=[pl.BlockSpec(memory_space=pltpu.SMEM), row(t, 6 * EP), row(t, 1), row(1, t), full(th), full(tl), full(gain)],
        out_specs=[row(t, 2 * EP), row(t, 2 * EP), row(t, 2 * EP), row(2, t, t), row(2, t, t)],
        out_shape=[
            jax.ShapeDtypeStruct((n, t, 2 * EP), bf16),
            jax.ShapeDtypeStruct((n, t, 2 * EP), f32),
            jax.ShapeDtypeStruct((n, t, 2 * EP), f32),
            jax.ShapeDtypeStruct((n, 2, t, t), f32),
            jax.ShapeDtypeStruct((n, 2, t, t), bf16),
        ],
        cost_estimate=pl.CostEstimate(flops=n * 2 * 3 * 2 * t * t * QWIN * t, bytes_accessed=n * t * t * 20, transcendentals=n * 2 * t * t),
        name="attend",
    )(mix, qkv, dcol, drow, th, tl, gain)


def bwd_kernel(mix_ref, qkv_ref, dcol_ref, drow_ref, tt_ref, gain_ref, dn_ref, xhat_ref, s_ref, p_ref, z_ref,
               dqkv_ref, gconv_ref, gmix_ref, gg_ref, m_ref):
    step, steps = pl.program_id(0), pl.num_programs(0)
    t = p_ref.shape[-1]

    @pl.when(step == 0)
    def _():
        m_ref[...] = jnp.zeros_like(m_ref)
        gmix_ref[...] = jnp.zeros_like(gmix_ref)
        gg_ref[...] = jnp.zeros_like(gg_ref)

    allowed = allowed_mask(dcol_ref[0], drow_ref[0])
    scale = 1.0 / math.sqrt(E)
    lane = lax.broadcasted_iota(jnp.int32, (1, EP), 1)
    p = [p_ref[0, 0], p_ref[0, 1]]
    dmixed = []
    for h in range(2):
        cols = slice(h * EP, (h + 1) * EP)
        dn, xhat = dn_ref[0, :, cols], xhat_ref[0, :, cols]
        gg_ref[0:1, cols] += jnp.sum(dn * xhat, axis=0, keepdims=True)
        dc = dn * gain_ref[0:1, cols]
        m1 = jnp.sum(dc, axis=1, keepdims=True) / E
        m2 = jnp.sum(dc * xhat, axis=1, keepdims=True) / E
        dh = jnp.where(lane < E, s_ref[0, :, cols] * (dc - m1 - xhat * m2), 0.0).astype(bf16)
        v = qkv_ref[0, :, (4 + h) * EP:(5 + h) * EP]
        mixed = (mix_ref[h, 0] * p[0] + mix_ref[h, 1] * p[1]).astype(bf16)
        dmixed.append(dot(dh, v, 1, 1))
        dqkv_ref[0, :, (4 + h) * EP:(5 + h) * EP] = dot(mixed, dh, 0, 0).astype(bf16)
    for h in range(2):
        for c in range(2):
            r = 2 * h + c
            gmix_ref[r:r + 1, :] += jnp.sum(dmixed[h] * p[c], axis=0, keepdims=True)
    for c in range(2):
        dp = mix_ref[0, c] * dmixed[0] + mix_ref[1, c] * dmixed[1]
        dconv = p[c] * (dp - jnp.sum(dp * p[c], axis=1, keepdims=True))
        ahead = jnp.concatenate([up(dconv, a).astype(bf16) for a in range(QWIN)], 1)
        m_ref[c] += dot(z_ref[0, c], ahead, 0, 0)
        ds = jnp.where(allowed, dot(ahead, tt_ref[c]), 0.0).astype(bf16)
        q = qkv_ref[0, :, c * EP:(c + 1) * EP]
        k = qkv_ref[0, :, (2 + c) * EP:(3 + c) * EP]
        dqkv_ref[0, :, c * EP:(c + 1) * EP] = (dot(ds, k) * scale).astype(bf16)
        dqkv_ref[0, :, (2 + c) * EP:(3 + c) * EP] = (dot(ds, q, 0, 0) * scale).astype(bf16)

    @pl.when(step == steps - 1)
    def _():
        lanes = lax.broadcasted_iota(jnp.int32, (8, t), 1)
        for h in range(2):
            for a in range(QWIN):
                total = jnp.zeros((8, t), f32)
                for first in range(0, t, 8):
                    rows = m_ref[h, first:first + 8, a * t:(a + 1) * t]
                    turned = pltpu.roll(rows, t - first, 1) if first else rows
                    total = total + jnp.where(lanes < t - first, turned, 0.0)
                gconv_ref[h, a] = total[:, :EP]


def attend_back(mix, qkv, dcol, drow, tt, gain, dn, xhat, s, p, z):
    n, t, _ = qkv.shape
    row = lambda *sh: pl.BlockSpec((1,) + sh, lambda i: (i,) + (0,) * len(sh))
    full = lambda a: pl.BlockSpec(a.shape, lambda i: (0,) * a.ndim)
    keep = lambda *sh: pl.BlockSpec(sh, lambda i: (0,) * len(sh))
    return pl.pallas_call(
        bwd_kernel,
        grid=(n,),
        in_specs=[pl.BlockSpec(memory_space=pltpu.SMEM), row(t, 6 * EP), row(t, 1), row(1, t), full(tt), full(gain),
                  row(t, 2 * EP), row(t, 2 * EP), row(t, 2 * EP), row(2, t, t), row(2, t, t)],
        out_specs=[row(t, 6 * EP), keep(2, QWIN, 8, EP), keep(8, t), keep(8, 2 * EP)],
        out_shape=[
            jax.ShapeDtypeStruct((n, t, 6 * EP), bf16),
            jax.ShapeDtypeStruct((2, QWIN, 8, EP), f32),
            jax.ShapeDtypeStruct((8, t), f32),
            jax.ShapeDtypeStruct((8, 2 * EP), f32),
        ],
        scratch_shapes=[pltpu.VMEM((2, t, QWIN * t), f32)],
        cost_estimate=pl.CostEstimate(flops=n * 2 * 2 * 2 * t * t * QWIN * t, bytes_accessed=n * t * t * 20, transcendentals=0),
        name="attend_back",
    )(mix, qkv, dcol, drow, tt, gain, dn, xhat, s, p, z)


def bands(kernel, t):
    diff = jnp.arange(t)[None, :] - jnp.arange(t)[:, None]
    band = jnp.zeros((2, QWIN, t, t), f32)
    back = jnp.zeros((2, QWIN, t, t), f32)
    for b in range(KWIN):
        tap = kernel[:, :, b][:, :, None, None]
        band = band + jnp.where(diff == b, tap, 0.0)
        back = back + jnp.where(diff == -b, tap, 0.0)
    th, tl = split(band)
    flat = lambda v: v.reshape(2, QWIN * t, t)
    return flat(th), flat(tl), flat(back.astype(bf16))


def diagonals(tiles):
    return sum(tiles[:, :, i, i:i + KWIN] for i in range(8))


FF = 4096
MESH = pl.DeviceIdType.MESH


class Net:
    def __init__(self):
        self.x, self.f = lax.axis_index("rep"), lax.axis_index("fsdp")
        self.z, self.y, self.c = self.f // 4, (self.f // 2) % 2, self.f % 2
        self.k = self.f % 4
        nx, fy, fc = 1 - self.x, 2 - 4 * self.y, 1 - 2 * self.c
        self.to = {
            "x": (nx, self.f),
            "y": (self.x, self.f + fy),
            "c": (self.x, self.f + fc),
            "xy": (nx, self.f + fy),
            "xc": (nx, self.f + fc),
            "yc": (self.x, self.f + fy + fc),
            "xyc": (nx, self.f + fy + fc),
            "up": (self.x, self.f + 4),
            "down": (self.x, self.f - 4),
        }

    def greet(self, names, line=True):
        barrier = pltpu.get_barrier_semaphore()
        for name in names:
            pl.semaphore_signal(barrier, inc=1, device_id=self.to[name], device_id_type=MESH)
        count = len(names)
        if line:

            @pl.when(self.z < 3)
            def _():
                pl.semaphore_signal(barrier, inc=1, device_id=self.to["up"], device_id_type=MESH)

            @pl.when(self.z > 0)
            def _():
                pl.semaphore_signal(barrier, inc=1, device_id=self.to["down"], device_id_type=MESH)

            count = count + (self.z + 3) // 4 + (6 - self.z) // 4
        pl.semaphore_wait(barrier, count)

    def copy(self, src, dst, sems, i, name):
        return pltpu.make_async_remote_copy(
            src_ref=src, dst_ref=dst, send_sem=sems[0].at[i], recv_sem=sems[1].at[i],
            device_id=self.to[name], device_id_type=MESH,
        )

    def send(self, src, dst, sems, i, name):
        copy = self.copy(src, dst, sems, i, name)
        copy.start()
        return copy


def tiles(start, size, body, step=32):
    def one(i, _):
        body(pl.ds(pl.multiple_of(start + i * step, step), step))
        return 0

    lax.fori_loop(0, size // step, one, 0)


def wide(v):
    return v.astype(f32)


class GatherLine:
    def __init__(self, net, src, out, sems, base, keep=None):
        self.net, self.src, self.out, self.sems, self.base = net, src, out, sems, base
        self.keep = keep or (lambda slot: net.z >= 0)

    def go(self, d, way, act):
        net = self.net
        slot = net.z - d if way == "up" else net.z + d
        inside = (net.z >= d) & (net.z < 3) if way == "up" else (net.z < 4 - d) & (net.z > 0)
        i = self.base + d + (0 if way == "up" else 3)

        @pl.when(inside & self.keep(slot))
        def _():
            src = self.src if d == 0 else self.out.at[slot]
            act(net.copy(src, self.out.at[slot], self.sems, i, way))

    def came(self, d, way):
        net = self.net
        slot = net.z - d if way == "up" else net.z + d
        inside = net.z >= d if way == "up" else net.z < 4 - d
        i = self.base + d - 1 + (0 if way == "up" else 3)

        @pl.when(inside & self.keep(slot))
        def _():
            net.copy(self.out.at[slot], self.out.at[slot], self.sems, i, way).wait_recv()

    def step(self, d):
        for way in ("up", "down"):
            if d > 0:
                self.came(d, way)
            if d < 3:
                self.go(d, way, lambda copy: copy.start())

    def finish(self):
        for d in range(3):
            for way in ("up", "down"):
                self.go(d, way, lambda copy: copy.wait_send())


class ScatterLine:
    def __init__(self, net, parts, got, made, sems, base):
        self.net, self.parts, self.got, self.made, self.sems, self.base = net, parts, got, made, sems, base
        self.n = parts.shape[1]

    def each(self, d, way):
        net = self.net
        t = net.z + (3 - d) if way == 0 else net.z - (3 - d)
        inside = (t < 4) if way == 0 else (t >= 0)
        first = (net.z == 0) if way == 0 else (net.z == 3)
        return t, inside, first, self.base + d + 3 * way, ("up", "down")[way]

    def step(self, d):
        for way in range(2):
            t, inside, first, i, name = self.each(d, way)

            @pl.when(inside & first)
            def _():
                self.net.copy(self.parts.at[t], self.got.at[way, d], self.sems, i, name).start()

            if d == 0:
                continue

            @pl.when(inside & jnp.logical_not(first))
            def _():
                self.net.copy(self.got.at[way, d - 1], self.got.at[way, d - 1], self.sems, i - 1, name).wait_recv()

                def body(rows):
                    self.made[way, d - 1, rows] = (wide(self.parts[t, rows]) + wide(self.got[way, d - 1, rows])).astype(bf16)

                tiles(0, self.n, body)
                self.net.copy(self.made.at[way, d - 1], self.got.at[way, d], self.sems, i, name).start()

    def finish(self, store):
        net = self.net
        below, above = net.z > 0, net.z < 3

        @pl.when(below)
        def _():
            net.copy(self.got.at[0, 2], self.got.at[0, 2], self.sems, self.base + 2, "up").wait_recv()

        @pl.when(above)
        def _():
            net.copy(self.got.at[1, 2], self.got.at[1, 2], self.sems, self.base + 5, "down").wait_recv()

        def put(low, high):
            def body(rows):
                total = wide(self.parts[net.z, rows])
                if low:
                    total = total + wide(self.got[0, 2, rows])
                if high:
                    total = total + wide(self.got[1, 2, rows])
                store(rows, total)

            tiles(0, self.n, body)

        @pl.when(below & above)
        def _():
            put(True, True)

        @pl.when(jnp.logical_not(below))
        def _():
            put(False, True)

        @pl.when(jnp.logical_not(above))
        def _():
            put(True, False)

        for d in range(3):
            for way in range(2):
                t, inside, first, i, name = self.each(d, way)

                @pl.when(inside & first)
                def _():
                    net.copy(self.parts.at[t], self.got.at[way, d], self.sems, i, name).wait_send()

                if d > 0:

                    @pl.when(inside & jnp.logical_not(first))
                    def _():
                        net.copy(self.made.at[way, d - 1], self.got.at[way, d], self.sems, i, name).wait_send()


def line_scratch(n, w):
    return [pltpu.VMEM((2, 3, n, w), bf16), pltpu.VMEM((2, 2, n, w), bf16)]


LINE_COPIES = 6


class Later:
    def __init__(self, make):
        self.make = make
        make().start()

    def wait_recv(self):
        self.make().wait_recv()

    def wait_send(self):
        self.make().wait_send()


def gather_steps(net, v, out, sems, base, ready):
    n = v.shape[0]
    A, B = pl.ds(0, n // 2), pl.ds(n // 2, n // 2)
    go = {}
    ready(0)
    go["xA"] = Later(lambda: net.copy(v.at[A], out.at[1, 0, A], sems, base + 0, "x"))
    go["yA"] = Later(lambda: net.copy(v.at[A], out.at[2, 0, A], sems, base + 3, "y"))
    go["0A"] = Later(lambda: net.copy(v.at[A], out.at[0, 1, A], sems, base + 4, "c"))
    ready(1)
    go["yB"] = Later(lambda: net.copy(v.at[B], out.at[2, 0, B], sems, base + 2, "y"))
    go["xB"] = Later(lambda: net.copy(v.at[B], out.at[1, 0, B], sems, base + 1, "x"))
    go["0B"] = Later(lambda: net.copy(v.at[B], out.at[0, 1, B], sems, base + 5, "c"))
    yield
    go["xA"].wait_recv()
    go["dA"] = Later(lambda: net.copy(out.at[1, 0, A], out.at[3, 0, A], sems, base + 6, "y"))
    go["1A"] = Later(lambda: net.copy(out.at[1, 0, A], out.at[1, 1, A], sems, base + 8, "c"))
    go["yA"].wait_recv()
    go["2A"] = Later(lambda: net.copy(out.at[2, 0, A], out.at[2, 1, A], sems, base + 10, "c"))
    yield
    go["yB"].wait_recv()
    go["dB"] = Later(lambda: net.copy(out.at[2, 0, B], out.at[3, 0, B], sems, base + 7, "x"))
    go["2B"] = Later(lambda: net.copy(out.at[2, 0, B], out.at[2, 1, B], sems, base + 9, "c"))
    go["xB"].wait_recv()
    go["1B"] = Later(lambda: net.copy(out.at[1, 0, B], out.at[1, 1, B], sems, base + 11, "c"))
    yield
    go["dA"].wait_recv()
    go["3A"] = Later(lambda: net.copy(out.at[3, 0, A], out.at[3, 1, A], sems, base + 12, "c"))
    go["dB"].wait_recv()
    go["3B"] = Later(lambda: net.copy(out.at[3, 0, B], out.at[3, 1, B], sems, base + 13, "c"))
    yield
    for name in ("0A", "0B", "1A", "2B", "2A", "1B", "3A", "3B"):
        go[name].wait_recv()
    for copy in go.values():
        copy.wait_send()


def gather_rows(net, v, out, sems, base, ready, poll):
    for _ in gather_steps(net, v, out, sems, base, ready):
        poll()


GATHER_COPIES = 14
SCATTER_COPIES = 10


def scatter_steps(net, parts, rc, rd, rx, ry, td, tx, ty, sems, base):
    n = parts.shape[2]
    A, B = pl.ds(0, n // 2), pl.ds(n // 2, n // 2)
    go = {}
    for i, chip in enumerate((3, 1, 2, 0)):
        go[chip] = Later(lambda i=i, chip=chip: net.copy(parts.at[chip, 1], rc.at[chip], sems, base + i, "c"))

    def add(dst, chip, start, more=None):
        def body(rows):
            total = wide(parts[chip, 0, rows]) + wide(rc[chip, rows])
            if more is not None:
                total = total + wide(more[rows])
            dst[rows] = total.astype(bf16)

        tiles(start, n // 2, body)

    yield None
    go[3].wait_recv()
    add(td, 3, 0)
    go["dA"] = Later(lambda: net.copy(td.at[A], rd.at[A], sems, base + 4, "x"))
    add(td, 3, n // 2)
    go["dB"] = Later(lambda: net.copy(td.at[B], rd.at[B], sems, base + 5, "y"))
    go[1].wait_recv()
    add(tx, 1, 0)
    go["xA"] = Later(lambda: net.copy(tx.at[A], rx.at[A], sems, base + 6, "x"))
    go[2].wait_recv()
    add(ty, 2, n // 2)
    go["yB"] = Later(lambda: net.copy(ty.at[B], ry.at[B], sems, base + 7, "y"))
    yield None
    go["dA"].wait_recv()
    add(ty, 2, 0, rd)
    go["yA"] = Later(lambda: net.copy(ty.at[A], ry.at[A], sems, base + 8, "y"))
    go["dB"].wait_recv()
    add(tx, 1, n // 2, rd)
    go["xB"] = Later(lambda: net.copy(tx.at[B], rx.at[B], sems, base + 9, "x"))
    go[0].wait_recv()

    def done(half):
        for name in (("xA", "yA"), ("xB", "yB"))[half]:
            go[name].wait_recv()
        if half == 1:
            for copy in go.values():
                copy.wait_send()

    yield done


def scatter_rows(net, parts, rc, rd, rx, ry, td, tx, ty, sems, base, poll):
    steps = scatter_steps(net, parts, rc, rd, rx, ry, td, tx, ty, sems, base)
    next(steps)
    next(steps)
    poll()
    return next(steps)


def scatter_scratch(n, w):
    return [pltpu.VMEM((4, n, w), bf16)] + [pltpu.VMEM((n, w), bf16)] * 6


def dma_sems(count):
    return [pltpu.SemaphoreType.DMA((count,)), pltpu.SemaphoreType.DMA((count,))]


VM = pl.BlockSpec(memory_space=pltpu.VMEM)
ANY = pl.BlockSpec(memory_space=pl.ANY)


def polls(*acts):
    left = list(acts)

    def poll():
        if left:
            left.pop(0)()

    def drain():
        while left:
            poll()

    return poll, drain


def comm_call(body, name, ident, ins, in_specs, outs, out_specs, scratch):
    return pl.pallas_call(
        body,
        in_specs=in_specs,
        out_specs=out_specs,
        out_shape=outs,
        scratch_shapes=scratch,
        compiler_params=pltpu.CompilerParams(collective_id=ident, has_side_effects=True, vmem_limit_bytes=60 << 20),
        name=name,
    )(*ins)


def shape(dims, dtype):
    return jax.ShapeDtypeStruct(dims, dtype)


PLANE = ("x", "y", "c", "xy", "xc", "yc", "xyc")
PLACES = {"c": (0, 1), "x": (1, 0), "xc": (1, 1), "y": (2, 0), "yc": (2, 1), "xy": (3, 0), "xyc": (3, 1)}


def start_call(x, dy, docs, gains, taps, w_qkv, w_gate, w_up, w_out, ident):
    n, w = x.shape
    rows = w_qkv.shape[0]

    def body(x_ref, dy_ref, docs_ref, g_ref, taps_ref, wq_ref, gate_ref, up_ref, wo_ref,
             a1_ref, dys_ref, docs_out, gains_ref, qkv_out, gu_out, wo_out, th_ref, tl_ref, tt_ref,
             xs, gains_out, slots, gus, local, send, recv):
        net = Net()
        sems = (send, recv)
        base = 2 * GATHER_COPIES
        line_q = GatherLine(net, qkv_out.at[net.z], qkv_out, sems, base)
        line_o = GatherLine(net, wo_ref, wo_out, sems, base + 6, lambda slot: slot // 2 == net.x)
        line_g = GatherLine(net, gains_out.at[net.z], gains_out, sems, base + 12)
        base += 18
        gains_out[net.z, net.k] = g_ref[...]
        slots[...] = jnp.zeros_like(slots)
        for half in range(2):

            @pl.when(net.x == half)
            def _():
                for k in range(4):
                    pair = 4 * half + 2 * (k % 2) + k // 2
                    for m in range(6):
                        col = (m // 2) * MODEL_WIDTH + (2 * pair + m % 2) * E
                        slots[k, :, m * EP : m * EP + E] = wq_ref[:, col : col + E]
                    for m in range(8):
                        src = gate_ref if m < 4 else up_ref
                        col = 256 * (4 * (m % 4) + k) + 128 * half
                        gus[k, :, m * 128 : (m + 1) * 128] = src[:, col : col + 128]

        net.greet(PLANE)
        own = [
            pltpu.make_async_copy(slots.at[net.k], qkv_out.at[net.z, net.k], local.at[0]),
            pltpu.make_async_copy(dy_ref, dys_ref.at[0, 0], local.at[1]),
            pltpu.make_async_copy(gus.at[net.k], gu_out.at[net.k], local.at[2]),
            pltpu.make_async_copy(docs_ref, docs_out.at[0, 0], local.at[3]),
            pltpu.make_async_copy(wo_ref, wo_out.at[net.z], local.at[4]),
        ]
        for copy in own:
            copy.start()
        qkv_parts, gain_parts, small = [], [], []
        flips = {"c": net.k + 1 - 2 * net.c, "y": net.k + 2 - 4 * net.y, "yc": net.k + 1 - 2 * net.c + 2 - 4 * net.y}
        for j, name in enumerate(("y", "yc", "c")):
            gain_parts.append(net.send(g_ref, gains_out.at[net.z, net.k], sems, base + 6 + j, name))
            qkv_parts.append(net.send(slots.at[flips[name]], qkv_out.at[net.z, net.k], sems, base + j, name))
        line_o.step(0)
        for j, (name, (chip, core)) in enumerate(PLACES.items()):
            small.append(net.send(docs_ref, docs_out.at[chip, core], sems, base + 9 + j, name))
        gather_x = gather_steps(net, x_ref, xs, sems, 0, lambda half: None)
        next(gather_x)
        gather_dy = gather_steps(net, dy_ref, dys_ref, sems, GATHER_COPIES, lambda half: None)
        next(gather_dy)
        for copy in gain_parts:
            copy.wait_recv()
        line_g.step(0)
        own[0].wait()
        for copy in qkv_parts:
            copy.wait_recv()
        line_q.step(0)
        line_g.step(1)

        diff = lax.broadcasted_iota(jnp.int32, (n, n), 1) - lax.broadcasted_iota(jnp.int32, (n, n), 0)

        def bands_of(first, count):
            def one(i, _):
                band = jnp.zeros((n, n), f32)
                back = jnp.zeros((n, n), f32)
                for b in range(KWIN):
                    tap = taps_ref[(first + i) * KWIN + b]
                    band = jnp.where(diff == b, tap, band)
                    back = jnp.where(diff == -b, tap, back)
                h, a = (first + i) // QWIN, (first + i) % QWIN
                at = pl.ds(pl.multiple_of(a * n, n), n)
                th_ref[h, at], tl_ref[h, at] = split(band)
                tt_ref[h, at] = back.astype(bf16)
                return 0

            lax.fori_loop(0, count, one, 0)

        bands_of(0, QWIN)
        line_g.step(2)
        next(gather_x)
        line_q.step(1)
        line_g.step(3)
        line_o.step(1)
        for i in range(16):
            gains_ref[:, i * rows : (i + 1) * rows] = wide(gains_out[i // 4, i % 4, 0:8, 0:rows])
        bands_of(QWIN, QWIN)
        next(gather_x)
        next(gather_dy)
        for j, name in enumerate(("y", "yc", "c")):
            small.append(net.send(gus.at[flips[name]], gu_out.at[net.k], sems, base + 3 + j, name))
        next(gather_dy)
        gain = gains_ref[0:1]

        def norm(chip, core, src):
            def body(at):
                xf = wide(src[at])
                r = lax.rsqrt(jnp.mean(xf * xf, axis=1, keepdims=True) + 1e-06)
                a1_ref[chip, core, at] = (xf * r * gain).astype(bf16)

            tiles(0, n, body)

        norm(0, 0, x_ref)
        line_q.step(2)
        line_o.step(2)
        for _ in gather_x:
            pass
        next(gather_dy)
        for chip in range(4):
            for core in range(2):
                if (chip, core) != (0, 0):
                    norm(chip, core, xs.at[chip, core])
        line_q.step(3)
        line_o.step(3)
        for _ in gather_dy:
            pass
        for line in (line_q, line_g, line_o):
            line.finish()
        for copy in own[1:]:
            copy.wait()
        for copy in small:
            copy.wait_recv()
        for copy in qkv_parts + gain_parts + small:
            copy.wait_send()

    return comm_call(
        body, "start", ident, (x, dy, docs, gains, taps, w_qkv, w_gate, w_up, w_out),
        [VM] * 4 + [pl.BlockSpec(memory_space=pltpu.SMEM)] + [VM] * 4,
        [shape((4, 2, n, w), bf16), shape((4, 2, n, w), bf16), shape((4, 2) + docs.shape, docs.dtype), shape((8, w), f32),
         shape((4, 4, rows, 6 * EP), bf16), shape((4, rows, FF // 4), bf16), shape((4, rows, MODEL_WIDTH), bf16)]
        + [shape((2, QWIN * n, n), bf16)] * 3,
        [VM, ANY, ANY, VM, ANY, ANY, ANY, VM, VM, VM],
        [pltpu.VMEM((4, 2, n, w), bf16), pltpu.VMEM((4, 4) + gains.shape, bf16),
         pltpu.VMEM((4, rows, 6 * EP), bf16), pltpu.VMEM((4, rows, FF // 4), bf16), pltpu.SemaphoreType.DMA((5,))]
        + dma_sems(2 * GATHER_COPIES + 18 + 16),
    )


def forward_call(mix, a1, dcol, drow, th, tl, group, qkv_w, out_w, x, gain, gu, w_down, ident):
    rows, t, w = a1.shape
    n = x.shape[0]
    down = w_down.shape[0] // 2

    def body(mix_ref, a1_ref, dcol_ref, drow_ref, th_ref, tl_ref, group_ref, qw_ref, ow_ref, x_ref, g_ref, gu_ref, wd_ref,
             qkv_ref, normed_ref, xhat_ref, s_ref, p_ref, z_ref, resid_ref, out_ref, gu_out, wd_out,
             parts, v, local, rc, rd, rx, ry, td, tx, ty, send, recv):
        net = Net()
        sems = (send, recv)
        step = pl.program_id(0)
        base = SCATTER_COPIES + GATHER_COPIES
        mine = wd_ref.at[pl.ds(pl.multiple_of(down * net.x, down), down)]
        line_g = GatherLine(net, gu_ref, gu_out, sems, base)
        line_d = GatherLine(net, mine, wd_out, sems, base + LINE_COPIES)
        own_g = lambda: pltpu.make_async_copy(gu_ref, gu_out.at[net.z], local.at[1])
        own_d = lambda: pltpu.make_async_copy(mine, wd_out.at[net.z], local.at[2])
        A, B = pl.ds(0, n // 2), pl.ds(n // 2, n // 2)
        go = {}

        def at(i):
            def run(act):
                pl.when(step == i)(act)

            return run

        @at(0)
        def _():
            net.greet("xyc")
            line_g.step(0)
            line_d.step(0)
            own_g().start()
            own_d().start()

        qkv_ref[0] = dot(a1_ref[0], qw_ref[...]).astype(bf16)
        attend_row(mix_ref, qkv_ref, dcol_ref, drow_ref, th_ref, tl_ref, group_ref, normed_ref, xhat_ref, s_ref, p_ref, z_ref)
        parts[3 - step // 2, step % 2] = dot(normed_ref[0], ow_ref[...]).astype(bf16)

        def swap(chip, i):
            go[chip] = Later(lambda: net.copy(parts.at[chip, 1], rc.at[chip], sems, i, "c"))

        def add(dst, chip, start, more=None):
            def one(r):
                total = wide(parts[chip, 0, r]) + wide(rc[chip, r])
                if more is not None:
                    total = total + wide(more[r])
                dst[r] = total.astype(bf16)

            tiles(start, n // 2, one)

        @at(1)
        def _():
            swap(3, 0)

        @at(2)
        def _():
            go[3].wait_recv()
            add(td, 3, 0)
            go["dA"] = Later(lambda: net.copy(td.at[A], rd.at[A], sems, 4, "x"))
            add(td, 3, n // 2)
            go["dB"] = Later(lambda: net.copy(td.at[B], rd.at[B], sems, 5, "y"))

        @at(3)
        def _():
            swap(2, 2)
            line_g.step(1)

        @at(4)
        def _():
            go[2].wait_recv()
            add(ty, 2, n // 2)
            go["yB"] = Later(lambda: net.copy(ty.at[B], ry.at[B], sems, 7, "y"))
            go["dA"].wait_recv()
            add(ty, 2, 0, rd)
            go["yA"] = Later(lambda: net.copy(ty.at[A], ry.at[A], sems, 8, "y"))

        @at(5)
        def _():
            swap(1, 1)
            line_d.step(1)

        @at(6)
        def _():
            go[1].wait_recv()
            add(tx, 1, 0)
            go["xA"] = Later(lambda: net.copy(tx.at[A], rx.at[A], sems, 6, "x"))
            go["dB"].wait_recv()
            add(tx, 1, n // 2, rd)
            go["xB"] = Later(lambda: net.copy(tx.at[B], rx.at[B], sems, 9, "x"))

        @at(rows - 1)
        def _():
            swap(0, 3)
            line_g.step(2)
            go[0].wait_recv()

            def ready(half):
                for name in (("yA", "xA"), ("yB", "xB"))[half]:
                    go[name].wait_recv()

                def rows_of(r):
                    total = wide(parts[0, 0, r]) + wide(rc[0, r]) + wide(rx[r]) + wide(ry[r])
                    resid = wide(x_ref[r]) + total
                    resid_ref[r] = resid
                    inv = lax.rsqrt(jnp.mean(resid * resid, axis=1, keepdims=True) + 1e-06)
                    v[r] = (resid * inv * g_ref[...]).astype(bf16)

                tiles(half * (n // 2), n // 2, rows_of)

            poll, drain = polls(lambda: line_d.step(2), lambda: line_g.step(3), lambda: line_d.step(3))
            gather_rows(net, v, out_ref, sems, SCATTER_COPIES, ready, poll)
            drain()
            last = pltpu.make_async_copy(v, out_ref.at[0, 0], local.at[0])
            last.start()
            line_g.finish()
            line_d.finish()
            own_g().wait()
            own_d().wait()
            for copy in go.values():
                copy.wait_send()
            last.wait()

    where = lambda i: 2 * (3 - i // 2) + i % 2
    row = lambda *sh: pl.BlockSpec((1,) + sh, lambda i: (where(i),) + (0,) * len(sh))
    full = lambda v: pl.BlockSpec(v.shape, lambda i: (0,) * v.ndim, pipeline_mode=pl.Buffered(1))
    keep = lambda *sh: pl.BlockSpec(sh, lambda i: (0,) * len(sh))
    return pl.pallas_call(
        body,
        grid=(rows,),
        in_specs=[pl.BlockSpec(memory_space=pltpu.SMEM), row(t, w), row(t, 1), row(1, t), full(th), full(tl), full(group), full(qkv_w),
                  full(out_w), full(x), full(gain), full(gu), full(w_down)],
        out_specs=[row(t, 6 * EP), row(t, 2 * EP), row(t, 2 * EP), row(t, 2 * EP), row(2, t, t), row(2, t, t), keep(n, w), ANY, ANY, ANY],
        out_shape=[
            shape((rows, t, 6 * EP), bf16),
            shape((rows, t, 2 * EP), bf16),
            shape((rows, t, 2 * EP), f32),
            shape((rows, t, 2 * EP), f32),
            shape((rows, 2, t, t), f32),
            shape((rows, 2, t, t), bf16),
            shape((n, w), f32),
            shape((4, 2, n, w), bf16),
            shape((4,) + gu.shape, bf16),
            shape((4, down, w), bf16),
        ],
        scratch_shapes=[pltpu.VMEM((4, 2, n, w), bf16), pltpu.VMEM((n, w), bf16), pltpu.SemaphoreType.DMA((3,))] + scatter_scratch(n, w)
        + dma_sems(SCATTER_COPIES + GATHER_COPIES + 2 * LINE_COPIES),
        compiler_params=pltpu.CompilerParams(collective_id=ident, has_side_effects=True, vmem_limit_bytes=60 << 20),
        name="forward",
    )(mix, a1, dcol, drow, th, tl, group, qkv_w, out_w, x, gain, gu, w_down)


def mid_back_call(parts, dy, resid, gain, down, gate, ident):
    n, w = parts.shape[2:]

    def body(p_ref, dy_ref, r_ref, g_ref, down_ref, gate_ref, dresid_ref, out_ref, sum_ref, down_out, gate_out,
             v, local, rc, rd, rx, ry, td, tx, ty, d_got, d_made, g_got, g_made, send, recv):
        net = Net()
        sems = (send, recv)
        net.greet("xyc")
        base = SCATTER_COPIES + GATHER_COPIES
        line_d = ScatterLine(net, down_ref, d_got, d_made, sems, base)
        line_g = ScatterLine(net, gate_ref, g_got, g_made, sems, base + LINE_COPIES)
        line_g.step(0)
        line_d.step(0)
        poll, drain = polls(
            lambda: (line_g.step(1), line_d.step(1)), lambda: None, lambda: (line_g.step(2), line_d.step(2))
        )
        sum_ref[...] = jnp.zeros_like(sum_ref)
        done = scatter_rows(net, p_ref, rc, rd, rx, ry, td, tx, ty, sems, 0, poll)
        poll()

        def ready(half):
            done(half)

            def rows_of(rows):
                da2 = wide(p_ref[0, 0, rows]) + wide(rc[0, rows]) + wide(rx[rows]) + wide(ry[rows])
                res = r_ref[rows]
                r = lax.rsqrt(jnp.mean(res * res, axis=1, keepdims=True) + 1e-06)
                unit = res * r
                sum_ref[0:1] += jnp.sum(da2 * unit, axis=0, keepdims=True)
                dn = da2 * g_ref[...]
                dresid = wide(dy_ref[rows]) + r * (dn - unit * r * jnp.mean(dn * res, axis=1, keepdims=True))
                dresid_ref[rows] = dresid
                v[rows] = dresid.astype(bf16)

            tiles(half * (n // 2), n // 2, rows_of)

        gather_rows(net, v, out_ref, sems, SCATTER_COPIES, ready, poll)
        drain()
        last = pltpu.make_async_copy(v, out_ref.at[0, 0], local)
        last.start()

        def put(ref):
            def store(rows, total):
                ref[rows] = total.astype(bf16)

            return store

        line_g.finish(put(gate_out))
        line_d.finish(put(down_out))
        last.wait()

    return comm_call(
        body, "mid_back", ident, (parts, dy, resid, gain, down, gate), [VM] * 6,
        [shape((n, w), f32), shape((4, 2, n, w), bf16), shape((8, w), f32), shape(down.shape[1:], bf16),
         shape(gate.shape[1:], bf16)],
        [VM, ANY, VM, VM, VM],
        [pltpu.VMEM((n, w), bf16), pltpu.SemaphoreType.DMA] + scatter_scratch(n, w) + line_scratch(*down.shape[1:])
        + line_scratch(*gate.shape[1:]) + dma_sems(SCATTER_COPIES + GATHER_COPIES + 2 * LINE_COPIES),
    )


class Home:
    def __init__(self, net, zq, cq, fq, sems, base):
        self.net, self.zq, self.cq, self.fq, self.sems, self.base = net, zq, cq, fq, sems, base
        self.r = cq.shape[2]

    def rows(self, i, j):
        return pl.ds(pl.multiple_of((2 * i + j) * self.r, self.r), self.r)

    def over_c(self, i):
        net = self.net
        return net.copy(self.zq.at[self.rows(i, 1 - net.c)], self.cq.at[i, net.c], self.sems, self.base + i, "c")

    def over_y(self):
        net = self.net
        return net.copy(self.cq.at[1 - net.y], self.fq.at[net.x, net.y], self.sems, self.base + 2, "y")

    def over_x(self):
        net = self.net
        return net.copy(self.fq.at[net.x], self.fq.at[net.x], self.sems, self.base + 3, "x")

    def step(self, d):
        net = self.net
        if d == 0:
            for i in range(2):
                self.over_c(i).start()
                self.cq[i, net.c] = self.zq[self.rows(i, net.c)]
        elif d == 1:
            for i in range(2):
                self.over_c(i).wait_recv()
            self.over_y().start()
            self.fq[net.x, net.y] = self.cq[net.y]
        elif d == 2:
            self.over_y().wait_recv()
            self.over_x().start()
        else:
            self.over_x().wait_recv()

    def finish(self):
        for i in range(2):
            self.over_c(i).wait_send()
        self.over_y().wait_send()
        self.over_x().wait_send()

    def spread(self, dst):
        for i in range(2):
            for k in range(4):
                for m in range(4):
                    col = 256 * (4 * m + k) + 128 * i
                    dst[:, col : col + 128] = wide(self.fq[i, k // 2, k % 2, :, m * 128 : (m + 1) * 128])


HOME_COPIES = 4


def home_scratch(r, k):
    return [pltpu.VMEM((2, 2, r, k), bf16), pltpu.VMEM((2, 2, 2, r, k), bf16)]


def end_call(da_parts, qkv, wo, gate_up, small, x, dresid, gain, ident):
    n, w = da_parts.shape[2:]
    rows, wide_q = qkv.shape[2] // 4, qkv.shape[3]

    def body(da_ref, q_ref, wo_ref, up_ref, small_ref, x_ref, dresid_ref, g_ref,
             gx_ref, gq_ref, go_ref, gu_ref, total_ref,
             rc, rd, rx, ry, td, tx, ty, q_got, q_made, zq, cq, fq, cu, fu, ro, s_got, s_sum, s_line, send, recv):
        net = Net()
        sems = (send, recv)
        net.greet("xyc")
        base = SCATTER_COPIES
        lines = [ScatterLine(net, q_ref.at[i], q_got.at[i], q_made.at[i], sems, base + 6 * i) for i in range(2)]
        line_s = GatherLine(net, s_sum.at[2], s_line, sems, base + 12)
        base += 18
        homes = [Home(net, zq.at[i], cq.at[i], fq.at[i], sems, base + 4 * i) for i in range(2)]
        home_u = Home(net, up_ref, cu, fu, sems, base + 8)
        base += 12
        for line in lines:
            line.step(0)
        hops = [net.send(small_ref, s_got.at[0], sems, base, "c")]
        home_u.step(0)

        def small_step(i):
            hops[i].wait_recv()
            s_sum[i] = (small_ref[...] if i == 0 else s_sum[i - 1]) + s_got[i]
            if i < 2:
                hops.append(net.send(s_sum.at[i], s_got.at[i + 1], sems, base + 1 + i, "yx"[i]))
            else:
                line_s.step(0)

        scatter = scatter_steps(net, da_ref, rc, rd, rx, ry, td, tx, ty, sems, 0)
        next(scatter)
        small_step(0)
        next(scatter)
        home_u.step(1)
        swap_o = net.send(wo_ref, ro, sems, base + 3, "x")
        lines[0].step(1)
        small_step(1)
        done = next(scatter)
        lines[1].step(1)
        home_u.step(2)
        small_step(2)
        lines[0].step(2)
        line_s.step(1)
        lines[1].step(2)
        line_s.step(2)
        for half in range(2):
            done(half)

            def rows_of(at):
                da = wide(da_ref[0, 0, at]) + wide(rc[0, at]) + wide(rx[at]) + wide(ry[at])
                xf = wide(x_ref[at])
                r = lax.rsqrt(jnp.mean(xf * xf, axis=1, keepdims=True) + 1e-06)
                dn = da * g_ref[...]
                gx_ref[at] = dresid_ref[at] + r * (dn - xf * r * r * jnp.mean(dn * xf, axis=1, keepdims=True))

            tiles(half * (n // 2), n // 2, rows_of)

        for i in range(2):

            def put(at, total):
                zq[i, at] = total.astype(bf16)

            lines[i].finish(put)
            homes[i].step(0)
        homes[0].step(1)
        homes[1].step(1)
        homes[0].step(2)
        homes[1].step(2)
        line_s.step(3)
        s_line[net.z] = s_sum[2]
        total_ref[...] = (s_line[0] + s_line[1]) + (s_line[2] + s_line[3])
        swap_o.wait_recv()
        go_ref[...] = wide(wo_ref[...]) + wide(ro[...])
        home_u.step(3)
        home_u.spread(gu_ref)
        for part in range(2):
            homes[part].step(3)
            for i in range(2):
                for k in range(4):
                    pair = 4 * i + 2 * (k % 2) + k // 2
                    for m in range(3):
                        to = 3 * part + m
                        col = (to // 2) * MODEL_WIDTH + (2 * pair + to % 2) * E
                        gq_ref[:, col : col + E] = wide(fq[part, i, k // 2, k % 2, :, m * EP : m * EP + E])
        line_s.finish()
        for home in homes + [home_u]:
            home.finish()
        for copy in hops + [swap_o]:
            copy.wait_send()

    two = lambda specs: [pltpu.VMEM((2,) + v.shape, v.dtype) for v in specs]
    return comm_call(
        body, "end", ident, (da_parts, qkv, wo, gate_up, small, x, dresid, gain), [VM] * 8,
        [shape((n, w), f32), shape((rows, 3 * MODEL_WIDTH), f32), shape(wo.shape, f32), shape((rows, FF), f32), shape(small.shape, f32)],
        [VM] * 5,
        scatter_scratch(n, w) + two(line_scratch(4 * rows, wide_q)) + two([pltpu.VMEM((4 * rows, wide_q), bf16)])
        + two(home_scratch(rows, wide_q)) + home_scratch(rows, FF // 8) + [pltpu.VMEM(wo.shape, bf16)]
        + [pltpu.VMEM((3,) + small.shape, f32), pltpu.VMEM((3,) + small.shape, f32), pltpu.VMEM((4,) + small.shape, f32)]
        + dma_sems(SCATTER_COPIES + 18 + 12 + 4),
    )


def back_call(mix, qkv, dcol, drow, tt, gain, dattn, xhat, s, p, z, a1, out_w, qkv_w, out_parts, up_parts, wo, gate, down, resid, ident):
    rows, t, _ = qkv.shape
    n, w = out_parts.shape[2:]
    rows_o, rows_d, wide_q = wo.shape[1], down.shape[0], 3 * EP

    def body(mix_ref, qkv_ref, dcol_ref, drow_ref, tt_ref, gain_ref, dattn_ref, xhat_ref, s_ref, p_ref, z_ref, a1_ref,
             ow_ref, qw_ref, op_ref, gu_ref, wo_ref, gate_ref, down_ref, resid_ref,
             da_ref, q16_ref, sum_ref, gconv_ref, gmix_ref, gg_ref, out_ref, gu_out, go_out, gg_out, gd_ref,
             m_ref, gq_ref, dq, rc, rd, rx, ry, td, tx, ty, g_got, g_made, o_got, o_made, po, cg, fg, fd, send, recv):
        net = Net()
        sems = (send, recv)
        step = pl.program_id(0)
        base = SCATTER_COPIES
        line = ScatterLine(net, gu_ref, g_got, g_made, sems, base)
        line_o = ScatterLine(net, po, o_got, o_made, sems, base + 6)
        home = Home(net, gate_ref, cg, fg, sems, base + 12)
        x, c = net.x, net.c
        to_c = lambda: net.copy(wo_ref.at[1 - c], po.at[2 * x + c], sems, base + 16, "c")
        to_x = lambda: net.copy(down_ref, fd.at[x], sems, base + 17, "x")
        scatter = scatter_steps(net, op_ref, rc, rd, rx, ry, td, tx, ty, sems, 0)

        @pl.when(step == 0)
        def _():
            net.greet("xyc")
            line.step(0)
            to_c().start()
            next(scatter)
            home.step(0)
            po[2 * (1 - x)] = jnp.zeros((rows_o, w), bf16)
            po[2 * (1 - x) + 1] = jnp.zeros((rows_o, w), bf16)
            po[2 * x + c] = wo_ref[c]
            fd[x] = down_ref[...]
            m_ref[...] = jnp.zeros_like(m_ref)
            gmix_ref[...] = jnp.zeros_like(gmix_ref)
            gg_ref[...] = jnp.zeros_like(gg_ref)
            gq_ref[...] = jnp.zeros_like(gq_ref)

        allowed = allowed_mask(dcol_ref[0], drow_ref[0])
        scale = 1.0 / math.sqrt(E)
        lane = lax.broadcasted_iota(jnp.int32, (1, EP), 1)
        prob = [p_ref[0, 0], p_ref[0, 1]]
        dmixed = []
        for h in range(2):
            cols = slice(h * EP, (h + 1) * EP)
            dn, xh = dot(dattn_ref[0], ow_ref[cols], 1, 1), xhat_ref[0, :, cols]
            gg_ref[0:1, cols] += jnp.sum(dn * xh, axis=0, keepdims=True)
            dc = dn * gain_ref[0:1, cols]
            m1 = jnp.sum(dc, axis=1, keepdims=True) / E
            m2 = jnp.sum(dc * xh, axis=1, keepdims=True) / E
            dh = jnp.where(lane < E, s_ref[0, :, cols] * (dc - m1 - xh * m2), 0.0).astype(bf16)
            v = qkv_ref[0, :, (4 + h) * EP : (5 + h) * EP]
            mixed = (mix_ref[h, 0] * prob[0] + mix_ref[h, 1] * prob[1]).astype(bf16)
            dmixed.append(dot(dh, v, 1, 1))
            dq[:, (4 + h) * EP : (5 + h) * EP] = dot(mixed, dh, 0, 0).astype(bf16)
        for h in range(2):
            for c in range(2):
                r = 2 * h + c
                gmix_ref[r : r + 1, :] += jnp.sum(dmixed[h] * prob[c], axis=0, keepdims=True)
        for c in range(2):
            dp = mix_ref[0, c] * dmixed[0] + mix_ref[1, c] * dmixed[1]
            dconv = prob[c] * (dp - jnp.sum(dp * prob[c], axis=1, keepdims=True))
            ahead = jnp.concatenate([up(dconv, a).astype(bf16) for a in range(QWIN)], 1)
            m_ref[c] += dot(z_ref[0, c], ahead, 0, 0)
            ds = jnp.where(allowed, dot(ahead, tt_ref[c]), 0.0).astype(bf16)
            q = qkv_ref[0, :, c * EP : (c + 1) * EP]
            k = qkv_ref[0, :, (2 + c) * EP : (3 + c) * EP]
            dq[:, c * EP : (c + 1) * EP] = (dot(ds, k) * scale).astype(bf16)
            dq[:, (2 + c) * EP : (3 + c) * EP] = (dot(ds, q, 0, 0) * scale).astype(bf16)
        da_ref[0] = dot(dq[...], qw_ref[...], 1, 1).astype(bf16)
        for i in range(0, w, 384):
            gq_ref[i : i + 384] += dot(a1_ref[0, :, i : i + 384], dq[...], 0, 0)

        done = []

        @pl.when(step == 1)
        def _():
            next(scatter)
            to_c().wait_recv()
            line_o.step(0)
            home.step(1)
            to_x().start()

        @pl.when(step == 2)
        def _():
            line.step(1)
            done.append(next(scatter))

        @pl.when(step == 3)
        def _():
            line_o.step(1)
            home.step(2)

        @pl.when(step == 4)
        def _():
            line.step(2)

        @pl.when(step == 5)
        def _():
            line_o.step(2)

        @pl.when(step == rows - 1)
        def _():
            lanes = lax.broadcasted_iota(jnp.int32, (8, t), 1)
            for h in range(2):
                for a in range(QWIN):
                    total = jnp.zeros((8, t), f32)
                    for first in range(0, t, 8):
                        part = m_ref[h, first : first + 8, a * t : (a + 1) * t]
                        turned = pltpu.roll(part, t - first, 1) if first else part
                        total = total + jnp.where(lanes < t - first, turned, 0.0)
                    gconv_ref[h, a] = total[:, :EP]
            for half in range(2):
                done[0](half)

                def sum_of(at):
                    total = wide(op_ref[0, 0, at]) + wide(rc[0, at]) + wide(rx[at]) + wide(ry[at])
                    out_ref[at] = (resid_ref[at] + total).astype(bf16)

                tiles(half * (n // 2), n // 2, sum_of)

            def put(at, total):
                gu_out[at] = total.astype(bf16)

            line.finish(put)

            def put_o(at, total):
                go_out[at] = total.astype(bf16)

            line_o.finish(put_o)
            to_x().wait_recv()
            for i in range(2):
                gd_ref[i * rows_d : (i + 1) * rows_d] = wide(fd[i])
            home.step(3)
            home.spread(gg_out)
            home.finish()
            to_x().wait_send()
            to_c().wait_send()
            for i in range(0, w, 384):
                part = gq_ref[i : i + 384]
                for j in range(2):
                    q16_ref[j, i : i + 384] = part[:, j * wide_q : (j + 1) * wide_q].astype(bf16)
                sum_ref[:, i : i + 384] = lax.dot_general(
                    jnp.ones((8, 6 * EP), f32), part * wide(qw_ref[i : i + 384]), (((1,), (1,)), ((), ())),
                    precision=lax.Precision.HIGHEST, preferred_element_type=f32,
                )

    row = lambda *sh: pl.BlockSpec((1,) + sh, lambda i: (i,) + (0,) * len(sh))
    full = lambda v: pl.BlockSpec(v.shape, lambda i: (0,) * v.ndim, pipeline_mode=pl.Buffered(1))
    keep = lambda *sh: pl.BlockSpec(sh, lambda i: (0,) * len(sh))
    return pl.pallas_call(
        body,
        grid=(rows,),
        in_specs=[pl.BlockSpec(memory_space=pltpu.SMEM), row(t, 6 * EP), row(t, 1), row(1, t), full(tt), full(gain),
                  row(t, w), row(t, 2 * EP), row(t, 2 * EP), row(2, t, t), row(2, t, t), row(t, w),
                  full(out_w), full(qkv_w), full(out_parts), full(up_parts), full(wo), full(gate), full(down), full(resid)],
        out_specs=[row(t, w), keep(2, w, wide_q), keep(8, w), keep(2, QWIN, 8, EP), keep(8, t), keep(8, 2 * EP), keep(n, w),
                   keep(*up_parts.shape[1:]), keep(rows_o, w), keep(rows_o, FF), keep(2 * rows_d, w)],
        out_shape=[
            shape((rows, t, w), bf16),
            shape((2, w, wide_q), bf16),
            shape((8, w), f32),
            shape((2, QWIN, 8, EP), f32),
            shape((8, t), f32),
            shape((8, 2 * EP), f32),
            shape((n, w), bf16),
            shape(up_parts.shape[1:], bf16),
            shape((rows_o, w), bf16),
            shape((rows_o, FF), f32),
            shape((2 * rows_d, w), f32),
        ],
        scratch_shapes=[pltpu.VMEM((2, t, QWIN * t), f32), pltpu.VMEM((w, 6 * EP), f32), pltpu.VMEM((t, 6 * EP), bf16)] + scatter_scratch(n, w)
        + line_scratch(*up_parts.shape[1:]) + line_scratch(rows_o, w) + [pltpu.VMEM((4, rows_o, w), bf16)]
        + home_scratch(rows_o, FF // 8) + [pltpu.VMEM((2, rows_d, w), bf16)] + dma_sems(SCATTER_COPIES + 18),
        compiler_params=pltpu.CompilerParams(collective_id=ident, has_side_effects=True, vmem_limit_bytes=63 << 20),
        name="back",
    )(mix, qkv, dcol, drow, tt, gain, dattn, xhat, s, p, z, a1, out_w, qkv_w, out_parts, up_parts, wo, gate, down, resid)


def rms_scale(values):
    return lax.rsqrt(jnp.mean(values * values, axis=1, keepdims=True) + 1e-06)


class Links:
    def __init__(self, fsdp):
        self.fsdp = fsdp
        index = lax.axis_index("fsdp")
        self.x = lax.axis_index("rep")
        self.z, self.y, self.c = index // 4, (index // 2) % 2, index % 2

    def across(self, flip, v):
        if flip == "x":
            return lax.ppermute(v, "rep", [(0, 1), (1, 0)])
        bit = {"y": 2, "c": 1}[flip]
        return lax.ppermute(v, "fsdp", [(f, f ^ bit) for f in range(self.fsdp)])

    def along(self, v, step):
        pairs = [(f, f + 4 * step) for f in range(self.fsdp) if 0 <= f + 4 * step < self.fsdp]
        return lax.ppermute(v, "fsdp", pairs)

    def ordered(self, bit, mine, other, axis):
        first, second = jnp.where(bit == 0, mine, other), jnp.where(bit == 0, other, mine)
        return jnp.stack([first, second], axis)

    def gather_z(self, v):
        left, right = [], []
        a = b = v
        for _ in range(3):
            a, b = self.along(a, 1), self.along(b, -1)
            left.append(a)
            right.append(b)
        line = jnp.stack(left[::-1] + [v] + right)
        return lax.dynamic_slice_in_dim(line, 3 - self.z, 4, 0)

    def scatter_z(self, parts):
        zero = jnp.zeros((3,) + parts.shape[1:], parts.dtype)
        line = lax.dynamic_slice_in_dim(jnp.concatenate([zero, parts, zero]), self.z, 7, 0)
        low = lambda v: v.astype(bf16)
        a = self.along(low(line[6]), 1)
        b = self.along(low(line[0]), -1)
        for step in (1, 2):
            a = self.along(low(line[6 - step] + a.astype(f32)), 1)
            b = self.along(low(line[step] + b.astype(f32)), -1)
        return line[3] + a.astype(f32) + b.astype(f32)

    def gather_plane(self, v):
        n = v.shape[0] // 2
        vx, vy = self.across("x", v), self.across("y", v)
        vd = jnp.concatenate([self.across("y", vx[:n]), self.across("x", vy[n:])])
        return [jnp.concatenate([u, self.across("c", u)]) for u in (v, vx, vy, vd)]

    def scatter_plane(self, parts):
        low = lambda v: v.astype(bf16)
        n = parts[0].shape[0] // 2
        s = [p[:n] + self.across("c", low(p[n:])).astype(f32) for p in parts]
        m = n // 2
        dx, dy = self.across("x", low(s[3][:m])), self.across("y", low(s[3][m:]))
        to_x = jnp.concatenate([s[1][:m], s[1][m:] + dy.astype(f32)])
        to_y = jnp.concatenate([s[2][:m] + dx.astype(f32), s[2][m:]])
        return s[0] + self.across("x", low(to_x)).astype(f32) + self.across("y", low(to_y)).astype(f32)


class Weights:
    def __init__(self, links):
        self.links = links
        self.line = links.fsdp == 16
        x, y, c = links.x, links.y, links.c
        self.pair = 4 * x + 2 * c + y
        self.slot = 4 * x + 2 * y + c

    def spread(self, shard, dims):
        l = self.links
        ax, ay, ac = dims
        v = lax.dynamic_index_in_dim(shard, l.x, ax, keepdims=True)
        keep = lax.dynamic_index_in_dim(v, l.y, ay, keepdims=True)
        sent = l.across("y", lax.dynamic_index_in_dim(v, 1 - l.y, ay, keepdims=True))
        v = l.ordered(l.y, keep, sent, 0)
        keep = lax.dynamic_index_in_dim(v, l.c, ac + 1, keepdims=True)
        sent = l.across("c", lax.dynamic_index_in_dim(v, 1 - l.c, ac + 1, keepdims=True))
        v = l.ordered(l.c, keep, sent, 1)
        return l.gather_z(v)

    def collect(self, grad, dims):
        l = self.links
        ax, ay, ac = dims
        low = lambda v: v.astype(bf16)
        v = l.scatter_z(grad)
        keep = lax.dynamic_index_in_dim(v, l.c, 1, keepdims=False)
        sent = l.across("c", low(lax.dynamic_index_in_dim(v, 1 - l.c, 1, keepdims=False)))
        v = self.join(l.c, keep, sent.astype(f32), ac + 1)
        keep = lax.dynamic_index_in_dim(v, l.y, 0, keepdims=False)
        sent = l.across("y", low(lax.dynamic_index_in_dim(v, 1 - l.y, 0, keepdims=False)))
        v = low(self.join(l.y, keep, sent.astype(f32), ay))
        return self.join(l.x, v, l.across("x", v), ax).astype(f32)

    def join(self, bit, mine, other, axis):
        first, second = jnp.where(bit == 0, mine, other), jnp.where(bit == 0, other, mine)
        return jnp.concatenate([first, second], axis)

    def whole(self, shard):
        return lax.all_gather(shard, "fsdp", axis=0, tiled=True)

    def owned(self, grad):
        part = lax.psum_scatter(grad, "fsdp", scatter_dimension=0, tiled=True)
        return lax.psum(part.astype(bf16), "rep").astype(f32)

    def qkv(self, shard):
        rows = shard.shape[0]
        if self.line:
            v = self.spread(shard.reshape(rows, 3, 2, 2, 2, 2 * E), (2, 4, 3))
            v = v.reshape(MODEL_WIDTH, 3, 2, E)
        else:
            v = self.whole(shard).reshape(MODEL_WIDTH, 3, 8, 2, E)
            v = lax.dynamic_index_in_dim(v, self.pair, 2, keepdims=False)
        return jnp.pad(v, ((0, 0), (0, 0), (0, 0), (0, EP - E))).reshape(MODEL_WIDTH, 6 * EP)

    def qkv_back(self, grad):
        g = grad.reshape(MODEL_WIDTH, 3, 2, EP)[..., :E]
        if self.line:
            return self.collect(g.reshape(4, 2, 2, -1, 3, 1, 1, 1, 2 * E), (2, 4, 3)).reshape(-1, 3 * MODEL_WIDTH)
        zero = jnp.zeros((MODEL_WIDTH, 3, 8, 2, E), f32)
        return self.owned(lax.dynamic_update_index_in_dim(zero, g, self.pair, 2).reshape(MODEL_WIDTH, 3 * MODEL_WIDTH))

    def out(self, shard):
        l = self.links
        if self.line:
            v = l.gather_z(shard)
            keep = lax.dynamic_index_in_dim(v, 2 * l.x + l.c, 0, keepdims=False)
            sent = l.across("c", lax.dynamic_index_in_dim(v, 2 * l.x + 1 - l.c, 0, keepdims=False))
            v = l.ordered(l.c, keep, sent, 0)
        else:
            v = self.whole(shard).reshape(8, 2, E, MODEL_WIDTH)
            v = lax.dynamic_index_in_dim(v, self.pair, 0, keepdims=False)
        return jnp.pad(v, ((0, 0), (0, EP - E), (0, 0))).reshape(2 * EP, MODEL_WIDTH)

    def out_back(self, grad):
        l = self.links
        g = grad.reshape(2, EP, MODEL_WIDTH)[:, :E]
        if self.line:
            keep = lax.dynamic_index_in_dim(g, l.c, 0, keepdims=False)
            sent = l.across("c", lax.dynamic_index_in_dim(g, 1 - l.c, 0, keepdims=False).astype(bf16)).astype(f32)
            at = jnp.arange(4)[:, None, None]
            parts = jnp.where(at == 2 * l.x + l.c, keep[None], jnp.where(at == 2 * l.x + 1 - l.c, sent[None], 0.0))
            v = l.scatter_z(parts).astype(bf16)
            return (v + l.across("x", v)).astype(f32)
        zero = jnp.zeros((8, 2, E, MODEL_WIDTH), f32)
        return self.owned(lax.dynamic_update_index_in_dim(zero, g, self.pair, 0).reshape(MODEL_WIDTH, MODEL_WIDTH))

    def ffn_in(self, gate, up_):
        rows = gate.shape[0]
        both = jnp.stack([gate, up_], 1)
        if self.line:
            v = self.spread(both.reshape(rows, 2, 4, 2, 2, 2, FF // 32), (5, 3, 4))
            return v.reshape(MODEL_WIDTH, FF // 4)
        v = self.whole(both).reshape(MODEL_WIDTH, 2, 8, FF // 8)
        return lax.dynamic_index_in_dim(v, self.slot, 2, keepdims=False).reshape(MODEL_WIDTH, FF // 4)

    def ffn_in_back(self, grad):
        if self.line:
            v = self.collect(grad.reshape(4, 2, 2, -1, 2, 4, 1, 1, 1, FF // 32), (5, 3, 4)).reshape(-1, 2, FF)
        else:
            zero = jnp.zeros((MODEL_WIDTH, 2, 8, FF // 8), f32)
            g = grad.reshape(MODEL_WIDTH, 2, FF // 8)
            v = self.owned(lax.dynamic_update_index_in_dim(zero, g, self.slot, 2).reshape(MODEL_WIDTH, 2, FF))
        return v[:, 0], v[:, 1]

    def ffn_out(self, shard):
        l = self.links
        if self.line:
            v = lax.dynamic_index_in_dim(shard.reshape(2, FF // 32, MODEL_WIDTH), l.x, 0, keepdims=False)
            return l.gather_z(v).reshape(FF // 8, MODEL_WIDTH)
        v = self.whole(shard).reshape(8, FF // 8, MODEL_WIDTH)
        return lax.dynamic_index_in_dim(v, self.slot, 0, keepdims=False)

    def ffn_out_back(self, grad):
        l = self.links
        if self.line:
            v = l.scatter_z(grad.reshape(4, FF // 32, MODEL_WIDTH)).astype(bf16)
            return self.join(l.x, v, l.across("x", v), 0).astype(f32)
        zero = jnp.zeros((8, FF // 8, MODEL_WIDTH), f32)
        return self.owned(lax.dynamic_update_index_in_dim(zero, grad, self.slot, 0).reshape(FF, MODEL_WIDTH))

    def gains(self, *shards):
        l = self.links
        v = jnp.stack(shards)
        if self.line:
            v = l.ordered(l.c, v, l.across("c", v), 0)
            v = l.ordered(l.y, v, l.across("y", v), 0)
            v = l.gather_z(v)
            v = v.reshape(16, len(shards), -1).transpose(1, 0, 2).reshape(len(shards), MODEL_WIDTH)
        else:
            v = lax.all_gather(v, "fsdp", axis=1, tiled=True)
        return [v[i].astype(f32) for i in range(len(shards))]


def per_device(
    fsdp,
    x_in,
    doc_ids,
    w_qkv,
    w_out,
    gain_attn,
    gain_group,
    conv_kernel,
    head_mix,
    gain_ffn,
    w_gate,
    w_up,
    w_down,
    cotangent,
):
    links = Links(fsdp)
    weights = Weights(links)
    tokens = x_in.shape[1]

    x_all = jnp.concatenate(links.gather_plane(x_in[0]))
    qkv_w = weights.qkv(w_qkv)
    gain_a, gain_g, gain_f = weights.gains(gain_attn, gain_group, gain_ffn)
    docs = doc_ids
    for flip in ("y", "x"):
        docs = jnp.concatenate([docs, links.across(flip, docs)])
    docs = jnp.stack([docs, links.across("c", docs)], 1)
    docs = docs[jnp.array([0, 2, 1, 3])].reshape(8, tokens)
    out_w = weights.out(w_out)
    in_w = weights.ffn_in(w_gate, w_up)
    down_w = weights.ffn_out(w_down)
    upstream_chips = links.gather_plane(cotangent[0])

    kernel = lax.dynamic_slice_in_dim(conv_kernel, 2 * weights.pair, 2, 0)
    mix = lax.dynamic_slice_in_dim(head_mix, 2 * weights.pair, 2, 0)
    th, tl, tt = bands(kernel, tokens)
    group = lax.dynamic_slice_in_dim(gain_g.reshape(8, 2, E), weights.pair, 1, 0)
    group = jnp.pad(group, ((0, 0), (0, 0), (0, EP - E))).reshape(1, 2 * EP)
    doc_col, doc_row = docs[:, :, None], docs[:, None, :]

    xf_all = x_all.astype(f32)
    a1 = (xf_all * rms_scale(xf_all) * gain_a).astype(bf16)
    qkv = dot(a1, qkv_w).astype(bf16).reshape(8, tokens, 6 * EP)
    normed, xhat, s, probs, zeroed = attend(mix, qkv, doc_col, doc_row, th, tl, group)
    normed = normed.reshape(4, 2 * tokens, 2 * EP)
    xf = x_in[0].astype(f32)
    resid = xf + links.scatter_plane([dot(normed[i], out_w) for i in range(4)])

    r2 = rms_scale(resid)
    a2_chips = links.gather_plane((resid * r2 * gain_f).astype(bf16))
    out_parts, back_parts, hiddens, dgus = [], [], [], []
    half = FF // 8
    for a2, dffn in zip(a2_chips, upstream_chips):
        gu = dot(a2, in_w)
        gate, up_act = gu[:, :half], gu[:, half:]
        sig = jax.nn.sigmoid(gate)
        silu = gate * sig
        hidden = (silu * up_act).astype(bf16)
        dhidden = dot(dffn, down_w, 1, 1)
        dgate = (dhidden * up_act * sig * (1.0 + gate * (1.0 - sig))).astype(bf16)
        dup = (dhidden * silu).astype(bf16)
        dgu = jnp.concatenate([dgate, dup], 1)
        hiddens.append(hidden)
        dgus.append(dgu)
        back_parts.append(dot(dgu, in_w, 1, 1))
        out_parts.append(dot(hidden, down_w))
    da2 = links.scatter_plane(back_parts)
    output = (resid + links.scatter_plane(out_parts)).astype(bf16)

    dy = cotangent[0].astype(f32)
    sum_gain_ffn = jnp.sum(da2 * resid * r2, axis=0)
    dn2 = da2 * gain_f
    dresid = dy + r2 * (dn2 - resid * r2 * r2 * jnp.mean(dn2 * resid, axis=1, keepdims=True))
    dattn = jnp.concatenate(links.gather_plane(dresid.astype(bf16)))

    a2_all, dgu_all = jnp.concatenate(a2_chips), jnp.concatenate(dgus)
    hidden_all, dffn_all = jnp.concatenate(hiddens), jnp.concatenate(upstream_chips)
    grad_gate, grad_up = weights.ffn_in_back(dot(a2_all, dgu_all, 0, 0))
    grad_down = weights.ffn_out_back(dot(hidden_all, dffn_all, 0, 0))

    dnormed = dot(dattn, out_w, 1, 1).reshape(8, tokens, 2 * EP)
    dqkv, conv_tiles, mix_sums, group_sums = attend_back(
        mix, qkv, doc_col, doc_row, tt, group, dnormed, xhat, s, probs, zeroed
    )
    dqkv = dqkv.reshape(4, 2 * tokens, 6 * EP)
    da1 = links.scatter_plane([dot(dqkv[i], qkv_w, 1, 1) for i in range(4)])
    grad_out = weights.out_back(dot(normed.reshape(8 * tokens, 2 * EP), dattn, 0, 0))
    grad_qkv = weights.qkv_back(dot(a1, dqkv.reshape(8 * tokens, 6 * EP), 0, 0))

    r1 = rms_scale(xf)
    sum_gain_attn = jnp.sum(da1 * xf * r1, axis=0)
    dn1 = da1 * gain_a
    grad_x = dresid + r1 * (dn1 - xf * r1 * r1 * jnp.mean(dn1 * xf, axis=1, keepdims=True))

    place = lambda v: lax.dynamic_update_index_in_dim(jnp.zeros((8,) + v.shape, f32), v, weights.pair, 0)
    small = [
        sum_gain_attn,
        sum_gain_ffn,
        place(group_sums[0].reshape(2, EP)[:, :E].reshape(-1)),
        place(diagonals(conv_tiles)),
        place(jnp.sum(mix_sums[:4], axis=1)),
    ]
    sizes = [v.size for v in small]
    total = lax.psum(jnp.concatenate([v.reshape(-1) for v in small]), ("rep", "fsdp"))
    cut = [0]
    for size in sizes:
        cut.append(cut[-1] + size)
    gain_a_sum, gain_f_sum, group_sum, conv_sum, mix_sum = (total[cut[i] : cut[i + 1]] for i in range(5))
    rows = gain_attn.shape[0]
    own = lambda v: lax.dynamic_slice_in_dim(v, lax.axis_index("fsdp") * rows, rows, 0)
    return (
        output[None],
        grad_x[None],
        grad_qkv,
        grad_out,
        own(gain_a_sum),
        own(group_sum),
        conv_sum.reshape(H, QWIN, KWIN),
        mix_sum.reshape(H, 2),
        own(gain_f_sum),
        grad_gate,
        grad_up,
        grad_down,
    )


def join(bit, mine, other, axis):
    first, second = jnp.where(bit == 0, mine, other), jnp.where(bit == 0, other, mine)
    return jnp.stack([first, second], axis)


def fast(
    x_in,
    doc_ids,
    w_qkv,
    w_out,
    gain_attn,
    gain_group,
    conv_kernel,
    head_mix,
    gain_ffn,
    w_gate,
    w_up,
    w_down,
    cotangent,
):
    links = Links(16)
    pair = 4 * links.x + 2 * links.c + links.y
    tokens = x_in.shape[1]
    x, dy = x_in[0], cotangent[0]
    rows = w_qkv.shape[0]

    kernel = lax.dynamic_slice_in_dim(conv_kernel, 2 * pair, 2, 0)
    mix = lax.dynamic_slice_in_dim(head_mix, 2 * pair, 2, 0)
    gains = jnp.pad(jnp.stack([gain_attn, gain_group, gain_ffn]), ((0, 13), (0, 128 - rows)))
    docs = jnp.broadcast_to(doc_ids, (8, tokens))
    a1, dffn_all, docs, gains, qkv_w, gu_plane, out_w, th, tl, tt = start_call(
        x, dy, docs, gains, kernel.reshape(-1), w_qkv, w_gate, w_up, w_out, 1
    )
    docs = docs.reshape(8, 8, tokens)[:, 0]
    gain_a, gain_g, gain_f = gains[0:1], gains[1], gains[2:3]
    qkv_w = qkv_w.reshape(MODEL_WIDTH, 6 * EP)
    keep = lax.dynamic_index_in_dim(out_w, 2 * links.x + links.c, 0, keepdims=False)
    other = links.across("c", lax.dynamic_index_in_dim(out_w, 2 * links.x + 1 - links.c, 0, keepdims=False))
    out_w = jnp.pad(join(links.c, keep, other, 0), ((0, 0), (0, EP - E), (0, 0))).reshape(2 * EP, MODEL_WIDTH)

    group = lax.dynamic_slice_in_dim(gain_g.reshape(8, 2, E), pair, 1, 0)
    group = jnp.pad(group, ((0, 0), (0, 0), (0, EP - E))).reshape(1, 2 * EP)
    doc_col, doc_row = docs[:, :, None], docs[:, None, :]

    dffn_all = dffn_all.reshape(8 * tokens, MODEL_WIDTH)
    by_chip = lambda v: v.astype(bf16).reshape(4, 2, tokens, MODEL_WIDTH)
    by_row = lambda v: v.reshape(8, tokens, -1)
    qkv, normed, xhat, s, probs, zeroed, resid, a2, gu_w, down_w = forward_call(
        mix, by_row(a1), doc_col, doc_row, th, tl, group, qkv_w, out_w, x, gain_f, gu_plane, w_down, 2
    )
    normed = normed.reshape(8 * tokens, 2 * EP)

    a2 = a2.reshape(8 * tokens, MODEL_WIDTH)
    gu_w = gu_w.reshape(MODEL_WIDTH, FF // 4)
    down_w = down_w.reshape(FF // 8, MODEL_WIDTH)
    half = FF // 8
    gu = dot(a2, gu_w)
    gate, up_act = gu[:, :half], gu[:, half:]
    sig = jax.nn.sigmoid(gate)
    silu = gate * sig
    hidden = (silu * up_act).astype(bf16)
    dhidden = dot(dffn_all, down_w, 1, 1)
    dgate = (dhidden * up_act * sig * (1.0 + gate * (1.0 - sig))).astype(bf16)
    dup = (dhidden * silu).astype(bf16)
    dgu = jnp.concatenate([dgate, dup], 1)
    grad_gate = dot(a2, dgate, 0, 0).astype(bf16).reshape(4, 4 * rows, half)
    grad_up = dot(a2, dup, 0, 0).astype(bf16).reshape(4, 4 * rows, half)
    grad_down = dot(hidden, dffn_all, 0, 0).astype(bf16).reshape(4, FF // 32, MODEL_WIDTH)
    out_parts = by_chip(dot(hidden, down_w))
    dresid, dattn, sum_f, grad_down, grad_gate = mid_back_call(
        by_chip(dot(dgu, gu_w, 1, 1)), dy, resid, gain_f, grad_down, grad_gate, 3
    )
    grad_out = dot(normed, dattn.reshape(8 * tokens, MODEL_WIDTH), 0, 0).astype(bf16).reshape(2, EP, MODEL_WIDTH)[:, :rows]
    da_parts, grad_qkv, sum_a, conv_tiles, mix_sums, group_sums, out, grad_up, grad_out, grad_gate, grad_down = back_call(
        mix, qkv, doc_col, doc_row, tt, group, by_row(dattn), xhat, s, probs, zeroed, by_row(a1), out_w, qkv_w,
        out_parts, grad_up, grad_out, grad_gate, grad_down, resid, 5
    )
    sum_a = sum_a[0] / gain_a[0]
    place = lambda v: lax.dynamic_update_index_in_dim(jnp.zeros((8,) + v.shape, f32), v, pair, 0)
    small = [
        sum_a,
        sum_f[0],
        place(group_sums[0].reshape(2, EP)[:, :E].reshape(-1)),
        place(diagonals(conv_tiles)),
        place(jnp.sum(mix_sums[:4], axis=1)),
    ]
    cut = [0]
    for v in small:
        cut.append(cut[-1] + v.size)
    room = 48 * 128
    flat = jnp.concatenate([v.reshape(-1) for v in small] + [jnp.zeros((room - cut[-1],), f32)]).reshape(48, 128)
    grad_x, grad_qkv, grad_out, grad_up, total = end_call(
        by_chip(da_parts),
        grad_qkv.reshape(2, 4, 4 * rows, 3 * EP),
        grad_out,
        grad_up,
        flat,
        x,
        dresid,
        gain_a,
        4,
    )
    total = total.reshape(-1)
    gain_a_sum, gain_f_sum, group_sum, conv_sum, mix_sum = (total[cut[i] : cut[i + 1]] for i in range(5))
    own = lambda v: lax.dynamic_slice_in_dim(v, lax.axis_index("fsdp") * rows, rows, 0)
    return (
        out[None],
        grad_x[None],
        grad_qkv,
        grad_out,
        own(gain_a_sum),
        own(group_sum),
        conv_sum.reshape(H, QWIN, KWIN),
        mix_sum.reshape(H, 2),
        own(gain_f_sum),
        grad_gate,
        grad_up,
        grad_down,
    )


def solution(mesh):
    fsdp = mesh.shape["fsdp"]
    assert mesh.shape["rep"] == 2 and fsdp % 4 == 0
    rows, shard, part = P(("rep", "fsdp"), None, None), P("fsdp", None), P("fsdp")
    placed = (rows, P(("rep", "fsdp"), None), shard, shard, part, part, P(), P(), part, shard, shard, shard, rows)
    return jax.shard_map(
        fast if fsdp == 16 else (lambda *args: per_device(fsdp, *args)),
        mesh=mesh,
        in_specs=placed,
        out_specs=(rows, rows, shard, shard, part, part, P(), P(), part, shard, shard, shard),
        check_vma=False,
    )
```

```python
import math

import jax
import jax.numpy as jnp
from jax import lax
from jax.experimental import pallas as pl
from jax.experimental.pallas import tpu as pltpu
from jax.sharding import PartitionSpec as P

MODEL_WIDTH = 1536
H = 16
E = 96
EP = 128
QWIN = 6
KWIN = 11
bf16, f32 = jnp.bfloat16, jnp.float32


def allowed_mask(doc_col, doc_row):
    n = doc_row.shape[-1]
    i = lax.broadcasted_iota(jnp.int32, (n, n), 0)
    j = lax.broadcasted_iota(jnp.int32, (n, n), 1)
    return (j <= i) & (doc_col == doc_row)


def down(v, a):
    if a == 0:
        return v
    i = lax.broadcasted_iota(jnp.int32, v.shape, 0)
    return jnp.where(i >= a, pltpu.roll(v, a, 0), 0.0)


def up(v, a):
    if a == 0:
        return v
    n = v.shape[0]
    i = lax.broadcasted_iota(jnp.int32, v.shape, 0)
    return jnp.where(i < n - a, pltpu.roll(v, n - a, 0), 0.0)


def dot(a, b, ca=1, cb=0):
    return lax.dot_general(a, b, (((ca,), (cb,)), ((), ())), preferred_element_type=f32)


def split(v):
    hi = v.astype(bf16)
    return hi, (v - hi.astype(f32)).astype(bf16)


def attend_row(mix_ref, qkv_ref, dcol_ref, drow_ref, th_ref, tl_ref, gain_ref,
               normed_ref, xhat_ref, s_ref, p_ref, z_ref):
    allowed = allowed_mask(dcol_ref[0], drow_ref[0])
    scale = 1.0 / math.sqrt(E)
    probs = []
    for h in range(2):
        q = qkv_ref[0, :, h * EP:(h + 1) * EP]
        k = qkv_ref[0, :, (2 + h) * EP:(3 + h) * EP]
        zeroed = jnp.where(allowed, dot(q, k, 1, 1) * scale, 0.0)
        z_ref[0, h] = zeroed.astype(bf16)
        his, los = [], []
        for a in range(QWIN):
            hi, lo = split(down(zeroed, a))
            his.append(hi)
            los.append(lo)
        his, los = jnp.concatenate(his, 1), jnp.concatenate(los, 1)
        th, tl = th_ref[h], tl_ref[h]
        conv = dot(his, th) + (dot(his, tl) + dot(los, th))
        masked = jnp.where(allowed, conv, -jnp.inf)
        e = jnp.exp(masked - jnp.max(masked, axis=1, keepdims=True))
        p = e / jnp.sum(e, axis=1, keepdims=True)
        p_ref[0, h] = p
        probs.append(p)
    lane = lax.broadcasted_iota(jnp.int32, (1, EP), 1)
    for h in range(2):
        v = qkv_ref[0, :, (4 + h) * EP:(5 + h) * EP]
        mixed = (mix_ref[h, 0] * probs[0] + mix_ref[h, 1] * probs[1]).astype(bf16)
        ho = dot(mixed, v)
        centered = jnp.where(lane < E, ho - jnp.sum(ho, axis=1, keepdims=True) / E, 0.0)
        s = lax.rsqrt(jnp.sum(centered * centered, axis=1, keepdims=True) / E + 1e-05)
        xhat = centered * s
        cols = slice(h * EP, (h + 1) * EP)
        xhat_ref[0, :, cols] = xhat
        s_ref[0, :, cols] = jnp.broadcast_to(s, xhat.shape)
        normed_ref[0, :, cols] = (xhat * gain_ref[0:1, cols]).astype(bf16)


def attend(mix, qkv, dcol, drow, th, tl, gain):
    n, t, _ = qkv.shape
    row = lambda *s: pl.BlockSpec((1,) + s, lambda i: (i,) + (0,) * len(s))
    full = lambda a: pl.BlockSpec(a.shape, lambda i: (0,) * a.ndim)
    return pl.pallas_call(
        attend_row,
        grid=(n,),
        in_specs=[pl.BlockSpec(memory_space=pltpu.SMEM), row(t, 6 * EP), row(t, 1), row(1, t), full(th), full(tl), full(gain)],
        out_specs=[row(t, 2 * EP), row(t, 2 * EP), row(t, 2 * EP), row(2, t, t), row(2, t, t)],
        out_shape=[
            jax.ShapeDtypeStruct((n, t, 2 * EP), bf16),
            jax.ShapeDtypeStruct((n, t, 2 * EP), f32),
            jax.ShapeDtypeStruct((n, t, 2 * EP), f32),
            jax.ShapeDtypeStruct((n, 2, t, t), f32),
            jax.ShapeDtypeStruct((n, 2, t, t), bf16),
        ],
        cost_estimate=pl.CostEstimate(flops=n * 2 * 3 * 2 * t * t * QWIN * t, bytes_accessed=n * t * t * 20, transcendentals=n * 2 * t * t),
        name="attend",
    )(mix, qkv, dcol, drow, th, tl, gain)


def bwd_kernel(mix_ref, qkv_ref, dcol_ref, drow_ref, tt_ref, gain_ref, dn_ref, xhat_ref, s_ref, p_ref, z_ref,
               dqkv_ref, gconv_ref, gmix_ref, gg_ref, m_ref):
    step, steps = pl.program_id(0), pl.num_programs(0)
    t = p_ref.shape[-1]

    @pl.when(step == 0)
    def _():
        m_ref[...] = jnp.zeros_like(m_ref)
        gmix_ref[...] = jnp.zeros_like(gmix_ref)
        gg_ref[...] = jnp.zeros_like(gg_ref)

    allowed = allowed_mask(dcol_ref[0], drow_ref[0])
    scale = 1.0 / math.sqrt(E)
    lane = lax.broadcasted_iota(jnp.int32, (1, EP), 1)
    p = [p_ref[0, 0], p_ref[0, 1]]
    dmixed = []
    for h in range(2):
        cols = slice(h * EP, (h + 1) * EP)
        dn, xhat = dn_ref[0, :, cols], xhat_ref[0, :, cols]
        gg_ref[0:1, cols] += jnp.sum(dn * xhat, axis=0, keepdims=True)
        dc = dn * gain_ref[0:1, cols]
        m1 = jnp.sum(dc, axis=1, keepdims=True) / E
        m2 = jnp.sum(dc * xhat, axis=1, keepdims=True) / E
        dh = jnp.where(lane < E, s_ref[0, :, cols] * (dc - m1 - xhat * m2), 0.0).astype(bf16)
        v = qkv_ref[0, :, (4 + h) * EP:(5 + h) * EP]
        mixed = (mix_ref[h, 0] * p[0] + mix_ref[h, 1] * p[1]).astype(bf16)
        dmixed.append(dot(dh, v, 1, 1))
        dqkv_ref[0, :, (4 + h) * EP:(5 + h) * EP] = dot(mixed, dh, 0, 0).astype(bf16)
    for h in range(2):
        for c in range(2):
            r = 2 * h + c
            gmix_ref[r:r + 1, :] += jnp.sum(dmixed[h] * p[c], axis=0, keepdims=True)
    for c in range(2):
        dp = mix_ref[0, c] * dmixed[0] + mix_ref[1, c] * dmixed[1]
        dconv = p[c] * (dp - jnp.sum(dp * p[c], axis=1, keepdims=True))
        ahead = jnp.concatenate([up(dconv, a).astype(bf16) for a in range(QWIN)], 1)
        m_ref[c] += dot(z_ref[0, c], ahead, 0, 0)
        ds = jnp.where(allowed, dot(ahead, tt_ref[c]), 0.0).astype(bf16)
        q = qkv_ref[0, :, c * EP:(c + 1) * EP]
        k = qkv_ref[0, :, (2 + c) * EP:(3 + c) * EP]
        dqkv_ref[0, :, c * EP:(c + 1) * EP] = (dot(ds, k) * scale).astype(bf16)
        dqkv_ref[0, :, (2 + c) * EP:(3 + c) * EP] = (dot(ds, q, 0, 0) * scale).astype(bf16)

    @pl.when(step == steps - 1)
    def _():
        lanes = lax.broadcasted_iota(jnp.int32, (8, t), 1)
        for h in range(2):
            for a in range(QWIN):
                total = jnp.zeros((8, t), f32)
                for first in range(0, t, 8):
                    rows = m_ref[h, first:first + 8, a * t:(a + 1) * t]
                    turned = pltpu.roll(rows, t - first, 1) if first else rows
                    total = total + jnp.where(lanes < t - first, turned, 0.0)
                gconv_ref[h, a] = total[:, :EP]


def attend_back(mix, qkv, dcol, drow, tt, gain, dn, xhat, s, p, z):
    n, t, _ = qkv.shape
    row = lambda *sh: pl.BlockSpec((1,) + sh, lambda i: (i,) + (0,) * len(sh))
    full = lambda a: pl.BlockSpec(a.shape, lambda i: (0,) * a.ndim)
    keep = lambda *sh: pl.BlockSpec(sh, lambda i: (0,) * len(sh))
    return pl.pallas_call(
        bwd_kernel,
        grid=(n,),
        in_specs=[pl.BlockSpec(memory_space=pltpu.SMEM), row(t, 6 * EP), row(t, 1), row(1, t), full(tt), full(gain),
                  row(t, 2 * EP), row(t, 2 * EP), row(t, 2 * EP), row(2, t, t), row(2, t, t)],
        out_specs=[row(t, 6 * EP), keep(2, QWIN, 8, EP), keep(8, t), keep(8, 2 * EP)],
        out_shape=[
            jax.ShapeDtypeStruct((n, t, 6 * EP), bf16),
            jax.ShapeDtypeStruct((2, QWIN, 8, EP), f32),
            jax.ShapeDtypeStruct((8, t), f32),
            jax.ShapeDtypeStruct((8, 2 * EP), f32),
        ],
        scratch_shapes=[pltpu.VMEM((2, t, QWIN * t), f32)],
        cost_estimate=pl.CostEstimate(flops=n * 2 * 2 * 2 * t * t * QWIN * t, bytes_accessed=n * t * t * 20, transcendentals=0),
        name="attend_back",
    )(mix, qkv, dcol, drow, tt, gain, dn, xhat, s, p, z)


def bands(kernel, t):
    diff = jnp.arange(t)[None, :] - jnp.arange(t)[:, None]
    band = jnp.zeros((2, QWIN, t, t), f32)
    back = jnp.zeros((2, QWIN, t, t), f32)
    for b in range(KWIN):
        tap = kernel[:, :, b][:, :, None, None]
        band = band + jnp.where(diff == b, tap, 0.0)
        back = back + jnp.where(diff == -b, tap, 0.0)
    th, tl = split(band)
    flat = lambda v: v.reshape(2, QWIN * t, t)
    return flat(th), flat(tl), flat(back.astype(bf16))


def diagonals(tiles):
    return sum(tiles[:, :, i, i:i + KWIN] for i in range(8))


FF = 4096
MESH = pl.DeviceIdType.MESH


class Net:
    def __init__(self):
        self.x, self.f = lax.axis_index("rep"), lax.axis_index("fsdp")
        self.z, self.y, self.c = self.f // 4, (self.f // 2) % 2, self.f % 2
        self.k = self.f % 4
        nx, fy, fc = 1 - self.x, 2 - 4 * self.y, 1 - 2 * self.c
        self.to = {
            "x": (nx, self.f),
            "y": (self.x, self.f + fy),
            "c": (self.x, self.f + fc),
            "xy": (nx, self.f + fy),
            "xc": (nx, self.f + fc),
            "yc": (self.x, self.f + fy + fc),
            "xyc": (nx, self.f + fy + fc),
            "up": (self.x, self.f + 4),
            "down": (self.x, self.f - 4),
        }

    def greet(self, names, line=True):
        barrier = pltpu.get_barrier_semaphore()
        for name in names:
            pl.semaphore_signal(barrier, inc=1, device_id=self.to[name], device_id_type=MESH)
        count = len(names)
        if line:

            @pl.when(self.z < 3)
            def _():
                pl.semaphore_signal(barrier, inc=1, device_id=self.to["up"], device_id_type=MESH)

            @pl.when(self.z > 0)
            def _():
                pl.semaphore_signal(barrier, inc=1, device_id=self.to["down"], device_id_type=MESH)

            count = count + (self.z + 3) // 4 + (6 - self.z) // 4
        pl.semaphore_wait(barrier, count)

    def copy(self, src, dst, sems, i, name):
        return pltpu.make_async_remote_copy(
            src_ref=src, dst_ref=dst, send_sem=sems[0].at[i], recv_sem=sems[1].at[i],
            device_id=self.to[name], device_id_type=MESH,
        )

    def send(self, src, dst, sems, i, name):
        copy = self.copy(src, dst, sems, i, name)
        copy.start()
        return copy


def tiles(start, size, body, step=32):
    def one(i, _):
        body(pl.ds(pl.multiple_of(start + i * step, step), step))
        return 0

    lax.fori_loop(0, size // step, one, 0)


def wide(v):
    return v.astype(f32)


class GatherLine:
    def __init__(self, net, src, out, sems, base, keep=None):
        self.net, self.src, self.out, self.sems, self.base = net, src, out, sems, base
        self.keep = keep or (lambda slot: net.z >= 0)

    def go(self, d, way, act):
        net = self.net
        slot = net.z - d if way == "up" else net.z + d
        inside = (net.z >= d) & (net.z < 3) if way == "up" else (net.z < 4 - d) & (net.z > 0)
        i = self.base + d + (0 if way == "up" else 3)

        @pl.when(inside & self.keep(slot))
        def _():
            src = self.src if d == 0 else self.out.at[slot]
            act(net.copy(src, self.out.at[slot], self.sems, i, way))

    def came(self, d, way):
        net = self.net
        slot = net.z - d if way == "up" else net.z + d
        inside = net.z >= d if way == "up" else net.z < 4 - d
        i = self.base + d - 1 + (0 if way == "up" else 3)

        @pl.when(inside & self.keep(slot))
        def _():
            net.copy(self.out.at[slot], self.out.at[slot], self.sems, i, way).wait_recv()

    def step(self, d):
        for way in ("up", "down"):
            if d > 0:
                self.came(d, way)
            if d < 3:
                self.go(d, way, lambda copy: copy.start())

    def finish(self):
        for d in range(3):
            for way in ("up", "down"):
                self.go(d, way, lambda copy: copy.wait_send())


class ScatterLine:
    def __init__(self, net, parts, got, made, sems, base):
        self.net, self.parts, self.got, self.made, self.sems, self.base = net, parts, got, made, sems, base
        self.n = parts.shape[1]

    def each(self, d, way):
        net = self.net
        t = net.z + (3 - d) if way == 0 else net.z - (3 - d)
        inside = (t < 4) if way == 0 else (t >= 0)
        first = (net.z == 0) if way == 0 else (net.z == 3)
        return t, inside, first, self.base + d + 3 * way, ("up", "down")[way]

    def step(self, d):
        for way in range(2):
            t, inside, first, i, name = self.each(d, way)

            @pl.when(inside & first)
            def _():
                self.net.copy(self.parts.at[t], self.got.at[way, d], self.sems, i, name).start()

            if d == 0:
                continue

            @pl.when(inside & jnp.logical_not(first))
            def _():
                self.net.copy(self.got.at[way, d - 1], self.got.at[way, d - 1], self.sems, i - 1, name).wait_recv()

                def body(rows):
                    self.made[way, d - 1, rows] = (wide(self.parts[t, rows]) + wide(self.got[way, d - 1, rows])).astype(bf16)

                tiles(0, self.n, body)
                self.net.copy(self.made.at[way, d - 1], self.got.at[way, d], self.sems, i, name).start()

    def finish(self, store):
        net = self.net
        below, above = net.z > 0, net.z < 3

        @pl.when(below)
        def _():
            net.copy(self.got.at[0, 2], self.got.at[0, 2], self.sems, self.base + 2, "up").wait_recv()

        @pl.when(above)
        def _():
            net.copy(self.got.at[1, 2], self.got.at[1, 2], self.sems, self.base + 5, "down").wait_recv()

        def put(low, high):
            def body(rows):
                total = wide(self.parts[net.z, rows])
                if low:
                    total = total + wide(self.got[0, 2, rows])
                if high:
                    total = total + wide(self.got[1, 2, rows])
                store(rows, total)

            tiles(0, self.n, body)

        @pl.when(below & above)
        def _():
            put(True, True)

        @pl.when(jnp.logical_not(below))
        def _():
            put(False, True)

        @pl.when(jnp.logical_not(above))
        def _():
            put(True, False)

        for d in range(3):
            for way in range(2):
                t, inside, first, i, name = self.each(d, way)

                @pl.when(inside & first)
                def _():
                    net.copy(self.parts.at[t], self.got.at[way, d], self.sems, i, name).wait_send()

                if d > 0:

                    @pl.when(inside & jnp.logical_not(first))
                    def _():
                        net.copy(self.made.at[way, d - 1], self.got.at[way, d], self.sems, i, name).wait_send()


def line_scratch(n, w):
    return [pltpu.VMEM((2, 3, n, w), bf16), pltpu.VMEM((2, 2, n, w), bf16)]


LINE_COPIES = 6


class Later:
    def __init__(self, make):
        self.make = make
        make().start()

    def wait_recv(self):
        self.make().wait_recv()

    def wait_send(self):
        self.make().wait_send()


def gather_steps(net, v, out, sems, base, ready):
    n = v.shape[0]
    A, B = pl.ds(0, n // 2), pl.ds(n // 2, n // 2)
    go = {}
    ready(0)
    go["xA"] = Later(lambda: net.copy(v.at[A], out.at[1, 0, A], sems, base + 0, "x"))
    go["yA"] = Later(lambda: net.copy(v.at[A], out.at[2, 0, A], sems, base + 3, "y"))
    go["0A"] = Later(lambda: net.copy(v.at[A], out.at[0, 1, A], sems, base + 4, "c"))
    ready(1)
    go["yB"] = Later(lambda: net.copy(v.at[B], out.at[2, 0, B], sems, base + 2, "y"))
    go["xB"] = Later(lambda: net.copy(v.at[B], out.at[1, 0, B], sems, base + 1, "x"))
    go["0B"] = Later(lambda: net.copy(v.at[B], out.at[0, 1, B], sems, base + 5, "c"))
    yield
    go["xA"].wait_recv()
    go["dA"] = Later(lambda: net.copy(out.at[1, 0, A], out.at[3, 0, A], sems, base + 6, "y"))
    go["1A"] = Later(lambda: net.copy(out.at[1, 0, A], out.at[1, 1, A], sems, base + 8, "c"))
    go["yA"].wait_recv()
    go["2A"] = Later(lambda: net.copy(out.at[2, 0, A], out.at[2, 1, A], sems, base + 10, "c"))
    yield
    go["yB"].wait_recv()
    go["dB"] = Later(lambda: net.copy(out.at[2, 0, B], out.at[3, 0, B], sems, base + 7, "x"))
    go["2B"] = Later(lambda: net.copy(out.at[2, 0, B], out.at[2, 1, B], sems, base + 9, "c"))
    go["xB"].wait_recv()
    go["1B"] = Later(lambda: net.copy(out.at[1, 0, B], out.at[1, 1, B], sems, base + 11, "c"))
    yield
    go["dA"].wait_recv()
    go["3A"] = Later(lambda: net.copy(out.at[3, 0, A], out.at[3, 1, A], sems, base + 12, "c"))
    go["dB"].wait_recv()
    go["3B"] = Later(lambda: net.copy(out.at[3, 0, B], out.at[3, 1, B], sems, base + 13, "c"))
    yield
    for name in ("0A", "0B", "1A", "2B", "2A", "1B", "3A", "3B"):
        go[name].wait_recv()
    for copy in go.values():
        copy.wait_send()


def gather_rows(net, v, out, sems, base, ready, poll):
    for _ in gather_steps(net, v, out, sems, base, ready):
        poll()


GATHER_COPIES = 14
SCATTER_COPIES = 10


def scatter_steps(net, parts, rc, rd, rx, ry, td, tx, ty, sems, base):
    n = parts.shape[2]
    A, B = pl.ds(0, n // 2), pl.ds(n // 2, n // 2)
    go = {}
    for i, chip in enumerate((3, 1, 2, 0)):
        go[chip] = Later(lambda i=i, chip=chip: net.copy(parts.at[chip, 1], rc.at[chip], sems, base + i, "c"))

    def add(dst, chip, start, more=None):
        def body(rows):
            total = wide(parts[chip, 0, rows]) + wide(rc[chip, rows])
            if more is not None:
                total = total + wide(more[rows])
            dst[rows] = total.astype(bf16)

        tiles(start, n // 2, body)

    yield None
    go[3].wait_recv()
    add(td, 3, 0)
    go["dA"] = Later(lambda: net.copy(td.at[A], rd.at[A], sems, base + 4, "x"))
    add(td, 3, n // 2)
    go["dB"] = Later(lambda: net.copy(td.at[B], rd.at[B], sems, base + 5, "y"))
    go[1].wait_recv()
    add(tx, 1, 0)
    go["xA"] = Later(lambda: net.copy(tx.at[A], rx.at[A], sems, base + 6, "x"))
    go[2].wait_recv()
    add(ty, 2, n // 2)
    go["yB"] = Later(lambda: net.copy(ty.at[B], ry.at[B], sems, base + 7, "y"))
    yield None
    go["dA"].wait_recv()
    add(ty, 2, 0, rd)
    go["yA"] = Later(lambda: net.copy(ty.at[A], ry.at[A], sems, base + 8, "y"))
    go["dB"].wait_recv()
    add(tx, 1, n // 2, rd)
    go["xB"] = Later(lambda: net.copy(tx.at[B], rx.at[B], sems, base + 9, "x"))
    go[0].wait_recv()

    def done(half):
        for name in (("xA", "yA"), ("xB", "yB"))[half]:
            go[name].wait_recv()
        if half == 1:
            for copy in go.values():
                copy.wait_send()

    yield done


def scatter_rows(net, parts, rc, rd, rx, ry, td, tx, ty, sems, base, poll):
    steps = scatter_steps(net, parts, rc, rd, rx, ry, td, tx, ty, sems, base)
    next(steps)
    next(steps)
    poll()
    return next(steps)


def scatter_scratch(n, w):
    return [pltpu.VMEM((4, n, w), bf16)] + [pltpu.VMEM((n, w), bf16)] * 6


def dma_sems(count):
    return [pltpu.SemaphoreType.DMA((count,)), pltpu.SemaphoreType.DMA((count,))]


VM = pl.BlockSpec(memory_space=pltpu.VMEM)
ANY = pl.BlockSpec(memory_space=pl.ANY)


def polls(*acts):
    left = list(acts)

    def poll():
        if left:
            left.pop(0)()

    def drain():
        while left:
            poll()

    return poll, drain


def comm_call(body, name, ident, ins, in_specs, outs, out_specs, scratch):
    return pl.pallas_call(
        body,
        in_specs=in_specs,
        out_specs=out_specs,
        out_shape=outs,
        scratch_shapes=scratch,
        compiler_params=pltpu.CompilerParams(collective_id=ident, has_side_effects=True, vmem_limit_bytes=63 << 20),
        name=name,
    )(*ins)


def shape(dims, dtype):
    return jax.ShapeDtypeStruct(dims, dtype)


PLANE = ("x", "y", "c", "xy", "xc", "yc", "xyc")
PLACES = {"c": (0, 1), "x": (1, 0), "xc": (1, 1), "y": (2, 0), "yc": (2, 1), "xy": (3, 0), "xyc": (3, 1)}


def start_call(x, dy, docs, gains, taps, w_qkv, w_gate, w_up, w_out, ident):
    n, w = x.shape
    rows = w_qkv.shape[0]

    def body(x_ref, dy_ref, docs_ref, g_ref, taps_ref, wq_ref, gate_ref, up_ref, wo_ref,
             a1_ref, dys_ref, docs_out, gains_ref, qkv_out, gu_out, wo_out, th_ref, tl_ref, tt_ref,
             xs, gains_out, slots, gus, local, send, recv):
        net = Net()
        sems = (send, recv)
        base = 2 * GATHER_COPIES
        mine = dy_ref.at[pl.ds(0, n // 2)]
        line_q = GatherLine(net, qkv_out.at[net.z], qkv_out, sems, base)
        line_o = GatherLine(net, wo_ref, wo_out, sems, base + 6, lambda slot: slot // 2 == net.x)
        line_g = GatherLine(net, gains_out.at[net.z], gains_out, sems, base + 12)
        base += 18
        gains_out[net.z, net.k] = g_ref[...]
        slots[...] = jnp.zeros_like(slots)
        for half in range(2):

            @pl.when(net.x == half)
            def _():
                for k in range(4):
                    pair = 4 * half + 2 * (k % 2) + k // 2
                    for m in range(6):
                        col = (m // 2) * MODEL_WIDTH + (2 * pair + m % 2) * E
                        slots[k, :, m * EP : m * EP + E] = wq_ref[:, col : col + E]
                    for m in range(8):
                        src = gate_ref if m < 4 else up_ref
                        col = 256 * (4 * (m % 4) + k) + 128 * half
                        gus[k, :, m * 128 : (m + 1) * 128] = src[:, col : col + 128]

        net.greet(PLANE)
        own = [
            pltpu.make_async_copy(mine, dys_ref.at[0, 0], local.at[1]),
            pltpu.make_async_copy(slots.at[net.k], qkv_out.at[net.z, net.k], local.at[0]),
            pltpu.make_async_copy(gus.at[net.k], gu_out.at[net.k], local.at[2]),
            pltpu.make_async_copy(docs_ref, docs_out.at[0, 0], local.at[3]),
            pltpu.make_async_copy(wo_ref, wo_out.at[net.z], local.at[4]),
        ]
        for copy in own:
            copy.start()
        qkv_parts, gain_parts, small = [], [], []
        flips = {"c": net.k + 1 - 2 * net.c, "y": net.k + 2 - 4 * net.y, "yc": net.k + 1 - 2 * net.c + 2 - 4 * net.y}
        for j, name in enumerate(("y", "yc", "c")):
            gain_parts.append(net.send(g_ref, gains_out.at[net.z, net.k], sems, base + 6 + j, name))
            qkv_parts.append(net.send(slots.at[flips[name]], qkv_out.at[net.z, net.k], sems, base + j, name))
        line_o.step(0)
        for j, (name, (chip, core)) in enumerate(PLACES.items()):
            small.append(net.send(docs_ref, docs_out.at[chip, core], sems, base + 9 + j, name))
        gather_x = gather_steps(net, x_ref, xs, sems, 0, lambda half: None)
        next(gather_x)
        gather_dy = gather_steps(net, mine, dys_ref, sems, GATHER_COPIES, lambda half: None)
        next(gather_dy)
        for copy in gain_parts:
            copy.wait_recv()
        line_g.step(0)
        own[1].wait()
        for copy in qkv_parts:
            copy.wait_recv()
        line_q.step(0)
        line_g.step(1)

        diff = lax.broadcasted_iota(jnp.int32, (n, n), 1) - lax.broadcasted_iota(jnp.int32, (n, n), 0)

        def bands_of(first, count):
            def one(i, _):
                band = jnp.zeros((n, n), f32)
                back = jnp.zeros((n, n), f32)
                for b in range(KWIN):
                    tap = taps_ref[(first + i) * KWIN + b]
                    band = jnp.where(diff == b, tap, band)
                    back = jnp.where(diff == -b, tap, back)
                h, a = (first + i) // QWIN, (first + i) % QWIN
                at = pl.ds(pl.multiple_of(a * n, n), n)
                th_ref[h, at], tl_ref[h, at] = split(band)
                tt_ref[h, at] = back.astype(bf16)
                return 0

            lax.fori_loop(0, count, one, 0)

        bands_of(0, QWIN)
        line_g.step(2)
        next(gather_x)
        line_q.step(1)
        line_g.step(3)
        line_o.step(1)
        for i in range(16):
            gains_ref[:, i * rows : (i + 1) * rows] = wide(gains_out[i // 4, i % 4, 0:8, 0:rows])
        bands_of(QWIN, QWIN)
        next(gather_x)
        for j, name in enumerate(("y", "yc", "c")):
            small.append(net.send(gus.at[flips[name]], gu_out.at[net.k], sems, base + 3 + j, name))
        gain = gains_ref[0:1]

        def norm(chip, core, src):
            def body(at):
                xf = wide(src[at])
                r = lax.rsqrt(jnp.mean(xf * xf, axis=1, keepdims=True) + 1e-06)
                a1_ref[chip, core, at] = (xf * r * gain).astype(bf16)

            tiles(0, n, body)

        norm(0, 0, x_ref)
        line_q.step(2)
        line_o.step(2)
        for _ in gather_x:
            pass
        next(gather_dy)
        next(gather_dy)
        for chip in range(4):
            for core in range(2):
                if (chip, core) != (0, 0):
                    norm(chip, core, xs.at[chip, core])
        next(gather_dy)
        line_q.step(3)
        for _ in gather_dy:
            pass
        line_o.step(3)
        for line in (line_q, line_g, line_o):
            line.finish()
        for copy in own[:1] + own[2:]:
            copy.wait()
        for copy in small:
            copy.wait_recv()
        for copy in qkv_parts + gain_parts + small:
            copy.wait_send()

    return comm_call(
        body, "start", ident, (x, dy, docs, gains, taps, w_qkv, w_gate, w_up, w_out),
        [VM] * 4 + [pl.BlockSpec(memory_space=pltpu.SMEM)] + [VM] * 4,
        [shape((4, 2, n, w), bf16), shape((4, 2, n // 2, w), bf16), shape((4, 2) + docs.shape, docs.dtype), shape((8, w), f32),
         shape((4, 4, rows, 6 * EP), bf16), shape((4, rows, FF // 4), bf16), shape((4, rows, MODEL_WIDTH), bf16)]
        + [shape((2, QWIN * n, n), bf16)] * 3,
        [VM, ANY, ANY, VM, ANY, ANY, ANY, VM, VM, VM],
        [pltpu.VMEM((4, 2, n, w), bf16), pltpu.VMEM((4, 4) + gains.shape, bf16),
         pltpu.VMEM((4, rows, 6 * EP), bf16), pltpu.VMEM((4, rows, FF // 4), bf16), pltpu.SemaphoreType.DMA((5,))]
        + dma_sems(2 * GATHER_COPIES + 18 + 16),
    )


def forward_call(mix, a1, dcol, drow, th, tl, group, qkv_w, out_w, x, dy, gain, gu, w_down, ident):
    rows, t, w = a1.shape
    n = x.shape[0]
    down = w_down.shape[0] // 2

    def body(mix_ref, a1_ref, dcol_ref, drow_ref, th_ref, tl_ref, group_ref, qw_ref, ow_ref, x_ref, dy_ref, g_ref, gu_ref, wd_ref,
             qkv_ref, normed_ref, xhat_ref, s_ref, p_ref, z_ref, resid_ref, out_ref, dys_ref, gu_out, wd_out,
             parts, v, local, rc, rd, rx, ry, td, tx, ty, send, recv):
        net = Net()
        sems = (send, recv)
        step = pl.program_id(0)
        base = SCATTER_COPIES + GATHER_COPIES
        mine = wd_ref.at[pl.ds(pl.multiple_of(down * net.x, down), down)]
        line_g = GatherLine(net, gu_ref, gu_out, sems, base)
        line_d = GatherLine(net, mine, wd_out, sems, base + LINE_COPIES)
        own_g = lambda: pltpu.make_async_copy(gu_ref, gu_out.at[net.z], local.at[1])
        own_d = lambda: pltpu.make_async_copy(mine, wd_out.at[net.z], local.at[2])
        A, B = pl.ds(0, n // 2), pl.ds(n // 2, n // 2)
        go = {}
        half_dy = dy_ref.at[pl.ds(n // 2, n // 2)]
        own_dy = lambda: pltpu.make_async_copy(half_dy, dys_ref.at[0, 0], local.at[3])
        gather_dy = gather_steps(net, half_dy, dys_ref, sems, base + 2 * LINE_COPIES, lambda half: None)

        def at(i):
            def run(act):
                pl.when(step == i)(act)

            return run

        @at(0)
        def _():
            net.greet("xyc")
            line_g.step(0)
            line_d.step(0)
            own_g().start()
            own_d().start()
            own_dy().start()
            next(gather_dy)

        qkv_ref[0] = dot(a1_ref[0], qw_ref[...]).astype(bf16)
        attend_row(mix_ref, qkv_ref, dcol_ref, drow_ref, th_ref, tl_ref, group_ref, normed_ref, xhat_ref, s_ref, p_ref, z_ref)
        parts[3 - step // 2, step % 2] = dot(normed_ref[0], ow_ref[...]).astype(bf16)

        def swap(chip, i):
            go[chip] = Later(lambda: net.copy(parts.at[chip, 1], rc.at[chip], sems, i, "c"))

        def add(dst, chip, start, more=None):
            def one(r):
                total = wide(parts[chip, 0, r]) + wide(rc[chip, r])
                if more is not None:
                    total = total + wide(more[r])
                dst[r] = total.astype(bf16)

            tiles(start, n // 2, one)

        @at(1)
        def _():
            swap(3, 0)

        @at(2)
        def _():
            go[3].wait_recv()
            add(td, 3, 0)
            go["dA"] = Later(lambda: net.copy(td.at[A], rd.at[A], sems, 4, "x"))
            add(td, 3, n // 2)
            go["dB"] = Later(lambda: net.copy(td.at[B], rd.at[B], sems, 5, "y"))

        @at(3)
        def _():
            swap(2, 2)
            line_g.step(1)
            next(gather_dy)

        @at(4)
        def _():
            go[2].wait_recv()
            add(ty, 2, n // 2)
            go["yB"] = Later(lambda: net.copy(ty.at[B], ry.at[B], sems, 7, "y"))
            go["dA"].wait_recv()
            add(ty, 2, 0, rd)
            go["yA"] = Later(lambda: net.copy(ty.at[A], ry.at[A], sems, 8, "y"))
            next(gather_dy)

        @at(5)
        def _():
            swap(1, 1)
            line_d.step(1)
            next(gather_dy)

        @at(6)
        def _():
            go[1].wait_recv()
            add(tx, 1, 0)
            go["xA"] = Later(lambda: net.copy(tx.at[A], rx.at[A], sems, 6, "x"))
            go["dB"].wait_recv()
            add(tx, 1, n // 2, rd)
            go["xB"] = Later(lambda: net.copy(tx.at[B], rx.at[B], sems, 9, "x"))

        @at(rows - 1)
        def _():
            swap(0, 3)
            line_g.step(2)
            for _ in gather_dy:
                pass
            go[0].wait_recv()

            def ready(half):
                for name in (("yA", "xA"), ("yB", "xB"))[half]:
                    go[name].wait_recv()

                def rows_of(r):
                    total = wide(parts[0, 0, r]) + wide(rc[0, r]) + wide(rx[r]) + wide(ry[r])
                    resid = wide(x_ref[r]) + total
                    resid_ref[r] = resid
                    inv = lax.rsqrt(jnp.mean(resid * resid, axis=1, keepdims=True) + 1e-06)
                    v[r] = (resid * inv * g_ref[...]).astype(bf16)

                tiles(half * (n // 2), n // 2, rows_of)

            poll, drain = polls(lambda: line_d.step(2), lambda: line_g.step(3), lambda: line_d.step(3))
            gather_rows(net, v, out_ref, sems, SCATTER_COPIES, ready, poll)
            drain()
            last = pltpu.make_async_copy(v, out_ref.at[0, 0], local.at[0])
            last.start()
            line_g.finish()
            line_d.finish()
            own_g().wait()
            own_d().wait()
            own_dy().wait()
            for copy in go.values():
                copy.wait_send()
            last.wait()

    where = lambda i: 2 * (3 - i // 2) + i % 2
    row = lambda *sh: pl.BlockSpec((1,) + sh, lambda i: (where(i),) + (0,) * len(sh))
    full = lambda v: pl.BlockSpec(v.shape, lambda i: (0,) * v.ndim, pipeline_mode=pl.Buffered(1))
    keep = lambda *sh: pl.BlockSpec(sh, lambda i: (0,) * len(sh))
    return pl.pallas_call(
        body,
        grid=(rows,),
        in_specs=[pl.BlockSpec(memory_space=pltpu.SMEM), row(t, w), row(t, 1), row(1, t), full(th), full(tl), full(group), full(qkv_w),
                  full(out_w), full(x), full(dy), full(gain), full(gu), full(w_down)],
        out_specs=[row(t, 6 * EP), row(t, 2 * EP), row(t, 2 * EP), row(t, 2 * EP), row(2, t, t), row(2, t, t), keep(n, w), ANY, ANY, ANY, ANY],
        out_shape=[
            shape((rows, t, 6 * EP), bf16),
            shape((rows, t, 2 * EP), bf16),
            shape((rows, t, 2 * EP), f32),
            shape((rows, t, 2 * EP), f32),
            shape((rows, 2, t, t), f32),
            shape((rows, 2, t, t), bf16),
            shape((n, w), f32),
            shape((4, 2, n, w), bf16),
            shape((4, 2, n // 2, w), bf16),
            shape((4,) + gu.shape, bf16),
            shape((4, down, w), bf16),
        ],
        scratch_shapes=[pltpu.VMEM((4, 2, n, w), bf16), pltpu.VMEM((n, w), bf16), pltpu.SemaphoreType.DMA((4,))] + scatter_scratch(n, w)
        + dma_sems(SCATTER_COPIES + 2 * GATHER_COPIES + 2 * LINE_COPIES),
        compiler_params=pltpu.CompilerParams(collective_id=ident, has_side_effects=True, vmem_limit_bytes=60 << 20),
        name="forward",
    )(mix, a1, dcol, drow, th, tl, group, qkv_w, out_w, x, dy, gain, gu, w_down)


def ffn_call(a2, first, second, gu_w, down_w):
    count, w = a2.shape
    half = down_w.shape[0]
    m = count // 4
    part = half // 2

    def body(a2_ref, df1_ref, df2_ref, gw_ref, dw_ref, dgu_ref, hid_ref, gd_ref, df_ref, total):
        step = pl.program_id(0)

        @pl.when(step == 0)
        def _():
            total[...] = jnp.zeros_like(total)

        q = m // 4
        for i in range(2):
            df_ref[2 * i * q : (2 * i + 1) * q] = df1_ref[i * q : (i + 1) * q]
            df_ref[(2 * i + 1) * q : (2 * i + 2) * q] = df2_ref[i * q : (i + 1) * q]
        for j in range(2):
            cols, more = slice(j * part, (j + 1) * part), slice(half + j * part, half + (j + 1) * part)
            gate, up_act = dot(a2_ref[...], gw_ref[:, cols]), dot(a2_ref[...], gw_ref[:, more])
            dhidden = dot(df_ref[...], dw_ref[cols], 1, 1)
            sig = jax.nn.sigmoid(gate)
            silu = gate * sig
            hid_ref[:, cols] = (silu * up_act).astype(bf16)
            dgu_ref[:, cols] = (dhidden * up_act * sig * (1.0 + gate * (1.0 - sig))).astype(bf16)
            dgu_ref[:, more] = (dhidden * silu).astype(bf16)
        total[...] += dot(hid_ref[...], df_ref[...], 0, 0)

        @pl.when(step == 3)
        def _():
            gd_ref[...] = total[...].astype(bf16)

    row = lambda k, m=m: pl.BlockSpec((m, k), lambda i: (i, 0))
    full = lambda v: pl.BlockSpec(v.shape, lambda i: (0, 0), pipeline_mode=pl.Buffered(1))
    return pl.pallas_call(
        body,
        grid=(4,),
        in_specs=[row(w), row(w, m // 2), row(w, m // 2), full(gu_w), full(down_w)],
        out_specs=[row(2 * half), row(half), pl.BlockSpec((half, w), lambda i: (0, 0))],
        out_shape=[shape((count, 2 * half), bf16), shape((count, half), bf16), shape((half, w), bf16)],
        scratch_shapes=[pltpu.VMEM((m, w), bf16), pltpu.VMEM((half, w), f32)],
        compiler_params=pltpu.CompilerParams(vmem_limit_bytes=40 << 20),
        name="ffn",
    )(a2, first, second, gu_w, down_w)


def mid_back_call(dgu, gu_w, a2, hidden, down_w, dy, resid, gain, down, ident):
    n, w = dy.shape
    m, half = dgu.shape[0] // 4, gu_w.shape[1] // 2

    def body(dgu_ref, gw_ref, a2_ref, hid_ref, dw_ref, dy_ref, r_ref, g_ref, down_ref,
             dresid_ref, out_ref, sum_ref, down_out, gate_out, up_out, op_out,
             parts, a2s, hids, dws, stage, gates, v, local, rc, rd, rx, ry, td, tx, ty, d_got, d_made, g_got, g_made, send, recv):
        net = Net()
        sems = (send, recv)
        net.greet("xyc")
        base = SCATTER_COPIES + GATHER_COPIES
        line_d = ScatterLine(net, down_ref, d_got, d_made, sems, base)
        line_g = ScatterLine(net, gates, g_got, g_made, sems, base + LINE_COPIES)
        line_d.step(0)
        loads = [pltpu.make_async_copy(src, dst, local.at[i]) for i, (src, dst) in enumerate(((a2_ref, a2s), (hid_ref, hids), (dw_ref, dws)))]
        for copy in loads:
            copy.start()
        A, B = pl.ds(0, n // 2), pl.ds(n // 2, n // 2)
        go = {}

        def part(chip):
            for j in range(3):
                cols = slice(j * (w // 3), (j + 1) * (w // 3))
                total = dot(dgu_ref[chip * m : (chip + 1) * m], gw_ref[cols], 1, 1)
                parts[chip, :, :, cols] = total.astype(bf16).reshape(2, n, w // 3)

        def swap(chip, i):
            go[chip] = Later(lambda: net.copy(parts.at[chip, 1], rc.at[chip], sems, i, "c"))

        def add(dst, chip, start, more=None):
            def one(r):
                total = wide(parts[chip, 0, r]) + wide(rc[chip, r])
                if more is not None:
                    total = total + wide(more[r])
                dst[r] = total.astype(bf16)

            tiles(start, n // 2, one)

        def weights(first, last):
            for i in range(first, last):
                rows = slice(i * (w // 4), (i + 1) * (w // 4))
                total = dot(a2s[:, rows], dgu_ref[...], 0, 0)
                gates[i] = total[:, :half].astype(bf16)
                up_out[i] = total[:, half:].astype(bf16)

        def put_back(chip):
            return pltpu.make_async_copy(stage.at[chip % 2], op_out.at[chip], local.at[4 + chip % 2])

        def forward(chip):
            if chip >= 2:
                put_back(chip - 2).wait()
            for j in range(3):
                cols = slice(j * (w // 3), (j + 1) * (w // 3))
                total = dot(hids[chip * m : (chip + 1) * m], dws[:, cols])
                stage[chip % 2, :, :, cols] = total.astype(bf16).reshape(2, n, w // 3)
            put_back(chip).start()

        part(3)
        swap(3, 0)
        part(2)
        swap(2, 2)
        go[3].wait_recv()
        add(td, 3, 0)
        go["dA"] = Later(lambda: net.copy(td.at[A], rd.at[A], sems, 4, "x"))
        add(td, 3, n // 2)
        go["dB"] = Later(lambda: net.copy(td.at[B], rd.at[B], sems, 5, "y"))
        part(1)
        swap(1, 1)
        go[2].wait_recv()
        add(ty, 2, n // 2)
        go["yB"] = Later(lambda: net.copy(ty.at[B], ry.at[B], sems, 7, "y"))
        part(0)
        swap(0, 3)
        go[1].wait_recv()
        add(tx, 1, 0)
        go["xA"] = Later(lambda: net.copy(tx.at[A], rx.at[A], sems, 6, "x"))
        loads[0].wait()
        go["dA"].wait_recv()
        add(ty, 2, 0, rd)
        go["yA"] = Later(lambda: net.copy(ty.at[A], ry.at[A], sems, 8, "y"))
        go["dB"].wait_recv()
        add(tx, 1, n // 2, rd)
        go["xB"] = Later(lambda: net.copy(tx.at[B], rx.at[B], sems, 9, "x"))
        weights(0, 4)
        line_g.step(0)
        line_d.step(1)
        loads[1].wait()
        loads[2].wait()
        sum_ref[...] = jnp.zeros_like(sum_ref)
        go[0].wait_recv()

        def ready(side):
            for name in (("xA", "yA"), ("xB", "yB"))[side]:
                go[name].wait_recv()

            def rows_of(r):
                da2 = wide(parts[0, 0, r]) + wide(rc[0, r]) + wide(rx[r]) + wide(ry[r])
                res = r_ref[r]
                inv = lax.rsqrt(jnp.mean(res * res, axis=1, keepdims=True) + 1e-06)
                unit = res * inv
                sum_ref[0:1] += jnp.sum(da2 * unit, axis=0, keepdims=True)
                dn = da2 * g_ref[...]
                dresid = wide(dy_ref[r]) + inv * (dn - unit * inv * jnp.mean(dn * res, axis=1, keepdims=True))
                dresid_ref[r] = dresid
                v[r] = dresid.astype(bf16)

            tiles(side * (n // 2), n // 2, rows_of)

        poll, drain = polls(
            lambda: (forward(0), forward(1)), lambda: (line_d.step(2), line_g.step(1)), lambda: (forward(2), forward(3)), lambda: line_g.step(2)
        )
        gather_rows(net, v, out_ref, sems, SCATTER_COPIES, ready, poll)
        drain()
        last = pltpu.make_async_copy(v, out_ref.at[0, 0], local.at[3])
        last.start()

        def put(ref):
            def store(r, total):
                ref[r] = total.astype(bf16)

            return store

        line_d.finish(put(down_out))
        line_g.finish(put(gate_out))
        for copy in go.values():
            copy.wait_send()
        put_back(2).wait()
        put_back(3).wait()
        last.wait()

    return comm_call(
        body, "mid_back", ident, (dgu, gu_w, a2, hidden, down_w, dy, resid, gain, down), [VM] * 2 + [ANY] * 3 + [VM] * 4,
        [shape((n, w), f32), shape((4, 2, n, w), bf16), shape((8, w), f32), shape(down.shape[1:], bf16), shape((w // 4, half), bf16),
         shape((4, w // 4, half), bf16), shape((4, 2, n, w), bf16)],
        [VM, ANY, VM, VM, VM, VM, ANY],
        [pltpu.VMEM((4, 2, n, w), bf16), pltpu.VMEM(a2.shape, bf16), pltpu.VMEM(hidden.shape, bf16), pltpu.VMEM(down_w.shape, bf16),
         pltpu.VMEM((2, 2, n, w), bf16), pltpu.VMEM((4, w // 4, half), bf16), pltpu.VMEM((n, w), bf16), pltpu.SemaphoreType.DMA((6,))]
        + scatter_scratch(n, w) + line_scratch(*down.shape[1:]) + line_scratch(w // 4, half)
        + dma_sems(SCATTER_COPIES + GATHER_COPIES + 2 * LINE_COPIES),
    )


class Home:
    def __init__(self, net, zq, cq, fq, sems, base):
        self.net, self.zq, self.cq, self.fq, self.sems, self.base = net, zq, cq, fq, sems, base
        self.r = cq.shape[2]

    def rows(self, i, j):
        return pl.ds(pl.multiple_of((2 * i + j) * self.r, self.r), self.r)

    def over_c(self, i):
        net = self.net
        return net.copy(self.zq.at[self.rows(i, 1 - net.c)], self.cq.at[i, net.c], self.sems, self.base + i, "c")

    def over_y(self):
        net = self.net
        return net.copy(self.cq.at[1 - net.y], self.fq.at[net.x, net.y], self.sems, self.base + 2, "y")

    def over_x(self):
        net = self.net
        return net.copy(self.fq.at[net.x], self.fq.at[net.x], self.sems, self.base + 3, "x")

    def step(self, d):
        net = self.net
        if d == 0:
            for i in range(2):
                self.over_c(i).start()
                self.cq[i, net.c] = self.zq[self.rows(i, net.c)]
        elif d == 1:
            for i in range(2):
                self.over_c(i).wait_recv()
            self.over_y().start()
            self.fq[net.x, net.y] = self.cq[net.y]
        elif d == 2:
            self.over_y().wait_recv()
            self.over_x().start()
        else:
            self.over_x().wait_recv()

    def finish(self):
        for i in range(2):
            self.over_c(i).wait_send()
        self.over_y().wait_send()
        self.over_x().wait_send()

    def spread(self, dst):
        for i in range(2):
            for k in range(4):
                for m in range(4):
                    col = 256 * (4 * m + k) + 128 * i
                    dst[:, col : col + 128] = wide(self.fq[i, k // 2, k % 2, :, m * 128 : (m + 1) * 128])


HOME_COPIES = 4


def home_scratch(r, k):
    return [pltpu.VMEM((2, 2, r, k), bf16), pltpu.VMEM((2, 2, 2, r, k), bf16)]


def end_call(da_parts, qkv, wo, gate_up, small, x, dresid, gain, ident):
    n, w = da_parts.shape[2:]
    rows, wide_q = qkv.shape[2] // 4, qkv.shape[3]

    def body(da_ref, q_ref, wo_ref, up_ref, small_ref, x_ref, dresid_ref, g_ref,
             gx_ref, gq_ref, go_ref, gu_ref, total_ref,
             rc, rd, rx, ry, td, tx, ty, q_got, q_made, zq, cq, fq, cu, fu, ro, s_got, s_sum, s_line, send, recv):
        net = Net()
        sems = (send, recv)
        net.greet("xyc")
        base = SCATTER_COPIES
        lines = [ScatterLine(net, q_ref.at[i], q_got.at[i], q_made.at[i], sems, base + 6 * i) for i in range(2)]
        line_s = GatherLine(net, s_sum.at[2], s_line, sems, base + 12)
        base += 18
        homes = [Home(net, zq.at[i], cq.at[i], fq.at[i], sems, base + 4 * i) for i in range(2)]
        home_u = Home(net, up_ref, cu, fu, sems, base + 8)
        base += 12
        for line in lines:
            line.step(0)
        hops = [net.send(small_ref, s_got.at[0], sems, base, "c")]
        home_u.step(0)

        def small_step(i):
            hops[i].wait_recv()
            s_sum[i] = (small_ref[...] if i == 0 else s_sum[i - 1]) + s_got[i]
            if i < 2:
                hops.append(net.send(s_sum.at[i], s_got.at[i + 1], sems, base + 1 + i, "yx"[i]))
            else:
                line_s.step(0)

        scatter = scatter_steps(net, da_ref, rc, rd, rx, ry, td, tx, ty, sems, 0)
        next(scatter)
        small_step(0)
        next(scatter)
        home_u.step(1)
        swap_o = net.send(wo_ref, ro, sems, base + 3, "x")
        lines[0].step(1)
        small_step(1)
        done = next(scatter)
        lines[1].step(1)
        home_u.step(2)
        small_step(2)
        lines[0].step(2)
        line_s.step(1)
        lines[1].step(2)
        line_s.step(2)
        for half in range(2):
            done(half)

            def rows_of(at):
                da = wide(da_ref[0, 0, at]) + wide(rc[0, at]) + wide(rx[at]) + wide(ry[at])
                xf = wide(x_ref[at])
                r = lax.rsqrt(jnp.mean(xf * xf, axis=1, keepdims=True) + 1e-06)
                dn = da * g_ref[...]
                gx_ref[at] = dresid_ref[at] + r * (dn - xf * r * r * jnp.mean(dn * xf, axis=1, keepdims=True))

            tiles(half * (n // 2), n // 2, rows_of)

        for i in range(2):

            def put(at, total):
                zq[i, at] = total.astype(bf16)

            lines[i].finish(put)
            homes[i].step(0)
        homes[0].step(1)
        homes[1].step(1)
        homes[0].step(2)
        homes[1].step(2)
        line_s.step(3)
        s_line[net.z] = s_sum[2]
        total_ref[...] = (s_line[0] + s_line[1]) + (s_line[2] + s_line[3])
        swap_o.wait_recv()
        go_ref[...] = wide(wo_ref[...]) + wide(ro[...])
        home_u.step(3)
        home_u.spread(gu_ref)
        for part in range(2):
            homes[part].step(3)
            for i in range(2):
                for k in range(4):
                    pair = 4 * i + 2 * (k % 2) + k // 2
                    for m in range(3):
                        to = 3 * part + m
                        col = (to // 2) * MODEL_WIDTH + (2 * pair + to % 2) * E
                        gq_ref[:, col : col + E] = wide(fq[part, i, k // 2, k % 2, :, m * EP : m * EP + E])
        line_s.finish()
        for home in homes + [home_u]:
            home.finish()
        for copy in hops + [swap_o]:
            copy.wait_send()

    two = lambda specs: [pltpu.VMEM((2,) + v.shape, v.dtype) for v in specs]
    return comm_call(
        body, "end", ident, (da_parts, qkv, wo, gate_up, small, x, dresid, gain), [VM] * 8,
        [shape((n, w), f32), shape((rows, 3 * MODEL_WIDTH), f32), shape(wo.shape, f32), shape((rows, FF), f32), shape(small.shape, f32)],
        [VM] * 5,
        scatter_scratch(n, w) + two(line_scratch(4 * rows, wide_q)) + two([pltpu.VMEM((4 * rows, wide_q), bf16)])
        + two(home_scratch(rows, wide_q)) + home_scratch(rows, FF // 8) + [pltpu.VMEM(wo.shape, bf16)]
        + [pltpu.VMEM((3,) + small.shape, f32), pltpu.VMEM((3,) + small.shape, f32), pltpu.VMEM((4,) + small.shape, f32)]
        + dma_sems(SCATTER_COPIES + 18 + 12 + 4),
    )


def back_call(mix, qkv, dcol, drow, tt, gain, dattn, xhat, s, p, z, a1, out_w, qkv_w, out_parts, up_parts, wo, gate, down, resid, ident):
    rows, t, _ = qkv.shape
    n, w = out_parts.shape[2:]
    rows_o, rows_d, wide_q = wo.shape[1], down.shape[0], 3 * EP

    def body(mix_ref, qkv_ref, dcol_ref, drow_ref, tt_ref, gain_ref, dattn_ref, xhat_ref, s_ref, p_ref, z_ref, a1_ref,
             ow_ref, qw_ref, op_ref, gu_ref, wo_ref, gate_ref, down_ref, resid_ref,
             da_ref, q16_ref, sum_ref, gconv_ref, gmix_ref, gg_ref, out_ref, gu_out, go_out, gg_out, gd_ref,
             m_ref, gq_ref, dq, rc, rd, rx, ry, td, tx, ty, g_got, g_made, o_got, o_made, po, cg, fg, fd, send, recv):
        net = Net()
        sems = (send, recv)
        step = pl.program_id(0)
        base = SCATTER_COPIES
        line = ScatterLine(net, gu_ref, g_got, g_made, sems, base)
        line_o = ScatterLine(net, po, o_got, o_made, sems, base + 6)
        home = Home(net, gate_ref, cg, fg, sems, base + 12)
        x, c = net.x, net.c
        to_c = lambda: net.copy(wo_ref.at[1 - c], po.at[2 * x + c], sems, base + 16, "c")
        to_x = lambda: net.copy(down_ref, fd.at[x], sems, base + 17, "x")
        scatter = scatter_steps(net, op_ref, rc, rd, rx, ry, td, tx, ty, sems, 0)

        @pl.when(step == 0)
        def _():
            net.greet("xyc")
            line.step(0)
            to_c().start()
            next(scatter)
            home.step(0)
            po[2 * (1 - x)] = jnp.zeros((rows_o, w), bf16)
            po[2 * (1 - x) + 1] = jnp.zeros((rows_o, w), bf16)
            po[2 * x + c] = wo_ref[c]
            fd[x] = down_ref[...]
            m_ref[...] = jnp.zeros_like(m_ref)
            gmix_ref[...] = jnp.zeros_like(gmix_ref)
            gg_ref[...] = jnp.zeros_like(gg_ref)
            gq_ref[...] = jnp.zeros_like(gq_ref)

        allowed = allowed_mask(dcol_ref[0], drow_ref[0])
        scale = 1.0 / math.sqrt(E)
        lane = lax.broadcasted_iota(jnp.int32, (1, EP), 1)
        prob = [p_ref[0, 0], p_ref[0, 1]]
        dmixed = []
        for h in range(2):
            cols = slice(h * EP, (h + 1) * EP)
            dn, xh = dot(dattn_ref[0], ow_ref[cols], 1, 1), xhat_ref[0, :, cols]
            gg_ref[0:1, cols] += jnp.sum(dn * xh, axis=0, keepdims=True)
            dc = dn * gain_ref[0:1, cols]
            m1 = jnp.sum(dc, axis=1, keepdims=True) / E
            m2 = jnp.sum(dc * xh, axis=1, keepdims=True) / E
            dh = jnp.where(lane < E, s_ref[0, :, cols] * (dc - m1 - xh * m2), 0.0).astype(bf16)
            v = qkv_ref[0, :, (4 + h) * EP : (5 + h) * EP]
            mixed = (mix_ref[h, 0] * prob[0] + mix_ref[h, 1] * prob[1]).astype(bf16)
            dmixed.append(dot(dh, v, 1, 1))
            dq[:, (4 + h) * EP : (5 + h) * EP] = dot(mixed, dh, 0, 0).astype(bf16)
        for h in range(2):
            for c in range(2):
                r = 2 * h + c
                gmix_ref[r : r + 1, :] += jnp.sum(dmixed[h] * prob[c], axis=0, keepdims=True)
        for c in range(2):
            dp = mix_ref[0, c] * dmixed[0] + mix_ref[1, c] * dmixed[1]
            dconv = prob[c] * (dp - jnp.sum(dp * prob[c], axis=1, keepdims=True))
            ahead = jnp.concatenate([up(dconv, a).astype(bf16) for a in range(QWIN)], 1)
            m_ref[c] += dot(z_ref[0, c], ahead, 0, 0)
            ds = jnp.where(allowed, dot(ahead, tt_ref[c]), 0.0).astype(bf16)
            q = qkv_ref[0, :, c * EP : (c + 1) * EP]
            k = qkv_ref[0, :, (2 + c) * EP : (3 + c) * EP]
            dq[:, c * EP : (c + 1) * EP] = (dot(ds, k) * scale).astype(bf16)
            dq[:, (2 + c) * EP : (3 + c) * EP] = (dot(ds, q, 0, 0) * scale).astype(bf16)
        da_ref[0] = dot(dq[...], qw_ref[...], 1, 1).astype(bf16)
        for i in range(0, w, 384):
            gq_ref[i : i + 384] += dot(a1_ref[0, :, i : i + 384], dq[...], 0, 0)

        done = []

        @pl.when(step == 1)
        def _():
            next(scatter)
            to_c().wait_recv()
            line_o.step(0)
            home.step(1)
            to_x().start()

        @pl.when(step == 2)
        def _():
            line.step(1)
            done.append(next(scatter))

        @pl.when(step == 3)
        def _():
            line_o.step(1)
            home.step(2)

        @pl.when(step == 4)
        def _():
            line.step(2)

        @pl.when(step == 5)
        def _():
            line_o.step(2)

        @pl.when(step == rows - 1)
        def _():
            lanes = lax.broadcasted_iota(jnp.int32, (8, t), 1)
            for h in range(2):
                for a in range(QWIN):
                    total = jnp.zeros((8, t), f32)
                    for first in range(0, t, 8):
                        part = m_ref[h, first : first + 8, a * t : (a + 1) * t]
                        turned = pltpu.roll(part, t - first, 1) if first else part
                        total = total + jnp.where(lanes < t - first, turned, 0.0)
                    gconv_ref[h, a] = total[:, :EP]
            for half in range(2):
                done[0](half)

                def sum_of(at):
                    total = wide(op_ref[0, 0, at]) + wide(rc[0, at]) + wide(rx[at]) + wide(ry[at])
                    out_ref[at] = (resid_ref[at] + total).astype(bf16)

                tiles(half * (n // 2), n // 2, sum_of)

            def put(at, total):
                gu_out[at] = total.astype(bf16)

            line.finish(put)

            def put_o(at, total):
                go_out[at] = total.astype(bf16)

            line_o.finish(put_o)
            to_x().wait_recv()
            for i in range(2):
                gd_ref[i * rows_d : (i + 1) * rows_d] = wide(fd[i])
            home.step(3)
            home.spread(gg_out)
            home.finish()
            to_x().wait_send()
            to_c().wait_send()
            for i in range(0, w, 384):
                part = gq_ref[i : i + 384]
                for j in range(2):
                    q16_ref[j, i : i + 384] = part[:, j * wide_q : (j + 1) * wide_q].astype(bf16)
                sum_ref[:, i : i + 384] = lax.dot_general(
                    jnp.ones((8, 6 * EP), f32), part * wide(qw_ref[i : i + 384]), (((1,), (1,)), ((), ())),
                    precision=lax.Precision.HIGHEST, preferred_element_type=f32,
                )

    row = lambda *sh: pl.BlockSpec((1,) + sh, lambda i: (i,) + (0,) * len(sh))
    full = lambda v: pl.BlockSpec(v.shape, lambda i: (0,) * v.ndim, pipeline_mode=pl.Buffered(1))
    keep = lambda *sh: pl.BlockSpec(sh, lambda i: (0,) * len(sh))
    return pl.pallas_call(
        body,
        grid=(rows,),
        in_specs=[pl.BlockSpec(memory_space=pltpu.SMEM), row(t, 6 * EP), row(t, 1), row(1, t), full(tt), full(gain),
                  row(t, w), row(t, 2 * EP), row(t, 2 * EP), row(2, t, t), row(2, t, t), row(t, w),
                  full(out_w), full(qkv_w), full(out_parts), full(up_parts), full(wo), full(gate), full(down), full(resid)],
        out_specs=[row(t, w), keep(2, w, wide_q), keep(8, w), keep(2, QWIN, 8, EP), keep(8, t), keep(8, 2 * EP), keep(n, w),
                   keep(*up_parts.shape[1:]), keep(rows_o, w), keep(rows_o, FF), keep(2 * rows_d, w)],
        out_shape=[
            shape((rows, t, w), bf16),
            shape((2, w, wide_q), bf16),
            shape((8, w), f32),
            shape((2, QWIN, 8, EP), f32),
            shape((8, t), f32),
            shape((8, 2 * EP), f32),
            shape((n, w), bf16),
            shape(up_parts.shape[1:], bf16),
            shape((rows_o, w), bf16),
            shape((rows_o, FF), f32),
            shape((2 * rows_d, w), f32),
        ],
        scratch_shapes=[pltpu.VMEM((2, t, QWIN * t), f32), pltpu.VMEM((w, 6 * EP), f32), pltpu.VMEM((t, 6 * EP), bf16)] + scatter_scratch(n, w)
        + line_scratch(*up_parts.shape[1:]) + line_scratch(rows_o, w) + [pltpu.VMEM((4, rows_o, w), bf16)]
        + home_scratch(rows_o, FF // 8) + [pltpu.VMEM((2, rows_d, w), bf16)] + dma_sems(SCATTER_COPIES + 18),
        compiler_params=pltpu.CompilerParams(collective_id=ident, has_side_effects=True, vmem_limit_bytes=63 << 20),
        name="back",
    )(mix, qkv, dcol, drow, tt, gain, dattn, xhat, s, p, z, a1, out_w, qkv_w, out_parts, up_parts, wo, gate, down, resid)


def rms_scale(values):
    return lax.rsqrt(jnp.mean(values * values, axis=1, keepdims=True) + 1e-06)


class Links:
    def __init__(self, fsdp):
        self.fsdp = fsdp
        index = lax.axis_index("fsdp")
        self.x = lax.axis_index("rep")
        self.z, self.y, self.c = index // 4, (index // 2) % 2, index % 2

    def across(self, flip, v):
        if flip == "x":
            return lax.ppermute(v, "rep", [(0, 1), (1, 0)])
        bit = {"y": 2, "c": 1}[flip]
        return lax.ppermute(v, "fsdp", [(f, f ^ bit) for f in range(self.fsdp)])

    def along(self, v, step):
        pairs = [(f, f + 4 * step) for f in range(self.fsdp) if 0 <= f + 4 * step < self.fsdp]
        return lax.ppermute(v, "fsdp", pairs)

    def ordered(self, bit, mine, other, axis):
        first, second = jnp.where(bit == 0, mine, other), jnp.where(bit == 0, other, mine)
        return jnp.stack([first, second], axis)

    def gather_z(self, v):
        left, right = [], []
        a = b = v
        for _ in range(3):
            a, b = self.along(a, 1), self.along(b, -1)
            left.append(a)
            right.append(b)
        line = jnp.stack(left[::-1] + [v] + right)
        return lax.dynamic_slice_in_dim(line, 3 - self.z, 4, 0)

    def scatter_z(self, parts):
        zero = jnp.zeros((3,) + parts.shape[1:], parts.dtype)
        line = lax.dynamic_slice_in_dim(jnp.concatenate([zero, parts, zero]), self.z, 7, 0)
        low = lambda v: v.astype(bf16)
        a = self.along(low(line[6]), 1)
        b = self.along(low(line[0]), -1)
        for step in (1, 2):
            a = self.along(low(line[6 - step] + a.astype(f32)), 1)
            b = self.along(low(line[step] + b.astype(f32)), -1)
        return line[3] + a.astype(f32) + b.astype(f32)

    def gather_plane(self, v):
        n = v.shape[0] // 2
        vx, vy = self.across("x", v), self.across("y", v)
        vd = jnp.concatenate([self.across("y", vx[:n]), self.across("x", vy[n:])])
        return [jnp.concatenate([u, self.across("c", u)]) for u in (v, vx, vy, vd)]

    def scatter_plane(self, parts):
        low = lambda v: v.astype(bf16)
        n = parts[0].shape[0] // 2
        s = [p[:n] + self.across("c", low(p[n:])).astype(f32) for p in parts]
        m = n // 2
        dx, dy = self.across("x", low(s[3][:m])), self.across("y", low(s[3][m:]))
        to_x = jnp.concatenate([s[1][:m], s[1][m:] + dy.astype(f32)])
        to_y = jnp.concatenate([s[2][:m] + dx.astype(f32), s[2][m:]])
        return s[0] + self.across("x", low(to_x)).astype(f32) + self.across("y", low(to_y)).astype(f32)


class Weights:
    def __init__(self, links):
        self.links = links
        self.line = links.fsdp == 16
        x, y, c = links.x, links.y, links.c
        self.pair = 4 * x + 2 * c + y
        self.slot = 4 * x + 2 * y + c

    def spread(self, shard, dims):
        l = self.links
        ax, ay, ac = dims
        v = lax.dynamic_index_in_dim(shard, l.x, ax, keepdims=True)
        keep = lax.dynamic_index_in_dim(v, l.y, ay, keepdims=True)
        sent = l.across("y", lax.dynamic_index_in_dim(v, 1 - l.y, ay, keepdims=True))
        v = l.ordered(l.y, keep, sent, 0)
        keep = lax.dynamic_index_in_dim(v, l.c, ac + 1, keepdims=True)
        sent = l.across("c", lax.dynamic_index_in_dim(v, 1 - l.c, ac + 1, keepdims=True))
        v = l.ordered(l.c, keep, sent, 1)
        return l.gather_z(v)

    def collect(self, grad, dims):
        l = self.links
        ax, ay, ac = dims
        low = lambda v: v.astype(bf16)
        v = l.scatter_z(grad)
        keep = lax.dynamic_index_in_dim(v, l.c, 1, keepdims=False)
        sent = l.across("c", low(lax.dynamic_index_in_dim(v, 1 - l.c, 1, keepdims=False)))
        v = self.join(l.c, keep, sent.astype(f32), ac + 1)
        keep = lax.dynamic_index_in_dim(v, l.y, 0, keepdims=False)
        sent = l.across("y", low(lax.dynamic_index_in_dim(v, 1 - l.y, 0, keepdims=False)))
        v = low(self.join(l.y, keep, sent.astype(f32), ay))
        return self.join(l.x, v, l.across("x", v), ax).astype(f32)

    def join(self, bit, mine, other, axis):
        first, second = jnp.where(bit == 0, mine, other), jnp.where(bit == 0, other, mine)
        return jnp.concatenate([first, second], axis)

    def whole(self, shard):
        return lax.all_gather(shard, "fsdp", axis=0, tiled=True)

    def owned(self, grad):
        part = lax.psum_scatter(grad, "fsdp", scatter_dimension=0, tiled=True)
        return lax.psum(part.astype(bf16), "rep").astype(f32)

    def qkv(self, shard):
        rows = shard.shape[0]
        if self.line:
            v = self.spread(shard.reshape(rows, 3, 2, 2, 2, 2 * E), (2, 4, 3))
            v = v.reshape(MODEL_WIDTH, 3, 2, E)
        else:
            v = self.whole(shard).reshape(MODEL_WIDTH, 3, 8, 2, E)
            v = lax.dynamic_index_in_dim(v, self.pair, 2, keepdims=False)
        return jnp.pad(v, ((0, 0), (0, 0), (0, 0), (0, EP - E))).reshape(MODEL_WIDTH, 6 * EP)

    def qkv_back(self, grad):
        g = grad.reshape(MODEL_WIDTH, 3, 2, EP)[..., :E]
        if self.line:
            return self.collect(g.reshape(4, 2, 2, -1, 3, 1, 1, 1, 2 * E), (2, 4, 3)).reshape(-1, 3 * MODEL_WIDTH)
        zero = jnp.zeros((MODEL_WIDTH, 3, 8, 2, E), f32)
        return self.owned(lax.dynamic_update_index_in_dim(zero, g, self.pair, 2).reshape(MODEL_WIDTH, 3 * MODEL_WIDTH))

    def out(self, shard):
        l = self.links
        if self.line:
            v = l.gather_z(shard)
            keep = lax.dynamic_index_in_dim(v, 2 * l.x + l.c, 0, keepdims=False)
            sent = l.across("c", lax.dynamic_index_in_dim(v, 2 * l.x + 1 - l.c, 0, keepdims=False))
            v = l.ordered(l.c, keep, sent, 0)
        else:
            v = self.whole(shard).reshape(8, 2, E, MODEL_WIDTH)
            v = lax.dynamic_index_in_dim(v, self.pair, 0, keepdims=False)
        return jnp.pad(v, ((0, 0), (0, EP - E), (0, 0))).reshape(2 * EP, MODEL_WIDTH)

    def out_back(self, grad):
        l = self.links
        g = grad.reshape(2, EP, MODEL_WIDTH)[:, :E]
        if self.line:
            keep = lax.dynamic_index_in_dim(g, l.c, 0, keepdims=False)
            sent = l.across("c", lax.dynamic_index_in_dim(g, 1 - l.c, 0, keepdims=False).astype(bf16)).astype(f32)
            at = jnp.arange(4)[:, None, None]
            parts = jnp.where(at == 2 * l.x + l.c, keep[None], jnp.where(at == 2 * l.x + 1 - l.c, sent[None], 0.0))
            v = l.scatter_z(parts).astype(bf16)
            return (v + l.across("x", v)).astype(f32)
        zero = jnp.zeros((8, 2, E, MODEL_WIDTH), f32)
        return self.owned(lax.dynamic_update_index_in_dim(zero, g, self.pair, 0).reshape(MODEL_WIDTH, MODEL_WIDTH))

    def ffn_in(self, gate, up_):
        rows = gate.shape[0]
        both = jnp.stack([gate, up_], 1)
        if self.line:
            v = self.spread(both.reshape(rows, 2, 4, 2, 2, 2, FF // 32), (5, 3, 4))
            return v.reshape(MODEL_WIDTH, FF // 4)
        v = self.whole(both).reshape(MODEL_WIDTH, 2, 8, FF // 8)
        return lax.dynamic_index_in_dim(v, self.slot, 2, keepdims=False).reshape(MODEL_WIDTH, FF // 4)

    def ffn_in_back(self, grad):
        if self.line:
            v = self.collect(grad.reshape(4, 2, 2, -1, 2, 4, 1, 1, 1, FF // 32), (5, 3, 4)).reshape(-1, 2, FF)
        else:
            zero = jnp.zeros((MODEL_WIDTH, 2, 8, FF // 8), f32)
            g = grad.reshape(MODEL_WIDTH, 2, FF // 8)
            v = self.owned(lax.dynamic_update_index_in_dim(zero, g, self.slot, 2).reshape(MODEL_WIDTH, 2, FF))
        return v[:, 0], v[:, 1]

    def ffn_out(self, shard):
        l = self.links
        if self.line:
            v = lax.dynamic_index_in_dim(shard.reshape(2, FF // 32, MODEL_WIDTH), l.x, 0, keepdims=False)
            return l.gather_z(v).reshape(FF // 8, MODEL_WIDTH)
        v = self.whole(shard).reshape(8, FF // 8, MODEL_WIDTH)
        return lax.dynamic_index_in_dim(v, self.slot, 0, keepdims=False)

    def ffn_out_back(self, grad):
        l = self.links
        if self.line:
            v = l.scatter_z(grad.reshape(4, FF // 32, MODEL_WIDTH)).astype(bf16)
            return self.join(l.x, v, l.across("x", v), 0).astype(f32)
        zero = jnp.zeros((8, FF // 8, MODEL_WIDTH), f32)
        return self.owned(lax.dynamic_update_index_in_dim(zero, grad, self.slot, 0).reshape(FF, MODEL_WIDTH))

    def gains(self, *shards):
        l = self.links
        v = jnp.stack(shards)
        if self.line:
            v = l.ordered(l.c, v, l.across("c", v), 0)
            v = l.ordered(l.y, v, l.across("y", v), 0)
            v = l.gather_z(v)
            v = v.reshape(16, len(shards), -1).transpose(1, 0, 2).reshape(len(shards), MODEL_WIDTH)
        else:
            v = lax.all_gather(v, "fsdp", axis=1, tiled=True)
        return [v[i].astype(f32) for i in range(len(shards))]


def per_device(
    fsdp,
    x_in,
    doc_ids,
    w_qkv,
    w_out,
    gain_attn,
    gain_group,
    conv_kernel,
    head_mix,
    gain_ffn,
    w_gate,
    w_up,
    w_down,
    cotangent,
):
    links = Links(fsdp)
    weights = Weights(links)
    tokens = x_in.shape[1]

    x_all = jnp.concatenate(links.gather_plane(x_in[0]))
    qkv_w = weights.qkv(w_qkv)
    gain_a, gain_g, gain_f = weights.gains(gain_attn, gain_group, gain_ffn)
    docs = doc_ids
    for flip in ("y", "x"):
        docs = jnp.concatenate([docs, links.across(flip, docs)])
    docs = jnp.stack([docs, links.across("c", docs)], 1)
    docs = docs[jnp.array([0, 2, 1, 3])].reshape(8, tokens)
    out_w = weights.out(w_out)
    in_w = weights.ffn_in(w_gate, w_up)
    down_w = weights.ffn_out(w_down)
    upstream_chips = links.gather_plane(cotangent[0])

    kernel = lax.dynamic_slice_in_dim(conv_kernel, 2 * weights.pair, 2, 0)
    mix = lax.dynamic_slice_in_dim(head_mix, 2 * weights.pair, 2, 0)
    th, tl, tt = bands(kernel, tokens)
    group = lax.dynamic_slice_in_dim(gain_g.reshape(8, 2, E), weights.pair, 1, 0)
    group = jnp.pad(group, ((0, 0), (0, 0), (0, EP - E))).reshape(1, 2 * EP)
    doc_col, doc_row = docs[:, :, None], docs[:, None, :]

    xf_all = x_all.astype(f32)
    a1 = (xf_all * rms_scale(xf_all) * gain_a).astype(bf16)
    qkv = dot(a1, qkv_w).astype(bf16).reshape(8, tokens, 6 * EP)
    normed, xhat, s, probs, zeroed = attend(mix, qkv, doc_col, doc_row, th, tl, group)
    normed = normed.reshape(4, 2 * tokens, 2 * EP)
    xf = x_in[0].astype(f32)
    resid = xf + links.scatter_plane([dot(normed[i], out_w) for i in range(4)])

    r2 = rms_scale(resid)
    a2_chips = links.gather_plane((resid * r2 * gain_f).astype(bf16))
    out_parts, back_parts, hiddens, dgus = [], [], [], []
    half = FF // 8
    for a2, dffn in zip(a2_chips, upstream_chips):
        gu = dot(a2, in_w)
        gate, up_act = gu[:, :half], gu[:, half:]
        sig = jax.nn.sigmoid(gate)
        silu = gate * sig
        hidden = (silu * up_act).astype(bf16)
        dhidden = dot(dffn, down_w, 1, 1)
        dgate = (dhidden * up_act * sig * (1.0 + gate * (1.0 - sig))).astype(bf16)
        dup = (dhidden * silu).astype(bf16)
        dgu = jnp.concatenate([dgate, dup], 1)
        hiddens.append(hidden)
        dgus.append(dgu)
        back_parts.append(dot(dgu, in_w, 1, 1))
        out_parts.append(dot(hidden, down_w))
    da2 = links.scatter_plane(back_parts)
    output = (resid + links.scatter_plane(out_parts)).astype(bf16)

    dy = cotangent[0].astype(f32)
    sum_gain_ffn = jnp.sum(da2 * resid * r2, axis=0)
    dn2 = da2 * gain_f
    dresid = dy + r2 * (dn2 - resid * r2 * r2 * jnp.mean(dn2 * resid, axis=1, keepdims=True))
    dattn = jnp.concatenate(links.gather_plane(dresid.astype(bf16)))

    a2_all, dgu_all = jnp.concatenate(a2_chips), jnp.concatenate(dgus)
    hidden_all, dffn_all = jnp.concatenate(hiddens), jnp.concatenate(upstream_chips)
    grad_gate, grad_up = weights.ffn_in_back(dot(a2_all, dgu_all, 0, 0))
    grad_down = weights.ffn_out_back(dot(hidden_all, dffn_all, 0, 0))

    dnormed = dot(dattn, out_w, 1, 1).reshape(8, tokens, 2 * EP)
    dqkv, conv_tiles, mix_sums, group_sums = attend_back(
        mix, qkv, doc_col, doc_row, tt, group, dnormed, xhat, s, probs, zeroed
    )
    dqkv = dqkv.reshape(4, 2 * tokens, 6 * EP)
    da1 = links.scatter_plane([dot(dqkv[i], qkv_w, 1, 1) for i in range(4)])
    grad_out = weights.out_back(dot(normed.reshape(8 * tokens, 2 * EP), dattn, 0, 0))
    grad_qkv = weights.qkv_back(dot(a1, dqkv.reshape(8 * tokens, 6 * EP), 0, 0))

    r1 = rms_scale(xf)
    sum_gain_attn = jnp.sum(da1 * xf * r1, axis=0)
    dn1 = da1 * gain_a
    grad_x = dresid + r1 * (dn1 - xf * r1 * r1 * jnp.mean(dn1 * xf, axis=1, keepdims=True))

    place = lambda v: lax.dynamic_update_index_in_dim(jnp.zeros((8,) + v.shape, f32), v, weights.pair, 0)
    small = [
        sum_gain_attn,
        sum_gain_ffn,
        place(group_sums[0].reshape(2, EP)[:, :E].reshape(-1)),
        place(diagonals(conv_tiles)),
        place(jnp.sum(mix_sums[:4], axis=1)),
    ]
    sizes = [v.size for v in small]
    total = lax.psum(jnp.concatenate([v.reshape(-1) for v in small]), ("rep", "fsdp"))
    cut = [0]
    for size in sizes:
        cut.append(cut[-1] + size)
    gain_a_sum, gain_f_sum, group_sum, conv_sum, mix_sum = (total[cut[i] : cut[i + 1]] for i in range(5))
    rows = gain_attn.shape[0]
    own = lambda v: lax.dynamic_slice_in_dim(v, lax.axis_index("fsdp") * rows, rows, 0)
    return (
        output[None],
        grad_x[None],
        grad_qkv,
        grad_out,
        own(gain_a_sum),
        own(group_sum),
        conv_sum.reshape(H, QWIN, KWIN),
        mix_sum.reshape(H, 2),
        own(gain_f_sum),
        grad_gate,
        grad_up,
        grad_down,
    )


def join(bit, mine, other, axis):
    first, second = jnp.where(bit == 0, mine, other), jnp.where(bit == 0, other, mine)
    return jnp.stack([first, second], axis)


def fast(
    x_in,
    doc_ids,
    w_qkv,
    w_out,
    gain_attn,
    gain_group,
    conv_kernel,
    head_mix,
    gain_ffn,
    w_gate,
    w_up,
    w_down,
    cotangent,
):
    links = Links(16)
    pair = 4 * links.x + 2 * links.c + links.y
    tokens = x_in.shape[1]
    x, dy = x_in[0], cotangent[0]
    rows = w_qkv.shape[0]

    kernel = lax.dynamic_slice_in_dim(conv_kernel, 2 * pair, 2, 0)
    mix = lax.dynamic_slice_in_dim(head_mix, 2 * pair, 2, 0)
    gains = jnp.pad(jnp.stack([gain_attn, gain_group, gain_ffn]), ((0, 13), (0, 128 - rows)))
    docs = jnp.broadcast_to(doc_ids, (8, tokens))
    a1, dffn_1, docs, gains, qkv_w, gu_plane, out_w, th, tl, tt = start_call(
        x, dy, docs, gains, kernel.reshape(-1), w_qkv, w_gate, w_up, w_out, 1
    )
    docs = docs.reshape(8, 8, tokens)[:, 0]
    gain_a, gain_g, gain_f = gains[0:1], gains[1], gains[2:3]
    qkv_w = qkv_w.reshape(MODEL_WIDTH, 6 * EP)
    keep = lax.dynamic_index_in_dim(out_w, 2 * links.x + links.c, 0, keepdims=False)
    other = links.across("c", lax.dynamic_index_in_dim(out_w, 2 * links.x + 1 - links.c, 0, keepdims=False))
    out_w = jnp.pad(join(links.c, keep, other, 0), ((0, 0), (0, EP - E), (0, 0))).reshape(2 * EP, MODEL_WIDTH)

    group = lax.dynamic_slice_in_dim(gain_g.reshape(8, 2, E), pair, 1, 0)
    group = jnp.pad(group, ((0, 0), (0, 0), (0, EP - E))).reshape(1, 2 * EP)
    doc_col, doc_row = docs[:, :, None], docs[:, None, :]

    by_chip = lambda v: v.astype(bf16).reshape(4, 2, tokens, MODEL_WIDTH)
    by_row = lambda v: v.reshape(8, tokens, -1)
    qkv, normed, xhat, s, probs, zeroed, resid, a2, dffn_2, gu_w, down_w = forward_call(
        mix, by_row(a1), doc_col, doc_row, th, tl, group, qkv_w, out_w, x, dy, gain_f, gu_plane, w_down, 2
    )
    normed = normed.reshape(8 * tokens, 2 * EP)

    a2 = a2.reshape(8 * tokens, MODEL_WIDTH)
    flat = lambda v: v.reshape(-1, MODEL_WIDTH)
    gu_w = gu_w.reshape(MODEL_WIDTH, FF // 4)
    down_w = down_w.reshape(FF // 8, MODEL_WIDTH)
    dgu, hidden, grad_down = ffn_call(a2, flat(dffn_1), flat(dffn_2), gu_w, down_w)
    grad_down = grad_down.reshape(4, FF // 32, MODEL_WIDTH)
    dresid, dattn, sum_f, grad_down, grad_gate, grad_up, out_parts = mid_back_call(
        dgu, gu_w, a2, hidden, down_w, dy, resid, gain_f, grad_down, 3
    )

    grad_out = dot(normed, dattn.reshape(8 * tokens, MODEL_WIDTH), 0, 0).astype(bf16).reshape(2, EP, MODEL_WIDTH)[:, :rows]
    da_parts, grad_qkv, sum_a, conv_tiles, mix_sums, group_sums, out, grad_up, grad_out, grad_gate, grad_down = back_call(
        mix, qkv, doc_col, doc_row, tt, group, by_row(dattn), xhat, s, probs, zeroed, by_row(a1), out_w, qkv_w,
        out_parts, grad_up, grad_out, grad_gate, grad_down, resid, 5
    )
    sum_a = sum_a[0] / gain_a[0]
    place = lambda v: lax.dynamic_update_index_in_dim(jnp.zeros((8,) + v.shape, f32), v, pair, 0)
    small = [
        sum_a,
        sum_f[0],
        place(group_sums[0].reshape(2, EP)[:, :E].reshape(-1)),
        place(diagonals(conv_tiles)),
        place(jnp.sum(mix_sums[:4], axis=1)),
    ]
    cut = [0]
    for v in small:
        cut.append(cut[-1] + v.size)
    room = 48 * 128
    flat = jnp.concatenate([v.reshape(-1) for v in small] + [jnp.zeros((room - cut[-1],), f32)]).reshape(48, 128)
    grad_x, grad_qkv, grad_out, grad_up, total = end_call(
        by_chip(da_parts),
        grad_qkv.reshape(2, 4, 4 * rows, 3 * EP),
        grad_out,
        grad_up,
        flat,
        x,
        dresid,
        gain_a,
        4,
    )
    total = total.reshape(-1)
    gain_a_sum, gain_f_sum, group_sum, conv_sum, mix_sum = (total[cut[i] : cut[i + 1]] for i in range(5))
    own = lambda v: lax.dynamic_slice_in_dim(v, lax.axis_index("fsdp") * rows, rows, 0)
    return (
        out[None],
        grad_x[None],
        grad_qkv,
        grad_out,
        own(gain_a_sum),
        own(group_sum),
        conv_sum.reshape(H, QWIN, KWIN),
        mix_sum.reshape(H, 2),
        own(gain_f_sum),
        grad_gate,
        grad_up,
        grad_down,
    )


def solution(mesh):
    fsdp = mesh.shape["fsdp"]
    assert mesh.shape["rep"] == 2 and fsdp % 4 == 0
    rows, shard, part = P(("rep", "fsdp"), None, None), P("fsdp", None), P("fsdp")
    placed = (rows, P(("rep", "fsdp"), None), shard, shard, part, part, P(), P(), part, shard, shard, shard, rows)
    return jax.shard_map(
        fast if fsdp == 16 else (lambda *args: per_device(fsdp, *args)),
        mesh=mesh,
        in_specs=placed,
        out_specs=(rows, rows, shard, shard, part, part, P(), P(), part, shard, shard, shard),
        check_vma=False,
    )
```

```python
import math

import jax
import jax.numpy as jnp
from jax import lax
from jax.experimental import pallas as pl
from jax.experimental.pallas import tpu as pltpu
from jax.sharding import PartitionSpec as P

MODEL_WIDTH = 1536
H = 16
E = 96
EP = 128
QWIN = 6
KWIN = 11
bf16, f32 = jnp.bfloat16, jnp.float32


def allowed_mask(doc_col, doc_row):
    n = doc_row.shape[-1]
    i = lax.broadcasted_iota(jnp.int32, (n, n), 0)
    j = lax.broadcasted_iota(jnp.int32, (n, n), 1)
    return (j <= i) & (doc_col == doc_row)


def down(v, a):
    if a == 0:
        return v
    i = lax.broadcasted_iota(jnp.int32, v.shape, 0)
    return jnp.where(i >= a, pltpu.roll(v, a, 0), 0.0)


def up(v, a):
    if a == 0:
        return v
    n = v.shape[0]
    i = lax.broadcasted_iota(jnp.int32, v.shape, 0)
    return jnp.where(i < n - a, pltpu.roll(v, n - a, 0), 0.0)


def dot(a, b, ca=1, cb=0):
    return lax.dot_general(a, b, (((ca,), (cb,)), ((), ())), preferred_element_type=f32)


def split(v):
    hi = v.astype(bf16)
    return hi, (v - hi.astype(f32)).astype(bf16)


def attend_row(mix_ref, qkv_ref, dcol_ref, drow_ref, th_ref, tl_ref, gain_ref,
               normed_ref, xhat_ref, s_ref, p_ref, z_ref):
    allowed = allowed_mask(dcol_ref[0], drow_ref[0])
    scale = 1.0 / math.sqrt(E)
    probs = []
    for h in range(2):
        q = qkv_ref[0, :, h * EP:(h + 1) * EP]
        k = qkv_ref[0, :, (2 + h) * EP:(3 + h) * EP]
        zeroed = jnp.where(allowed, dot(q, k, 1, 1) * scale, 0.0)
        z_ref[0, h] = zeroed.astype(bf16)
        his, los = [], []
        for a in range(QWIN):
            hi, lo = split(down(zeroed, a))
            his.append(hi)
            los.append(lo)
        his, los = jnp.concatenate(his, 1), jnp.concatenate(los, 1)
        th, tl = th_ref[h], tl_ref[h]
        conv = dot(his, th) + (dot(his, tl) + dot(los, th))
        masked = jnp.where(allowed, conv, -jnp.inf)
        e = jnp.exp(masked - jnp.max(masked, axis=1, keepdims=True))
        p = e / jnp.sum(e, axis=1, keepdims=True)
        p_ref[0, h] = p
        probs.append(p)
    lane = lax.broadcasted_iota(jnp.int32, (1, EP), 1)
    for h in range(2):
        v = qkv_ref[0, :, (4 + h) * EP:(5 + h) * EP]
        mixed = (mix_ref[h, 0] * probs[0] + mix_ref[h, 1] * probs[1]).astype(bf16)
        ho = dot(mixed, v)
        centered = jnp.where(lane < E, ho - jnp.sum(ho, axis=1, keepdims=True) / E, 0.0)
        s = lax.rsqrt(jnp.sum(centered * centered, axis=1, keepdims=True) / E + 1e-05)
        xhat = centered * s
        cols = slice(h * EP, (h + 1) * EP)
        xhat_ref[0, :, cols] = xhat
        s_ref[0, :, cols] = jnp.broadcast_to(s, xhat.shape)
        normed_ref[0, :, cols] = (xhat * gain_ref[0:1, cols]).astype(bf16)


def attend(mix, qkv, dcol, drow, th, tl, gain):
    n, t, _ = qkv.shape
    row = lambda *s: pl.BlockSpec((1,) + s, lambda i: (i,) + (0,) * len(s))
    full = lambda a: pl.BlockSpec(a.shape, lambda i: (0,) * a.ndim)
    return pl.pallas_call(
        attend_row,
        grid=(n,),
        in_specs=[pl.BlockSpec(memory_space=pltpu.SMEM), row(t, 6 * EP), row(t, 1), row(1, t), full(th), full(tl), full(gain)],
        out_specs=[row(t, 2 * EP), row(t, 2 * EP), row(t, 2 * EP), row(2, t, t), row(2, t, t)],
        out_shape=[
            jax.ShapeDtypeStruct((n, t, 2 * EP), bf16),
            jax.ShapeDtypeStruct((n, t, 2 * EP), f32),
            jax.ShapeDtypeStruct((n, t, 2 * EP), f32),
            jax.ShapeDtypeStruct((n, 2, t, t), f32),
            jax.ShapeDtypeStruct((n, 2, t, t), bf16),
        ],
        cost_estimate=pl.CostEstimate(flops=n * 2 * 3 * 2 * t * t * QWIN * t, bytes_accessed=n * t * t * 20, transcendentals=n * 2 * t * t),
        name="attend",
    )(mix, qkv, dcol, drow, th, tl, gain)


def bwd_kernel(mix_ref, qkv_ref, dcol_ref, drow_ref, tt_ref, gain_ref, dn_ref, xhat_ref, s_ref, p_ref, z_ref,
               dqkv_ref, gconv_ref, gmix_ref, gg_ref, m_ref):
    step, steps = pl.program_id(0), pl.num_programs(0)
    t = p_ref.shape[-1]

    @pl.when(step == 0)
    def _():
        m_ref[...] = jnp.zeros_like(m_ref)
        gmix_ref[...] = jnp.zeros_like(gmix_ref)
        gg_ref[...] = jnp.zeros_like(gg_ref)

    allowed = allowed_mask(dcol_ref[0], drow_ref[0])
    scale = 1.0 / math.sqrt(E)
    lane = lax.broadcasted_iota(jnp.int32, (1, EP), 1)
    p = [p_ref[0, 0], p_ref[0, 1]]
    dmixed = []
    for h in range(2):
        cols = slice(h * EP, (h + 1) * EP)
        dn, xhat = dn_ref[0, :, cols], xhat_ref[0, :, cols]
        gg_ref[0:1, cols] += jnp.sum(dn * xhat, axis=0, keepdims=True)
        dc = dn * gain_ref[0:1, cols]
        m1 = jnp.sum(dc, axis=1, keepdims=True) / E
        m2 = jnp.sum(dc * xhat, axis=1, keepdims=True) / E
        dh = jnp.where(lane < E, s_ref[0, :, cols] * (dc - m1 - xhat * m2), 0.0).astype(bf16)
        v = qkv_ref[0, :, (4 + h) * EP:(5 + h) * EP]
        mixed = (mix_ref[h, 0] * p[0] + mix_ref[h, 1] * p[1]).astype(bf16)
        dmixed.append(dot(dh, v, 1, 1))
        dqkv_ref[0, :, (4 + h) * EP:(5 + h) * EP] = dot(mixed, dh, 0, 0).astype(bf16)
    for h in range(2):
        for c in range(2):
            r = 2 * h + c
            gmix_ref[r:r + 1, :] += jnp.sum(dmixed[h] * p[c], axis=0, keepdims=True)
    for c in range(2):
        dp = mix_ref[0, c] * dmixed[0] + mix_ref[1, c] * dmixed[1]
        dconv = p[c] * (dp - jnp.sum(dp * p[c], axis=1, keepdims=True))
        ahead = jnp.concatenate([up(dconv, a).astype(bf16) for a in range(QWIN)], 1)
        m_ref[c] += dot(z_ref[0, c], ahead, 0, 0)
        ds = jnp.where(allowed, dot(ahead, tt_ref[c]), 0.0).astype(bf16)
        q = qkv_ref[0, :, c * EP:(c + 1) * EP]
        k = qkv_ref[0, :, (2 + c) * EP:(3 + c) * EP]
        dqkv_ref[0, :, c * EP:(c + 1) * EP] = (dot(ds, k) * scale).astype(bf16)
        dqkv_ref[0, :, (2 + c) * EP:(3 + c) * EP] = (dot(ds, q, 0, 0) * scale).astype(bf16)

    @pl.when(step == steps - 1)
    def _():
        lanes = lax.broadcasted_iota(jnp.int32, (8, t), 1)
        for h in range(2):
            for a in range(QWIN):
                total = jnp.zeros((8, t), f32)
                for first in range(0, t, 8):
                    rows = m_ref[h, first:first + 8, a * t:(a + 1) * t]
                    turned = pltpu.roll(rows, t - first, 1) if first else rows
                    total = total + jnp.where(lanes < t - first, turned, 0.0)
                gconv_ref[h, a] = total[:, :EP]


def attend_back(mix, qkv, dcol, drow, tt, gain, dn, xhat, s, p, z):
    n, t, _ = qkv.shape
    row = lambda *sh: pl.BlockSpec((1,) + sh, lambda i: (i,) + (0,) * len(sh))
    full = lambda a: pl.BlockSpec(a.shape, lambda i: (0,) * a.ndim)
    keep = lambda *sh: pl.BlockSpec(sh, lambda i: (0,) * len(sh))
    return pl.pallas_call(
        bwd_kernel,
        grid=(n,),
        in_specs=[pl.BlockSpec(memory_space=pltpu.SMEM), row(t, 6 * EP), row(t, 1), row(1, t), full(tt), full(gain),
                  row(t, 2 * EP), row(t, 2 * EP), row(t, 2 * EP), row(2, t, t), row(2, t, t)],
        out_specs=[row(t, 6 * EP), keep(2, QWIN, 8, EP), keep(8, t), keep(8, 2 * EP)],
        out_shape=[
            jax.ShapeDtypeStruct((n, t, 6 * EP), bf16),
            jax.ShapeDtypeStruct((2, QWIN, 8, EP), f32),
            jax.ShapeDtypeStruct((8, t), f32),
            jax.ShapeDtypeStruct((8, 2 * EP), f32),
        ],
        scratch_shapes=[pltpu.VMEM((2, t, QWIN * t), f32)],
        cost_estimate=pl.CostEstimate(flops=n * 2 * 2 * 2 * t * t * QWIN * t, bytes_accessed=n * t * t * 20, transcendentals=0),
        name="attend_back",
    )(mix, qkv, dcol, drow, tt, gain, dn, xhat, s, p, z)


def bands(kernel, t):
    diff = jnp.arange(t)[None, :] - jnp.arange(t)[:, None]
    band = jnp.zeros((2, QWIN, t, t), f32)
    back = jnp.zeros((2, QWIN, t, t), f32)
    for b in range(KWIN):
        tap = kernel[:, :, b][:, :, None, None]
        band = band + jnp.where(diff == b, tap, 0.0)
        back = back + jnp.where(diff == -b, tap, 0.0)
    th, tl = split(band)
    flat = lambda v: v.reshape(2, QWIN * t, t)
    return flat(th), flat(tl), flat(back.astype(bf16))


def diagonals(tiles):
    return sum(tiles[:, :, i, i:i + KWIN] for i in range(8))


FF = 4096
MESH = pl.DeviceIdType.MESH


class Net:
    def __init__(self):
        self.x, self.f = lax.axis_index("rep"), lax.axis_index("fsdp")
        self.z, self.y, self.c = self.f // 4, (self.f // 2) % 2, self.f % 2
        self.k = self.f % 4
        nx, fy, fc = 1 - self.x, 2 - 4 * self.y, 1 - 2 * self.c
        self.to = {
            "x": (nx, self.f),
            "y": (self.x, self.f + fy),
            "c": (self.x, self.f + fc),
            "xy": (nx, self.f + fy),
            "xc": (nx, self.f + fc),
            "yc": (self.x, self.f + fy + fc),
            "xyc": (nx, self.f + fy + fc),
            "up": (self.x, self.f + 4),
            "down": (self.x, self.f - 4),
        }

    def greet(self, names, line=True):
        barrier = pltpu.get_barrier_semaphore()
        for name in names:
            pl.semaphore_signal(barrier, inc=1, device_id=self.to[name], device_id_type=MESH)
        count = len(names)
        if line:

            @pl.when(self.z < 3)
            def _():
                pl.semaphore_signal(barrier, inc=1, device_id=self.to["up"], device_id_type=MESH)

            @pl.when(self.z > 0)
            def _():
                pl.semaphore_signal(barrier, inc=1, device_id=self.to["down"], device_id_type=MESH)

            count = count + (self.z + 3) // 4 + (6 - self.z) // 4
        pl.semaphore_wait(barrier, count)

    def copy(self, src, dst, sems, i, name):
        return pltpu.make_async_remote_copy(
            src_ref=src, dst_ref=dst, send_sem=sems[0].at[i], recv_sem=sems[1].at[i],
            device_id=self.to[name], device_id_type=MESH,
        )

    def send(self, src, dst, sems, i, name):
        copy = self.copy(src, dst, sems, i, name)
        copy.start()
        return copy


def tiles(start, size, body, step=32):
    def one(i, _):
        body(pl.ds(pl.multiple_of(start + i * step, step), step))
        return 0

    lax.fori_loop(0, size // step, one, 0)


def wide(v):
    return v.astype(f32)


class GatherLine:
    def __init__(self, net, src, out, sems, base, keep=None):
        self.net, self.src, self.out, self.sems, self.base = net, src, out, sems, base
        self.keep = keep or (lambda slot: net.z >= 0)

    def go(self, d, way, act):
        net = self.net
        slot = net.z - d if way == "up" else net.z + d
        inside = (net.z >= d) & (net.z < 3) if way == "up" else (net.z < 4 - d) & (net.z > 0)
        i = self.base + d + (0 if way == "up" else 3)

        @pl.when(inside & self.keep(slot))
        def _():
            src = self.src if d == 0 else self.out.at[slot]
            act(net.copy(src, self.out.at[slot], self.sems, i, way))

    def came(self, d, way):
        net = self.net
        slot = net.z - d if way == "up" else net.z + d
        inside = net.z >= d if way == "up" else net.z < 4 - d
        i = self.base + d - 1 + (0 if way == "up" else 3)

        @pl.when(inside & self.keep(slot))
        def _():
            net.copy(self.out.at[slot], self.out.at[slot], self.sems, i, way).wait_recv()

    def step(self, d):
        for way in ("up", "down"):
            if d > 0:
                self.came(d, way)
            if d < 3:
                self.go(d, way, lambda copy: copy.start())

    def finish(self):
        for d in range(3):
            for way in ("up", "down"):
                self.go(d, way, lambda copy: copy.wait_send())


class ScatterLine:
    def __init__(self, net, parts, got, made, sems, base):
        self.net, self.parts, self.got, self.made, self.sems, self.base = net, parts, got, made, sems, base
        self.n = parts.shape[1]

    def each(self, d, way):
        net = self.net
        t = net.z + (3 - d) if way == 0 else net.z - (3 - d)
        inside = (t < 4) if way == 0 else (t >= 0)
        first = (net.z == 0) if way == 0 else (net.z == 3)
        return t, inside, first, self.base + d + 3 * way, ("up", "down")[way]

    def step(self, d):
        for way in range(2):
            t, inside, first, i, name = self.each(d, way)

            @pl.when(inside & first)
            def _():
                self.net.copy(self.parts.at[t], self.got.at[way, d], self.sems, i, name).start()

            if d == 0:
                continue

            @pl.when(inside & jnp.logical_not(first))
            def _():
                self.net.copy(self.got.at[way, d - 1], self.got.at[way, d - 1], self.sems, i - 1, name).wait_recv()

                def body(rows):
                    self.made[way, d - 1, rows] = (wide(self.parts[t, rows]) + wide(self.got[way, d - 1, rows])).astype(bf16)

                tiles(0, self.n, body)
                self.net.copy(self.made.at[way, d - 1], self.got.at[way, d], self.sems, i, name).start()

    def finish(self, store):
        net = self.net
        below, above = net.z > 0, net.z < 3

        @pl.when(below)
        def _():
            net.copy(self.got.at[0, 2], self.got.at[0, 2], self.sems, self.base + 2, "up").wait_recv()

        @pl.when(above)
        def _():
            net.copy(self.got.at[1, 2], self.got.at[1, 2], self.sems, self.base + 5, "down").wait_recv()

        def put(low, high):
            def body(rows):
                total = wide(self.parts[net.z, rows])
                if low:
                    total = total + wide(self.got[0, 2, rows])
                if high:
                    total = total + wide(self.got[1, 2, rows])
                store(rows, total)

            tiles(0, self.n, body)

        @pl.when(below & above)
        def _():
            put(True, True)

        @pl.when(jnp.logical_not(below))
        def _():
            put(False, True)

        @pl.when(jnp.logical_not(above))
        def _():
            put(True, False)

        for d in range(3):
            for way in range(2):
                t, inside, first, i, name = self.each(d, way)

                @pl.when(inside & first)
                def _():
                    net.copy(self.parts.at[t], self.got.at[way, d], self.sems, i, name).wait_send()

                if d > 0:

                    @pl.when(inside & jnp.logical_not(first))
                    def _():
                        net.copy(self.made.at[way, d - 1], self.got.at[way, d], self.sems, i, name).wait_send()


def line_scratch(n, w):
    return [pltpu.VMEM((2, 3, n, w), bf16), pltpu.VMEM((2, 2, n, w), bf16)]


LINE_COPIES = 6


class Later:
    def __init__(self, make):
        self.make = make
        make().start()

    def wait_recv(self):
        self.make().wait_recv()

    def wait_send(self):
        self.make().wait_send()


def gather_steps(net, v, out, sems, base, ready):
    n = v.shape[0]
    A, B = pl.ds(0, n // 2), pl.ds(n // 2, n // 2)
    go = {}
    ready(0)
    go["xA"] = Later(lambda: net.copy(v.at[A], out.at[1, 0, A], sems, base + 0, "x"))
    go["yA"] = Later(lambda: net.copy(v.at[A], out.at[2, 0, A], sems, base + 3, "y"))
    go["0A"] = Later(lambda: net.copy(v.at[A], out.at[0, 1, A], sems, base + 4, "c"))
    ready(1)
    go["yB"] = Later(lambda: net.copy(v.at[B], out.at[2, 0, B], sems, base + 2, "y"))
    go["xB"] = Later(lambda: net.copy(v.at[B], out.at[1, 0, B], sems, base + 1, "x"))
    go["0B"] = Later(lambda: net.copy(v.at[B], out.at[0, 1, B], sems, base + 5, "c"))
    yield
    go["xA"].wait_recv()
    go["dA"] = Later(lambda: net.copy(out.at[1, 0, A], out.at[3, 0, A], sems, base + 6, "y"))
    go["1A"] = Later(lambda: net.copy(out.at[1, 0, A], out.at[1, 1, A], sems, base + 8, "c"))
    go["yA"].wait_recv()
    go["2A"] = Later(lambda: net.copy(out.at[2, 0, A], out.at[2, 1, A], sems, base + 10, "c"))
    yield
    go["yB"].wait_recv()
    go["dB"] = Later(lambda: net.copy(out.at[2, 0, B], out.at[3, 0, B], sems, base + 7, "x"))
    go["2B"] = Later(lambda: net.copy(out.at[2, 0, B], out.at[2, 1, B], sems, base + 9, "c"))
    go["xB"].wait_recv()
    go["1B"] = Later(lambda: net.copy(out.at[1, 0, B], out.at[1, 1, B], sems, base + 11, "c"))
    yield
    go["dA"].wait_recv()
    go["3A"] = Later(lambda: net.copy(out.at[3, 0, A], out.at[3, 1, A], sems, base + 12, "c"))
    go["dB"].wait_recv()
    go["3B"] = Later(lambda: net.copy(out.at[3, 0, B], out.at[3, 1, B], sems, base + 13, "c"))
    yield
    for name in ("0A", "0B", "1A", "2B", "2A", "1B", "3A", "3B"):
        go[name].wait_recv()
    for copy in go.values():
        copy.wait_send()


def gather_rows(net, v, out, sems, base, ready, poll):
    for _ in gather_steps(net, v, out, sems, base, ready):
        poll()


GATHER_COPIES = 14
SCATTER_COPIES = 10


def scatter_steps(net, parts, rc, rd, rx, ry, td, tx, ty, sems, base):
    n = parts.shape[2]
    A, B = pl.ds(0, n // 2), pl.ds(n // 2, n // 2)
    go = {}
    for i, chip in enumerate((3, 1, 2, 0)):
        go[chip] = Later(lambda i=i, chip=chip: net.copy(parts.at[chip, 1], rc.at[chip], sems, base + i, "c"))

    def add(dst, chip, start, more=None):
        def body(rows):
            total = wide(parts[chip, 0, rows]) + wide(rc[chip, rows])
            if more is not None:
                total = total + wide(more[rows])
            dst[rows] = total.astype(bf16)

        tiles(start, n // 2, body)

    yield None
    go[3].wait_recv()
    add(td, 3, 0)
    go["dA"] = Later(lambda: net.copy(td.at[A], rd.at[A], sems, base + 4, "x"))
    add(td, 3, n // 2)
    go["dB"] = Later(lambda: net.copy(td.at[B], rd.at[B], sems, base + 5, "y"))
    go[1].wait_recv()
    add(tx, 1, 0)
    go["xA"] = Later(lambda: net.copy(tx.at[A], rx.at[A], sems, base + 6, "x"))
    go[2].wait_recv()
    add(ty, 2, n // 2)
    go["yB"] = Later(lambda: net.copy(ty.at[B], ry.at[B], sems, base + 7, "y"))
    yield None
    go["dA"].wait_recv()
    add(ty, 2, 0, rd)
    go["yA"] = Later(lambda: net.copy(ty.at[A], ry.at[A], sems, base + 8, "y"))
    go["dB"].wait_recv()
    add(tx, 1, n // 2, rd)
    go["xB"] = Later(lambda: net.copy(tx.at[B], rx.at[B], sems, base + 9, "x"))
    go[0].wait_recv()

    def done(half):
        for name in (("xA", "yA"), ("xB", "yB"))[half]:
            go[name].wait_recv()
        if half == 1:
            for copy in go.values():
                copy.wait_send()

    yield done


def scatter_rows(net, parts, rc, rd, rx, ry, td, tx, ty, sems, base, poll):
    steps = scatter_steps(net, parts, rc, rd, rx, ry, td, tx, ty, sems, base)
    next(steps)
    next(steps)
    poll()
    return next(steps)


def scatter_scratch(n, w):
    return [pltpu.VMEM((4, n, w), bf16)] + [pltpu.VMEM((n, w), bf16)] * 6


def dma_sems(count):
    return [pltpu.SemaphoreType.DMA((count,)), pltpu.SemaphoreType.DMA((count,))]


VM = pl.BlockSpec(memory_space=pltpu.VMEM)
ANY = pl.BlockSpec(memory_space=pl.ANY)


def polls(*acts):
    left = list(acts)

    def poll():
        if left:
            left.pop(0)()

    def drain():
        while left:
            poll()

    return poll, drain


def comm_call(body, name, ident, ins, in_specs, outs, out_specs, scratch):
    return pl.pallas_call(
        body,
        in_specs=in_specs,
        out_specs=out_specs,
        out_shape=outs,
        scratch_shapes=scratch,
        compiler_params=pltpu.CompilerParams(collective_id=ident, has_side_effects=True, vmem_limit_bytes=63 << 20),
        name=name,
    )(*ins)


def shape(dims, dtype):
    return jax.ShapeDtypeStruct(dims, dtype)


PLANE = ("x", "y", "c", "xy", "xc", "yc", "xyc")
PLACES = {"c": (0, 1), "x": (1, 0), "xc": (1, 1), "y": (2, 0), "yc": (2, 1), "xy": (3, 0), "xyc": (3, 1)}


def start_call(x, dy, docs, gains, taps, w_qkv, w_gate, w_up, w_out, ident):
    n, w = x.shape
    rows = w_qkv.shape[0]

    def body(x_ref, dy_ref, docs_ref, g_ref, taps_ref, wq_ref, gate_ref, up_ref, wo_ref,
             a1_ref, dys_ref, docs_out, gains_ref, qkv_out, gu_out, wo_out, th_ref, tl_ref, tt_ref,
             xs, gains_out, slots, gus, local, send, recv):
        net = Net()
        sems = (send, recv)
        base = 2 * GATHER_COPIES
        mine = dy_ref.at[pl.ds(0, n // 2)]
        line_q = GatherLine(net, qkv_out.at[net.z], qkv_out, sems, base)
        line_o = GatherLine(net, wo_ref, wo_out, sems, base + 6, lambda slot: slot // 2 == net.x)
        line_g = GatherLine(net, gains_out.at[net.z], gains_out, sems, base + 12)
        base += 18
        gains_out[net.z, net.k] = g_ref[...]
        slots[...] = jnp.zeros_like(slots)
        for half in range(2):

            @pl.when(net.x == half)
            def _():
                for k in range(4):
                    pair = 4 * half + 2 * (k % 2) + k // 2
                    for m in range(6):
                        col = (m // 2) * MODEL_WIDTH + (2 * pair + m % 2) * E
                        slots[k, :, m * EP : m * EP + E] = wq_ref[:, col : col + E]
                    for m in range(8):
                        src = gate_ref if m < 4 else up_ref
                        col = 256 * (4 * (m % 4) + k) + 128 * half
                        gus[k, :, m * 128 : (m + 1) * 128] = src[:, col : col + 128]

        net.greet(PLANE)
        own = [
            pltpu.make_async_copy(mine, dys_ref.at[0, 0], local.at[1]),
            pltpu.make_async_copy(slots.at[net.k], qkv_out.at[net.z, net.k], local.at[0]),
            pltpu.make_async_copy(gus.at[net.k], gu_out.at[net.k], local.at[2]),
            pltpu.make_async_copy(docs_ref, docs_out.at[0, 0], local.at[3]),
            pltpu.make_async_copy(wo_ref, wo_out.at[net.z], local.at[4]),
        ]
        for copy in own:
            copy.start()
        qkv_parts, gain_parts, small = [], [], []
        flips = {"c": net.k + 1 - 2 * net.c, "y": net.k + 2 - 4 * net.y, "yc": net.k + 1 - 2 * net.c + 2 - 4 * net.y}
        for j, name in enumerate(("y", "yc", "c")):
            gain_parts.append(net.send(g_ref, gains_out.at[net.z, net.k], sems, base + 6 + j, name))
            qkv_parts.append(net.send(slots.at[flips[name]], qkv_out.at[net.z, net.k], sems, base + j, name))
        line_o.step(0)
        for j, (name, (chip, core)) in enumerate(PLACES.items()):
            small.append(net.send(docs_ref, docs_out.at[chip, core], sems, base + 9 + j, name))
        gather_x = gather_steps(net, x_ref, xs, sems, 0, lambda half: None)
        next(gather_x)
        gather_dy = gather_steps(net, mine, dys_ref, sems, GATHER_COPIES, lambda half: None)
        next(gather_dy)
        for copy in gain_parts:
            copy.wait_recv()
        line_g.step(0)
        own[1].wait()
        for copy in qkv_parts:
            copy.wait_recv()
        line_q.step(0)
        line_g.step(1)

        diff = lax.broadcasted_iota(jnp.int32, (n, n), 1) - lax.broadcasted_iota(jnp.int32, (n, n), 0)

        def bands_of(first, count):
            def one(i, _):
                band = jnp.zeros((n, n), f32)
                back = jnp.zeros((n, n), f32)
                for b in range(KWIN):
                    tap = taps_ref[(first + i) * KWIN + b]
                    band = jnp.where(diff == b, tap, band)
                    back = jnp.where(diff == -b, tap, back)
                h, a = (first + i) // QWIN, (first + i) % QWIN
                at = pl.ds(pl.multiple_of(a * n, n), n)
                th_ref[h, at], tl_ref[h, at] = split(band)
                tt_ref[h, at] = back.astype(bf16)
                return 0

            lax.fori_loop(0, count, one, 0)

        bands_of(0, QWIN)
        line_g.step(2)
        next(gather_x)
        line_q.step(1)
        line_g.step(3)
        line_o.step(1)
        for i in range(16):
            gains_ref[:, i * rows : (i + 1) * rows] = wide(gains_out[i // 4, i % 4, 0:8, 0:rows])
        bands_of(QWIN, QWIN)
        next(gather_x)
        for j, name in enumerate(("y", "yc", "c")):
            small.append(net.send(gus.at[flips[name]], gu_out.at[net.k], sems, base + 3 + j, name))
        gain = gains_ref[0:1]

        def norm(chip, core, src):
            def body(at):
                xf = wide(src[at])
                r = lax.rsqrt(jnp.mean(xf * xf, axis=1, keepdims=True) + 1e-06)
                a1_ref[chip, core, at] = (xf * r * gain).astype(bf16)

            tiles(0, n, body)

        norm(0, 0, x_ref)
        line_q.step(2)
        line_o.step(2)
        for _ in gather_x:
            pass
        next(gather_dy)
        next(gather_dy)
        for chip in range(4):
            for core in range(2):
                if (chip, core) != (0, 0):
                    norm(chip, core, xs.at[chip, core])
        next(gather_dy)
        line_q.step(3)
        for _ in gather_dy:
            pass
        line_o.step(3)
        for line in (line_q, line_g, line_o):
            line.finish()
        for copy in own[:1] + own[2:]:
            copy.wait()
        for copy in small:
            copy.wait_recv()
        for copy in qkv_parts + gain_parts + small:
            copy.wait_send()

    return comm_call(
        body, "start", ident, (x, dy, docs, gains, taps, w_qkv, w_gate, w_up, w_out),
        [VM] * 4 + [pl.BlockSpec(memory_space=pltpu.SMEM)] + [VM] * 4,
        [shape((4, 2, n, w), bf16), shape((4, 2, n // 2, w), bf16), shape((4, 2) + docs.shape, docs.dtype), shape((8, w), f32),
         shape((4, 4, rows, 6 * EP), bf16), shape((4, rows, FF // 4), bf16), shape((4, rows, MODEL_WIDTH), bf16)]
        + [shape((2, QWIN * n, n), bf16)] * 3,
        [VM, ANY, ANY, VM, ANY, ANY, ANY, VM, VM, VM],
        [pltpu.VMEM((4, 2, n, w), bf16), pltpu.VMEM((4, 4) + gains.shape, bf16),
         pltpu.VMEM((4, rows, 6 * EP), bf16), pltpu.VMEM((4, rows, FF // 4), bf16), pltpu.SemaphoreType.DMA((5,))]
        + dma_sems(2 * GATHER_COPIES + 18 + 16),
    )


def turn(docs):
    return jnp.transpose(docs)[:, 0:1], docs[0:1]


def forward_call(mix, a1, docs, th, tl, group, qkv_w, out_w, x, dy, gain, gu, w_down, ident):
    rows, t, w = a1.shape
    n = x.shape[0]
    down = w_down.shape[0] // 2

    def body(mix_ref, a1_ref, docs_ref, th_ref, tl_ref, group_ref, qw_ref, ow_ref, x_ref, dy_ref, g_ref, gu_ref, wd_ref,
             qkv_ref, normed_ref, xhat_ref, s_ref, p_ref, z_ref, resid_ref, out_ref, dys_ref, gu_out, wd_out,
             parts, v, local, rc, rd, rx, ry, td, tx, ty, send, recv):
        net = Net()
        sems = (send, recv)
        step = pl.program_id(0)
        base = SCATTER_COPIES + GATHER_COPIES
        mine = wd_ref.at[pl.ds(pl.multiple_of(down * net.x, down), down)]
        line_g = GatherLine(net, gu_ref, gu_out, sems, base)
        line_d = GatherLine(net, mine, wd_out, sems, base + LINE_COPIES)
        own_g = lambda: pltpu.make_async_copy(gu_ref, gu_out.at[net.z], local.at[1])
        own_d = lambda: pltpu.make_async_copy(mine, wd_out.at[net.z], local.at[2])
        A, B = pl.ds(0, n // 2), pl.ds(n // 2, n // 2)
        go = {}
        half_dy = dy_ref.at[pl.ds(n // 2, n // 2)]
        own_dy = lambda: pltpu.make_async_copy(half_dy, dys_ref.at[0, 0], local.at[3])
        gather_dy = gather_steps(net, half_dy, dys_ref, sems, base + 2 * LINE_COPIES, lambda half: None)

        def at(i):
            def run(act):
                pl.when(step == i)(act)

            return run

        @at(0)
        def _():
            net.greet("xyc")
            line_g.step(0)
            line_d.step(0)
            own_g().start()
            own_d().start()
            own_dy().start()
            next(gather_dy)

        qkv_ref[0] = dot(a1_ref[0], qw_ref[...]).astype(bf16)
        col, across = turn(docs_ref[0])
        attend_row(mix_ref, qkv_ref, [col], [across], th_ref, tl_ref, group_ref, normed_ref, xhat_ref, s_ref, p_ref, z_ref)
        parts[3 - step // 2, step % 2] = dot(normed_ref[0], ow_ref[...]).astype(bf16)

        def swap(chip, i):
            go[chip] = Later(lambda: net.copy(parts.at[chip, 1], rc.at[chip], sems, i, "c"))

        def add(dst, chip, start, more=None):
            def one(r):
                total = wide(parts[chip, 0, r]) + wide(rc[chip, r])
                if more is not None:
                    total = total + wide(more[r])
                dst[r] = total.astype(bf16)

            tiles(start, n // 2, one)

        @at(1)
        def _():
            swap(3, 0)

        @at(2)
        def _():
            go[3].wait_recv()
            add(td, 3, 0)
            go["dA"] = Later(lambda: net.copy(td.at[A], rd.at[A], sems, 4, "x"))
            add(td, 3, n // 2)
            go["dB"] = Later(lambda: net.copy(td.at[B], rd.at[B], sems, 5, "y"))

        @at(3)
        def _():
            swap(2, 2)
            line_g.step(1)
            next(gather_dy)

        @at(4)
        def _():
            go[2].wait_recv()
            add(ty, 2, n // 2)
            go["yB"] = Later(lambda: net.copy(ty.at[B], ry.at[B], sems, 7, "y"))
            go["dA"].wait_recv()
            add(ty, 2, 0, rd)
            go["yA"] = Later(lambda: net.copy(ty.at[A], ry.at[A], sems, 8, "y"))
            next(gather_dy)

        @at(5)
        def _():
            swap(1, 1)
            line_d.step(1)
            next(gather_dy)

        @at(6)
        def _():
            go[1].wait_recv()
            add(tx, 1, 0)
            go["xA"] = Later(lambda: net.copy(tx.at[A], rx.at[A], sems, 6, "x"))
            go["dB"].wait_recv()
            add(tx, 1, n // 2, rd)
            go["xB"] = Later(lambda: net.copy(tx.at[B], rx.at[B], sems, 9, "x"))

        @at(rows - 1)
        def _():
            swap(0, 3)
            line_g.step(2)
            for _ in gather_dy:
                pass
            go[0].wait_recv()

            def ready(half):
                for name in (("yA", "xA"), ("yB", "xB"))[half]:
                    go[name].wait_recv()

                def rows_of(r):
                    total = wide(parts[0, 0, r]) + wide(rc[0, r]) + wide(rx[r]) + wide(ry[r])
                    resid = wide(x_ref[r]) + total
                    resid_ref[r] = resid
                    inv = lax.rsqrt(jnp.mean(resid * resid, axis=1, keepdims=True) + 1e-06)
                    v[r] = (resid * inv * g_ref[...]).astype(bf16)

                tiles(half * (n // 2), n // 2, rows_of)

            poll, drain = polls(lambda: line_d.step(2), lambda: line_g.step(3), lambda: line_d.step(3))
            gather_rows(net, v, out_ref, sems, SCATTER_COPIES, ready, poll)
            drain()
            last = pltpu.make_async_copy(v, out_ref.at[0, 0], local.at[0])
            last.start()
            line_g.finish()
            line_d.finish()
            own_g().wait()
            own_d().wait()
            own_dy().wait()
            for copy in go.values():
                copy.wait_send()
            last.wait()

    where = lambda i: 2 * (3 - i // 2) + i % 2
    row = lambda *sh: pl.BlockSpec((1,) + sh, lambda i: (where(i),) + (0,) * len(sh))
    full = lambda v: pl.BlockSpec(v.shape, lambda i: (0,) * v.ndim, pipeline_mode=pl.Buffered(1))
    keep = lambda *sh: pl.BlockSpec(sh, lambda i: (0,) * len(sh))
    return pl.pallas_call(
        body,
        grid=(rows,),
        in_specs=[pl.BlockSpec(memory_space=pltpu.SMEM), row(t, w), row(8, t), full(th), full(tl), full(group), full(qkv_w),
                  full(out_w), full(x), full(dy), full(gain), full(gu), full(w_down)],
        out_specs=[row(t, 6 * EP), row(t, 2 * EP), row(t, 2 * EP), row(t, 2 * EP), row(2, t, t), row(2, t, t), keep(n, w), ANY, ANY, ANY, ANY],
        out_shape=[
            shape((rows, t, 6 * EP), bf16),
            shape((rows, t, 2 * EP), bf16),
            shape((rows, t, 2 * EP), f32),
            shape((rows, t, 2 * EP), f32),
            shape((rows, 2, t, t), f32),
            shape((rows, 2, t, t), bf16),
            shape((n, w), f32),
            shape((4, 2, n, w), bf16),
            shape((4, 2, n // 2, w), bf16),
            shape((4,) + gu.shape, bf16),
            shape((4, down, w), bf16),
        ],
        scratch_shapes=[pltpu.VMEM((4, 2, n, w), bf16), pltpu.VMEM((n, w), bf16), pltpu.SemaphoreType.DMA((4,))] + scatter_scratch(n, w)
        + dma_sems(SCATTER_COPIES + 2 * GATHER_COPIES + 2 * LINE_COPIES),
        compiler_params=pltpu.CompilerParams(collective_id=ident, has_side_effects=True, vmem_limit_bytes=60 << 20),
        name="forward",
    )(mix, a1, docs, th, tl, group, qkv_w, out_w, x, dy, gain, gu, w_down)


def ffn_call(a2, first, second, gu_w, down_w):
    count, w = a2.shape
    half = down_w.shape[0]
    m = count // 4
    part = half // 2

    def body(a2_ref, df1_ref, df2_ref, gw_ref, dw_ref, dgu_ref, hid_ref, gd_ref, df_ref, total):
        step = pl.program_id(0)

        @pl.when(step == 0)
        def _():
            total[...] = jnp.zeros_like(total)

        q = m // 4
        for i in range(2):
            df_ref[2 * i * q : (2 * i + 1) * q] = df1_ref[i * q : (i + 1) * q]
            df_ref[(2 * i + 1) * q : (2 * i + 2) * q] = df2_ref[i * q : (i + 1) * q]
        for j in range(2):
            cols, more = slice(j * part, (j + 1) * part), slice(half + j * part, half + (j + 1) * part)
            gate, up_act = dot(a2_ref[...], gw_ref[:, cols]), dot(a2_ref[...], gw_ref[:, more])
            dhidden = dot(df_ref[...], dw_ref[cols], 1, 1)
            sig = jax.nn.sigmoid(gate)
            silu = gate * sig
            hid_ref[:, cols] = (silu * up_act).astype(bf16)
            dgu_ref[:, cols] = (dhidden * up_act * sig * (1.0 + gate * (1.0 - sig))).astype(bf16)
            dgu_ref[:, more] = (dhidden * silu).astype(bf16)
        total[...] += dot(hid_ref[...], df_ref[...], 0, 0)

        @pl.when(step == 3)
        def _():
            gd_ref[...] = total[...].astype(bf16)

    row = lambda k, m=m: pl.BlockSpec((m, k), lambda i: (i, 0))
    full = lambda v: pl.BlockSpec(v.shape, lambda i: (0, 0), pipeline_mode=pl.Buffered(1))
    return pl.pallas_call(
        body,
        grid=(4,),
        in_specs=[row(w), row(w, m // 2), row(w, m // 2), full(gu_w), full(down_w)],
        out_specs=[row(2 * half), row(half), pl.BlockSpec((half, w), lambda i: (0, 0))],
        out_shape=[shape((count, 2 * half), bf16), shape((count, half), bf16), shape((half, w), bf16)],
        scratch_shapes=[pltpu.VMEM((m, w), bf16), pltpu.VMEM((half, w), f32)],
        compiler_params=pltpu.CompilerParams(vmem_limit_bytes=40 << 20),
        name="ffn",
    )(a2, first, second, gu_w, down_w)


def mid_back_call(dgu, gu_w, a2, hidden, down_w, dy, resid, gain, down, ident):
    n, w = dy.shape
    m, half = dgu.shape[0] // 4, gu_w.shape[1] // 2

    def body(dgu_ref, gw_ref, a2_ref, hid_ref, dw_ref, dy_ref, r_ref, g_ref, down_ref,
             dresid_ref, out_ref, sum_ref, down_out, gate_out, up_out, op_out,
             parts, a2s, hids, dws, stage, gates, v, local, rc, rd, rx, ry, td, tx, ty, d_got, d_made, g_got, g_made, send, recv):
        net = Net()
        sems = (send, recv)
        net.greet("xyc")
        base = SCATTER_COPIES + GATHER_COPIES
        line_d = ScatterLine(net, down_ref, d_got, d_made, sems, base)
        line_g = ScatterLine(net, gates, g_got, g_made, sems, base + LINE_COPIES)
        line_d.step(0)
        loads = [pltpu.make_async_copy(src, dst, local.at[i]) for i, (src, dst) in enumerate(((a2_ref, a2s), (hid_ref, hids), (dw_ref, dws)))]
        for copy in loads:
            copy.start()
        A, B = pl.ds(0, n // 2), pl.ds(n // 2, n // 2)
        go = {}

        def part(chip):
            for j in range(3):
                cols = slice(j * (w // 3), (j + 1) * (w // 3))
                total = dot(dgu_ref[chip * m : (chip + 1) * m], gw_ref[cols], 1, 1)
                parts[chip, :, :, cols] = total.astype(bf16).reshape(2, n, w // 3)

        def swap(chip, i):
            go[chip] = Later(lambda: net.copy(parts.at[chip, 1], rc.at[chip], sems, i, "c"))

        def add(dst, chip, start, more=None):
            def one(r):
                total = wide(parts[chip, 0, r]) + wide(rc[chip, r])
                if more is not None:
                    total = total + wide(more[r])
                dst[r] = total.astype(bf16)

            tiles(start, n // 2, one)

        def weights(first, last):
            for i in range(first, last):
                rows = slice(i * (w // 4), (i + 1) * (w // 4))
                total = dot(a2s[:, rows], dgu_ref[...], 0, 0)
                gates[i] = total[:, :half].astype(bf16)
                up_out[i] = total[:, half:].astype(bf16)

        def put_back(chip):
            return pltpu.make_async_copy(stage.at[chip % 2], op_out.at[chip], local.at[4 + chip % 2])

        def forward(chip):
            if chip >= 2:
                put_back(chip - 2).wait()
            for j in range(3):
                cols = slice(j * (w // 3), (j + 1) * (w // 3))
                total = dot(hids[chip * m : (chip + 1) * m], dws[:, cols])
                stage[chip % 2, :, :, cols] = total.astype(bf16).reshape(2, n, w // 3)
            put_back(chip).start()

        part(3)
        swap(3, 0)
        part(2)
        swap(2, 2)
        go[3].wait_recv()
        add(td, 3, 0)
        go["dA"] = Later(lambda: net.copy(td.at[A], rd.at[A], sems, 4, "x"))
        add(td, 3, n // 2)
        go["dB"] = Later(lambda: net.copy(td.at[B], rd.at[B], sems, 5, "y"))
        part(1)
        swap(1, 1)
        go[2].wait_recv()
        add(ty, 2, n // 2)
        go["yB"] = Later(lambda: net.copy(ty.at[B], ry.at[B], sems, 7, "y"))
        part(0)
        swap(0, 3)
        go[1].wait_recv()
        add(tx, 1, 0)
        go["xA"] = Later(lambda: net.copy(tx.at[A], rx.at[A], sems, 6, "x"))
        loads[0].wait()
        go["dA"].wait_recv()
        add(ty, 2, 0, rd)
        go["yA"] = Later(lambda: net.copy(ty.at[A], ry.at[A], sems, 8, "y"))
        go["dB"].wait_recv()
        add(tx, 1, n // 2, rd)
        go["xB"] = Later(lambda: net.copy(tx.at[B], rx.at[B], sems, 9, "x"))
        weights(0, 4)
        line_g.step(0)
        line_d.step(1)
        loads[1].wait()
        loads[2].wait()
        sum_ref[...] = jnp.zeros_like(sum_ref)
        go[0].wait_recv()

        def ready(side):
            for name in (("xA", "yA"), ("xB", "yB"))[side]:
                go[name].wait_recv()

            def rows_of(r):
                da2 = wide(parts[0, 0, r]) + wide(rc[0, r]) + wide(rx[r]) + wide(ry[r])
                res = r_ref[r]
                inv = lax.rsqrt(jnp.mean(res * res, axis=1, keepdims=True) + 1e-06)
                unit = res * inv
                sum_ref[0:1] += jnp.sum(da2 * unit, axis=0, keepdims=True)
                dn = da2 * g_ref[...]
                dresid = wide(dy_ref[r]) + inv * (dn - unit * inv * jnp.mean(dn * res, axis=1, keepdims=True))
                dresid_ref[r] = dresid
                v[r] = dresid.astype(bf16)

            tiles(side * (n // 2), n // 2, rows_of)

        poll, drain = polls(
            lambda: (forward(0), forward(1)), lambda: (line_d.step(2), line_g.step(1)), lambda: (forward(2), forward(3)), lambda: line_g.step(2)
        )
        gather_rows(net, v, out_ref, sems, SCATTER_COPIES, ready, poll)
        drain()
        last = pltpu.make_async_copy(v, out_ref.at[0, 0], local.at[3])
        last.start()

        def put(ref):
            def store(r, total):
                ref[r] = total.astype(bf16)

            return store

        line_d.finish(put(down_out))
        line_g.finish(put(gate_out))
        for copy in go.values():
            copy.wait_send()
        put_back(2).wait()
        put_back(3).wait()
        last.wait()

    return comm_call(
        body, "mid_back", ident, (dgu, gu_w, a2, hidden, down_w, dy, resid, gain, down), [VM] * 2 + [ANY] * 3 + [VM] * 4,
        [shape((n, w), f32), shape((4, 2, n, w), bf16), shape((8, w), f32), shape(down.shape[1:], bf16), shape((w // 4, half), bf16),
         shape((4, w // 4, half), bf16), shape((4, 2, n, w), bf16)],
        [VM, ANY, VM, VM, VM, VM, ANY],
        [pltpu.VMEM((4, 2, n, w), bf16), pltpu.VMEM(a2.shape, bf16), pltpu.VMEM(hidden.shape, bf16), pltpu.VMEM(down_w.shape, bf16),
         pltpu.VMEM((2, 2, n, w), bf16), pltpu.VMEM((4, w // 4, half), bf16), pltpu.VMEM((n, w), bf16), pltpu.SemaphoreType.DMA((6,))]
        + scatter_scratch(n, w) + line_scratch(*down.shape[1:]) + line_scratch(w // 4, half)
        + dma_sems(SCATTER_COPIES + GATHER_COPIES + 2 * LINE_COPIES),
    )


class Home:
    def __init__(self, net, zq, cq, fq, sems, base):
        self.net, self.zq, self.cq, self.fq, self.sems, self.base = net, zq, cq, fq, sems, base
        self.r = cq.shape[2]

    def rows(self, i, j):
        return pl.ds(pl.multiple_of((2 * i + j) * self.r, self.r), self.r)

    def over_c(self, i):
        net = self.net
        return net.copy(self.zq.at[self.rows(i, 1 - net.c)], self.cq.at[i, net.c], self.sems, self.base + i, "c")

    def over_y(self):
        net = self.net
        return net.copy(self.cq.at[1 - net.y], self.fq.at[net.x, net.y], self.sems, self.base + 2, "y")

    def over_x(self):
        net = self.net
        return net.copy(self.fq.at[net.x], self.fq.at[net.x], self.sems, self.base + 3, "x")

    def step(self, d):
        net = self.net
        if d == 0:
            for i in range(2):
                self.over_c(i).start()
                self.cq[i, net.c] = self.zq[self.rows(i, net.c)]
        elif d == 1:
            for i in range(2):
                self.over_c(i).wait_recv()
            self.over_y().start()
            self.fq[net.x, net.y] = self.cq[net.y]
        elif d == 2:
            self.over_y().wait_recv()
            self.over_x().start()
        else:
            self.over_x().wait_recv()

    def finish(self):
        for i in range(2):
            self.over_c(i).wait_send()
        self.over_y().wait_send()
        self.over_x().wait_send()

    def spread(self, dst):
        for i in range(2):
            for k in range(4):
                for m in range(4):
                    col = 256 * (4 * m + k) + 128 * i
                    dst[:, col : col + 128] = wide(self.fq[i, k // 2, k % 2, :, m * 128 : (m + 1) * 128])


HOME_COPIES = 4


def home_scratch(r, k):
    return [pltpu.VMEM((2, 2, r, k), bf16), pltpu.VMEM((2, 2, 2, r, k), bf16)]


def end_call(da_parts, qkv, wo, gate_up, small, x, dresid, gain, ident):
    n, w = da_parts.shape[2:]
    rows, wide_q = qkv.shape[2] // 4, qkv.shape[3]

    def body(da_ref, q_ref, wo_ref, up_ref, small_ref, x_ref, dresid_ref, g_ref,
             gx_ref, gq_ref, go_ref, gu_ref, total_ref, own_ref,
             rc, rd, rx, ry, td, tx, ty, q_got, q_made, zq, cq, fq, cu, fu, ro, s_got, s_sum, s_line, send, recv):
        net = Net()
        sems = (send, recv)
        net.greet("xyc")
        base = SCATTER_COPIES
        lines = [ScatterLine(net, q_ref.at[i], q_got.at[i], q_made.at[i], sems, base + 6 * i) for i in range(2)]
        line_s = GatherLine(net, s_sum.at[2], s_line, sems, base + 12)
        base += 18
        homes = [Home(net, zq.at[i], cq.at[i], fq.at[i], sems, base + 4 * i) for i in range(2)]
        home_u = Home(net, up_ref, cu, fu, sems, base + 8)
        base += 12
        for line in lines:
            line.step(0)
        hops = [net.send(small_ref, s_got.at[0], sems, base, "c")]
        home_u.step(0)

        def small_step(i):
            hops[i].wait_recv()
            s_sum[i] = (small_ref[...] if i == 0 else s_sum[i - 1]) + s_got[i]
            if i < 2:
                hops.append(net.send(s_sum.at[i], s_got.at[i + 1], sems, base + 1 + i, "yx"[i]))
            else:
                line_s.step(0)

        scatter = scatter_steps(net, da_ref, rc, rd, rx, ry, td, tx, ty, sems, 0)
        next(scatter)
        small_step(0)
        next(scatter)
        home_u.step(1)
        swap_o = net.send(wo_ref, ro, sems, base + 3, "x")
        lines[0].step(1)
        small_step(1)
        done = next(scatter)
        lines[1].step(1)
        home_u.step(2)
        small_step(2)
        lines[0].step(2)
        line_s.step(1)
        lines[1].step(2)
        line_s.step(2)
        for half in range(2):
            done(half)

            def rows_of(at):
                da = wide(da_ref[0, 0, at]) + wide(rc[0, at]) + wide(rx[at]) + wide(ry[at])
                xf = wide(x_ref[at])
                r = lax.rsqrt(jnp.mean(xf * xf, axis=1, keepdims=True) + 1e-06)
                dn = da * g_ref[...]
                gx_ref[at] = dresid_ref[at] + r * (dn - xf * r * r * jnp.mean(dn * xf, axis=1, keepdims=True))

            tiles(half * (n // 2), n // 2, rows_of)

        for i in range(2):

            def put(at, total):
                zq[i, at] = total.astype(bf16)

            lines[i].finish(put)
            homes[i].step(0)
        homes[0].step(1)
        homes[1].step(1)
        homes[0].step(2)
        homes[1].step(2)
        line_s.step(3)
        s_line[net.z] = s_sum[2]
        total_ref[...] = (s_line[0] + s_line[1]) + (s_line[2] + s_line[3])
        own_ref[...] = jnp.zeros_like(own_ref)
        for i in range(3):
            own_ref[i : i + 1] = total_ref[pl.ds(16 * i + net.f, 1)]
        swap_o.wait_recv()
        go_ref[...] = wide(wo_ref[...]) + wide(ro[...])
        home_u.step(3)
        home_u.spread(gu_ref)
        for part in range(2):
            homes[part].step(3)
            for i in range(2):
                for k in range(4):
                    pair = 4 * i + 2 * (k % 2) + k // 2
                    for m in range(3):
                        to = 3 * part + m
                        col = (to // 2) * MODEL_WIDTH + (2 * pair + to % 2) * E
                        gq_ref[:, col : col + E] = wide(fq[part, i, k // 2, k % 2, :, m * EP : m * EP + E])
        line_s.finish()
        for home in homes + [home_u]:
            home.finish()
        for copy in hops + [swap_o]:
            copy.wait_send()

    two = lambda specs: [pltpu.VMEM((2,) + v.shape, v.dtype) for v in specs]
    return comm_call(
        body, "end", ident, (da_parts, qkv, wo, gate_up, small, x, dresid, gain), [VM] * 8,
        [shape((n, w), f32), shape((rows, 3 * MODEL_WIDTH), f32), shape(wo.shape, f32), shape((rows, FF), f32), shape(small.shape, f32),
         shape((8, small.shape[1]), f32)],
        [VM] * 6,
        scatter_scratch(n, w) + two(line_scratch(4 * rows, wide_q)) + two([pltpu.VMEM((4 * rows, wide_q), bf16)])
        + two(home_scratch(rows, wide_q)) + home_scratch(rows, FF // 8) + [pltpu.VMEM(wo.shape, bf16)]
        + [pltpu.VMEM((3,) + small.shape, f32), pltpu.VMEM((3,) + small.shape, f32), pltpu.VMEM((4,) + small.shape, f32)]
        + dma_sems(SCATTER_COPIES + 18 + 12 + 4),
    )


def back_call(mix, qkv, docs, tt, gain, dattn, xhat, s, p, z, a1, out_w, qkv_w, out_parts, up_parts, wo, gate, down, resid, ident):
    rows, t, _ = qkv.shape
    n, w = out_parts.shape[2:]
    rows_o, rows_d, wide_q = wo.shape[1], down.shape[0], 3 * EP

    def body(mix_ref, qkv_ref, docs_ref, tt_ref, gain_ref, dattn_ref, xhat_ref, s_ref, p_ref, z_ref, a1_ref,
             ow_ref, qw_ref, op_ref, gu_ref, wo_ref, gate_ref, down_ref, resid_ref,
             da_ref, q16_ref, sum_ref, gconv_ref, gmix_ref, gg_ref, out_ref, gu_out, go_out, gg_out, gd_ref,
             m_ref, gq_ref, dq, rc, rd, rx, ry, td, tx, ty, g_got, g_made, o_got, o_made, po, cg, fg, fd, send, recv):
        net = Net()
        sems = (send, recv)
        step = pl.program_id(0)
        base = SCATTER_COPIES
        line = ScatterLine(net, gu_ref, g_got, g_made, sems, base)
        line_o = ScatterLine(net, po, o_got, o_made, sems, base + 6)
        home = Home(net, gate_ref, cg, fg, sems, base + 12)
        x, c = net.x, net.c
        to_c = lambda: net.copy(wo_ref.at[1 - c], po.at[2 * x + c], sems, base + 16, "c")
        to_x = lambda: net.copy(down_ref, fd.at[x], sems, base + 17, "x")
        scatter = scatter_steps(net, op_ref, rc, rd, rx, ry, td, tx, ty, sems, 0)

        @pl.when(step == 0)
        def _():
            net.greet("xyc")
            line.step(0)
            to_c().start()
            next(scatter)
            home.step(0)
            po[2 * (1 - x)] = jnp.zeros((rows_o, w), bf16)
            po[2 * (1 - x) + 1] = jnp.zeros((rows_o, w), bf16)
            po[2 * x + c] = wo_ref[c]
            fd[x] = down_ref[...]
            m_ref[...] = jnp.zeros_like(m_ref)
            gmix_ref[...] = jnp.zeros_like(gmix_ref)
            gg_ref[...] = jnp.zeros_like(gg_ref)
            gq_ref[...] = jnp.zeros_like(gq_ref)

        allowed = allowed_mask(*turn(docs_ref[0]))
        scale = 1.0 / math.sqrt(E)
        lane = lax.broadcasted_iota(jnp.int32, (1, EP), 1)
        prob = [p_ref[0, 0], p_ref[0, 1]]
        dmixed = []
        for h in range(2):
            cols = slice(h * EP, (h + 1) * EP)
            dn, xh = dot(dattn_ref[0], ow_ref[cols], 1, 1), xhat_ref[0, :, cols]
            gg_ref[0:1, cols] += jnp.sum(dn * xh, axis=0, keepdims=True)
            dc = dn * gain_ref[0:1, cols]
            m1 = jnp.sum(dc, axis=1, keepdims=True) / E
            m2 = jnp.sum(dc * xh, axis=1, keepdims=True) / E
            dh = jnp.where(lane < E, s_ref[0, :, cols] * (dc - m1 - xh * m2), 0.0).astype(bf16)
            v = qkv_ref[0, :, (4 + h) * EP : (5 + h) * EP]
            mixed = (mix_ref[h, 0] * prob[0] + mix_ref[h, 1] * prob[1]).astype(bf16)
            dmixed.append(dot(dh, v, 1, 1))
            dq[:, (4 + h) * EP : (5 + h) * EP] = dot(mixed, dh, 0, 0).astype(bf16)
        for h in range(2):
            for c in range(2):
                r = 2 * h + c
                gmix_ref[r : r + 1, :] += jnp.sum(dmixed[h] * prob[c], axis=0, keepdims=True)
        for c in range(2):
            dp = mix_ref[0, c] * dmixed[0] + mix_ref[1, c] * dmixed[1]
            dconv = prob[c] * (dp - jnp.sum(dp * prob[c], axis=1, keepdims=True))
            ahead = jnp.concatenate([up(dconv, a).astype(bf16) for a in range(QWIN)], 1)
            m_ref[c] += dot(z_ref[0, c], ahead, 0, 0)
            ds = jnp.where(allowed, dot(ahead, tt_ref[c]), 0.0).astype(bf16)
            q = qkv_ref[0, :, c * EP : (c + 1) * EP]
            k = qkv_ref[0, :, (2 + c) * EP : (3 + c) * EP]
            dq[:, c * EP : (c + 1) * EP] = (dot(ds, k) * scale).astype(bf16)
            dq[:, (2 + c) * EP : (3 + c) * EP] = (dot(ds, q, 0, 0) * scale).astype(bf16)
        da_ref[0] = dot(dq[...], qw_ref[...], 1, 1).astype(bf16)
        for i in range(0, w, 384):
            gq_ref[i : i + 384] += dot(a1_ref[0, :, i : i + 384], dq[...], 0, 0)

        done = []

        @pl.when(step == 1)
        def _():
            next(scatter)
            to_c().wait_recv()
            line_o.step(0)
            home.step(1)
            to_x().start()

        @pl.when(step == 2)
        def _():
            line.step(1)
            done.append(next(scatter))

        @pl.when(step == 3)
        def _():
            line_o.step(1)
            home.step(2)

        @pl.when(step == 4)
        def _():
            line.step(2)

        @pl.when(step == 5)
        def _():
            line_o.step(2)

        @pl.when(step == rows - 1)
        def _():
            lanes = lax.broadcasted_iota(jnp.int32, (8, t), 1)
            for h in range(2):
                for a in range(QWIN):
                    total = jnp.zeros((8, t), f32)
                    for first in range(0, t, 8):
                        part = m_ref[h, first : first + 8, a * t : (a + 1) * t]
                        turned = pltpu.roll(part, t - first, 1) if first else part
                        total = total + jnp.where(lanes < t - first, turned, 0.0)
                    gconv_ref[h, a] = total[:, :EP]
            for half in range(2):
                done[0](half)

                def sum_of(at):
                    total = wide(op_ref[0, 0, at]) + wide(rc[0, at]) + wide(rx[at]) + wide(ry[at])
                    out_ref[at] = (resid_ref[at] + total).astype(bf16)

                tiles(half * (n // 2), n // 2, sum_of)

            def put(at, total):
                gu_out[at] = total.astype(bf16)

            line.finish(put)

            def put_o(at, total):
                go_out[at] = total.astype(bf16)

            line_o.finish(put_o)
            to_x().wait_recv()
            for i in range(2):
                gd_ref[i * rows_d : (i + 1) * rows_d] = wide(fd[i])
            home.step(3)
            home.spread(gg_out)
            home.finish()
            to_x().wait_send()
            to_c().wait_send()
            for i in range(0, w, 384):
                part = gq_ref[i : i + 384]
                for j in range(2):
                    q16_ref[j, i : i + 384] = part[:, j * wide_q : (j + 1) * wide_q].astype(bf16)
                sum_ref[:, i : i + 384] = lax.dot_general(
                    jnp.ones((8, 6 * EP), f32), part * wide(qw_ref[i : i + 384]), (((1,), (1,)), ((), ())),
                    precision=lax.Precision.HIGHEST, preferred_element_type=f32,
                )

    row = lambda *sh: pl.BlockSpec((1,) + sh, lambda i: (i,) + (0,) * len(sh))
    full = lambda v: pl.BlockSpec(v.shape, lambda i: (0,) * v.ndim, pipeline_mode=pl.Buffered(1))
    keep = lambda *sh: pl.BlockSpec(sh, lambda i: (0,) * len(sh))
    return pl.pallas_call(
        body,
        grid=(rows,),
        in_specs=[pl.BlockSpec(memory_space=pltpu.SMEM), row(t, 6 * EP), row(8, t), full(tt), full(gain),
                  row(t, w), row(t, 2 * EP), row(t, 2 * EP), row(2, t, t), row(2, t, t), row(t, w),
                  full(out_w), full(qkv_w), full(out_parts), full(up_parts), full(wo), full(gate), full(down), full(resid)],
        out_specs=[row(t, w), keep(2, w, wide_q), keep(8, w), keep(2, QWIN, 8, EP), keep(8, t), keep(8, 2 * EP), keep(n, w),
                   keep(*up_parts.shape[1:]), keep(rows_o, w), keep(rows_o, FF), keep(2 * rows_d, w)],
        out_shape=[
            shape((rows, t, w), bf16),
            shape((2, w, wide_q), bf16),
            shape((8, w), f32),
            shape((2, QWIN, 8, EP), f32),
            shape((8, t), f32),
            shape((8, 2 * EP), f32),
            shape((n, w), bf16),
            shape(up_parts.shape[1:], bf16),
            shape((rows_o, w), bf16),
            shape((rows_o, FF), f32),
            shape((2 * rows_d, w), f32),
        ],
        scratch_shapes=[pltpu.VMEM((2, t, QWIN * t), f32), pltpu.VMEM((w, 6 * EP), f32), pltpu.VMEM((t, 6 * EP), bf16)] + scatter_scratch(n, w)
        + line_scratch(*up_parts.shape[1:]) + line_scratch(rows_o, w) + [pltpu.VMEM((4, rows_o, w), bf16)]
        + home_scratch(rows_o, FF // 8) + [pltpu.VMEM((2, rows_d, w), bf16)] + dma_sems(SCATTER_COPIES + 18),
        compiler_params=pltpu.CompilerParams(collective_id=ident, has_side_effects=True, vmem_limit_bytes=63 << 20),
        name="back",
    )(mix, qkv, docs, tt, gain, dattn, xhat, s, p, z, a1, out_w, qkv_w, out_parts, up_parts, wo, gate, down, resid)


def rms_scale(values):
    return lax.rsqrt(jnp.mean(values * values, axis=1, keepdims=True) + 1e-06)


class Links:
    def __init__(self, fsdp):
        self.fsdp = fsdp
        index = lax.axis_index("fsdp")
        self.x = lax.axis_index("rep")
        self.z, self.y, self.c = index // 4, (index // 2) % 2, index % 2

    def across(self, flip, v):
        if flip == "x":
            return lax.ppermute(v, "rep", [(0, 1), (1, 0)])
        bit = {"y": 2, "c": 1}[flip]
        return lax.ppermute(v, "fsdp", [(f, f ^ bit) for f in range(self.fsdp)])

    def along(self, v, step):
        pairs = [(f, f + 4 * step) for f in range(self.fsdp) if 0 <= f + 4 * step < self.fsdp]
        return lax.ppermute(v, "fsdp", pairs)

    def ordered(self, bit, mine, other, axis):
        first, second = jnp.where(bit == 0, mine, other), jnp.where(bit == 0, other, mine)
        return jnp.stack([first, second], axis)

    def gather_z(self, v):
        left, right = [], []
        a = b = v
        for _ in range(3):
            a, b = self.along(a, 1), self.along(b, -1)
            left.append(a)
            right.append(b)
        line = jnp.stack(left[::-1] + [v] + right)
        return lax.dynamic_slice_in_dim(line, 3 - self.z, 4, 0)

    def scatter_z(self, parts):
        zero = jnp.zeros((3,) + parts.shape[1:], parts.dtype)
        line = lax.dynamic_slice_in_dim(jnp.concatenate([zero, parts, zero]), self.z, 7, 0)
        low = lambda v: v.astype(bf16)
        a = self.along(low(line[6]), 1)
        b = self.along(low(line[0]), -1)
        for step in (1, 2):
            a = self.along(low(line[6 - step] + a.astype(f32)), 1)
            b = self.along(low(line[step] + b.astype(f32)), -1)
        return line[3] + a.astype(f32) + b.astype(f32)

    def gather_plane(self, v):
        n = v.shape[0] // 2
        vx, vy = self.across("x", v), self.across("y", v)
        vd = jnp.concatenate([self.across("y", vx[:n]), self.across("x", vy[n:])])
        return [jnp.concatenate([u, self.across("c", u)]) for u in (v, vx, vy, vd)]

    def scatter_plane(self, parts):
        low = lambda v: v.astype(bf16)
        n = parts[0].shape[0] // 2
        s = [p[:n] + self.across("c", low(p[n:])).astype(f32) for p in parts]
        m = n // 2
        dx, dy = self.across("x", low(s[3][:m])), self.across("y", low(s[3][m:]))
        to_x = jnp.concatenate([s[1][:m], s[1][m:] + dy.astype(f32)])
        to_y = jnp.concatenate([s[2][:m] + dx.astype(f32), s[2][m:]])
        return s[0] + self.across("x", low(to_x)).astype(f32) + self.across("y", low(to_y)).astype(f32)


class Weights:
    def __init__(self, links):
        self.links = links
        self.line = links.fsdp == 16
        x, y, c = links.x, links.y, links.c
        self.pair = 4 * x + 2 * c + y
        self.slot = 4 * x + 2 * y + c

    def spread(self, shard, dims):
        l = self.links
        ax, ay, ac = dims
        v = lax.dynamic_index_in_dim(shard, l.x, ax, keepdims=True)
        keep = lax.dynamic_index_in_dim(v, l.y, ay, keepdims=True)
        sent = l.across("y", lax.dynamic_index_in_dim(v, 1 - l.y, ay, keepdims=True))
        v = l.ordered(l.y, keep, sent, 0)
        keep = lax.dynamic_index_in_dim(v, l.c, ac + 1, keepdims=True)
        sent = l.across("c", lax.dynamic_index_in_dim(v, 1 - l.c, ac + 1, keepdims=True))
        v = l.ordered(l.c, keep, sent, 1)
        return l.gather_z(v)

    def collect(self, grad, dims):
        l = self.links
        ax, ay, ac = dims
        low = lambda v: v.astype(bf16)
        v = l.scatter_z(grad)
        keep = lax.dynamic_index_in_dim(v, l.c, 1, keepdims=False)
        sent = l.across("c", low(lax.dynamic_index_in_dim(v, 1 - l.c, 1, keepdims=False)))
        v = self.join(l.c, keep, sent.astype(f32), ac + 1)
        keep = lax.dynamic_index_in_dim(v, l.y, 0, keepdims=False)
        sent = l.across("y", low(lax.dynamic_index_in_dim(v, 1 - l.y, 0, keepdims=False)))
        v = low(self.join(l.y, keep, sent.astype(f32), ay))
        return self.join(l.x, v, l.across("x", v), ax).astype(f32)

    def join(self, bit, mine, other, axis):
        first, second = jnp.where(bit == 0, mine, other), jnp.where(bit == 0, other, mine)
        return jnp.concatenate([first, second], axis)

    def whole(self, shard):
        return lax.all_gather(shard, "fsdp", axis=0, tiled=True)

    def owned(self, grad):
        part = lax.psum_scatter(grad, "fsdp", scatter_dimension=0, tiled=True)
        return lax.psum(part.astype(bf16), "rep").astype(f32)

    def qkv(self, shard):
        rows = shard.shape[0]
        if self.line:
            v = self.spread(shard.reshape(rows, 3, 2, 2, 2, 2 * E), (2, 4, 3))
            v = v.reshape(MODEL_WIDTH, 3, 2, E)
        else:
            v = self.whole(shard).reshape(MODEL_WIDTH, 3, 8, 2, E)
            v = lax.dynamic_index_in_dim(v, self.pair, 2, keepdims=False)
        return jnp.pad(v, ((0, 0), (0, 0), (0, 0), (0, EP - E))).reshape(MODEL_WIDTH, 6 * EP)

    def qkv_back(self, grad):
        g = grad.reshape(MODEL_WIDTH, 3, 2, EP)[..., :E]
        if self.line:
            return self.collect(g.reshape(4, 2, 2, -1, 3, 1, 1, 1, 2 * E), (2, 4, 3)).reshape(-1, 3 * MODEL_WIDTH)
        zero = jnp.zeros((MODEL_WIDTH, 3, 8, 2, E), f32)
        return self.owned(lax.dynamic_update_index_in_dim(zero, g, self.pair, 2).reshape(MODEL_WIDTH, 3 * MODEL_WIDTH))

    def out(self, shard):
        l = self.links
        if self.line:
            v = l.gather_z(shard)
            keep = lax.dynamic_index_in_dim(v, 2 * l.x + l.c, 0, keepdims=False)
            sent = l.across("c", lax.dynamic_index_in_dim(v, 2 * l.x + 1 - l.c, 0, keepdims=False))
            v = l.ordered(l.c, keep, sent, 0)
        else:
            v = self.whole(shard).reshape(8, 2, E, MODEL_WIDTH)
            v = lax.dynamic_index_in_dim(v, self.pair, 0, keepdims=False)
        return jnp.pad(v, ((0, 0), (0, EP - E), (0, 0))).reshape(2 * EP, MODEL_WIDTH)

    def out_back(self, grad):
        l = self.links
        g = grad.reshape(2, EP, MODEL_WIDTH)[:, :E]
        if self.line:
            keep = lax.dynamic_index_in_dim(g, l.c, 0, keepdims=False)
            sent = l.across("c", lax.dynamic_index_in_dim(g, 1 - l.c, 0, keepdims=False).astype(bf16)).astype(f32)
            at = jnp.arange(4)[:, None, None]
            parts = jnp.where(at == 2 * l.x + l.c, keep[None], jnp.where(at == 2 * l.x + 1 - l.c, sent[None], 0.0))
            v = l.scatter_z(parts).astype(bf16)
            return (v + l.across("x", v)).astype(f32)
        zero = jnp.zeros((8, 2, E, MODEL_WIDTH), f32)
        return self.owned(lax.dynamic_update_index_in_dim(zero, g, self.pair, 0).reshape(MODEL_WIDTH, MODEL_WIDTH))

    def ffn_in(self, gate, up_):
        rows = gate.shape[0]
        both = jnp.stack([gate, up_], 1)
        if self.line:
            v = self.spread(both.reshape(rows, 2, 4, 2, 2, 2, FF // 32), (5, 3, 4))
            return v.reshape(MODEL_WIDTH, FF // 4)
        v = self.whole(both).reshape(MODEL_WIDTH, 2, 8, FF // 8)
        return lax.dynamic_index_in_dim(v, self.slot, 2, keepdims=False).reshape(MODEL_WIDTH, FF // 4)

    def ffn_in_back(self, grad):
        if self.line:
            v = self.collect(grad.reshape(4, 2, 2, -1, 2, 4, 1, 1, 1, FF // 32), (5, 3, 4)).reshape(-1, 2, FF)
        else:
            zero = jnp.zeros((MODEL_WIDTH, 2, 8, FF // 8), f32)
            g = grad.reshape(MODEL_WIDTH, 2, FF // 8)
            v = self.owned(lax.dynamic_update_index_in_dim(zero, g, self.slot, 2).reshape(MODEL_WIDTH, 2, FF))
        return v[:, 0], v[:, 1]

    def ffn_out(self, shard):
        l = self.links
        if self.line:
            v = lax.dynamic_index_in_dim(shard.reshape(2, FF // 32, MODEL_WIDTH), l.x, 0, keepdims=False)
            return l.gather_z(v).reshape(FF // 8, MODEL_WIDTH)
        v = self.whole(shard).reshape(8, FF // 8, MODEL_WIDTH)
        return lax.dynamic_index_in_dim(v, self.slot, 0, keepdims=False)

    def ffn_out_back(self, grad):
        l = self.links
        if self.line:
            v = l.scatter_z(grad.reshape(4, FF // 32, MODEL_WIDTH)).astype(bf16)
            return self.join(l.x, v, l.across("x", v), 0).astype(f32)
        zero = jnp.zeros((8, FF // 8, MODEL_WIDTH), f32)
        return self.owned(lax.dynamic_update_index_in_dim(zero, grad, self.slot, 0).reshape(FF, MODEL_WIDTH))

    def gains(self, *shards):
        l = self.links
        v = jnp.stack(shards)
        if self.line:
            v = l.ordered(l.c, v, l.across("c", v), 0)
            v = l.ordered(l.y, v, l.across("y", v), 0)
            v = l.gather_z(v)
            v = v.reshape(16, len(shards), -1).transpose(1, 0, 2).reshape(len(shards), MODEL_WIDTH)
        else:
            v = lax.all_gather(v, "fsdp", axis=1, tiled=True)
        return [v[i].astype(f32) for i in range(len(shards))]


def per_device(
    fsdp,
    x_in,
    doc_ids,
    w_qkv,
    w_out,
    gain_attn,
    gain_group,
    conv_kernel,
    head_mix,
    gain_ffn,
    w_gate,
    w_up,
    w_down,
    cotangent,
):
    links = Links(fsdp)
    weights = Weights(links)
    tokens = x_in.shape[1]

    x_all = jnp.concatenate(links.gather_plane(x_in[0]))
    qkv_w = weights.qkv(w_qkv)
    gain_a, gain_g, gain_f = weights.gains(gain_attn, gain_group, gain_ffn)
    docs = doc_ids
    for flip in ("y", "x"):
        docs = jnp.concatenate([docs, links.across(flip, docs)])
    docs = jnp.stack([docs, links.across("c", docs)], 1)
    docs = docs[jnp.array([0, 2, 1, 3])].reshape(8, tokens)
    out_w = weights.out(w_out)
    in_w = weights.ffn_in(w_gate, w_up)
    down_w = weights.ffn_out(w_down)
    upstream_chips = links.gather_plane(cotangent[0])

    kernel = lax.dynamic_slice_in_dim(conv_kernel, 2 * weights.pair, 2, 0)
    mix = lax.dynamic_slice_in_dim(head_mix, 2 * weights.pair, 2, 0)
    th, tl, tt = bands(kernel, tokens)
    group = lax.dynamic_slice_in_dim(gain_g.reshape(8, 2, E), weights.pair, 1, 0)
    group = jnp.pad(group, ((0, 0), (0, 0), (0, EP - E))).reshape(1, 2 * EP)
    doc_col, doc_row = docs[:, :, None], docs[:, None, :]

    xf_all = x_all.astype(f32)
    a1 = (xf_all * rms_scale(xf_all) * gain_a).astype(bf16)
    qkv = dot(a1, qkv_w).astype(bf16).reshape(8, tokens, 6 * EP)
    normed, xhat, s, probs, zeroed = attend(mix, qkv, doc_col, doc_row, th, tl, group)
    normed = normed.reshape(4, 2 * tokens, 2 * EP)
    xf = x_in[0].astype(f32)
    resid = xf + links.scatter_plane([dot(normed[i], out_w) for i in range(4)])

    r2 = rms_scale(resid)
    a2_chips = links.gather_plane((resid * r2 * gain_f).astype(bf16))
    out_parts, back_parts, hiddens, dgus = [], [], [], []
    half = FF // 8
    for a2, dffn in zip(a2_chips, upstream_chips):
        gu = dot(a2, in_w)
        gate, up_act = gu[:, :half], gu[:, half:]
        sig = jax.nn.sigmoid(gate)
        silu = gate * sig
        hidden = (silu * up_act).astype(bf16)
        dhidden = dot(dffn, down_w, 1, 1)
        dgate = (dhidden * up_act * sig * (1.0 + gate * (1.0 - sig))).astype(bf16)
        dup = (dhidden * silu).astype(bf16)
        dgu = jnp.concatenate([dgate, dup], 1)
        hiddens.append(hidden)
        dgus.append(dgu)
        back_parts.append(dot(dgu, in_w, 1, 1))
        out_parts.append(dot(hidden, down_w))
    da2 = links.scatter_plane(back_parts)
    output = (resid + links.scatter_plane(out_parts)).astype(bf16)

    dy = cotangent[0].astype(f32)
    sum_gain_ffn = jnp.sum(da2 * resid * r2, axis=0)
    dn2 = da2 * gain_f
    dresid = dy + r2 * (dn2 - resid * r2 * r2 * jnp.mean(dn2 * resid, axis=1, keepdims=True))
    dattn = jnp.concatenate(links.gather_plane(dresid.astype(bf16)))

    a2_all, dgu_all = jnp.concatenate(a2_chips), jnp.concatenate(dgus)
    hidden_all, dffn_all = jnp.concatenate(hiddens), jnp.concatenate(upstream_chips)
    grad_gate, grad_up = weights.ffn_in_back(dot(a2_all, dgu_all, 0, 0))
    grad_down = weights.ffn_out_back(dot(hidden_all, dffn_all, 0, 0))

    dnormed = dot(dattn, out_w, 1, 1).reshape(8, tokens, 2 * EP)
    dqkv, conv_tiles, mix_sums, group_sums = attend_back(
        mix, qkv, doc_col, doc_row, tt, group, dnormed, xhat, s, probs, zeroed
    )
    dqkv = dqkv.reshape(4, 2 * tokens, 6 * EP)
    da1 = links.scatter_plane([dot(dqkv[i], qkv_w, 1, 1) for i in range(4)])
    grad_out = weights.out_back(dot(normed.reshape(8 * tokens, 2 * EP), dattn, 0, 0))
    grad_qkv = weights.qkv_back(dot(a1, dqkv.reshape(8 * tokens, 6 * EP), 0, 0))

    r1 = rms_scale(xf)
    sum_gain_attn = jnp.sum(da1 * xf * r1, axis=0)
    dn1 = da1 * gain_a
    grad_x = dresid + r1 * (dn1 - xf * r1 * r1 * jnp.mean(dn1 * xf, axis=1, keepdims=True))

    place = lambda v: lax.dynamic_update_index_in_dim(jnp.zeros((8,) + v.shape, f32), v, weights.pair, 0)
    small = [
        sum_gain_attn,
        sum_gain_ffn,
        place(group_sums[0].reshape(2, EP)[:, :E].reshape(-1)),
        place(diagonals(conv_tiles)),
        place(jnp.sum(mix_sums[:4], axis=1)),
    ]
    sizes = [v.size for v in small]
    total = lax.psum(jnp.concatenate([v.reshape(-1) for v in small]), ("rep", "fsdp"))
    cut = [0]
    for size in sizes:
        cut.append(cut[-1] + size)
    gain_a_sum, gain_f_sum, group_sum, conv_sum, mix_sum = (total[cut[i] : cut[i + 1]] for i in range(5))
    rows = gain_attn.shape[0]
    own = lambda v: lax.dynamic_slice_in_dim(v, lax.axis_index("fsdp") * rows, rows, 0)
    return (
        output[None],
        grad_x[None],
        grad_qkv,
        grad_out,
        own(gain_a_sum),
        own(group_sum),
        conv_sum.reshape(H, QWIN, KWIN),
        mix_sum.reshape(H, 2),
        own(gain_f_sum),
        grad_gate,
        grad_up,
        grad_down,
    )


def join(bit, mine, other, axis):
    first, second = jnp.where(bit == 0, mine, other), jnp.where(bit == 0, other, mine)
    return jnp.stack([first, second], axis)


def fast(
    x_in,
    doc_ids,
    w_qkv,
    w_out,
    gain_attn,
    gain_group,
    conv_kernel,
    head_mix,
    gain_ffn,
    w_gate,
    w_up,
    w_down,
    cotangent,
):
    links = Links(16)
    pair = 4 * links.x + 2 * links.c + links.y
    tokens = x_in.shape[1]
    x, dy = x_in[0], cotangent[0]
    rows = w_qkv.shape[0]

    kernel = lax.dynamic_slice_in_dim(conv_kernel, 2 * pair, 2, 0)
    mix = lax.dynamic_slice_in_dim(head_mix, 2 * pair, 2, 0)
    gains = jnp.pad(jnp.stack([gain_attn, gain_group, gain_ffn]), ((0, 13), (0, 128 - rows)))
    docs = jnp.broadcast_to(doc_ids, (8, tokens))
    a1, dffn_1, docs, gains, qkv_w, gu_plane, out_w, th, tl, tt = start_call(
        x, dy, docs, gains, kernel.reshape(-1), w_qkv, w_gate, w_up, w_out, 1
    )
    docs = docs.reshape(8, 8, tokens)
    gain_a, gain_g, gain_f = gains[0:1], gains[1], gains[2:3]
    qkv_w = qkv_w.reshape(MODEL_WIDTH, 6 * EP)
    keep = lax.dynamic_index_in_dim(out_w, 2 * links.x + links.c, 0, keepdims=False)
    other = links.across("c", lax.dynamic_index_in_dim(out_w, 2 * links.x + 1 - links.c, 0, keepdims=False))
    out_w = jnp.pad(join(links.c, keep, other, 0), ((0, 0), (0, EP - E), (0, 0))).reshape(2 * EP, MODEL_WIDTH)

    group = lax.dynamic_slice_in_dim(gain_g.reshape(8, 2, E), pair, 1, 0)
    group = jnp.pad(group, ((0, 0), (0, 0), (0, EP - E))).reshape(1, 2 * EP)

    by_chip = lambda v: v.astype(bf16).reshape(4, 2, tokens, MODEL_WIDTH)
    by_row = lambda v: v.reshape(8, tokens, -1)
    qkv, normed, xhat, s, probs, zeroed, resid, a2, dffn_2, gu_w, down_w = forward_call(
        mix, by_row(a1), docs, th, tl, group, qkv_w, out_w, x, dy, gain_f, gu_plane, w_down, 2
    )
    normed = normed.reshape(8 * tokens, 2 * EP)

    a2 = a2.reshape(8 * tokens, MODEL_WIDTH)
    flat = lambda v: v.reshape(-1, MODEL_WIDTH)
    gu_w = gu_w.reshape(MODEL_WIDTH, FF // 4)
    down_w = down_w.reshape(FF // 8, MODEL_WIDTH)
    dgu, hidden, grad_down = ffn_call(a2, flat(dffn_1), flat(dffn_2), gu_w, down_w)
    grad_down = grad_down.reshape(4, FF // 32, MODEL_WIDTH)
    dresid, dattn, sum_f, grad_down, grad_gate, grad_up, out_parts = mid_back_call(
        dgu, gu_w, a2, hidden, down_w, dy, resid, gain_f, grad_down, 3
    )

    grad_out = dot(normed, dattn.reshape(8 * tokens, MODEL_WIDTH), 0, 0).astype(bf16).reshape(2, EP, MODEL_WIDTH)[:, :rows]
    da_parts, grad_qkv, sum_a, conv_tiles, mix_sums, group_sums, out, grad_up, grad_out, grad_gate, grad_down = back_call(
        mix, qkv, docs, tt, group, by_row(dattn), xhat, s, probs, zeroed, by_row(a1), out_w, qkv_w,
        out_parts, grad_up, grad_out, grad_gate, grad_down, resid, 5
    )
    sum_a = sum_a[0] / gain_a[0]
    place = lambda v: lax.dynamic_update_index_in_dim(jnp.zeros((8,) + v.shape, f32), v, pair, 0).reshape(16, -1)
    heads = jnp.concatenate([diagonals(conv_tiles).reshape(2, -1), jnp.sum(mix_sums[:4], axis=1).reshape(2, 2)], 1)
    small = [sum_a.reshape(16, -1), sum_f[0].reshape(16, -1), place(group_sums[0].reshape(2, EP)[:, :E]), place(heads)]
    small = jnp.concatenate([jnp.pad(v, ((0, 0), (0, 128 - v.shape[1]))) for v in small])
    grad_x, grad_qkv, grad_out, grad_up, total, own = end_call(
        by_chip(da_parts),
        grad_qkv.reshape(2, 4, 4 * rows, 3 * EP),
        grad_out,
        grad_up,
        small,
        x,
        dresid,
        gain_a,
        4,
    )
    heads = total[48:]
    taps = QWIN * KWIN
    return (
        out[None],
        grad_x[None],
        grad_qkv,
        grad_out,
        own[0, :rows],
        own[2, :rows],
        heads[:, :taps].reshape(H, QWIN, KWIN),
        heads[:, taps : taps + 2],
        own[1, :rows],
        grad_gate,
        grad_up,
        grad_down,
    )


def solution(mesh):
    fsdp = mesh.shape["fsdp"]
    assert mesh.shape["rep"] == 2 and fsdp % 4 == 0
    rows, shard, part = P(("rep", "fsdp"), None, None), P("fsdp", None), P("fsdp")
    placed = (rows, P(("rep", "fsdp"), None), shard, shard, part, part, P(), P(), part, shard, shard, shard, rows)
    return jax.shard_map(
        fast if fsdp == 16 else (lambda *args: per_device(fsdp, *args)),
        mesh=mesh,
        in_specs=placed,
        out_specs=(rows, rows, shard, shard, part, part, P(), P(), part, shard, shard, shard),
        check_vma=False,
    )
```

```python
import math

import jax
import jax.numpy as jnp
from jax import lax
from jax.experimental import pallas as pl
from jax.experimental.pallas import tpu as pltpu
from jax.sharding import PartitionSpec as P

MODEL_WIDTH = 1536
H = 16
E = 96
EP = 128
QWIN = 6
KWIN = 11
bf16, f32 = jnp.bfloat16, jnp.float32


def allowed_mask(doc_col, doc_row):
    n = doc_row.shape[-1]
    i = lax.broadcasted_iota(jnp.int32, (n, n), 0)
    j = lax.broadcasted_iota(jnp.int32, (n, n), 1)
    return (j <= i) & (doc_col == doc_row)


def down(v, a):
    if a == 0:
        return v
    i = lax.broadcasted_iota(jnp.int32, v.shape, 0)
    return jnp.where(i >= a, pltpu.roll(v, a, 0), 0.0)


def up(v, a):
    if a == 0:
        return v
    n = v.shape[0]
    i = lax.broadcasted_iota(jnp.int32, v.shape, 0)
    return jnp.where(i < n - a, pltpu.roll(v, n - a, 0), 0.0)


def dot(a, b, ca=1, cb=0):
    return lax.dot_general(a, b, (((ca,), (cb,)), ((), ())), preferred_element_type=f32)


def split(v):
    hi = v.astype(bf16)
    return hi, (v - hi.astype(f32)).astype(bf16)


def attend_row(mix_ref, qkv_ref, dcol_ref, drow_ref, th_ref, tl_ref, gain_ref,
               normed_ref, xhat_ref, s_ref, p_ref, z_ref):
    allowed = allowed_mask(dcol_ref[0], drow_ref[0])
    scale = 1.0 / math.sqrt(E)
    probs = []
    for h in range(2):
        q = qkv_ref[0, :, h * EP:(h + 1) * EP]
        k = qkv_ref[0, :, (2 + h) * EP:(3 + h) * EP]
        zeroed = jnp.where(allowed, dot(q, k, 1, 1) * scale, 0.0)
        z_ref[0, h] = zeroed.astype(bf16)
        his, los = [], []
        for a in range(QWIN):
            hi, lo = split(down(zeroed, a))
            his.append(hi)
            los.append(lo)
        his, los = jnp.concatenate(his, 1), jnp.concatenate(los, 1)
        th, tl = th_ref[h], tl_ref[h]
        conv = dot(his, th) + (dot(his, tl) + dot(los, th))
        masked = jnp.where(allowed, conv, -jnp.inf)
        e = jnp.exp(masked - jnp.max(masked, axis=1, keepdims=True))
        p = e / jnp.sum(e, axis=1, keepdims=True)
        p_ref[0, h] = p
        probs.append(p)
    lane = lax.broadcasted_iota(jnp.int32, (1, EP), 1)
    for h in range(2):
        v = qkv_ref[0, :, (4 + h) * EP:(5 + h) * EP]
        mixed = (mix_ref[h, 0] * probs[0] + mix_ref[h, 1] * probs[1]).astype(bf16)
        ho = dot(mixed, v)
        centered = jnp.where(lane < E, ho - jnp.sum(ho, axis=1, keepdims=True) / E, 0.0)
        s = lax.rsqrt(jnp.sum(centered * centered, axis=1, keepdims=True) / E + 1e-05)
        xhat = centered * s
        cols = slice(h * EP, (h + 1) * EP)
        xhat_ref[0, :, cols] = xhat
        s_ref[0, :, cols] = jnp.broadcast_to(s, xhat.shape)
        normed_ref[0, :, cols] = (xhat * gain_ref[0:1, cols]).astype(bf16)


def attend(mix, qkv, dcol, drow, th, tl, gain):
    n, t, _ = qkv.shape
    row = lambda *s: pl.BlockSpec((1,) + s, lambda i: (i,) + (0,) * len(s))
    full = lambda a: pl.BlockSpec(a.shape, lambda i: (0,) * a.ndim)
    return pl.pallas_call(
        attend_row,
        grid=(n,),
        in_specs=[pl.BlockSpec(memory_space=pltpu.SMEM), row(t, 6 * EP), row(t, 1), row(1, t), full(th), full(tl), full(gain)],
        out_specs=[row(t, 2 * EP), row(t, 2 * EP), row(t, 2 * EP), row(2, t, t), row(2, t, t)],
        out_shape=[
            jax.ShapeDtypeStruct((n, t, 2 * EP), bf16),
            jax.ShapeDtypeStruct((n, t, 2 * EP), f32),
            jax.ShapeDtypeStruct((n, t, 2 * EP), f32),
            jax.ShapeDtypeStruct((n, 2, t, t), f32),
            jax.ShapeDtypeStruct((n, 2, t, t), bf16),
        ],
        cost_estimate=pl.CostEstimate(flops=n * 2 * 3 * 2 * t * t * QWIN * t, bytes_accessed=n * t * t * 20, transcendentals=n * 2 * t * t),
        name="attend",
    )(mix, qkv, dcol, drow, th, tl, gain)


def bwd_kernel(mix_ref, qkv_ref, dcol_ref, drow_ref, tt_ref, gain_ref, dn_ref, xhat_ref, s_ref, p_ref, z_ref,
               dqkv_ref, gconv_ref, gmix_ref, gg_ref, m_ref):
    step, steps = pl.program_id(0), pl.num_programs(0)
    t = p_ref.shape[-1]

    @pl.when(step == 0)
    def _():
        m_ref[...] = jnp.zeros_like(m_ref)
        gmix_ref[...] = jnp.zeros_like(gmix_ref)
        gg_ref[...] = jnp.zeros_like(gg_ref)

    allowed = allowed_mask(dcol_ref[0], drow_ref[0])
    scale = 1.0 / math.sqrt(E)
    lane = lax.broadcasted_iota(jnp.int32, (1, EP), 1)
    p = [p_ref[0, 0], p_ref[0, 1]]
    dmixed = []
    for h in range(2):
        cols = slice(h * EP, (h + 1) * EP)
        dn, xhat = dn_ref[0, :, cols], xhat_ref[0, :, cols]
        gg_ref[0:1, cols] += jnp.sum(dn * xhat, axis=0, keepdims=True)
        dc = dn * gain_ref[0:1, cols]
        m1 = jnp.sum(dc, axis=1, keepdims=True) / E
        m2 = jnp.sum(dc * xhat, axis=1, keepdims=True) / E
        dh = jnp.where(lane < E, s_ref[0, :, cols] * (dc - m1 - xhat * m2), 0.0).astype(bf16)
        v = qkv_ref[0, :, (4 + h) * EP:(5 + h) * EP]
        mixed = (mix_ref[h, 0] * p[0] + mix_ref[h, 1] * p[1]).astype(bf16)
        dmixed.append(dot(dh, v, 1, 1))
        dqkv_ref[0, :, (4 + h) * EP:(5 + h) * EP] = dot(mixed, dh, 0, 0).astype(bf16)
    for h in range(2):
        for c in range(2):
            r = 2 * h + c
            gmix_ref[r:r + 1, :] += jnp.sum(dmixed[h] * p[c], axis=0, keepdims=True)
    for c in range(2):
        dp = mix_ref[0, c] * dmixed[0] + mix_ref[1, c] * dmixed[1]
        dconv = p[c] * (dp - jnp.sum(dp * p[c], axis=1, keepdims=True))
        ahead = jnp.concatenate([up(dconv, a).astype(bf16) for a in range(QWIN)], 1)
        m_ref[c] += dot(z_ref[0, c], ahead, 0, 0)
        ds = jnp.where(allowed, dot(ahead, tt_ref[c]), 0.0).astype(bf16)
        q = qkv_ref[0, :, c * EP:(c + 1) * EP]
        k = qkv_ref[0, :, (2 + c) * EP:(3 + c) * EP]
        dqkv_ref[0, :, c * EP:(c + 1) * EP] = (dot(ds, k) * scale).astype(bf16)
        dqkv_ref[0, :, (2 + c) * EP:(3 + c) * EP] = (dot(ds, q, 0, 0) * scale).astype(bf16)

    @pl.when(step == steps - 1)
    def _():
        lanes = lax.broadcasted_iota(jnp.int32, (8, t), 1)
        for h in range(2):
            for a in range(QWIN):
                total = jnp.zeros((8, t), f32)
                for first in range(0, t, 8):
                    rows = m_ref[h, first:first + 8, a * t:(a + 1) * t]
                    turned = pltpu.roll(rows, t - first, 1) if first else rows
                    total = total + jnp.where(lanes < t - first, turned, 0.0)
                gconv_ref[h, a] = total[:, :EP]


def attend_back(mix, qkv, dcol, drow, tt, gain, dn, xhat, s, p, z):
    n, t, _ = qkv.shape
    row = lambda *sh: pl.BlockSpec((1,) + sh, lambda i: (i,) + (0,) * len(sh))
    full = lambda a: pl.BlockSpec(a.shape, lambda i: (0,) * a.ndim)
    keep = lambda *sh: pl.BlockSpec(sh, lambda i: (0,) * len(sh))
    return pl.pallas_call(
        bwd_kernel,
        grid=(n,),
        in_specs=[pl.BlockSpec(memory_space=pltpu.SMEM), row(t, 6 * EP), row(t, 1), row(1, t), full(tt), full(gain),
                  row(t, 2 * EP), row(t, 2 * EP), row(t, 2 * EP), row(2, t, t), row(2, t, t)],
        out_specs=[row(t, 6 * EP), keep(2, QWIN, 8, EP), keep(8, t), keep(8, 2 * EP)],
        out_shape=[
            jax.ShapeDtypeStruct((n, t, 6 * EP), bf16),
            jax.ShapeDtypeStruct((2, QWIN, 8, EP), f32),
            jax.ShapeDtypeStruct((8, t), f32),
            jax.ShapeDtypeStruct((8, 2 * EP), f32),
        ],
        scratch_shapes=[pltpu.VMEM((2, t, QWIN * t), f32)],
        cost_estimate=pl.CostEstimate(flops=n * 2 * 2 * 2 * t * t * QWIN * t, bytes_accessed=n * t * t * 20, transcendentals=0),
        name="attend_back",
    )(mix, qkv, dcol, drow, tt, gain, dn, xhat, s, p, z)


def bands(kernel, t):
    diff = jnp.arange(t)[None, :] - jnp.arange(t)[:, None]
    band = jnp.zeros((2, QWIN, t, t), f32)
    back = jnp.zeros((2, QWIN, t, t), f32)
    for b in range(KWIN):
        tap = kernel[:, :, b][:, :, None, None]
        band = band + jnp.where(diff == b, tap, 0.0)
        back = back + jnp.where(diff == -b, tap, 0.0)
    th, tl = split(band)
    flat = lambda v: v.reshape(2, QWIN * t, t)
    return flat(th), flat(tl), flat(back.astype(bf16))


def diagonals(tiles):
    return sum(tiles[:, :, i, i:i + KWIN] for i in range(8))


FF = 4096
MESH = pl.DeviceIdType.MESH


class Net:
    def __init__(self):
        self.x, self.f = lax.axis_index("rep"), lax.axis_index("fsdp")
        self.z, self.y, self.c = self.f // 4, (self.f // 2) % 2, self.f % 2
        self.k = self.f % 4
        nx, fy, fc = 1 - self.x, 2 - 4 * self.y, 1 - 2 * self.c
        self.to = {
            "x": (nx, self.f),
            "y": (self.x, self.f + fy),
            "c": (self.x, self.f + fc),
            "xy": (nx, self.f + fy),
            "xc": (nx, self.f + fc),
            "yc": (self.x, self.f + fy + fc),
            "xyc": (nx, self.f + fy + fc),
            "up": (self.x, self.f + 4),
            "down": (self.x, self.f - 4),
        }

    def greet(self, names, line=True):
        barrier = pltpu.get_barrier_semaphore()
        for name in names:
            pl.semaphore_signal(barrier, inc=1, device_id=self.to[name], device_id_type=MESH)
        count = len(names)
        if line:

            @pl.when(self.z < 3)
            def _():
                pl.semaphore_signal(barrier, inc=1, device_id=self.to["up"], device_id_type=MESH)

            @pl.when(self.z > 0)
            def _():
                pl.semaphore_signal(barrier, inc=1, device_id=self.to["down"], device_id_type=MESH)

            count = count + (self.z + 3) // 4 + (6 - self.z) // 4
        pl.semaphore_wait(barrier, count)

    def copy(self, src, dst, sems, i, name):
        return pltpu.make_async_remote_copy(
            src_ref=src, dst_ref=dst, send_sem=sems[0].at[i], recv_sem=sems[1].at[i],
            device_id=self.to[name], device_id_type=MESH,
        )

    def send(self, src, dst, sems, i, name):
        copy = self.copy(src, dst, sems, i, name)
        copy.start()
        return copy


def tiles(start, size, body, step=32):
    def one(i, _):
        body(pl.ds(pl.multiple_of(start + i * step, step), step))
        return 0

    lax.fori_loop(0, size // step, one, 0)


def wide(v):
    return v.astype(f32)


class GatherLine:
    def __init__(self, net, src, out, sems, base, keep=None):
        self.net, self.src, self.out, self.sems, self.base = net, src, out, sems, base
        self.keep = keep or (lambda slot: net.z >= 0)

    def go(self, d, way, act):
        net = self.net
        slot = net.z - d if way == "up" else net.z + d
        inside = (net.z >= d) & (net.z < 3) if way == "up" else (net.z < 4 - d) & (net.z > 0)
        i = self.base + d + (0 if way == "up" else 3)

        @pl.when(inside & self.keep(slot))
        def _():
            src = self.src if d == 0 else self.out.at[slot]
            act(net.copy(src, self.out.at[slot], self.sems, i, way))

    def came(self, d, way):
        net = self.net
        slot = net.z - d if way == "up" else net.z + d
        inside = net.z >= d if way == "up" else net.z < 4 - d
        i = self.base + d - 1 + (0 if way == "up" else 3)

        @pl.when(inside & self.keep(slot))
        def _():
            net.copy(self.out.at[slot], self.out.at[slot], self.sems, i, way).wait_recv()

    def step(self, d):
        for way in ("up", "down"):
            if d > 0:
                self.came(d, way)
            if d < 3:
                self.go(d, way, lambda copy: copy.start())

    def finish(self):
        for d in range(3):
            for way in ("up", "down"):
                self.go(d, way, lambda copy: copy.wait_send())


class ScatterLine:
    def __init__(self, net, parts, got, made, sems, base):
        self.net, self.parts, self.got, self.made, self.sems, self.base = net, parts, got, made, sems, base
        self.n = parts.shape[1]

    def each(self, d, way):
        net = self.net
        t = net.z + (3 - d) if way == 0 else net.z - (3 - d)
        inside = (t < 4) if way == 0 else (t >= 0)
        first = (net.z == 0) if way == 0 else (net.z == 3)
        return t, inside, first, self.base + d + 3 * way, ("up", "down")[way]

    def step(self, d):
        for way in range(2):
            t, inside, first, i, name = self.each(d, way)

            @pl.when(inside & first)
            def _():
                self.net.copy(self.parts.at[t], self.got.at[way, d], self.sems, i, name).start()

            if d == 0:
                continue

            @pl.when(inside & jnp.logical_not(first))
            def _():
                self.net.copy(self.got.at[way, d - 1], self.got.at[way, d - 1], self.sems, i - 1, name).wait_recv()

                def body(rows):
                    self.made[way, d - 1, rows] = (wide(self.parts[t, rows]) + wide(self.got[way, d - 1, rows])).astype(bf16)

                tiles(0, self.n, body)
                self.net.copy(self.made.at[way, d - 1], self.got.at[way, d], self.sems, i, name).start()

    def finish(self, store):
        net = self.net
        below, above = net.z > 0, net.z < 3

        @pl.when(below)
        def _():
            net.copy(self.got.at[0, 2], self.got.at[0, 2], self.sems, self.base + 2, "up").wait_recv()

        @pl.when(above)
        def _():
            net.copy(self.got.at[1, 2], self.got.at[1, 2], self.sems, self.base + 5, "down").wait_recv()

        def put(low, high):
            def body(rows):
                total = wide(self.parts[net.z, rows])
                if low:
                    total = total + wide(self.got[0, 2, rows])
                if high:
                    total = total + wide(self.got[1, 2, rows])
                store(rows, total)

            tiles(0, self.n, body)

        @pl.when(below & above)
        def _():
            put(True, True)

        @pl.when(jnp.logical_not(below))
        def _():
            put(False, True)

        @pl.when(jnp.logical_not(above))
        def _():
            put(True, False)

        for d in range(3):
            for way in range(2):
                t, inside, first, i, name = self.each(d, way)

                @pl.when(inside & first)
                def _():
                    net.copy(self.parts.at[t], self.got.at[way, d], self.sems, i, name).wait_send()

                if d > 0:

                    @pl.when(inside & jnp.logical_not(first))
                    def _():
                        net.copy(self.made.at[way, d - 1], self.got.at[way, d], self.sems, i, name).wait_send()


def line_scratch(n, w):
    return [pltpu.VMEM((2, 3, n, w), bf16), pltpu.VMEM((2, 2, n, w), bf16)]


LINE_COPIES = 6


class Later:
    def __init__(self, make):
        self.make = make
        make().start()

    def wait_recv(self):
        self.make().wait_recv()

    def wait_send(self):
        self.make().wait_send()


def gather_steps(net, v, out, sems, base, ready):
    n = v.shape[0]
    A, B = pl.ds(0, n // 2), pl.ds(n // 2, n // 2)
    go = {}
    ready(0)
    go["xA"] = Later(lambda: net.copy(v.at[A], out.at[1, 0, A], sems, base + 0, "x"))
    go["yA"] = Later(lambda: net.copy(v.at[A], out.at[2, 0, A], sems, base + 3, "y"))
    go["0A"] = Later(lambda: net.copy(v.at[A], out.at[0, 1, A], sems, base + 4, "c"))
    ready(1)
    go["yB"] = Later(lambda: net.copy(v.at[B], out.at[2, 0, B], sems, base + 2, "y"))
    go["xB"] = Later(lambda: net.copy(v.at[B], out.at[1, 0, B], sems, base + 1, "x"))
    go["0B"] = Later(lambda: net.copy(v.at[B], out.at[0, 1, B], sems, base + 5, "c"))
    yield
    go["xA"].wait_recv()
    go["dA"] = Later(lambda: net.copy(out.at[1, 0, A], out.at[3, 0, A], sems, base + 6, "y"))
    go["1A"] = Later(lambda: net.copy(out.at[1, 0, A], out.at[1, 1, A], sems, base + 8, "c"))
    go["yA"].wait_recv()
    go["2A"] = Later(lambda: net.copy(out.at[2, 0, A], out.at[2, 1, A], sems, base + 10, "c"))
    yield
    go["yB"].wait_recv()
    go["dB"] = Later(lambda: net.copy(out.at[2, 0, B], out.at[3, 0, B], sems, base + 7, "x"))
    go["2B"] = Later(lambda: net.copy(out.at[2, 0, B], out.at[2, 1, B], sems, base + 9, "c"))
    go["xB"].wait_recv()
    go["1B"] = Later(lambda: net.copy(out.at[1, 0, B], out.at[1, 1, B], sems, base + 11, "c"))
    yield
    go["dA"].wait_recv()
    go["3A"] = Later(lambda: net.copy(out.at[3, 0, A], out.at[3, 1, A], sems, base + 12, "c"))
    go["dB"].wait_recv()
    go["3B"] = Later(lambda: net.copy(out.at[3, 0, B], out.at[3, 1, B], sems, base + 13, "c"))
    yield
    for name in ("0A", "0B", "1A", "2B", "2A", "1B", "3A", "3B"):
        go[name].wait_recv()
    for copy in go.values():
        copy.wait_send()


def gather_rows(net, v, out, sems, base, ready, poll):
    for _ in gather_steps(net, v, out, sems, base, ready):
        poll()


GATHER_COPIES = 14
SCATTER_COPIES = 10


def scatter_steps(net, parts, rc, rd, rx, ry, td, tx, ty, sems, base):
    n = parts.shape[2]
    A, B = pl.ds(0, n // 2), pl.ds(n // 2, n // 2)
    go = {}
    for i, chip in enumerate((3, 1, 2, 0)):
        go[chip] = Later(lambda i=i, chip=chip: net.copy(parts.at[chip, 1], rc.at[chip], sems, base + i, "c"))

    def add(dst, chip, start, more=None):
        def body(rows):
            total = wide(parts[chip, 0, rows]) + wide(rc[chip, rows])
            if more is not None:
                total = total + wide(more[rows])
            dst[rows] = total.astype(bf16)

        tiles(start, n // 2, body)

    yield None
    go[3].wait_recv()
    add(td, 3, 0)
    go["dA"] = Later(lambda: net.copy(td.at[A], rd.at[A], sems, base + 4, "x"))
    add(td, 3, n // 2)
    go["dB"] = Later(lambda: net.copy(td.at[B], rd.at[B], sems, base + 5, "y"))
    go[1].wait_recv()
    add(tx, 1, 0)
    go["xA"] = Later(lambda: net.copy(tx.at[A], rx.at[A], sems, base + 6, "x"))
    go[2].wait_recv()
    add(ty, 2, n // 2)
    go["yB"] = Later(lambda: net.copy(ty.at[B], ry.at[B], sems, base + 7, "y"))
    yield None
    go["dA"].wait_recv()
    add(ty, 2, 0, rd)
    go["yA"] = Later(lambda: net.copy(ty.at[A], ry.at[A], sems, base + 8, "y"))
    go["dB"].wait_recv()
    add(tx, 1, n // 2, rd)
    go["xB"] = Later(lambda: net.copy(tx.at[B], rx.at[B], sems, base + 9, "x"))
    go[0].wait_recv()

    def done(half):
        for name in (("xA", "yA"), ("xB", "yB"))[half]:
            go[name].wait_recv()
        if half == 1:
            for copy in go.values():
                copy.wait_send()

    yield done


def scatter_rows(net, parts, rc, rd, rx, ry, td, tx, ty, sems, base, poll):
    steps = scatter_steps(net, parts, rc, rd, rx, ry, td, tx, ty, sems, base)
    next(steps)
    next(steps)
    poll()
    return next(steps)


def scatter_scratch(n, w):
    return [pltpu.VMEM((4, n, w), bf16)] + [pltpu.VMEM((n, w), bf16)] * 6


def dma_sems(count):
    return [pltpu.SemaphoreType.DMA((count,)), pltpu.SemaphoreType.DMA((count,))]


VM = pl.BlockSpec(memory_space=pltpu.VMEM)
ANY = pl.BlockSpec(memory_space=pl.ANY)


def polls(*acts):
    left = list(acts)

    def poll():
        if left:
            left.pop(0)()

    def drain():
        while left:
            poll()

    return poll, drain


def comm_call(body, name, ident, ins, in_specs, outs, out_specs, scratch):
    return pl.pallas_call(
        body,
        in_specs=in_specs,
        out_specs=out_specs,
        out_shape=outs,
        scratch_shapes=scratch,
        compiler_params=pltpu.CompilerParams(collective_id=ident, has_side_effects=True, vmem_limit_bytes=63 << 20),
        name=name,
    )(*ins)


def shape(dims, dtype):
    return jax.ShapeDtypeStruct(dims, dtype)


PLANE = ("x", "y", "c", "xy", "xc", "yc", "xyc")
PLACES = {"c": (0, 1), "x": (1, 0), "xc": (1, 1), "y": (2, 0), "yc": (2, 1), "xy": (3, 0), "xyc": (3, 1)}


def start_call(x, dy, docs, gains, taps, w_qkv, w_gate, w_up, w_out, ident):
    n, w = x.shape
    rows = w_qkv.shape[0]

    def body(x_ref, dy_ref, docs_ref, g_ref, taps_ref, wq_ref, gate_ref, up_ref, wo_ref,
             a1_ref, dys_ref, docs_out, gains_ref, qkv_out, gu_out, wo_out, th_ref, tl_ref, tt_ref,
             xs, gains_out, slots, gus, local, send, recv):
        net = Net()
        sems = (send, recv)
        base = 2 * GATHER_COPIES
        mine = dy_ref.at[pl.ds(0, n // 2)]
        line_q = GatherLine(net, qkv_out.at[net.z], qkv_out, sems, base)
        line_o = GatherLine(net, wo_ref, wo_out, sems, base + 6, lambda slot: slot // 2 == net.x)
        line_g = GatherLine(net, gains_out.at[net.z], gains_out, sems, base + 12)
        base += 18
        gains_out[net.z, net.k] = g_ref[...]
        slots[...] = jnp.zeros_like(slots)
        for half in range(2):

            @pl.when(net.x == half)
            def _():
                for k in range(4):
                    pair = 4 * half + 2 * (k % 2) + k // 2
                    for m in range(6):
                        col = (m // 2) * MODEL_WIDTH + (2 * pair + m % 2) * E
                        slots[k, :, m * EP : m * EP + E] = wq_ref[:, col : col + E]
                    for m in range(8):
                        src = gate_ref if m < 4 else up_ref
                        col = 256 * (4 * (m % 4) + k) + 128 * half
                        gus[k, :, m * 128 : (m + 1) * 128] = src[:, col : col + 128]

        net.greet(PLANE)
        own = [
            pltpu.make_async_copy(mine, dys_ref.at[0, 0], local.at[1]),
            pltpu.make_async_copy(slots.at[net.k], qkv_out.at[net.z, net.k], local.at[0]),
            pltpu.make_async_copy(gus.at[net.k], gu_out.at[net.k], local.at[2]),
            pltpu.make_async_copy(docs_ref, docs_out.at[0, 0], local.at[3]),
            pltpu.make_async_copy(wo_ref, wo_out.at[net.z], local.at[4]),
        ]
        for copy in own:
            copy.start()
        qkv_parts, gain_parts, small = [], [], []
        flips = {"c": net.k + 1 - 2 * net.c, "y": net.k + 2 - 4 * net.y, "yc": net.k + 1 - 2 * net.c + 2 - 4 * net.y}
        for j, name in enumerate(("y", "yc", "c")):
            gain_parts.append(net.send(g_ref, gains_out.at[net.z, net.k], sems, base + 6 + j, name))
            qkv_parts.append(net.send(slots.at[flips[name]], qkv_out.at[net.z, net.k], sems, base + j, name))
        line_o.step(0)
        for j, (name, (chip, core)) in enumerate(PLACES.items()):
            small.append(net.send(docs_ref, docs_out.at[chip, core], sems, base + 9 + j, name))
        gather_x = gather_steps(net, x_ref, xs, sems, 0, lambda half: None)
        next(gather_x)
        gather_dy = gather_steps(net, mine, dys_ref, sems, GATHER_COPIES, lambda half: None)
        next(gather_dy)
        for copy in gain_parts:
            copy.wait_recv()
        line_g.step(0)
        own[1].wait()
        for copy in qkv_parts:
            copy.wait_recv()
        line_q.step(0)
        line_g.step(1)

        diff = lax.broadcasted_iota(jnp.int32, (n, n), 1) - lax.broadcasted_iota(jnp.int32, (n, n), 0)

        def bands_of(first, count):
            def one(i, _):
                band = jnp.zeros((n, n), f32)
                back = jnp.zeros((n, n), f32)
                for b in range(KWIN):
                    tap = taps_ref[(first + i) * KWIN + b]
                    band = jnp.where(diff == b, tap, band)
                    back = jnp.where(diff == -b, tap, back)
                h, a = (first + i) // QWIN, (first + i) % QWIN
                at = pl.ds(pl.multiple_of(a * n, n), n)
                th_ref[h, at], tl_ref[h, at] = split(band)
                tt_ref[h, at] = back.astype(bf16)
                return 0

            lax.fori_loop(0, count, one, 0)

        bands_of(0, QWIN)
        line_g.step(2)
        next(gather_x)
        line_q.step(1)
        line_g.step(3)
        line_o.step(1)
        for i in range(16):
            gains_ref[:, i * rows : (i + 1) * rows] = wide(gains_out[i // 4, i % 4, 0:8, 0:rows])
        bands_of(QWIN, QWIN)
        next(gather_x)
        for j, name in enumerate(("y", "yc", "c")):
            small.append(net.send(gus.at[flips[name]], gu_out.at[net.k], sems, base + 3 + j, name))
        gain = gains_ref[0:1]

        def norm(chip, core, src):
            def body(at):
                xf = wide(src[at])
                r = lax.rsqrt(jnp.mean(xf * xf, axis=1, keepdims=True) + 1e-06)
                a1_ref[chip, core, at] = (xf * r * gain).astype(bf16)

            tiles(0, n, body)

        norm(0, 0, x_ref)
        line_q.step(2)
        line_o.step(2)
        for _ in gather_x:
            pass
        next(gather_dy)
        next(gather_dy)
        for chip in range(4):
            for core in range(2):
                if (chip, core) != (0, 0):
                    norm(chip, core, xs.at[chip, core])
        next(gather_dy)
        line_q.step(3)
        for _ in gather_dy:
            pass
        line_o.step(3)
        for line in (line_q, line_g, line_o):
            line.finish()
        for copy in own[:1] + own[2:]:
            copy.wait()
        for copy in small:
            copy.wait_recv()
        for copy in qkv_parts + gain_parts + small:
            copy.wait_send()

    return comm_call(
        body, "start", ident, (x, dy, docs, gains, taps, w_qkv, w_gate, w_up, w_out),
        [VM] * 4 + [pl.BlockSpec(memory_space=pltpu.SMEM)] + [VM] * 4,
        [shape((4, 2, n, w), bf16), shape((4, 2, n // 2, w), bf16), shape((4, 2) + docs.shape, docs.dtype), shape((8, w), f32),
         shape((4, 4, rows, 6 * EP), bf16), shape((4, rows, FF // 4), bf16), shape((4, rows, MODEL_WIDTH), bf16)]
        + [shape((2, QWIN * n, n), bf16)] * 3,
        [VM, ANY, ANY, VM, ANY, ANY, ANY, VM, VM, VM],
        [pltpu.VMEM((4, 2, n, w), bf16), pltpu.VMEM((4, 4) + gains.shape, bf16),
         pltpu.VMEM((4, rows, 6 * EP), bf16), pltpu.VMEM((4, rows, FF // 4), bf16), pltpu.SemaphoreType.DMA((5,))]
        + dma_sems(2 * GATHER_COPIES + 18 + 16),
    )


def turn(docs):
    return jnp.transpose(docs)[:, 0:1], docs[0:1]


def forward_call(mix, a1, docs, th, tl, group, qkv_w, out_w, x, dy, gain, gu, w_down, ident):
    rows, t, w = a1.shape
    n = x.shape[0]
    down = w_down.shape[0] // 2

    def body(mix_ref, a1_ref, docs_ref, th_ref, tl_ref, group_ref, qw_ref, ow_ref, x_ref, dy_ref, g_ref, gu_ref, wd_ref,
             qkv_ref, normed_ref, xhat_ref, s_ref, p_ref, z_ref, resid_ref, out_ref, dys_ref, gu_out, wd_out,
             parts, v, local, rc, rd, rx, ry, td, tx, ty, send, recv):
        net = Net()
        sems = (send, recv)
        step = pl.program_id(0)
        base = SCATTER_COPIES + GATHER_COPIES
        mine = wd_ref.at[pl.ds(pl.multiple_of(down * net.x, down), down)]
        line_g = GatherLine(net, gu_ref, gu_out, sems, base)
        line_d = GatherLine(net, mine, wd_out, sems, base + LINE_COPIES)
        own_g = lambda: pltpu.make_async_copy(gu_ref, gu_out.at[net.z], local.at[1])
        own_d = lambda: pltpu.make_async_copy(mine, wd_out.at[net.z], local.at[2])
        A, B = pl.ds(0, n // 2), pl.ds(n // 2, n // 2)
        go = {}
        half_dy = dy_ref.at[pl.ds(n // 2, n // 2)]
        own_dy = lambda: pltpu.make_async_copy(half_dy, dys_ref.at[0, 0], local.at[3])
        gather_dy = gather_steps(net, half_dy, dys_ref, sems, base + 2 * LINE_COPIES, lambda half: None)

        def at(i):
            def run(act):
                pl.when(step == i)(act)

            return run

        @at(0)
        def _():
            net.greet("xyc")
            line_g.step(0)
            line_d.step(0)
            own_g().start()
            own_d().start()
            own_dy().start()
            next(gather_dy)

        qkv_ref[0] = dot(a1_ref[0], qw_ref[...]).astype(bf16)
        col, across = turn(docs_ref[0])
        attend_row(mix_ref, qkv_ref, [col], [across], th_ref, tl_ref, group_ref, normed_ref, xhat_ref, s_ref, p_ref, z_ref)
        parts[3 - step // 2, step % 2] = dot(normed_ref[0], ow_ref[...]).astype(bf16)

        def swap(chip, i):
            go[chip] = Later(lambda: net.copy(parts.at[chip, 1], rc.at[chip], sems, i, "c"))

        def add(dst, chip, start, more=None):
            def one(r):
                total = wide(parts[chip, 0, r]) + wide(rc[chip, r])
                if more is not None:
                    total = total + wide(more[r])
                dst[r] = total.astype(bf16)

            tiles(start, n // 2, one)

        @at(1)
        def _():
            swap(3, 0)

        @at(2)
        def _():
            go[3].wait_recv()
            add(td, 3, 0)
            go["dA"] = Later(lambda: net.copy(td.at[A], rd.at[A], sems, 4, "x"))
            add(td, 3, n // 2)
            go["dB"] = Later(lambda: net.copy(td.at[B], rd.at[B], sems, 5, "y"))

        @at(3)
        def _():
            swap(2, 2)
            line_g.step(1)
            next(gather_dy)

        @at(4)
        def _():
            go[2].wait_recv()
            add(ty, 2, n // 2)
            go["yB"] = Later(lambda: net.copy(ty.at[B], ry.at[B], sems, 7, "y"))
            go["dA"].wait_recv()
            add(ty, 2, 0, rd)
            go["yA"] = Later(lambda: net.copy(ty.at[A], ry.at[A], sems, 8, "y"))
            next(gather_dy)

        @at(5)
        def _():
            swap(1, 1)
            line_d.step(1)
            next(gather_dy)

        @at(6)
        def _():
            go[1].wait_recv()
            add(tx, 1, 0)
            go["xA"] = Later(lambda: net.copy(tx.at[A], rx.at[A], sems, 6, "x"))
            go["dB"].wait_recv()
            add(tx, 1, n // 2, rd)
            go["xB"] = Later(lambda: net.copy(tx.at[B], rx.at[B], sems, 9, "x"))

        @at(rows - 1)
        def _():
            swap(0, 3)
            line_g.step(2)
            for _ in gather_dy:
                pass
            go[0].wait_recv()

            def ready(half):
                for name in (("yA", "xA"), ("yB", "xB"))[half]:
                    go[name].wait_recv()

                def rows_of(r):
                    total = wide(parts[0, 0, r]) + wide(rc[0, r]) + wide(rx[r]) + wide(ry[r])
                    resid = wide(x_ref[r]) + total
                    resid_ref[r] = resid
                    inv = lax.rsqrt(jnp.mean(resid * resid, axis=1, keepdims=True) + 1e-06)
                    v[r] = (resid * inv * g_ref[...]).astype(bf16)

                tiles(half * (n // 2), n // 2, rows_of)

            poll, drain = polls(lambda: line_d.step(2), lambda: line_g.step(3), lambda: line_d.step(3))
            gather_rows(net, v, out_ref, sems, SCATTER_COPIES, ready, poll)
            drain()
            last = pltpu.make_async_copy(v, out_ref.at[0, 0], local.at[0])
            last.start()
            line_g.finish()
            line_d.finish()
            own_g().wait()
            own_d().wait()
            own_dy().wait()
            for copy in go.values():
                copy.wait_send()
            last.wait()

    where = lambda i: 2 * (3 - i // 2) + i % 2
    row = lambda *sh: pl.BlockSpec((1,) + sh, lambda i: (where(i),) + (0,) * len(sh))
    full = lambda v: pl.BlockSpec(v.shape, lambda i: (0,) * v.ndim, pipeline_mode=pl.Buffered(1))
    keep = lambda *sh: pl.BlockSpec(sh, lambda i: (0,) * len(sh))
    return pl.pallas_call(
        body,
        grid=(rows,),
        in_specs=[pl.BlockSpec(memory_space=pltpu.SMEM), row(t, w), row(8, t), full(th), full(tl), full(group), full(qkv_w),
                  full(out_w), full(x), full(dy), full(gain), full(gu), full(w_down)],
        out_specs=[row(t, 6 * EP), row(t, 2 * EP), row(t, 2 * EP), row(t, 2 * EP), row(2, t, t), row(2, t, t), keep(n, w), ANY, ANY, ANY, ANY],
        out_shape=[
            shape((rows, t, 6 * EP), bf16),
            shape((rows, t, 2 * EP), bf16),
            shape((rows, t, 2 * EP), f32),
            shape((rows, t, 2 * EP), f32),
            shape((rows, 2, t, t), f32),
            shape((rows, 2, t, t), bf16),
            shape((n, w), f32),
            shape((4, 2, n, w), bf16),
            shape((4, 2, n // 2, w), bf16),
            shape((4,) + gu.shape, bf16),
            shape((4, down, w), bf16),
        ],
        scratch_shapes=[pltpu.VMEM((4, 2, n, w), bf16), pltpu.VMEM((n, w), bf16), pltpu.SemaphoreType.DMA((4,))] + scatter_scratch(n, w)
        + dma_sems(SCATTER_COPIES + 2 * GATHER_COPIES + 2 * LINE_COPIES),
        compiler_params=pltpu.CompilerParams(collective_id=ident, has_side_effects=True, vmem_limit_bytes=60 << 20),
        name="forward",
    )(mix, a1, docs, th, tl, group, qkv_w, out_w, x, dy, gain, gu, w_down)


def ffn_call(a2, first, second, gu_w, down_w):
    count, w = a2.shape
    half = down_w.shape[0]
    m = count // 4
    part = half // 2

    def body(a2_ref, df1_ref, df2_ref, gw_ref, dw_ref, dgu_ref, hid_ref, gd_ref, df_ref, total):
        step = pl.program_id(0)

        @pl.when(step == 0)
        def _():
            total[...] = jnp.zeros_like(total)

        q = m // 4
        for i in range(2):
            df_ref[2 * i * q : (2 * i + 1) * q] = df1_ref[i * q : (i + 1) * q]
            df_ref[(2 * i + 1) * q : (2 * i + 2) * q] = df2_ref[i * q : (i + 1) * q]
        for j in range(2):
            cols, more = slice(j * part, (j + 1) * part), slice(half + j * part, half + (j + 1) * part)
            gate, up_act = dot(a2_ref[...], gw_ref[:, cols]), dot(a2_ref[...], gw_ref[:, more])
            dhidden = dot(df_ref[...], dw_ref[cols], 1, 1)
            sig = jax.nn.sigmoid(gate)
            silu = gate * sig
            hid_ref[:, cols] = (silu * up_act).astype(bf16)
            dgu_ref[:, cols] = (dhidden * up_act * sig * (1.0 + gate * (1.0 - sig))).astype(bf16)
            dgu_ref[:, more] = (dhidden * silu).astype(bf16)
        total[...] += dot(hid_ref[...], df_ref[...], 0, 0)

        @pl.when(step == 3)
        def _():
            gd_ref[...] = total[...].astype(bf16)

    row = lambda k, m=m: pl.BlockSpec((m, k), lambda i: (i, 0))
    full = lambda v: pl.BlockSpec(v.shape, lambda i: (0, 0), pipeline_mode=pl.Buffered(1))
    return pl.pallas_call(
        body,
        grid=(4,),
        in_specs=[row(w), row(w, m // 2), row(w, m // 2), full(gu_w), full(down_w)],
        out_specs=[row(2 * half), row(half), pl.BlockSpec((half, w), lambda i: (0, 0))],
        out_shape=[shape((count, 2 * half), bf16), shape((count, half), bf16), shape((half, w), bf16)],
        scratch_shapes=[pltpu.VMEM((m, w), bf16), pltpu.VMEM((half, w), f32)],
        compiler_params=pltpu.CompilerParams(vmem_limit_bytes=63 << 20),
        name="ffn",
    )(a2, first, second, gu_w, down_w)


def mid_back_call(dgu, gu_w, a2, hidden, down_w, dy, resid, gain, down, ident):
    n, w = dy.shape
    m, half = dgu.shape[0] // 4, gu_w.shape[1] // 2

    def body(dgu_ref, gw_ref, a2_ref, hid_ref, dw_ref, dy_ref, r_ref, g_ref, down_ref,
             dresid_ref, out_ref, sum_ref, down_out, gate_out, up_out, op_out,
             parts, a2s, hids, dws, stage, gates, v, local, rc, rd, rx, ry, td, tx, ty, d_got, d_made, g_got, g_made, send, recv):
        net = Net()
        sems = (send, recv)
        net.greet("xyc")
        base = SCATTER_COPIES + GATHER_COPIES
        line_d = ScatterLine(net, down_ref, d_got, d_made, sems, base)
        line_g = ScatterLine(net, gates, g_got, g_made, sems, base + LINE_COPIES)
        line_d.step(0)
        loads = [pltpu.make_async_copy(src, dst, local.at[i]) for i, (src, dst) in enumerate(((a2_ref, a2s), (hid_ref, hids), (dw_ref, dws)))]
        for copy in loads:
            copy.start()
        A, B = pl.ds(0, n // 2), pl.ds(n // 2, n // 2)
        go = {}

        def part(chip):
            for j in range(3):
                cols = slice(j * (w // 3), (j + 1) * (w // 3))
                total = dot(dgu_ref[chip * m : (chip + 1) * m], gw_ref[cols], 1, 1)
                parts[chip, :, :, cols] = total.astype(bf16).reshape(2, n, w // 3)

        def swap(chip, i):
            go[chip] = Later(lambda: net.copy(parts.at[chip, 1], rc.at[chip], sems, i, "c"))

        def add(dst, chip, start, more=None):
            def one(r):
                total = wide(parts[chip, 0, r]) + wide(rc[chip, r])
                if more is not None:
                    total = total + wide(more[r])
                dst[r] = total.astype(bf16)

            tiles(start, n // 2, one)

        def weights(first, last):
            for i in range(first, last):
                rows = slice(i * (w // 4), (i + 1) * (w // 4))
                total = dot(a2s[:, rows], dgu_ref[...], 0, 0)
                gates[i] = total[:, :half].astype(bf16)
                up_out[i] = total[:, half:].astype(bf16)

        def put_back(chip):
            return pltpu.make_async_copy(stage.at[chip % 2], op_out.at[chip], local.at[4 + chip % 2])

        def forward(chip):
            if chip >= 2:
                put_back(chip - 2).wait()
            for j in range(3):
                cols = slice(j * (w // 3), (j + 1) * (w // 3))
                total = dot(hids[chip * m : (chip + 1) * m], dws[:, cols])
                stage[chip % 2, :, :, cols] = total.astype(bf16).reshape(2, n, w // 3)
            put_back(chip).start()

        part(3)
        swap(3, 0)
        part(2)
        swap(2, 2)
        go[3].wait_recv()
        add(td, 3, 0)
        go["dA"] = Later(lambda: net.copy(td.at[A], rd.at[A], sems, 4, "x"))
        add(td, 3, n // 2)
        go["dB"] = Later(lambda: net.copy(td.at[B], rd.at[B], sems, 5, "y"))
        part(1)
        swap(1, 1)
        go[2].wait_recv()
        add(ty, 2, n // 2)
        go["yB"] = Later(lambda: net.copy(ty.at[B], ry.at[B], sems, 7, "y"))
        part(0)
        swap(0, 3)
        go[1].wait_recv()
        add(tx, 1, 0)
        go["xA"] = Later(lambda: net.copy(tx.at[A], rx.at[A], sems, 6, "x"))
        loads[0].wait()
        go["dA"].wait_recv()
        add(ty, 2, 0, rd)
        go["yA"] = Later(lambda: net.copy(ty.at[A], ry.at[A], sems, 8, "y"))
        go["dB"].wait_recv()
        add(tx, 1, n // 2, rd)
        go["xB"] = Later(lambda: net.copy(tx.at[B], rx.at[B], sems, 9, "x"))
        weights(0, 4)
        line_g.step(0)
        line_d.step(1)
        loads[1].wait()
        loads[2].wait()
        sum_ref[...] = jnp.zeros_like(sum_ref)
        go[0].wait_recv()

        def ready(side):
            for name in (("xA", "yA"), ("xB", "yB"))[side]:
                go[name].wait_recv()

            def rows_of(r):
                da2 = wide(parts[0, 0, r]) + wide(rc[0, r]) + wide(rx[r]) + wide(ry[r])
                res = r_ref[r]
                inv = lax.rsqrt(jnp.mean(res * res, axis=1, keepdims=True) + 1e-06)
                unit = res * inv
                sum_ref[0:1] += jnp.sum(da2 * unit, axis=0, keepdims=True)
                dn = da2 * g_ref[...]
                dresid = wide(dy_ref[r]) + inv * (dn - unit * inv * jnp.mean(dn * res, axis=1, keepdims=True))
                dresid_ref[r] = dresid
                v[r] = dresid.astype(bf16)

            tiles(side * (n // 2), n // 2, rows_of)

        poll, drain = polls(
            lambda: (forward(0), forward(1)), lambda: (line_d.step(2), line_g.step(1)), lambda: (forward(2), forward(3)), lambda: line_g.step(2)
        )
        gather_rows(net, v, out_ref, sems, SCATTER_COPIES, ready, poll)
        drain()
        last = pltpu.make_async_copy(v, out_ref.at[0, 0], local.at[3])
        last.start()

        def put(ref):
            def store(r, total):
                ref[r] = total.astype(bf16)

            return store

        line_d.finish(put(down_out))
        line_g.finish(put(gate_out))
        for copy in go.values():
            copy.wait_send()
        put_back(2).wait()
        put_back(3).wait()
        last.wait()

    return comm_call(
        body, "mid_back", ident, (dgu, gu_w, a2, hidden, down_w, dy, resid, gain, down), [VM] * 2 + [ANY] * 3 + [VM] * 4,
        [shape((n, w), f32), shape((4, 2, n, w), bf16), shape((8, w), f32), shape(down.shape[1:], bf16), shape((w // 4, half), bf16),
         shape((4, w // 4, half), bf16), shape((4, 2, n, w), bf16)],
        [VM, ANY, VM, VM, VM, VM, ANY],
        [pltpu.VMEM((4, 2, n, w), bf16), pltpu.VMEM(a2.shape, bf16), pltpu.VMEM(hidden.shape, bf16), pltpu.VMEM(down_w.shape, bf16),
         pltpu.VMEM((2, 2, n, w), bf16), pltpu.VMEM((4, w // 4, half), bf16), pltpu.VMEM((n, w), bf16), pltpu.SemaphoreType.DMA((6,))]
        + scatter_scratch(n, w) + line_scratch(*down.shape[1:]) + line_scratch(w // 4, half)
        + dma_sems(SCATTER_COPIES + GATHER_COPIES + 2 * LINE_COPIES),
    )


class Home:
    def __init__(self, net, zq, cq, fq, sems, base):
        self.net, self.zq, self.cq, self.fq, self.sems, self.base = net, zq, cq, fq, sems, base
        self.r = cq.shape[2]

    def rows(self, i, j):
        return pl.ds(pl.multiple_of((2 * i + j) * self.r, self.r), self.r)

    def over_c(self, i):
        net = self.net
        return net.copy(self.zq.at[self.rows(i, 1 - net.c)], self.cq.at[i, net.c], self.sems, self.base + i, "c")

    def over_y(self):
        net = self.net
        return net.copy(self.cq.at[1 - net.y], self.fq.at[net.x, net.y], self.sems, self.base + 2, "y")

    def over_x(self):
        net = self.net
        return net.copy(self.fq.at[net.x], self.fq.at[net.x], self.sems, self.base + 3, "x")

    def step(self, d):
        net = self.net
        if d == 0:
            for i in range(2):
                self.over_c(i).start()
                self.cq[i, net.c] = self.zq[self.rows(i, net.c)]
        elif d == 1:
            for i in range(2):
                self.over_c(i).wait_recv()
            self.over_y().start()
            self.fq[net.x, net.y] = self.cq[net.y]
        elif d == 2:
            self.over_y().wait_recv()
            self.over_x().start()
        else:
            self.over_x().wait_recv()

    def finish(self):
        for i in range(2):
            self.over_c(i).wait_send()
        self.over_y().wait_send()
        self.over_x().wait_send()

    def spread(self, dst):
        for i in range(2):
            for k in range(4):
                for m in range(4):
                    col = 256 * (4 * m + k) + 128 * i
                    dst[:, col : col + 128] = wide(self.fq[i, k // 2, k % 2, :, m * 128 : (m + 1) * 128])


HOME_COPIES = 4


def home_scratch(r, k):
    return [pltpu.VMEM((2, 2, r, k), bf16), pltpu.VMEM((2, 2, 2, r, k), bf16)]


def end_call(da_parts, qkv, wo, gate_up, small, x, dresid, gain, ident):
    n, w = da_parts.shape[2:]
    rows, wide_q = qkv.shape[2] // 4, qkv.shape[3]

    def body(da_ref, q_ref, wo_ref, up_ref, small_ref, x_ref, dresid_ref, g_ref,
             gx_ref, gq_ref, go_ref, gu_ref, total_ref, own_ref,
             rc, rd, rx, ry, td, tx, ty, q_got, q_made, zq, cq, fq, cu, fu, ro, s_got, s_sum, s_line, send, recv):
        net = Net()
        sems = (send, recv)
        net.greet("xyc")
        base = SCATTER_COPIES
        lines = [ScatterLine(net, q_ref.at[i], q_got.at[i], q_made.at[i], sems, base + 6 * i) for i in range(2)]
        line_s = GatherLine(net, s_sum.at[2], s_line, sems, base + 12)
        base += 18
        homes = [Home(net, zq.at[i], cq.at[i], fq.at[i], sems, base + 4 * i) for i in range(2)]
        home_u = Home(net, up_ref, cu, fu, sems, base + 8)
        base += 12
        for line in lines:
            line.step(0)
        hops = [net.send(small_ref, s_got.at[0], sems, base, "c")]
        home_u.step(0)

        def small_step(i):
            hops[i].wait_recv()
            s_sum[i] = (small_ref[...] if i == 0 else s_sum[i - 1]) + s_got[i]
            if i < 2:
                hops.append(net.send(s_sum.at[i], s_got.at[i + 1], sems, base + 1 + i, "yx"[i]))
            else:
                line_s.step(0)

        scatter = scatter_steps(net, da_ref, rc, rd, rx, ry, td, tx, ty, sems, 0)
        next(scatter)
        small_step(0)
        next(scatter)
        home_u.step(1)
        swap_o = net.send(wo_ref, ro, sems, base + 3, "x")
        lines[0].step(1)
        small_step(1)
        done = next(scatter)
        lines[1].step(1)
        home_u.step(2)
        small_step(2)
        lines[0].step(2)
        line_s.step(1)
        lines[1].step(2)
        line_s.step(2)
        for half in range(2):
            done(half)

            def rows_of(at):
                da = wide(da_ref[0, 0, at]) + wide(rc[0, at]) + wide(rx[at]) + wide(ry[at])
                xf = wide(x_ref[at])
                r = lax.rsqrt(jnp.mean(xf * xf, axis=1, keepdims=True) + 1e-06)
                dn = da * g_ref[...]
                gx_ref[at] = dresid_ref[at] + r * (dn - xf * r * r * jnp.mean(dn * xf, axis=1, keepdims=True))

            tiles(half * (n // 2), n // 2, rows_of)

        for i in range(2):

            def put(at, total):
                zq[i, at] = total.astype(bf16)

            lines[i].finish(put)
            homes[i].step(0)
        homes[0].step(1)
        homes[1].step(1)
        homes[0].step(2)
        homes[1].step(2)
        line_s.step(3)
        s_line[net.z] = s_sum[2]
        total_ref[...] = (s_line[0] + s_line[1]) + (s_line[2] + s_line[3])
        own_ref[...] = jnp.zeros_like(own_ref)
        for i in range(3):
            own_ref[i : i + 1] = total_ref[pl.ds(16 * i + net.f, 1)]
        swap_o.wait_recv()
        go_ref[...] = wide(wo_ref[...]) + wide(ro[...])
        home_u.step(3)
        home_u.spread(gu_ref)
        for part in range(2):
            homes[part].step(3)
            for i in range(2):
                for k in range(4):
                    pair = 4 * i + 2 * (k % 2) + k // 2
                    for m in range(3):
                        to = 3 * part + m
                        col = (to // 2) * MODEL_WIDTH + (2 * pair + to % 2) * E
                        gq_ref[:, col : col + E] = wide(fq[part, i, k // 2, k % 2, :, m * EP : m * EP + E])
        line_s.finish()
        for home in homes + [home_u]:
            home.finish()
        for copy in hops + [swap_o]:
            copy.wait_send()

    two = lambda specs: [pltpu.VMEM((2,) + v.shape, v.dtype) for v in specs]
    return comm_call(
        body, "end", ident, (da_parts, qkv, wo, gate_up, small, x, dresid, gain), [VM] * 8,
        [shape((n, w), f32), shape((rows, 3 * MODEL_WIDTH), f32), shape(wo.shape, f32), shape((rows, FF), f32), shape(small.shape, f32),
         shape((8, small.shape[1]), f32)],
        [VM] * 6,
        scatter_scratch(n, w) + two(line_scratch(4 * rows, wide_q)) + two([pltpu.VMEM((4 * rows, wide_q), bf16)])
        + two(home_scratch(rows, wide_q)) + home_scratch(rows, FF // 8) + [pltpu.VMEM(wo.shape, bf16)]
        + [pltpu.VMEM((3,) + small.shape, f32), pltpu.VMEM((3,) + small.shape, f32), pltpu.VMEM((4,) + small.shape, f32)]
        + dma_sems(SCATTER_COPIES + 18 + 12 + 4),
    )


def back_call(mix, qkv, docs, tt, gain, dattn, xhat, s, p, z, a1, out_w, qkv_w, out_parts, up_parts, wo, gate, down, resid, ident):
    rows, t, _ = qkv.shape
    n, w = out_parts.shape[2:]
    rows_o, rows_d, wide_q = wo.shape[1], down.shape[0], 3 * EP

    def body(mix_ref, qkv_ref, docs_ref, tt_ref, gain_ref, dattn_ref, xhat_ref, s_ref, p_ref, z_ref, a1_ref,
             ow_ref, qw_ref, op_ref, gu_ref, wo_ref, gate_ref, down_ref, resid_ref,
             da_ref, q16_ref, sum_ref, gconv_ref, gmix_ref, gg_ref, out_ref, gu_out, go_out, gg_out, gd_ref,
             m_ref, gq_ref, dq, rc, rd, rx, ry, td, tx, ty, g_got, g_made, o_got, o_made, po, cg, fg, fd, send, recv):
        net = Net()
        sems = (send, recv)
        step = pl.program_id(0)
        base = SCATTER_COPIES
        line = ScatterLine(net, gu_ref, g_got, g_made, sems, base)
        line_o = ScatterLine(net, po, o_got, o_made, sems, base + 6)
        home = Home(net, gate_ref, cg, fg, sems, base + 12)
        x, c = net.x, net.c
        to_c = lambda: net.copy(wo_ref.at[1 - c], po.at[2 * x + c], sems, base + 16, "c")
        to_x = lambda: net.copy(down_ref, fd.at[x], sems, base + 17, "x")
        scatter = scatter_steps(net, op_ref, rc, rd, rx, ry, td, tx, ty, sems, 0)

        @pl.when(step == 0)
        def _():
            net.greet("xyc")
            line.step(0)
            to_c().start()
            next(scatter)
            home.step(0)
            po[2 * (1 - x)] = jnp.zeros((rows_o, w), bf16)
            po[2 * (1 - x) + 1] = jnp.zeros((rows_o, w), bf16)
            po[2 * x + c] = wo_ref[c]
            fd[x] = down_ref[...]
            m_ref[...] = jnp.zeros_like(m_ref)
            gmix_ref[...] = jnp.zeros_like(gmix_ref)
            gg_ref[...] = jnp.zeros_like(gg_ref)
            gq_ref[...] = jnp.zeros_like(gq_ref)

        allowed = allowed_mask(*turn(docs_ref[0]))
        scale = 1.0 / math.sqrt(E)
        lane = lax.broadcasted_iota(jnp.int32, (1, EP), 1)
        prob = [p_ref[0, 0], p_ref[0, 1]]
        dmixed = []
        for h in range(2):
            cols = slice(h * EP, (h + 1) * EP)
            dn, xh = dot(dattn_ref[0], ow_ref[cols], 1, 1), xhat_ref[0, :, cols]
            gg_ref[0:1, cols] += jnp.sum(dn * xh, axis=0, keepdims=True)
            dc = dn * gain_ref[0:1, cols]
            m1 = jnp.sum(dc, axis=1, keepdims=True) / E
            m2 = jnp.sum(dc * xh, axis=1, keepdims=True) / E
            dh = jnp.where(lane < E, s_ref[0, :, cols] * (dc - m1 - xh * m2), 0.0).astype(bf16)
            v = qkv_ref[0, :, (4 + h) * EP : (5 + h) * EP]
            mixed = (mix_ref[h, 0] * prob[0] + mix_ref[h, 1] * prob[1]).astype(bf16)
            dmixed.append(dot(dh, v, 1, 1))
            dq[:, (4 + h) * EP : (5 + h) * EP] = dot(mixed, dh, 0, 0).astype(bf16)
        for h in range(2):
            for c in range(2):
                r = 2 * h + c
                gmix_ref[r : r + 1, :] += jnp.sum(dmixed[h] * prob[c], axis=0, keepdims=True)
        for c in range(2):
            dp = mix_ref[0, c] * dmixed[0] + mix_ref[1, c] * dmixed[1]
            dconv = prob[c] * (dp - jnp.sum(dp * prob[c], axis=1, keepdims=True))
            ahead = jnp.concatenate([up(dconv, a).astype(bf16) for a in range(QWIN)], 1)
            m_ref[c] += dot(z_ref[0, c], ahead, 0, 0)
            ds = jnp.where(allowed, dot(ahead, tt_ref[c]), 0.0).astype(bf16)
            q = qkv_ref[0, :, c * EP : (c + 1) * EP]
            k = qkv_ref[0, :, (2 + c) * EP : (3 + c) * EP]
            dq[:, c * EP : (c + 1) * EP] = (dot(ds, k) * scale).astype(bf16)
            dq[:, (2 + c) * EP : (3 + c) * EP] = (dot(ds, q, 0, 0) * scale).astype(bf16)
        da_ref[0] = dot(dq[...], qw_ref[...], 1, 1).astype(bf16)
        for i in range(0, w, 384):
            gq_ref[i : i + 384] += dot(a1_ref[0, :, i : i + 384], dq[...], 0, 0)

        done = []

        @pl.when(step == 1)
        def _():
            next(scatter)
            to_c().wait_recv()
            line_o.step(0)
            home.step(1)
            to_x().start()

        @pl.when(step == 2)
        def _():
            line.step(1)
            done.append(next(scatter))

        @pl.when(step == 3)
        def _():
            line_o.step(1)
            home.step(2)

        @pl.when(step == 4)
        def _():
            line.step(2)

        @pl.when(step == 5)
        def _():
            line_o.step(2)

        @pl.when(step == rows - 1)
        def _():
            lanes = lax.broadcasted_iota(jnp.int32, (8, t), 1)
            for h in range(2):
                for a in range(QWIN):
                    total = jnp.zeros((8, t), f32)
                    for first in range(0, t, 8):
                        part = m_ref[h, first : first + 8, a * t : (a + 1) * t]
                        turned = pltpu.roll(part, t - first, 1) if first else part
                        total = total + jnp.where(lanes < t - first, turned, 0.0)
                    gconv_ref[h, a] = total[:, :EP]
            for half in range(2):
                done[0](half)

                def sum_of(at):
                    total = wide(op_ref[0, 0, at]) + wide(rc[0, at]) + wide(rx[at]) + wide(ry[at])
                    out_ref[at] = (resid_ref[at] + total).astype(bf16)

                tiles(half * (n // 2), n // 2, sum_of)

            def put(at, total):
                gu_out[at] = total.astype(bf16)

            line.finish(put)

            def put_o(at, total):
                go_out[at] = total.astype(bf16)

            line_o.finish(put_o)
            to_x().wait_recv()
            for i in range(2):
                gd_ref[i * rows_d : (i + 1) * rows_d] = wide(fd[i])
            home.step(3)
            home.spread(gg_out)
            home.finish()
            to_x().wait_send()
            to_c().wait_send()
            for i in range(0, w, 384):
                part = gq_ref[i : i + 384]
                for j in range(2):
                    q16_ref[j, i : i + 384] = part[:, j * wide_q : (j + 1) * wide_q].astype(bf16)
                sum_ref[:, i : i + 384] = lax.dot_general(
                    jnp.ones((8, 6 * EP), f32), part * wide(qw_ref[i : i + 384]), (((1,), (1,)), ((), ())),
                    precision=lax.Precision.HIGHEST, preferred_element_type=f32,
                )

    row = lambda *sh: pl.BlockSpec((1,) + sh, lambda i: (i,) + (0,) * len(sh))
    full = lambda v: pl.BlockSpec(v.shape, lambda i: (0,) * v.ndim, pipeline_mode=pl.Buffered(1))
    keep = lambda *sh: pl.BlockSpec(sh, lambda i: (0,) * len(sh))
    return pl.pallas_call(
        body,
        grid=(rows,),
        in_specs=[pl.BlockSpec(memory_space=pltpu.SMEM), row(t, 6 * EP), row(8, t), full(tt), full(gain),
                  row(t, w), row(t, 2 * EP), row(t, 2 * EP), row(2, t, t), row(2, t, t), row(t, w),
                  full(out_w), full(qkv_w), full(out_parts), full(up_parts), full(wo), full(gate), full(down), full(resid)],
        out_specs=[row(t, w), keep(2, w, wide_q), keep(8, w), keep(2, QWIN, 8, EP), keep(8, t), keep(8, 2 * EP), keep(n, w),
                   keep(*up_parts.shape[1:]), keep(rows_o, w), keep(rows_o, FF), keep(2 * rows_d, w)],
        out_shape=[
            shape((rows, t, w), bf16),
            shape((2, w, wide_q), bf16),
            shape((8, w), f32),
            shape((2, QWIN, 8, EP), f32),
            shape((8, t), f32),
            shape((8, 2 * EP), f32),
            shape((n, w), bf16),
            shape(up_parts.shape[1:], bf16),
            shape((rows_o, w), bf16),
            shape((rows_o, FF), f32),
            shape((2 * rows_d, w), f32),
        ],
        scratch_shapes=[pltpu.VMEM((2, t, QWIN * t), f32), pltpu.VMEM((w, 6 * EP), f32), pltpu.VMEM((t, 6 * EP), bf16)] + scatter_scratch(n, w)
        + line_scratch(*up_parts.shape[1:]) + line_scratch(rows_o, w) + [pltpu.VMEM((4, rows_o, w), bf16)]
        + home_scratch(rows_o, FF // 8) + [pltpu.VMEM((2, rows_d, w), bf16)] + dma_sems(SCATTER_COPIES + 18),
        compiler_params=pltpu.CompilerParams(collective_id=ident, has_side_effects=True, vmem_limit_bytes=63 << 20),
        name="back",
    )(mix, qkv, docs, tt, gain, dattn, xhat, s, p, z, a1, out_w, qkv_w, out_parts, up_parts, wo, gate, down, resid)


def rms_scale(values):
    return lax.rsqrt(jnp.mean(values * values, axis=1, keepdims=True) + 1e-06)


class Links:
    def __init__(self, fsdp):
        self.fsdp = fsdp
        index = lax.axis_index("fsdp")
        self.x = lax.axis_index("rep")
        self.z, self.y, self.c = index // 4, (index // 2) % 2, index % 2

    def across(self, flip, v):
        if flip == "x":
            return lax.ppermute(v, "rep", [(0, 1), (1, 0)])
        bit = {"y": 2, "c": 1}[flip]
        return lax.ppermute(v, "fsdp", [(f, f ^ bit) for f in range(self.fsdp)])

    def along(self, v, step):
        pairs = [(f, f + 4 * step) for f in range(self.fsdp) if 0 <= f + 4 * step < self.fsdp]
        return lax.ppermute(v, "fsdp", pairs)

    def ordered(self, bit, mine, other, axis):
        first, second = jnp.where(bit == 0, mine, other), jnp.where(bit == 0, other, mine)
        return jnp.stack([first, second], axis)

    def gather_z(self, v):
        left, right = [], []
        a = b = v
        for _ in range(3):
            a, b = self.along(a, 1), self.along(b, -1)
            left.append(a)
            right.append(b)
        line = jnp.stack(left[::-1] + [v] + right)
        return lax.dynamic_slice_in_dim(line, 3 - self.z, 4, 0)

    def scatter_z(self, parts):
        zero = jnp.zeros((3,) + parts.shape[1:], parts.dtype)
        line = lax.dynamic_slice_in_dim(jnp.concatenate([zero, parts, zero]), self.z, 7, 0)
        low = lambda v: v.astype(bf16)
        a = self.along(low(line[6]), 1)
        b = self.along(low(line[0]), -1)
        for step in (1, 2):
            a = self.along(low(line[6 - step] + a.astype(f32)), 1)
            b = self.along(low(line[step] + b.astype(f32)), -1)
        return line[3] + a.astype(f32) + b.astype(f32)

    def gather_plane(self, v):
        n = v.shape[0] // 2
        vx, vy = self.across("x", v), self.across("y", v)
        vd = jnp.concatenate([self.across("y", vx[:n]), self.across("x", vy[n:])])
        return [jnp.concatenate([u, self.across("c", u)]) for u in (v, vx, vy, vd)]

    def scatter_plane(self, parts):
        low = lambda v: v.astype(bf16)
        n = parts[0].shape[0] // 2
        s = [p[:n] + self.across("c", low(p[n:])).astype(f32) for p in parts]
        m = n // 2
        dx, dy = self.across("x", low(s[3][:m])), self.across("y", low(s[3][m:]))
        to_x = jnp.concatenate([s[1][:m], s[1][m:] + dy.astype(f32)])
        to_y = jnp.concatenate([s[2][:m] + dx.astype(f32), s[2][m:]])
        return s[0] + self.across("x", low(to_x)).astype(f32) + self.across("y", low(to_y)).astype(f32)


class Weights:
    def __init__(self, links):
        self.links = links
        self.line = links.fsdp == 16
        x, y, c = links.x, links.y, links.c
        self.pair = 4 * x + 2 * c + y
        self.slot = 4 * x + 2 * y + c

    def spread(self, shard, dims):
        l = self.links
        ax, ay, ac = dims
        v = lax.dynamic_index_in_dim(shard, l.x, ax, keepdims=True)
        keep = lax.dynamic_index_in_dim(v, l.y, ay, keepdims=True)
        sent = l.across("y", lax.dynamic_index_in_dim(v, 1 - l.y, ay, keepdims=True))
        v = l.ordered(l.y, keep, sent, 0)
        keep = lax.dynamic_index_in_dim(v, l.c, ac + 1, keepdims=True)
        sent = l.across("c", lax.dynamic_index_in_dim(v, 1 - l.c, ac + 1, keepdims=True))
        v = l.ordered(l.c, keep, sent, 1)
        return l.gather_z(v)

    def collect(self, grad, dims):
        l = self.links
        ax, ay, ac = dims
        low = lambda v: v.astype(bf16)
        v = l.scatter_z(grad)
        keep = lax.dynamic_index_in_dim(v, l.c, 1, keepdims=False)
        sent = l.across("c", low(lax.dynamic_index_in_dim(v, 1 - l.c, 1, keepdims=False)))
        v = self.join(l.c, keep, sent.astype(f32), ac + 1)
        keep = lax.dynamic_index_in_dim(v, l.y, 0, keepdims=False)
        sent = l.across("y", low(lax.dynamic_index_in_dim(v, 1 - l.y, 0, keepdims=False)))
        v = low(self.join(l.y, keep, sent.astype(f32), ay))
        return self.join(l.x, v, l.across("x", v), ax).astype(f32)

    def join(self, bit, mine, other, axis):
        first, second = jnp.where(bit == 0, mine, other), jnp.where(bit == 0, other, mine)
        return jnp.concatenate([first, second], axis)

    def whole(self, shard):
        return lax.all_gather(shard, "fsdp", axis=0, tiled=True)

    def owned(self, grad):
        part = lax.psum_scatter(grad, "fsdp", scatter_dimension=0, tiled=True)
        return lax.psum(part.astype(bf16), "rep").astype(f32)

    def qkv(self, shard):
        rows = shard.shape[0]
        if self.line:
            v = self.spread(shard.reshape(rows, 3, 2, 2, 2, 2 * E), (2, 4, 3))
            v = v.reshape(MODEL_WIDTH, 3, 2, E)
        else:
            v = self.whole(shard).reshape(MODEL_WIDTH, 3, 8, 2, E)
            v = lax.dynamic_index_in_dim(v, self.pair, 2, keepdims=False)
        return jnp.pad(v, ((0, 0), (0, 0), (0, 0), (0, EP - E))).reshape(MODEL_WIDTH, 6 * EP)

    def qkv_back(self, grad):
        g = grad.reshape(MODEL_WIDTH, 3, 2, EP)[..., :E]
        if self.line:
            return self.collect(g.reshape(4, 2, 2, -1, 3, 1, 1, 1, 2 * E), (2, 4, 3)).reshape(-1, 3 * MODEL_WIDTH)
        zero = jnp.zeros((MODEL_WIDTH, 3, 8, 2, E), f32)
        return self.owned(lax.dynamic_update_index_in_dim(zero, g, self.pair, 2).reshape(MODEL_WIDTH, 3 * MODEL_WIDTH))

    def out(self, shard):
        l = self.links
        if self.line:
            v = l.gather_z(shard)
            keep = lax.dynamic_index_in_dim(v, 2 * l.x + l.c, 0, keepdims=False)
            sent = l.across("c", lax.dynamic_index_in_dim(v, 2 * l.x + 1 - l.c, 0, keepdims=False))
            v = l.ordered(l.c, keep, sent, 0)
        else:
            v = self.whole(shard).reshape(8, 2, E, MODEL_WIDTH)
            v = lax.dynamic_index_in_dim(v, self.pair, 0, keepdims=False)
        return jnp.pad(v, ((0, 0), (0, EP - E), (0, 0))).reshape(2 * EP, MODEL_WIDTH)

    def out_back(self, grad):
        l = self.links
        g = grad.reshape(2, EP, MODEL_WIDTH)[:, :E]
        if self.line:
            keep = lax.dynamic_index_in_dim(g, l.c, 0, keepdims=False)
            sent = l.across("c", lax.dynamic_index_in_dim(g, 1 - l.c, 0, keepdims=False).astype(bf16)).astype(f32)
            at = jnp.arange(4)[:, None, None]
            parts = jnp.where(at == 2 * l.x + l.c, keep[None], jnp.where(at == 2 * l.x + 1 - l.c, sent[None], 0.0))
            v = l.scatter_z(parts).astype(bf16)
            return (v + l.across("x", v)).astype(f32)
        zero = jnp.zeros((8, 2, E, MODEL_WIDTH), f32)
        return self.owned(lax.dynamic_update_index_in_dim(zero, g, self.pair, 0).reshape(MODEL_WIDTH, MODEL_WIDTH))

    def ffn_in(self, gate, up_):
        rows = gate.shape[0]
        both = jnp.stack([gate, up_], 1)
        if self.line:
            v = self.spread(both.reshape(rows, 2, 4, 2, 2, 2, FF // 32), (5, 3, 4))
            return v.reshape(MODEL_WIDTH, FF // 4)
        v = self.whole(both).reshape(MODEL_WIDTH, 2, 8, FF // 8)
        return lax.dynamic_index_in_dim(v, self.slot, 2, keepdims=False).reshape(MODEL_WIDTH, FF // 4)

    def ffn_in_back(self, grad):
        if self.line:
            v = self.collect(grad.reshape(4, 2, 2, -1, 2, 4, 1, 1, 1, FF // 32), (5, 3, 4)).reshape(-1, 2, FF)
        else:
            zero = jnp.zeros((MODEL_WIDTH, 2, 8, FF // 8), f32)
            g = grad.reshape(MODEL_WIDTH, 2, FF // 8)
            v = self.owned(lax.dynamic_update_index_in_dim(zero, g, self.slot, 2).reshape(MODEL_WIDTH, 2, FF))
        return v[:, 0], v[:, 1]

    def ffn_out(self, shard):
        l = self.links
        if self.line:
            v = lax.dynamic_index_in_dim(shard.reshape(2, FF // 32, MODEL_WIDTH), l.x, 0, keepdims=False)
            return l.gather_z(v).reshape(FF // 8, MODEL_WIDTH)
        v = self.whole(shard).reshape(8, FF // 8, MODEL_WIDTH)
        return lax.dynamic_index_in_dim(v, self.slot, 0, keepdims=False)

    def ffn_out_back(self, grad):
        l = self.links
        if self.line:
            v = l.scatter_z(grad.reshape(4, FF // 32, MODEL_WIDTH)).astype(bf16)
            return self.join(l.x, v, l.across("x", v), 0).astype(f32)
        zero = jnp.zeros((8, FF // 8, MODEL_WIDTH), f32)
        return self.owned(lax.dynamic_update_index_in_dim(zero, grad, self.slot, 0).reshape(FF, MODEL_WIDTH))

    def gains(self, *shards):
        l = self.links
        v = jnp.stack(shards)
        if self.line:
            v = l.ordered(l.c, v, l.across("c", v), 0)
            v = l.ordered(l.y, v, l.across("y", v), 0)
            v = l.gather_z(v)
            v = v.reshape(16, len(shards), -1).transpose(1, 0, 2).reshape(len(shards), MODEL_WIDTH)
        else:
            v = lax.all_gather(v, "fsdp", axis=1, tiled=True)
        return [v[i].astype(f32) for i in range(len(shards))]


def per_device(
    fsdp,
    x_in,
    doc_ids,
    w_qkv,
    w_out,
    gain_attn,
    gain_group,
    conv_kernel,
    head_mix,
    gain_ffn,
    w_gate,
    w_up,
    w_down,
    cotangent,
):
    links = Links(fsdp)
    weights = Weights(links)
    tokens = x_in.shape[1]

    x_all = jnp.concatenate(links.gather_plane(x_in[0]))
    qkv_w = weights.qkv(w_qkv)
    gain_a, gain_g, gain_f = weights.gains(gain_attn, gain_group, gain_ffn)
    docs = doc_ids
    for flip in ("y", "x"):
        docs = jnp.concatenate([docs, links.across(flip, docs)])
    docs = jnp.stack([docs, links.across("c", docs)], 1)
    docs = docs[jnp.array([0, 2, 1, 3])].reshape(8, tokens)
    out_w = weights.out(w_out)
    in_w = weights.ffn_in(w_gate, w_up)
    down_w = weights.ffn_out(w_down)
    upstream_chips = links.gather_plane(cotangent[0])

    kernel = lax.dynamic_slice_in_dim(conv_kernel, 2 * weights.pair, 2, 0)
    mix = lax.dynamic_slice_in_dim(head_mix, 2 * weights.pair, 2, 0)
    th, tl, tt = bands(kernel, tokens)
    group = lax.dynamic_slice_in_dim(gain_g.reshape(8, 2, E), weights.pair, 1, 0)
    group = jnp.pad(group, ((0, 0), (0, 0), (0, EP - E))).reshape(1, 2 * EP)
    doc_col, doc_row = docs[:, :, None], docs[:, None, :]

    xf_all = x_all.astype(f32)
    a1 = (xf_all * rms_scale(xf_all) * gain_a).astype(bf16)
    qkv = dot(a1, qkv_w).astype(bf16).reshape(8, tokens, 6 * EP)
    normed, xhat, s, probs, zeroed = attend(mix, qkv, doc_col, doc_row, th, tl, group)
    normed = normed.reshape(4, 2 * tokens, 2 * EP)
    xf = x_in[0].astype(f32)
    resid = xf + links.scatter_plane([dot(normed[i], out_w) for i in range(4)])

    r2 = rms_scale(resid)
    a2_chips = links.gather_plane((resid * r2 * gain_f).astype(bf16))
    out_parts, back_parts, hiddens, dgus = [], [], [], []
    half = FF // 8
    for a2, dffn in zip(a2_chips, upstream_chips):
        gu = dot(a2, in_w)
        gate, up_act = gu[:, :half], gu[:, half:]
        sig = jax.nn.sigmoid(gate)
        silu = gate * sig
        hidden = (silu * up_act).astype(bf16)
        dhidden = dot(dffn, down_w, 1, 1)
        dgate = (dhidden * up_act * sig * (1.0 + gate * (1.0 - sig))).astype(bf16)
        dup = (dhidden * silu).astype(bf16)
        dgu = jnp.concatenate([dgate, dup], 1)
        hiddens.append(hidden)
        dgus.append(dgu)
        back_parts.append(dot(dgu, in_w, 1, 1))
        out_parts.append(dot(hidden, down_w))
    da2 = links.scatter_plane(back_parts)
    output = (resid + links.scatter_plane(out_parts)).astype(bf16)

    dy = cotangent[0].astype(f32)
    sum_gain_ffn = jnp.sum(da2 * resid * r2, axis=0)
    dn2 = da2 * gain_f
    dresid = dy + r2 * (dn2 - resid * r2 * r2 * jnp.mean(dn2 * resid, axis=1, keepdims=True))
    dattn = jnp.concatenate(links.gather_plane(dresid.astype(bf16)))

    a2_all, dgu_all = jnp.concatenate(a2_chips), jnp.concatenate(dgus)
    hidden_all, dffn_all = jnp.concatenate(hiddens), jnp.concatenate(upstream_chips)
    grad_gate, grad_up = weights.ffn_in_back(dot(a2_all, dgu_all, 0, 0))
    grad_down = weights.ffn_out_back(dot(hidden_all, dffn_all, 0, 0))

    dnormed = dot(dattn, out_w, 1, 1).reshape(8, tokens, 2 * EP)
    dqkv, conv_tiles, mix_sums, group_sums = attend_back(
        mix, qkv, doc_col, doc_row, tt, group, dnormed, xhat, s, probs, zeroed
    )
    dqkv = dqkv.reshape(4, 2 * tokens, 6 * EP)
    da1 = links.scatter_plane([dot(dqkv[i], qkv_w, 1, 1) for i in range(4)])
    grad_out = weights.out_back(dot(normed.reshape(8 * tokens, 2 * EP), dattn, 0, 0))
    grad_qkv = weights.qkv_back(dot(a1, dqkv.reshape(8 * tokens, 6 * EP), 0, 0))

    r1 = rms_scale(xf)
    sum_gain_attn = jnp.sum(da1 * xf * r1, axis=0)
    dn1 = da1 * gain_a
    grad_x = dresid + r1 * (dn1 - xf * r1 * r1 * jnp.mean(dn1 * xf, axis=1, keepdims=True))

    place = lambda v: lax.dynamic_update_index_in_dim(jnp.zeros((8,) + v.shape, f32), v, weights.pair, 0)
    small = [
        sum_gain_attn,
        sum_gain_ffn,
        place(group_sums[0].reshape(2, EP)[:, :E].reshape(-1)),
        place(diagonals(conv_tiles)),
        place(jnp.sum(mix_sums[:4], axis=1)),
    ]
    sizes = [v.size for v in small]
    total = lax.psum(jnp.concatenate([v.reshape(-1) for v in small]), ("rep", "fsdp"))
    cut = [0]
    for size in sizes:
        cut.append(cut[-1] + size)
    gain_a_sum, gain_f_sum, group_sum, conv_sum, mix_sum = (total[cut[i] : cut[i + 1]] for i in range(5))
    rows = gain_attn.shape[0]
    own = lambda v: lax.dynamic_slice_in_dim(v, lax.axis_index("fsdp") * rows, rows, 0)
    return (
        output[None],
        grad_x[None],
        grad_qkv,
        grad_out,
        own(gain_a_sum),
        own(group_sum),
        conv_sum.reshape(H, QWIN, KWIN),
        mix_sum.reshape(H, 2),
        own(gain_f_sum),
        grad_gate,
        grad_up,
        grad_down,
    )


def join(bit, mine, other, axis):
    first, second = jnp.where(bit == 0, mine, other), jnp.where(bit == 0, other, mine)
    return jnp.stack([first, second], axis)


def fast(
    x_in,
    doc_ids,
    w_qkv,
    w_out,
    gain_attn,
    gain_group,
    conv_kernel,
    head_mix,
    gain_ffn,
    w_gate,
    w_up,
    w_down,
    cotangent,
):
    links = Links(16)
    pair = 4 * links.x + 2 * links.c + links.y
    tokens = x_in.shape[1]
    x, dy = x_in[0], cotangent[0]
    rows = w_qkv.shape[0]

    kernel = lax.dynamic_slice_in_dim(conv_kernel, 2 * pair, 2, 0)
    mix = lax.dynamic_slice_in_dim(head_mix, 2 * pair, 2, 0)
    gains = jnp.pad(jnp.stack([gain_attn, gain_group, gain_ffn]), ((0, 13), (0, 128 - rows)))
    docs = jnp.broadcast_to(doc_ids, (8, tokens))
    a1, dffn_1, docs, gains, qkv_w, gu_plane, out_w, th, tl, tt = start_call(
        x, dy, docs, gains, kernel.reshape(-1), w_qkv, w_gate, w_up, w_out, 1
    )
    docs = docs.reshape(8, 8, tokens)
    gain_a, gain_g, gain_f = gains[0:1], gains[1], gains[2:3]
    qkv_w = qkv_w.reshape(MODEL_WIDTH, 6 * EP)
    keep = lax.dynamic_index_in_dim(out_w, 2 * links.x + links.c, 0, keepdims=False)
    other = links.across("c", lax.dynamic_index_in_dim(out_w, 2 * links.x + 1 - links.c, 0, keepdims=False))
    out_w = jnp.pad(join(links.c, keep, other, 0), ((0, 0), (0, EP - E), (0, 0))).reshape(2 * EP, MODEL_WIDTH)

    group = lax.dynamic_slice_in_dim(gain_g.reshape(8, 2, E), pair, 1, 0)
    group = jnp.pad(group, ((0, 0), (0, 0), (0, EP - E))).reshape(1, 2 * EP)

    by_chip = lambda v: v.astype(bf16).reshape(4, 2, tokens, MODEL_WIDTH)
    by_row = lambda v: v.reshape(8, tokens, -1)
    qkv, normed, xhat, s, probs, zeroed, resid, a2, dffn_2, gu_w, down_w = forward_call(
        mix, by_row(a1), docs, th, tl, group, qkv_w, out_w, x, dy, gain_f, gu_plane, w_down, 2
    )
    normed = normed.reshape(8 * tokens, 2 * EP)

    a2 = a2.reshape(8 * tokens, MODEL_WIDTH)
    flat = lambda v: v.reshape(-1, MODEL_WIDTH)
    gu_w = gu_w.reshape(MODEL_WIDTH, FF // 4)
    down_w = down_w.reshape(FF // 8, MODEL_WIDTH)
    dgu, hidden, grad_down = ffn_call(a2, flat(dffn_1), flat(dffn_2), gu_w, down_w)
    grad_down = grad_down.reshape(4, FF // 32, MODEL_WIDTH)
    dresid, dattn, sum_f, grad_down, grad_gate, grad_up, out_parts = mid_back_call(
        dgu, gu_w, a2, hidden, down_w, dy, resid, gain_f, grad_down, 3
    )

    grad_out = dot(normed, dattn.reshape(8 * tokens, MODEL_WIDTH), 0, 0).astype(bf16).reshape(2, EP, MODEL_WIDTH)[:, :rows]
    da_parts, grad_qkv, sum_a, conv_tiles, mix_sums, group_sums, out, grad_up, grad_out, grad_gate, grad_down = back_call(
        mix, qkv, docs, tt, group, by_row(dattn), xhat, s, probs, zeroed, by_row(a1), out_w, qkv_w,
        out_parts, grad_up, grad_out, grad_gate, grad_down, resid, 5
    )
    sum_a = sum_a[0] / gain_a[0]
    place = lambda v: lax.dynamic_update_index_in_dim(jnp.zeros((8,) + v.shape, f32), v, pair, 0).reshape(16, -1)
    heads = jnp.concatenate([diagonals(conv_tiles).reshape(2, -1), jnp.sum(mix_sums[:4], axis=1).reshape(2, 2)], 1)
    small = [sum_a.reshape(16, -1), sum_f[0].reshape(16, -1), place(group_sums[0].reshape(2, EP)[:, :E]), place(heads)]
    small = jnp.concatenate([jnp.pad(v, ((0, 0), (0, 128 - v.shape[1]))) for v in small])
    grad_x, grad_qkv, grad_out, grad_up, total, own = end_call(
        by_chip(da_parts),
        grad_qkv.reshape(2, 4, 4 * rows, 3 * EP),
        grad_out,
        grad_up,
        small,
        x,
        dresid,
        gain_a,
        4,
    )
    heads = total[48:]
    taps = QWIN * KWIN
    return (
        out[None],
        grad_x[None],
        grad_qkv,
        grad_out,
        own[0, :rows],
        own[2, :rows],
        heads[:, :taps].reshape(H, QWIN, KWIN),
        heads[:, taps : taps + 2],
        own[1, :rows],
        grad_gate,
        grad_up,
        grad_down,
    )


def solution(mesh):
    fsdp = mesh.shape["fsdp"]
    assert mesh.shape["rep"] == 2 and fsdp % 4 == 0
    rows, shard, part = P(("rep", "fsdp"), None, None), P("fsdp", None), P("fsdp")
    placed = (rows, P(("rep", "fsdp"), None), shard, shard, part, part, P(), P(), part, shard, shard, shard, rows)
    return jax.shard_map(
        fast if fsdp == 16 else (lambda *args: per_device(fsdp, *args)),
        mesh=mesh,
        in_specs=placed,
        out_specs=(rows, rows, shard, shard, part, part, P(), P(), part, shard, shard, shard),
        check_vma=False,
    )
```
